32 devices in a mesh: dp: 8 (over y, x, core), tensor: 4 (over z).
Axes of the slice: x: 2, y: 2, z: 4, core: 2. Of those that a mesh axis runs over, the one named last changes fastest.
Arguments:
- hidden_in: bfloat16 [8, 3072, 768], P('dp', 'tensor'), may hold values from -6 to 6
- segments: int32 [8, 3072], P('dp', 'tensor'), may hold values from 0 to 3, never falling along the last dimension, each value on 1 to 2000 neighbouring positions
- query_weight: bfloat16 [768, 768], P('dp', 'tensor'), may hold values from -0.21875 to 0.21875
- key_weight: bfloat16 [768, 768], P('dp', 'tensor'), may hold values from -0.21875 to 0.21875
- value_weight: bfloat16 [768, 768], P('dp', 'tensor'), may hold values from -0.21875 to 0.21875
- query_bias: float32 [768], P('tensor'), may hold values from -3 to 3
- value_bias: float32 [768], P('tensor'), may hold values from -3 to 3
- mixer_weight: bfloat16 [768, 768], P('tensor', 'dp'), may hold values from -1.75 to 1.75
- mixer_bias: float32 [768], replicated, may hold values from -3 to 3
- first_gain: float32 [768], replicated, may hold values from 0.5 to 1.5
- first_shift: float32 [768], replicated, may hold values from -3 to 3
- inner_weight: bfloat16 [768, 3072], P('dp', 'tensor'), may hold values from -0.21875 to 0.21875
- inner_bias: float32 [3072], P('tensor'), may hold values from -3 to 3
- outer_weight: bfloat16 [3072, 768], P('tensor', 'dp'), may hold values from -0.109375 to 0.109375
- outer_bias: float32 [768], replicated, may hold values from -3 to 3
- second_gain: float32 [768], replicated, may hold values from 0.5 to 1.5
- second_shift: float32 [768], replicated, may hold values from -3 to 3
- cotangent: bfloat16 [8, 3072, 768], P('dp', 'tensor'), may hold values from -6 to 6
Outputs:
- layer_out: bfloat16 [8, 3072, 768], P('dp', 'tensor')
- input_grad: bfloat16 [8, 3072, 768], P('dp', 'tensor')
- grad_query_weight: float32 [768, 768], P('dp', 'tensor')
- grad_key_weight: float32 [768, 768], P('dp', 'tensor')
- grad_value_weight: float32 [768, 768], P('dp', 'tensor')
- grad_query_bias: float32 [768], P('tensor')
- grad_value_bias: float32 [768], P('tensor')
- grad_mixer_weight: float32 [768, 768], P('tensor', 'dp')
- grad_mixer_bias: float32 [768], replicated
- grad_first_gain: float32 [768], replicated
- grad_first_shift: float32 [768], replicated
- grad_inner_weight: float32 [768, 3072], P('dp', 'tensor')
- grad_inner_bias: float32 [3072], P('tensor')
- grad_outer_weight: float32 [3072, 768], P('tensor', 'dp')
- grad_outer_bias: float32 [768], replicated
- grad_second_gain: float32 [768], replicated
- grad_second_shift: float32 [768], replicated
The draws below stay inside these ranges and needn't reach their ends.
Inputs may be any that keep to these rules, and one draw needn't show every extreme that they name: `segments`: segment numbers never fall along a sequence; a document holds at most 2000 positions, and in every sequence one holds exactly 2000.
All inputs are finite; a program needn't handle non-finite values.
Results may differ from the reference program's by a relative error of at most 0.02.
Values may be sent and summed in bfloat16 or wider, within the bound.
A program may use at most 128 MiB of HBM per device.

```python
import math
import jax
import jax.numpy as jnp
import numpy as np
from jax import lax

D = 768
HD = 64
FF = 3072
LEN = 3072
MOST = 2000
COUNT = 4
SEQS = 8


def with_spikes(values, key, source, target, shards_of, factor):
    owner, partner = [(jnp.arange(values.shape[dim]) // (values.shape[dim] // shards_of)).reshape([-1 if axis == dim else 1 for axis in range(values.ndim)]) for dim in (source, target)]
    chosen = jax.random.permutation(key, shards_of)[partner]
    strong = (owner == chosen) | (owner == (partner + shards_of // 2) % shards_of)
    return jnp.where(strong, factor * values, values)


def levels(stream_key, dims, split, low, top_value):
    def one(axis_at, shards_of):
        heights = jax.random.uniform(jax.random.fold_in(jax.random.fold_in(stream_key, 6), axis_at), (shards_of,), jnp.float32, low / len(split), top_value / len(split))
        return jnp.repeat(jnp.exp(heights), dims[axis_at] // shards_of).reshape((-1,) + (1,) * (len(dims) - axis_at - 1))

    level = one(*split[0])
    for cut in split[1:]:
        level = level * one(*cut)
    return level


def profile(amount, total, bound, lean):
    portions = [(1 << 20) // math.isqrt(grade ** lean) + 1 for grade in range(2, amount + 1)]
    rest, holding = total - bound - (amount - 1), [1] * (amount - 1)
    while rest > 0:
        free = [i for i in range(amount - 1) if holding[i] < bound]
        mass, remaining = sum([portions[i] for i in free]), rest
        for i in free:
            addition = min(bound - holding[i], max(1, remaining * portions[i] // mass), rest)
            holding[i] = holding[i] + addition
            rest = rest - addition
    return np.array([bound] + holding)


def ragged_sizes(stream_key, number_of, total, reach, lean):
    if number_of == 2:
        one = jax.random.randint(stream_key, (), max(1, total - reach), min(reach, total - 1) + 1)
        return jnp.stack([one, total - one])
    tallies = jnp.asarray(profile(number_of, total, reach, lean), jnp.int32)
    couples = (number_of - 1) // 2
    donor, sink = tallies[1:1 + 2 * couples:2], tallies[2:2 + 2 * couples:2]
    room = jnp.minimum(donor - 1, reach - sink)
    passed = jax.random.randint(jax.random.fold_in(stream_key, 1), (couples,), 0, 1 << 20) % (room + 1)
    tallies = tallies.at[1:1 + 2 * couples:2].set(donor - passed).at[2:2 + 2 * couples:2].set(sink + passed)
    return tallies[jax.random.permutation(jax.random.fold_in(stream_key, 2), number_of)]


def normal_values(own_key, shape, deviation, reach, shards=(), dtype=jnp.bfloat16):
    drawn = jax.random.normal(own_key, shape, jnp.float32) * deviation
    if len(shards) > 0:
        drawn = levels(own_key, shape, shards, -0.22, 0.18) * drawn
    return jnp.clip(drawn, min=-reach, max=reach).astype(dtype)


def heavy_noise(own_key, extent, spread, reach, split, heavy, dtype=jnp.bfloat16):
    entries = spread * jax.random.normal(own_key, extent, jnp.float32)
    if split:
        entries = entries * levels(own_key, extent, split, -0.22, 0.18)
    return jnp.clip(with_spikes(entries, jax.random.fold_in(own_key, 3), *heavy), -reach, reach).astype(dtype)


def setup_inputs(seed: int = 0) -> dict:
    key_list = jax.random.split(jax.random.key(seed), 19)
    return {
        "hidden_in": heavy_noise(key_list[0], (SEQS, LEN, D), 1.0, 6.0, ((0, 8), (1, 4)), (0, 2, 8, 2.0)),
        "segments": jax.vmap(lambda own: jnp.searchsorted(jnp.cumsum(ragged_sizes(own, COUNT, LEN, MOST, 1)), jnp.arange(LEN), side="right"))(jax.random.split(key_list[1], SEQS)).reshape((SEQS, LEN)).astype(jnp.int32),
        "query_weight": normal_values(key_list[2], (D, D), D ** -0.5, 0.21875, ((0, 8), (1, 4))),
        "key_weight": normal_values(key_list[3], (D, D), D ** -0.5, 0.21875, ((0, 8), (1, 4))),
        "value_weight": normal_values(key_list[4], (D, D), D ** -0.5, 0.21875, ((0, 8), (1, 4))),
        "query_bias": normal_values(key_list[5], (D,), 0.5, 3.0, ((0, 4),), jnp.float32),
        "value_bias": normal_values(key_list[6], (D,), 0.5, 3.0, ((0, 4),), jnp.float32),
        "mixer_weight": normal_values(key_list[7], (D, D), (D // 64) ** -0.5, 1.75, ((0, 4), (1, 8))),
        "mixer_bias": normal_values(key_list[8], (D,), 0.5, 3.0, (), jnp.float32),
        "first_gain": jnp.clip(1.0 + 0.1 * jax.random.normal(key_list[9], (D,), jnp.float32), 0.5, 1.5),
        "first_shift": normal_values(key_list[10], (D,), 0.5, 3.0, (), jnp.float32),
        "inner_weight": normal_values(key_list[11], (D, FF), D ** -0.5, 0.21875, ((0, 8), (1, 4))),
        "inner_bias": normal_values(key_list[12], (FF,), 0.5, 3.0, ((0, 4),), jnp.float32),
        "outer_weight": normal_values(key_list[13], (FF, D), FF ** -0.5, 0.109375, ((0, 4), (1, 8))),
        "outer_bias": normal_values(key_list[14], (D,), 0.5, 3.0, (), jnp.float32),
        "second_gain": jnp.clip(1.0 + 0.1 * jax.random.normal(key_list[15], (D,), jnp.float32), 0.5, 1.5),
        "second_shift": normal_values(key_list[16], (D,), 0.5, 3.0, (), jnp.float32),
        "cotangent": heavy_noise(key_list[17], (SEQS, LEN, D), 1.0, 6.0, ((0, 8), (1, 4)), (0, 2, 8, 2.0)),
    }


@jax.custom_vjp
def low(v):
    return lax.optimization_barrier(v.astype(jnp.bfloat16)).astype(jnp.float32)

@jax.custom_vjp
def low_back(v):
    return v

def low_keep(v):
    return (low(v), None)

def low_pass(kept, grad):
    return (grad,)

def back_keep(v):
    return (v, None)

def back_low(kept, grad):
    return (low(grad),)
low.defvjp(low_keep, low_pass)
low_back.defvjp(back_keep, back_low)
EPS = 1e-12
SCALE = 0.125
MASKED = -1e+30
ROOT_HALF = 0.7071067811865476

def matmul(left, right):
    return jnp.dot(left, right, preferred_element_type=jnp.float32, precision=lax.Precision.HIGHEST)

def rounded_both(value):
    return low(low_back(value))

def norm_apply(values_in, gain, shift):
    mean_row = lax.optimization_barrier(jnp.mean(values_in, -1, keepdims=True))
    centered = values_in - mean_row
    variance = lax.optimization_barrier(jnp.mean(centered * centered, -1, keepdims=True))
    return centered * lax.rsqrt(variance + EPS) * gain + shift

def gelu_exact(values_in):
    return 0.5 * values_in * (1.0 + jax.scipy.special.erf(values_in * ROOT_HALF))

def attend(queries, keys_all, values_all, segment_ids):
    length = queries.shape[0]
    head_count = queries.shape[1] // HD
    block_rows = min(512, length)
    block_count = length // block_rows
    segment_blocks = segment_ids.reshape(block_count, block_rows)

    def to_heads(flat):
        return flat.reshape(length, head_count, HD).transpose(1, 0, 2)

    def per_head(packed):
        query_head, key_head, value_head = packed

        def per_block(block_packed):
            query_block, segment_block = block_packed
            raw = low_back(matmul(query_block, key_head.T))
            scores = jnp.where(segment_block[:, None] == segment_ids[None, :], raw * SCALE, MASKED)
            row_max = lax.optimization_barrier(jnp.max(scores, -1, keepdims=True))
            exp_scores = jnp.exp(scores - row_max)
            probs = exp_scores / lax.optimization_barrier(jnp.sum(exp_scores, -1, keepdims=True))
            return matmul(low(probs), value_head)
        blocks_out = lax.map(jax.checkpoint(per_block), (query_head.reshape(block_count, block_rows, HD), segment_blocks))
        return blocks_out.reshape(length, HD)
    context = lax.map(per_head, (to_heads(queries), to_heads(keys_all), to_heads(values_all)))
    return context.transpose(1, 0, 2).reshape(length, head_count * HD)

def forward(hidden, segment_ids, params_in):
    query_weight, key_weight, value_weight, query_bias, value_bias, mixer_weight, mixer_bias, first_gain, first_shift, inner_weight, inner_bias, outer_weight, outer_bias, second_gain, second_shift = params_in
    queries = rounded_both(matmul(hidden, query_weight) + query_bias)
    keys_all = rounded_both(matmul(hidden, key_weight))
    values_all = rounded_both(matmul(hidden, value_weight) + value_bias)
    context = rounded_both(attend(queries, keys_all, values_all, segment_ids))
    mixed = low_back(matmul(context, mixer_weight))
    first = norm_apply(hidden + mixed + mixer_bias, first_gain, first_shift)
    inner = low_back(matmul(low(first), inner_weight) + inner_bias)
    active = low(gelu_exact(inner))
    outer = low_back(matmul(active, outer_weight))
    return norm_apply(first + outer + outer_bias, second_gain, second_shift)

def reference(hidden_in, segments, query_weight, key_weight, value_weight, query_bias, value_bias, mixer_weight, mixer_bias, first_gain, first_shift, inner_weight, inner_bias, outer_weight, outer_bias, second_gain, second_shift, cotangent):
    params_in = tuple((param.astype(jnp.float32) for param in (query_weight, key_weight, value_weight, query_bias, value_bias, mixer_weight, mixer_bias, first_gain, first_shift, inner_weight, inner_bias, outer_weight, outer_bias, second_gain, second_shift)))

    def per_sequence(totals, packed):
        hidden_seq, segment_seq, cot_seq = packed
        hidden_float = hidden_seq.astype(jnp.float32)
        result, pullback = jax.vjp(lambda hidden, params_now: forward(hidden, segment_seq, params_now), hidden_float, params_in)
        grad_hidden, grad_params = pullback(cot_seq.astype(jnp.float32))
        totals = jax.tree.map(lambda total, term: total + term, totals, grad_params)
        return (totals, (result.astype(jnp.bfloat16), grad_hidden.astype(jnp.bfloat16)))
    zero_totals = jax.tree.map(jnp.zeros_like, params_in)
    totals, (layer_out, input_grad) = lax.scan(per_sequence, zero_totals, (hidden_in, segments, cotangent))
    return (layer_out, input_grad, totals[0], totals[1], totals[2], totals[3], totals[4], totals[5], totals[6], totals[7], totals[8], totals[9], totals[10], totals[11], totals[12], totals[13], totals[14])
```

```python
import functools

import jax
import jax.numpy as jnp
from jax import lax
from jax.experimental import pallas as pl
from jax.experimental.pallas import tpu as pltpu
from jax.sharding import PartitionSpec as P

EPS = 1e-12
ROOT_HALF = 0.7071067811865476
INV_ROOT_TWO_PI = 0.3989422804014327
HD=64; SCALE=0.125; APART=-1e30
VM=pltpu.VMEM

def dot(a,b): return jnp.dot(a,b,preferred_element_type=jnp.float32)

def project_body(heads, x_ref, w_ref, b_ref, scol_ref, srow_ref, qt_ref, ka_ref, vt_ref, qn_ref, kt_ref, vn_ref):
    y = dot(x_ref[...], w_ref[...]) + b_ref[...]
    width = heads*HD
    low = y.astype(jnp.bfloat16)
    yt = y.T.astype(jnp.bfloat16)
    rows = y.shape[0]
    apart = jnp.where(lax.broadcasted_iota(jnp.int32,(HD,rows),0)==srow_ref[...],0.0,APART).astype(jnp.bfloat16)
    same = (lax.broadcasted_iota(jnp.int32,(rows,HD),1)==scol_ref[...]).astype(jnp.float32).astype(jnp.bfloat16)
    for h in range(heads):
        at=h*HD
        qt_ref[h,:HD,:]=yt[at:at+HD]*jnp.bfloat16(SCALE)
        qt_ref[h,HD:,:]=apart
        qn_ref[h]=low[:,at:at+HD]*jnp.bfloat16(SCALE)
        ka_ref[h]=jnp.concatenate([low[:,width+at:width+at+HD],same],axis=1)
        kt_ref[h]=yt[width+at:width+at+HD]
        vt_ref[h]=yt[2*width+at:2*width+at+HD]
        vn_ref[h]=low[:,2*width+at:2*width+at+HD]

def project(x,w,b,seg,rows=512):
    L,D=x.shape; heads=w.shape[1]//(3*HD)
    bf=jnp.bfloat16
    nat=lambda n: pl.BlockSpec((heads,rows,n),lambda i:(0,i,0))
    tr=lambda n: pl.BlockSpec((heads,n,rows),lambda i:(0,0,i))
    S=jax.ShapeDtypeStruct
    return pl.pallas_call(functools.partial(project_body,heads),grid=(L//rows,),
        in_specs=[pl.BlockSpec((rows,D),lambda i:(i,0)),pl.BlockSpec(w.shape,lambda i:(0,0)),pl.BlockSpec((1,w.shape[1]),lambda i:(0,0)),
                  pl.BlockSpec((rows,1),lambda i:(i,0)),pl.BlockSpec((1,rows),lambda i:(0,i))],
        out_specs=[tr(2*HD),nat(2*HD),tr(HD),nat(HD),tr(HD),nat(HD)],
        out_shape=[S((heads,2*HD,L),bf),S((heads,L,2*HD),bf),S((heads,HD,L),bf),S((heads,L,HD),bf),S((heads,HD,L),bf),S((heads,L,HD),bf)],
        compiler_params=pltpu.CompilerParams(vmem_limit_bytes=48<<20),
        cost_estimate=pl.CostEstimate(flops=2*L*D*w.shape[1],bytes_accessed=L*D*2+w.size*2+L*heads*HD*2*10,transcendentals=0),
        name="project")(x,w,b.reshape(1,-1),seg.reshape(-1,1),seg.reshape(1,-1))

def forward_body(heads, BK, lo_ref, hi_ref, qt_ref, ka_ref, vt_ref, ctx_ref, ot_ref, lse_ref, m_s, l_s, acc):
    i=pl.program_id(0)
    BQ=qt_ref.shape[2]
    m_s[...]=jnp.full(m_s.shape,-jnp.inf,jnp.float32)
    l_s[...]=jnp.zeros(l_s.shape,jnp.float32)
    acc[...]=jnp.zeros(acc.shape,jnp.float32)
    def step(j,_):
        at=pl.multiple_of(j*BK,BK)
        for h in range(heads):
            s=dot(ka_ref[h,pl.ds(at,BK),:],qt_ref[h])
            m_old=m_s[h]
            m_new=jnp.maximum(m_old,jnp.max(s,axis=0,keepdims=True))
            p=jnp.exp(s-m_new)
            alpha=jnp.exp(m_old-m_new)
            m_s[h]=m_new
            l_s[h]=l_s[h]*alpha+jnp.sum(p,axis=0,keepdims=True)
            acc[h]=acc[h]*alpha+dot(vt_ref[h,:,pl.ds(at,BK)],p.astype(jnp.bfloat16))
        return 0
    lax.fori_loop(lo_ref[i],hi_ref[i],step,0)
    outs=[]
    for h in range(heads):
        outs.append(acc[h]/l_s[h])
        lse_ref[h]=m_s[h]+jnp.log(l_s[h])
    o=jnp.concatenate(outs,axis=0)
    ot_ref[...]=o
    ctx_ref[...]=o.T.astype(jnp.bfloat16)

def attend_forward(qt,ka,vt,lo,hi,BQ=512,BK=512):
    heads,_,L=qt.shape
    S=jax.ShapeDtypeStruct; W=heads*HD
    return pl.pallas_call(functools.partial(forward_body,heads,BK),
        grid_spec=pltpu.PrefetchScalarGridSpec(num_scalar_prefetch=2,grid=(L//BQ,),
        in_specs=[pl.BlockSpec((heads,2*HD,BQ),lambda i,*_:(0,0,i)),pl.BlockSpec(ka.shape,lambda i,*_:(0,0,0)),pl.BlockSpec(vt.shape,lambda i,*_:(0,0,0))],
        out_specs=[pl.BlockSpec((BQ,W),lambda i,*_:(i,0)),pl.BlockSpec((W,BQ),lambda i,*_:(0,i)),pl.BlockSpec((heads,1,BQ),lambda i,*_:(0,0,i))],
        scratch_shapes=[VM((heads,1,BQ),jnp.float32),VM((heads,1,BQ),jnp.float32),VM((heads,HD,BQ),jnp.float32)]),
        out_shape=[S((L,W),jnp.bfloat16),S((W,L),jnp.float32),S((heads,1,L),jnp.float32)],
        compiler_params=pltpu.CompilerParams(vmem_limit_bytes=56<<20),
        cost_estimate=pl.CostEstimate(flops=2*L*L*HD*2*heads,bytes_accessed=L*heads*HD*2*8,transcendentals=L*L*heads),
        name="attend_forward")(lo,hi,qt,ka,vt)

def backward_body(heads, BQ, BK, lo_ref, hi_ref, go_ref, ot_ref, lse_ref, qt_ref, ka_ref, qn_ref, kt_ref, vn_ref, dq_ref, dk_ref, dv_ref, got, gon, delta, dqt, dk_s, dv_s):
    L=go_ref.shape[0]; W=heads*HD
    CH=512
    for c in range(L//CH):
        g=go_ref[c*CH:(c+1)*CH,:]
        gt=g.astype(jnp.float32).T
        prod=gt*ot_ref[:,c*CH:(c+1)*CH]
        for h in range(heads):
            got[h,:,c*CH:(c+1)*CH]=gt[h*HD:(h+1)*HD].astype(jnp.bfloat16)
            gon[h,c*CH:(c+1)*CH,:]=g[:,h*HD:(h+1)*HD]
            delta[h,:,c*CH:(c+1)*CH]=jnp.sum(prod[h*HD:(h+1)*HD],axis=0,keepdims=True)
    dqt[...]=jnp.zeros(dqt.shape,jnp.float32)
    def key_block(j,_):
        ka_at=pl.multiple_of(j*BK,BK)
        dk_s[...]=jnp.zeros(dk_s.shape,jnp.float32)
        dv_s[...]=jnp.zeros(dv_s.shape,jnp.float32)
        def query_block(i,_):
            at=pl.multiple_of(i*BQ,BQ)
            for h in range(heads):
                s=dot(ka_ref[h,pl.ds(ka_at,BK),:],qt_ref[h,:,pl.ds(at,BQ)])
                p=jnp.exp(s-lse_ref[h,:,pl.ds(at,BQ)])
                dp=dot(vn_ref[h,pl.ds(ka_at,BK),:],got[h,:,pl.ds(at,BQ)])
                ds=(p*(dp-delta[h,:,pl.ds(at,BQ)])).astype(jnp.bfloat16)
                dv_s[h]+=dot(p.astype(jnp.bfloat16),gon[h,pl.ds(at,BQ),:])
                dk_s[h]+=dot(ds,qn_ref[h,pl.ds(at,BQ),:])
                dqt[h,:,pl.ds(at,BQ)]+=dot(kt_ref[h,:,pl.ds(ka_at,BK)],ds)
            return 0
        lax.fori_loop(lo_ref[j],hi_ref[j],query_block,0)
        dk_ref[pl.ds(ka_at,BK),:]=jnp.concatenate([dk_s[h] for h in range(heads)],axis=1).astype(jnp.bfloat16)
        dv_ref[pl.ds(ka_at,BK),:]=jnp.concatenate([dv_s[h] for h in range(heads)],axis=1).astype(jnp.bfloat16)
        return 0
    lax.fori_loop(0,L//BK,key_block,0)
    for c in range(L//CH):
        dq_ref[c*CH:(c+1)*CH,:]=(jnp.concatenate([dqt[h,:,c*CH:(c+1)*CH] for h in range(heads)],axis=0).T*SCALE).astype(jnp.bfloat16)

def attend_backward(go,ot,lse,qt,ka,qn,kt,vn,lo,hi,BQ=512,BK=512):
    L,W=go.shape; heads=W//HD
    S=jax.ShapeDtypeStruct; f32=jnp.float32; bf=jnp.bfloat16
    ins=[go,ot,lse,qt,ka,qn,kt,vn]
    def full(a): return pl.BlockSpec(a.shape,lambda i,*_:(0,)*a.ndim)
    out=[S((L,W),bf)]*3
    return pl.pallas_call(functools.partial(backward_body,heads,BQ,BK),
        grid_spec=pltpu.PrefetchScalarGridSpec(num_scalar_prefetch=2,grid=(1,),
        in_specs=[pl.BlockSpec(a.shape,functools.partial(lambda n,i,*_:(0,)*n,a.ndim),pipeline_mode=pl.Buffered(1)) for a in ins],
        out_specs=[pl.BlockSpec((L,W),lambda i,*_:(0,0),pipeline_mode=pl.Buffered(1))]*3,
        scratch_shapes=[VM((heads,HD,L),bf),VM((heads,L,HD),bf),VM((heads,1,L),f32),VM((heads,HD,L),f32),VM((heads,BK,HD),f32),VM((heads,BK,HD),f32)]),
        out_shape=out,
        compiler_params=pltpu.CompilerParams(vmem_limit_bytes=60<<20),
        cost_estimate=pl.CostEstimate(flops=2*L*L*HD*5*heads,bytes_accessed=L*heads*HD*2*14,transcendentals=L*L*heads),
        name="attend_backward")(lo,hi,*ins)

def ranges(seg,BQ,BK):
    L=seg.shape[0]
    first=seg.reshape(-1,BQ)[:,0]; last=seg.reshape(-1,BQ)[:,-1]
    kf=seg.reshape(-1,BK)[:,0]; kl=seg.reshape(-1,BK)[:,-1]
    lo=jnp.sum((kl[None,:]<first[:,None]).astype(jnp.int32),1)
    hi=jnp.sum((kf[None,:]<=last[:,None]).astype(jnp.int32),1)
    return lo,hi


def dot_left_t(left, right):
    return lax.dot_general(
        left, right, (((0,), (0,)), ((), ())), preferred_element_type=jnp.float32
    )


def dot_right_t(left, right):
    return lax.dot_general(
        left, right, (((1,), (1,)), ((), ())), preferred_element_type=jnp.float32
    )


def layer_norm(values_in, gain, shift):
    mean_row = jnp.mean(values_in, -1, keepdims=True)
    centered = values_in - mean_row
    inverse = lax.rsqrt(jnp.mean(centered * centered, -1, keepdims=True) + EPS)
    normed = centered * inverse
    return (normed * gain + shift, normed, inverse)


def norm_back(grad_in, normed, inverse, gain):
    scaled = grad_in * gain
    return inverse * (
        scaled
        - jnp.mean(scaled, -1, keepdims=True)
        - normed * jnp.mean(scaled * normed, -1, keepdims=True)
    )


def gelu_value(inner):
    return 0.5 * inner * (1.0 + jax.scipy.special.erf(inner * ROOT_HALF))


def gelu_slope(inner):
    return (
        0.5 * (1.0 + jax.scipy.special.erf(inner * ROOT_HALF))
        + inner * jnp.exp(-0.5 * inner * inner) * INV_ROOT_TWO_PI
    )


def add_up(value):
    for axis in ("dp", "tensor"):
        size = lax.axis_size(axis)
        span = 1
        while span < size:
            value = value + lax.ppermute(value, axis, [(i, i ^ span) for i in range(size)])
            span *= 2
    return value


def body(hidden_in, segments, query_weight, key_weight, value_weight, query_bias, value_bias, mixer_weight, mixer_bias, first_gain, first_shift, inner_weight, inner_bias, outer_weight, outer_bias, second_gain, second_shift, cotangent):
    bf = jnp.bfloat16
    f32 = jnp.float32
    _, rows, width = hidden_in.shape
    parts = lax.axis_size("tensor")
    rank = lax.axis_index("tensor")
    own = query_weight.shape[1]
    units = inner_weight.shape[1]
    x_own = hidden_in[0]
    qkv_own = jnp.concatenate([query_weight, key_weight, value_weight], 1)
    qkv_all = lax.all_gather(qkv_own, "dp", axis=0, tiled=True)
    segment_all = lax.all_gather(segments[0], "tensor", axis=0, tiled=True)
    x_all = lax.all_gather(x_own, "tensor", axis=0, tiled=True)
    rest_own = jnp.concatenate([inner_weight, outer_weight.T, mixer_weight.T, qkv_own], 1)
    rest = lax.all_gather(rest_own, ("tensor", "dp"), axis=0, tiled=True)
    rest = rest.reshape(parts, width, rest_own.shape[1])
    biases = jnp.concatenate([query_bias, jnp.zeros_like(query_bias), value_bias])
    inner_bias_all = lax.all_gather(inner_bias, "tensor", axis=0, tiled=False)

    qt, ka, vt, qn, kt, vn = project(x_all, qkv_all, biases, segment_all)
    lo, hi = ranges(segment_all, 512, 512)
    context, context_t, lse = attend_forward(qt, ka, vt, lo, hi)
    context = lax.all_to_all(context.reshape(parts, rows, own), "tensor", 0, 0, tiled=True)
    parts_of = range(parts)
    w1 = [rest[t, :, :units] for t in parts_of]
    w2t = [rest[t, :, units : 2 * units] for t in parts_of]
    mt = [rest[t, :, 2 * units : 2 * units + own] for t in parts_of]
    context_own = jnp.concatenate([context[t] for t in parts_of], 1)
    mt_all = jnp.concatenate(mt, 1)
    mixed = dot_right_t(context_own, mt_all)
    attn_in = x_own.astype(f32) + mixed + mixer_bias
    first, first_norm, first_inv = layer_norm(attn_in, first_gain, first_shift)
    first_low = first.astype(bf)
    inner = [dot(first_low, w1[t]) + inner_bias_all[t] for t in parts_of]
    active = [gelu_value(inner[t]).astype(bf) for t in parts_of]
    outer = sum(dot_right_t(active[t], w2t[t]) for t in parts_of)
    second_in = first + outer + outer_bias
    second, second_norm, second_inv = layer_norm(second_in, second_gain, second_shift)
    layer_out = second.astype(bf)
    grad_out = cotangent[0].astype(f32)
    second_gain_grad = jnp.sum(grad_out * second_norm, 0)
    second_shift_grad = jnp.sum(grad_out, 0)
    grad_second = norm_back(grad_out, second_norm, second_inv, second_gain)
    outer_bias_grad = jnp.sum(grad_second, 0)
    second_low = grad_second.astype(bf)
    grad_inner = [(dot(second_low, w2t[t]) * gelu_slope(inner[t])).astype(bf) for t in parts_of]
    inner_bias_grad = jnp.stack([jnp.sum(g, 0, dtype=f32) for g in grad_inner])
    grad_first = grad_second + sum(dot_right_t(grad_inner[t], w1[t]) for t in parts_of)
    first_gain_grad = jnp.sum(grad_first * first_norm, 0)
    first_shift_grad = jnp.sum(grad_first, 0)
    grad_attn = norm_back(grad_first, first_norm, first_inv, first_gain)
    mixer_bias_grad = jnp.sum(grad_attn, 0)
    attn_low = grad_attn.astype(bf)
    grad_context = jnp.stack([dot(attn_low, mt[t]).astype(bf) for t in parts_of])
    grad_context = lax.all_to_all(grad_context, "tensor", 0, 0, tiled=True)
    weight_grads = jnp.stack(
        [
            jnp.concatenate(
                [
                    dot_left_t(first_low, grad_inner[t]),
                    dot_left_t(second_low, active[t]),
                    dot_left_t(attn_low, context[t]),
                ],
                1,
            ).astype(bf)
            for t in parts_of
        ]
    )
    weight_grads = lax.psum_scatter(weight_grads, "dp", scatter_dimension=1, tiled=True)
    weight_grads = lax.psum_scatter(weight_grads, "tensor", scatter_dimension=0, tiled=False)
    weight_grads = weight_grads.astype(f32)
    early = jnp.concatenate(
        [
            mixer_bias_grad,
            first_gain_grad,
            first_shift_grad,
            outer_bias_grad,
            second_gain_grad,
            second_shift_grad,
            inner_bias_grad.reshape(-1),
        ]
    )
    early = add_up(early)

    go = grad_context.reshape(parts * rows, own)
    grad_q, grad_k, grad_v = attend_backward(go, context_t, lse, qt, ka, qn, kt, vn, lo, hi)
    grad_qkv = jnp.concatenate([grad_q, grad_k, grad_v], 1)
    back = lax.all_to_all(grad_qkv.reshape(parts, rows, 3 * own), "tensor", 0, 0, tiled=True)
    qkv_grad = dot_left_t(x_all, grad_qkv).astype(bf)
    qkv_grad = lax.all_to_all(
        qkv_grad.reshape(-1, width // lax.axis_size("dp"), 3 * own), "dp", 0, 0, tiled=True
    )
    qkv_grad = jnp.sum(qkv_grad.astype(f32), 0)
    late = jnp.sum(grad_qkv, 0, dtype=f32)
    late = lax.psum(late, "dp")
    input_back = sum(dot_right_t(back[t], rest[t, :, 2 * units + own :]) for t in parts_of)
    input_grad = (grad_attn + input_back).astype(bf)
    stacked = early[: 6 * width].reshape(6, width)
    inner_bias_out = lax.dynamic_slice_in_dim(early, 6 * width + rank * units, units)
    return (
        layer_out[None],
        input_grad[None],
        qkv_grad[:, :own],
        qkv_grad[:, own : 2 * own],
        qkv_grad[:, 2 * own :],
        late[:own],
        late[2 * own :],
        weight_grads[:, 2 * units :].T,
        stacked[0],
        stacked[1],
        stacked[2],
        weight_grads[:, :units],
        inner_bias_out,
        weight_grads[:, units : 2 * units].T,
        stacked[3],
        stacked[4],
        stacked[5],
    )


def solution(mesh):
    placed = (
        P("dp", "tensor", None),
        P("dp", "tensor"),
        P("dp", "tensor"),
        P("dp", "tensor"),
        P("dp", "tensor"),
        P("tensor"),
        P("tensor"),
        P("tensor", "dp"),
        P(),
        P(),
        P(),
        P("dp", "tensor"),
        P("tensor"),
        P("tensor", "dp"),
        P(),
        P(),
        P(),
        P("dp", "tensor", None),
    )
    return jax.shard_map(
        body,
        mesh=mesh,
        in_specs=placed,
        out_specs=(
            P("dp", "tensor", None),
            P("dp", "tensor", None),
            P("dp", "tensor"),
            P("dp", "tensor"),
            P("dp", "tensor"),
            P("tensor"),
            P("tensor"),
            P("tensor", "dp"),
            P(),
            P(),
            P(),
            P("dp", "tensor"),
            P("tensor"),
            P("tensor", "dp"),
            P(),
            P(),
            P(),
        ),
        check_vma=False,
    )
```

```python
import functools

import jax
import jax.numpy as jnp
from jax import lax
from jax.experimental import pallas as pl
from jax.experimental.pallas import tpu as pltpu
from jax.sharding import PartitionSpec as P

EPS = 1e-12
ROOT_HALF = 0.7071067811865476
INV_ROOT_TWO_PI = 0.3989422804014327
HD=64; SCALE=0.125; APART=-1e30
VM=pltpu.VMEM

def dot(a,b): return jnp.dot(a,b,preferred_element_type=jnp.float32)

def project_body(heads, x_ref, w_ref, b_ref, scol_ref, srow_ref, qt_ref, ka_ref, vt_ref, qn_ref, kt_ref, vn_ref):
    y = dot(x_ref[...], w_ref[...]) + b_ref[...]
    low = y.astype(jnp.bfloat16)
    yt = y.T.astype(jnp.bfloat16)
    rows = y.shape[0]
    apart = jnp.where(lax.broadcasted_iota(jnp.int32,(HD,rows),0)==srow_ref[...],0.0,APART).astype(jnp.bfloat16)
    same = (lax.broadcasted_iota(jnp.int32,(rows,HD),1)==scol_ref[...]).astype(jnp.float32).astype(jnp.bfloat16)
    for h in range(heads):
        at=3*h*HD
        qt_ref[h,:HD,:]=yt[at:at+HD]*jnp.bfloat16(SCALE)
        qt_ref[h,HD:,:]=apart
        qn_ref[h]=low[:,at:at+HD]*jnp.bfloat16(SCALE)
        ka_ref[h]=jnp.concatenate([low[:,at+HD:at+2*HD],same],axis=1)
        kt_ref[h]=yt[at+HD:at+2*HD]
        vt_ref[h]=yt[at+2*HD:at+3*HD]
        vn_ref[h]=low[:,at+2*HD:at+3*HD]

def project(x,w,b,seg,rows=512):
    L,D=x.shape; heads=w.shape[1]//(3*HD)
    bf=jnp.bfloat16
    nat=lambda n: pl.BlockSpec((heads,rows,n),lambda i:(0,i,0))
    tr=lambda n: pl.BlockSpec((heads,n,rows),lambda i:(0,0,i))
    S=jax.ShapeDtypeStruct
    return pl.pallas_call(functools.partial(project_body,heads),grid=(L//rows,),
        in_specs=[pl.BlockSpec((rows,D),lambda i:(i,0)),pl.BlockSpec(w.shape,lambda i:(0,0)),pl.BlockSpec((1,w.shape[1]),lambda i:(0,0)),
                  pl.BlockSpec((rows,1),lambda i:(i,0)),pl.BlockSpec((1,rows),lambda i:(0,i))],
        out_specs=[tr(2*HD),nat(2*HD),tr(HD),nat(HD),tr(HD),nat(HD)],
        out_shape=[S((heads,2*HD,L),bf),S((heads,L,2*HD),bf),S((heads,HD,L),bf),S((heads,L,HD),bf),S((heads,HD,L),bf),S((heads,L,HD),bf)],
        compiler_params=pltpu.CompilerParams(vmem_limit_bytes=48<<20),
        cost_estimate=pl.CostEstimate(flops=2*L*D*w.shape[1],bytes_accessed=L*D*2+w.size*2+L*heads*HD*2*10,transcendentals=0),
        name="project")(x,w,b.reshape(1,-1),seg.reshape(-1,1),seg.reshape(1,-1))

def forward_body(BK, SUB, lo_ref, hi_ref, qt_ref, ka_ref, vt_ref, ctx_ref, ot_ref, lse_ref, m_s, l_s, acc):
    i=pl.program_id(0)
    heads,_,BQ=qt_ref.shape
    chains=[(h,slice(c*SUB,(c+1)*SUB)) for h in range(heads) for c in range(BQ//SUB)]
    m_s[...]=jnp.full(m_s.shape,-jnp.inf,jnp.float32)
    l_s[...]=jnp.zeros(l_s.shape,jnp.float32)
    acc[...]=jnp.zeros(acc.shape,jnp.float32)
    def step(j,_):
        at=pl.multiple_of(j*BK,BK)
        for h,cut in chains:
            s=dot(ka_ref[h,pl.ds(at,BK),:],qt_ref[h,:,cut])
            m_old=m_s[h,:,cut]
            m_new=jnp.maximum(m_old,jnp.max(s,axis=0,keepdims=True))
            p=jnp.exp(s-m_new)
            alpha=jnp.exp(m_old-m_new)
            m_s[h,:,cut]=m_new
            l_s[h,:,cut]=l_s[h,:,cut]*alpha+jnp.sum(p,axis=0,keepdims=True)
            acc[h,:,cut]=acc[h,:,cut]*alpha+dot(vt_ref[h,:,pl.ds(at,BK)],p.astype(jnp.bfloat16))
        return 0
    lax.fori_loop(lo_ref[i],hi_ref[i],step,0)
    for h in range(heads):
        o=acc[h]/l_s[h]
        lse_ref[h]=m_s[h]+jnp.log(l_s[h])
        ot_ref[h]=o
        ctx_ref[0,h*HD:(h+1)*HD,:]=o.astype(jnp.bfloat16)

def attend_forward(first,heads,parts,qt,ka,vt,lo,hi,BQ=384,BK=512,SUB=384):
    L=qt.shape[2]
    S=jax.ShapeDtypeStruct
    per=L//parts//BQ
    return pl.pallas_call(functools.partial(forward_body,BK,SUB),
        grid_spec=pltpu.PrefetchScalarGridSpec(num_scalar_prefetch=2,grid=(L//BQ,),
        in_specs=[pl.BlockSpec((heads,2*HD,BQ),lambda i,*_:(first//heads,0,i)),pl.BlockSpec((heads,L,2*HD),lambda i,*_:(first//heads,0,0)),pl.BlockSpec((heads,HD,L),lambda i,*_:(first//heads,0,0))],
        out_specs=[pl.BlockSpec((1,heads*HD,BQ),lambda i,*_:(i//per,0,i%per)),pl.BlockSpec((heads,HD,BQ),lambda i,*_:(0,0,i)),pl.BlockSpec((heads,1,BQ),lambda i,*_:(0,0,i))],
        scratch_shapes=[VM((heads,1,BQ),jnp.float32),VM((heads,1,BQ),jnp.float32),VM((heads,HD,BQ),jnp.float32)]),
        out_shape=[S((parts,heads*HD,L//parts),jnp.bfloat16),S((heads,HD,L),jnp.float32),S((heads,1,L),jnp.float32)],
        compiler_params=pltpu.CompilerParams(vmem_limit_bytes=56<<20),
        cost_estimate=pl.CostEstimate(flops=2*L*L*HD*2*heads,bytes_accessed=L*heads*HD*2*8,transcendentals=L*L*heads),
        name="attend_forward")(lo,hi,qt,ka,vt)

def backward_body(BQ, BK, SUB, lo_ref, hi_ref, go_ref, ot_ref, lse_ref, qt_ref, ka_ref, qn_ref, kt_ref, vn_ref, out_ref, got, gon, delta, dqt, dkt, dvt, dk_s, dv_s):
    parts,_,rows=go_ref.shape
    heads,_,L=qt_ref.shape
    CH=256
    for h in range(heads):
        for c in range(L//CH):
            p,at=c*CH//rows,c*CH%rows
            gt=go_ref[p,h*HD:(h+1)*HD,at:at+CH]
            wide=gt.astype(jnp.float32)
            got[h,:,c*CH:(c+1)*CH]=gt
            gon[h,c*CH:(c+1)*CH,:]=wide.T.astype(jnp.bfloat16)
            delta[h,:,c*CH:(c+1)*CH]=jnp.sum(wide*ot_ref[h,:,c*CH:(c+1)*CH],axis=0,keepdims=True)
    dqt[...]=jnp.zeros(dqt.shape,jnp.float32)
    def key_block(j,_):
        ka_at=pl.multiple_of(j*BK,BK)
        dk_s[...]=jnp.zeros(dk_s.shape,jnp.float32)
        dv_s[...]=jnp.zeros(dv_s.shape,jnp.float32)
        def query_block(i,_):
            for h,c in [(h,c) for h in range(heads) for c in range(BQ//SUB)]:
                at=pl.multiple_of(i*BQ+c*SUB,SUB)
                s=dot(ka_ref[h,pl.ds(ka_at,BK),:],qt_ref[h,:,pl.ds(at,SUB)])
                p=jnp.exp(s-lse_ref[h,:,pl.ds(at,SUB)])
                dp=dot(vn_ref[h,pl.ds(ka_at,BK),:],got[h,:,pl.ds(at,SUB)])
                ds=(p*(dp-delta[h,:,pl.ds(at,SUB)])).astype(jnp.bfloat16)
                dv_s[h]+=dot(p.astype(jnp.bfloat16),gon[h,pl.ds(at,SUB),:])
                dk_s[h]+=dot(ds,qn_ref[h,pl.ds(at,SUB),:])
                dqt[h,:,pl.ds(at,SUB)]+=dot(kt_ref[h,:,pl.ds(ka_at,BK)],ds)
            return 0
        lax.fori_loop(lo_ref[j],hi_ref[j],query_block,0)
        for h in range(heads):
            dkt[h,:,pl.ds(ka_at,BK)]=dk_s[h].T.astype(jnp.bfloat16)
            dvt[h,:,pl.ds(ka_at,BK)]=dv_s[h].T.astype(jnp.bfloat16)
        return 0
    lax.fori_loop(0,L//BK,key_block,0)
    for h in range(heads):
        for p in range(parts):
            cut=slice(p*rows,(p+1)*rows)
            out_ref[p,3*h*HD:(3*h+1)*HD,:]=(dqt[h,:,cut]*SCALE).astype(jnp.bfloat16)
            out_ref[p,(3*h+1)*HD:(3*h+2)*HD,:]=dkt[h,:,cut]
            out_ref[p,(3*h+2)*HD:(3*h+3)*HD,:]=dvt[h,:,cut]

def attend_backward(first,heads,go,ot,lse,qt,ka,qn,kt,vn,lo,hi,BQ=512,BK=512,SUB=512):
    parts,_,rows=go.shape; L=parts*rows
    S=jax.ShapeDtypeStruct; f32=jnp.float32; bf=jnp.bfloat16
    whole=lambda a: pl.BlockSpec(a.shape,lambda i,*_:(0,0,0),pipeline_mode=pl.Buffered(1))
    some=lambda a: pl.BlockSpec((heads,)+a.shape[1:],lambda i,*_:(first//heads,0,0),pipeline_mode=pl.Buffered(1))
    return pl.pallas_call(functools.partial(backward_body,BQ,BK,SUB),
        grid_spec=pltpu.PrefetchScalarGridSpec(num_scalar_prefetch=2,grid=(1,),
        in_specs=[whole(go),whole(ot),whole(lse)]+[some(a) for a in (qt,ka,qn,kt,vn)],
        out_specs=pl.BlockSpec((parts,3*heads*HD,rows),lambda i,*_:(0,0,0),pipeline_mode=pl.Buffered(1)),
        scratch_shapes=[VM((heads,HD,L),bf),VM((heads,L,HD),bf),VM((heads,1,L),f32),VM((heads,HD,L),f32),VM((heads,HD,L),bf),VM((heads,HD,L),bf),VM((heads,BK,HD),f32),VM((heads,BK,HD),f32)]),
        out_shape=S((parts,3*heads*HD,rows),bf),
        compiler_params=pltpu.CompilerParams(vmem_limit_bytes=60<<20),
        cost_estimate=pl.CostEstimate(flops=2*L*L*HD*5*heads,bytes_accessed=L*heads*HD*2*14,transcendentals=L*L*heads),
        name="attend_backward")(lo,hi,go,ot,lse,qt,ka,qn,kt,vn)

def ranges(seg,BQ,BK):
    L=seg.shape[0]
    first=seg.reshape(-1,BQ)[:,0]; last=seg.reshape(-1,BQ)[:,-1]
    kf=seg.reshape(-1,BK)[:,0]; kl=seg.reshape(-1,BK)[:,-1]
    lo=jnp.sum((kl[None,:]<first[:,None]).astype(jnp.int32),1)
    hi=jnp.sum((kf[None,:]<=last[:,None]).astype(jnp.int32),1)
    return lo,hi


def dot_left_t(left, right):
    return lax.dot_general(
        left, right, (((0,), (0,)), ((), ())), preferred_element_type=jnp.float32
    )


def dot_right_t(left, right):
    return lax.dot_general(
        left, right, (((1,), (1,)), ((), ())), preferred_element_type=jnp.float32
    )


def layer_norm(values_in, gain, shift):
    mean_row = jnp.mean(values_in, -1, keepdims=True)
    centered = values_in - mean_row
    inverse = lax.rsqrt(jnp.mean(centered * centered, -1, keepdims=True) + EPS)
    normed = centered * inverse
    return (normed * gain + shift, normed, inverse)


def norm_back(grad_in, normed, inverse, gain):
    scaled = grad_in * gain
    return inverse * (
        scaled
        - jnp.mean(scaled, -1, keepdims=True)
        - normed * jnp.mean(scaled * normed, -1, keepdims=True)
    )


def gelu_value(inner):
    return 0.5 * inner * (1.0 + jax.scipy.special.erf(inner * ROOT_HALF))


def gelu_slope(inner):
    return (
        0.5 * (1.0 + jax.scipy.special.erf(inner * ROOT_HALF))
        + inner * jnp.exp(-0.5 * inner * inner) * INV_ROOT_TWO_PI
    )


def weight_grads_body(parts, first_ref, second_ref, attn_ref, inner_ref, active_ref, context_ref, out_ref, ft, st):
    j = pl.program_id(0)

    @pl.when(j == 0)
    def _():
        ft[...] = first_ref[...].T
        st[...] = second_ref[...].T

    @pl.when((j < 2 * parts) & (j % 2 == 0))
    def _():
        out_ref[...] = dot(ft[...], inner_ref[0]).astype(out_ref.dtype)

    @pl.when((j < 2 * parts) & (j % 2 == 1))
    def _():
        out_ref[...] = dot(st[...], active_ref[0]).astype(out_ref.dtype)

    @pl.when(j == 2 * parts)
    def _():
        out_ref[...] = dot_right_t(attn_ref[...].T, context_ref[...]).astype(out_ref.dtype)


def weight_grads_of(first_low, second_low, attn_low, grad_inner, active, context):
    parts, rows, units = active.shape
    width = first_low.shape[1]
    features = context.shape[0]
    fixed = pl.BlockSpec((rows, width), lambda j: (0, 0))
    moving = lambda shift: pl.BlockSpec((1, rows, units), lambda j: (jnp.clip((j - shift) // 2, 0, parts - 1), 0, 0))
    return pl.pallas_call(
        functools.partial(weight_grads_body, parts),
        grid=(2 * parts + 1,),
        in_specs=[fixed, fixed, fixed, moving(0), moving(1), pl.BlockSpec((features, rows), lambda j: (0, 0))],
        out_specs=pl.BlockSpec((width, units), lambda j: (0, j)),
        out_shape=jax.ShapeDtypeStruct((width, units * 2 * parts + features), jnp.bfloat16),
        scratch_shapes=[VM((width, rows), jnp.bfloat16), VM((width, rows), jnp.bfloat16)],
        compiler_params=pltpu.CompilerParams(vmem_limit_bytes=40 << 20),
        cost_estimate=pl.CostEstimate(flops=2 * rows * width * (2 * parts * units + features), bytes_accessed=rows * units * 2 * parts * 4, transcendentals=0),
        name="weight_grads",
    )(first_low, second_low, attn_low, grad_inner, active, context)

def add_up(value):
    for axis in ("dp", "tensor"):
        size = lax.axis_size(axis)
        span = 1
        while span < size:
            value = value + lax.ppermute(value, axis, [(i, i ^ span) for i in range(size)])
            span *= 2
    return value


def body(hidden_in, segments, query_weight, key_weight, value_weight, query_bias, value_bias, mixer_weight, mixer_bias, first_gain, first_shift, inner_weight, inner_bias, outer_weight, outer_bias, second_gain, second_shift, cotangent):
    bf = jnp.bfloat16
    f32 = jnp.float32
    _, rows, width = hidden_in.shape
    parts = lax.axis_size("tensor")
    groups = lax.axis_size("dp")
    rank = lax.axis_index("tensor")
    own = query_weight.shape[1]
    heads = own // HD
    three = 3 * HD
    units = inner_weight.shape[1]
    parts_of = range(parts)
    by_head = lambda q, k, v: jnp.stack([a.reshape(a.shape[:-1] + (heads, HD)) for a in (q, k, v)], -2).reshape(q.shape[:-1] + (3 * own,))
    x_own = hidden_in[0]
    qkv_own = by_head(query_weight, key_weight, value_weight)
    qkv_all = lax.all_gather(qkv_own, "dp", axis=0, tiled=True)
    small = jnp.concatenate([segments[0].astype(f32), inner_bias])
    small = lax.all_gather(small[None], "tensor", axis=0, tiled=True)
    segment_all = small[:, :rows].astype(jnp.int32).reshape(-1)
    inner_bias_all = small[:, rows:]
    x_all = lax.all_gather(x_own, "tensor", axis=0, tiled=True)
    rest_own = jnp.concatenate([inner_weight, outer_weight.T, mixer_weight.T, qkv_own], 1)
    rest = lax.all_gather(rest_own, ("tensor", "dp"), axis=0, tiled=True)
    rest = rest.reshape(parts, width, rest_own.shape[1])
    biases = by_head(query_bias, jnp.zeros_like(query_bias), value_bias)

    qt, ka, vt, qn, kt, vn = project(x_all, qkv_all, biases, segment_all)
    lo, hi = ranges(segment_all, 384, 512)
    context, context_t, lse = attend_forward(0, heads, parts, qt, ka, vt, lo, hi)
    context = lax.all_to_all(context, "tensor", 0, 0, tiled=True)
    w1 = [rest[t, :, :units] for t in parts_of]
    w2t = [rest[t, :, units : 2 * units] for t in parts_of]
    mt = [rest[t, :, 2 * units : 2 * units + own] for t in parts_of]
    contract = lambda a, b, i, j: lax.dot_general(a, b, (((i,), (j,)), ((), ())), preferred_element_type=f32)
    mixed = sum(contract(context[t], mt[t], 0, 1) for t in parts_of)
    attn_in = x_own.astype(f32) + mixed + mixer_bias
    first, first_norm, first_inv = layer_norm(attn_in, first_gain, first_shift)
    first_low = first.astype(bf)
    inner = [dot(first_low, w1[t]) + inner_bias_all[t] for t in parts_of]
    active = [gelu_value(inner[t]).astype(bf) for t in parts_of]
    outer = sum(dot_right_t(active[t], w2t[t]) for t in parts_of)
    second_in = first + outer + outer_bias
    second, second_norm, second_inv = layer_norm(second_in, second_gain, second_shift)
    layer_out = second.astype(bf)
    grad_out = cotangent[0].astype(f32)
    second_gain_grad = jnp.sum(grad_out * second_norm, 0)
    second_shift_grad = jnp.sum(grad_out, 0)
    grad_second = norm_back(grad_out, second_norm, second_inv, second_gain)
    outer_bias_grad = jnp.sum(grad_second, 0)
    second_low = grad_second.astype(bf)
    grad_inner = [(dot(second_low, w2t[t]) * gelu_slope(inner[t])).astype(bf) for t in parts_of]
    inner_bias_grad = jnp.stack([jnp.sum(g, 0, dtype=f32) for g in grad_inner])
    grad_first = grad_second + sum(dot_right_t(grad_inner[t], w1[t]) for t in parts_of)
    first_gain_grad = jnp.sum(grad_first * first_norm, 0)
    first_shift_grad = jnp.sum(grad_first, 0)
    grad_attn = norm_back(grad_first, first_norm, first_inv, first_gain)
    mixer_bias_grad = jnp.sum(grad_attn, 0)
    attn_low = grad_attn.astype(bf)
    grad_context = jnp.stack([contract(mt[t], attn_low, 0, 1).astype(bf) for t in parts_of])
    go = [
        lax.all_to_all(grad_context[:, h * HD : (h + 1) * HD], "tensor", 0, 0, tiled=True)
        for h in range(heads)
    ]
    weight_grads = weight_grads_of(
        first_low, second_low, attn_low, jnp.stack(grad_inner), jnp.stack(active), context.reshape(-1, rows)
    )
    weight_grads = lax.psum_scatter(weight_grads, "dp", scatter_dimension=0, tiled=True)
    weight_grads = jnp.concatenate(
        [
            weight_grads[:, : 2 * units * parts].reshape(-1, parts, 2 * units),
            weight_grads[:, 2 * units * parts :].reshape(-1, parts, own),
        ],
        2,
    ).transpose(1, 0, 2)
    weight_grads = lax.all_to_all(weight_grads, "tensor", 0, 0, tiled=True)
    weight_grads = jnp.sum(weight_grads.astype(f32), 0)
    early = jnp.concatenate(
        [
            mixer_bias_grad,
            first_gain_grad,
            first_shift_grad,
            outer_bias_grad,
            second_gain_grad,
            second_shift_grad,
            inner_bias_grad.reshape(-1),
        ]
    )
    early = add_up(early)

    lo, hi = ranges(segment_all, 512, 512)
    x_parts = x_all.reshape(parts, rows, width)
    input_back = grad_attn
    qkv_grad = []
    bias_grad = []
    for h in range(heads):
        grads = attend_backward(h, 1, go[h], context_t[h : h + 1], lse[h : h + 1], qt, ka, qn, kt, vn, lo, hi)
        back = lax.all_to_all(grads, "tensor", 0, 0, tiled=True)
        qkv_grad.append(sum(contract(x_parts[p], grads[p], 0, 1) for p in parts_of))
        bias_grad.append(jnp.sum(grads, (0, 2), dtype=f32))
        at = 2 * units + own + h * three
        input_back = input_back + sum(contract(back[t], rest[t, :, at : at + three], 0, 1) for t in parts_of)
    input_grad = input_back.astype(bf)
    bias_grad = jnp.concatenate(bias_grad)
    high = bias_grad.astype(bf)
    low = (bias_grad - high.astype(f32)).astype(bf)
    each = width // groups
    qkv_grad = jnp.concatenate(qkv_grad, 1).astype(bf).reshape(groups, each, 3 * own)
    extra = jnp.broadcast_to(jnp.stack([high, low])[None], (groups, 2, 3 * own))
    qkv_grad = lax.all_to_all(jnp.concatenate([qkv_grad, extra], 1), "dp", 0, 0, tiled=True)
    qkv_grad = jnp.sum(qkv_grad.astype(f32), 0)
    bias_grad = qkv_grad[each] + qkv_grad[each + 1]
    pick = lambda a, n: a.reshape(a.shape[:-1] + (heads, 3, HD))[..., n, :].reshape(a.shape[:-1] + (own,))
    stacked = early[: 6 * width].reshape(6, width)
    inner_bias_out = lax.dynamic_slice_in_dim(early, 6 * width + rank * units, units)
    return (
        layer_out[None],
        input_grad[None],
        pick(qkv_grad[:each], 0),
        pick(qkv_grad[:each], 1),
        pick(qkv_grad[:each], 2),
        pick(bias_grad, 0),
        pick(bias_grad, 2),
        weight_grads[:, 2 * units :].T,
        stacked[0],
        stacked[1],
        stacked[2],
        weight_grads[:, :units],
        inner_bias_out,
        weight_grads[:, units : 2 * units].T,
        stacked[3],
        stacked[4],
        stacked[5],
    )


def solution(mesh):
    placed = (
        P("dp", "tensor", None),
        P("dp", "tensor"),
        P("dp", "tensor"),
        P("dp", "tensor"),
        P("dp", "tensor"),
        P("tensor"),
        P("tensor"),
        P("tensor", "dp"),
        P(),
        P(),
        P(),
        P("dp", "tensor"),
        P("tensor"),
        P("tensor", "dp"),
        P(),
        P(),
        P(),
        P("dp", "tensor", None),
    )
    return jax.shard_map(
        body,
        mesh=mesh,
        in_specs=placed,
        out_specs=(
            P("dp", "tensor", None),
            P("dp", "tensor", None),
            P("dp", "tensor"),
            P("dp", "tensor"),
            P("dp", "tensor"),
            P("tensor"),
            P("tensor"),
            P("tensor", "dp"),
            P(),
            P(),
            P(),
            P("dp", "tensor"),
            P("tensor"),
            P("tensor", "dp"),
            P(),
            P(),
            P(),
        ),
        check_vma=False,
    )
```

```python
import functools

import jax
import jax.numpy as jnp
from jax import lax
from jax.experimental import pallas as pl
from jax.experimental.pallas import tpu as pltpu
from jax.sharding import PartitionSpec as P


EPS = 1e-12
ROOT_HALF = 0.7071067811865476
INV_ROOT_TWO_PI = 0.3989422804014327
HD=64; SCALE=0.125; APART=-1e30
VM=pltpu.VMEM


def dot(a,b): return jnp.dot(a,b,preferred_element_type=jnp.float32)


def project_body(heads, x_ref, w_ref, b_ref, scol_ref, srow_ref, qt_ref, ka_ref, vt_ref, qn_ref, kt_ref, vn_ref):
    y = dot(x_ref[...], w_ref[...]) + b_ref[...]
    low = y.astype(jnp.bfloat16)
    yt = y.T.astype(jnp.bfloat16)
    rows = y.shape[0]
    apart = jnp.where(lax.broadcasted_iota(jnp.int32,(HD,rows),0)==srow_ref[...],0.0,APART).astype(jnp.bfloat16)
    same = (lax.broadcasted_iota(jnp.int32,(rows,HD),1)==scol_ref[...]).astype(jnp.float32).astype(jnp.bfloat16)
    for h in range(heads):
        at=3*h*HD
        qt_ref[h,:HD,:]=yt[at:at+HD]*jnp.bfloat16(SCALE)
        qt_ref[h,HD:,:]=apart
        qn_ref[h]=low[:,at:at+HD]*jnp.bfloat16(SCALE)
        ka_ref[h]=jnp.concatenate([low[:,at+HD:at+2*HD],same],axis=1)
        kt_ref[h]=yt[at+HD:at+2*HD]
        vt_ref[h]=yt[at+2*HD:at+3*HD]
        vn_ref[h]=low[:,at+2*HD:at+3*HD]


def project(x,w,b,seg,rows=512):
    L,D=x.shape; heads=w.shape[1]//(3*HD)
    bf=jnp.bfloat16
    nat=lambda n: pl.BlockSpec((heads,rows,n),lambda i:(0,i,0))
    tr=lambda n: pl.BlockSpec((heads,n,rows),lambda i:(0,0,i))
    S=jax.ShapeDtypeStruct
    return pl.pallas_call(functools.partial(project_body,heads),grid=(L//rows,),
        in_specs=[pl.BlockSpec((rows,D),lambda i:(i,0)),pl.BlockSpec(w.shape,lambda i:(0,0)),pl.BlockSpec((1,w.shape[1]),lambda i:(0,0)),
                  pl.BlockSpec((rows,1),lambda i:(i,0)),pl.BlockSpec((1,rows),lambda i:(0,i))],
        out_specs=[tr(2*HD),nat(2*HD),tr(HD),nat(HD),tr(HD),nat(HD)],
        out_shape=[S((heads,2*HD,L),bf),S((heads,L,2*HD),bf),S((heads,HD,L),bf),S((heads,L,HD),bf),S((heads,HD,L),bf),S((heads,L,HD),bf)],
        compiler_params=pltpu.CompilerParams(vmem_limit_bytes=48<<20),
        cost_estimate=pl.CostEstimate(flops=2*L*D*w.shape[1],bytes_accessed=L*D*2+w.size*2+L*heads*HD*2*10,transcendentals=0),
        name="project")(x,w,b.reshape(1,-1),seg.reshape(-1,1),seg.reshape(1,-1))


def forward_body(BK, SUB, lo_ref, hi_ref, qt_ref, ka_ref, vt_ref, ctx_ref, ot_ref, lse_ref, m_s, l_s, acc):
    i=pl.program_id(0)
    heads,_,BQ=qt_ref.shape
    chains=[(h,slice(c*SUB,(c+1)*SUB)) for h in range(heads) for c in range(BQ//SUB)]
    m_s[...]=jnp.full(m_s.shape,-jnp.inf,jnp.float32)
    l_s[...]=jnp.zeros(l_s.shape,jnp.float32)
    acc[...]=jnp.zeros(acc.shape,jnp.float32)

    def step(j,_):
        at=pl.multiple_of(j*BK,BK)
        for h,cut in chains:
            s=dot(ka_ref[h,pl.ds(at,BK),:],qt_ref[h,:,cut])
            m_old=m_s[h,:,cut]
            m_new=jnp.maximum(m_old,jnp.max(s,axis=0,keepdims=True))
            p=jnp.exp(s-m_new)
            alpha=jnp.exp(m_old-m_new)
            m_s[h,:,cut]=m_new
            l_s[h,:,cut]=l_s[h,:,cut]*alpha+jnp.sum(p,axis=0,keepdims=True)
            acc[h,:,cut]=acc[h,:,cut]*alpha+dot(vt_ref[h,:,pl.ds(at,BK)],p.astype(jnp.bfloat16))
        return 0

    lax.fori_loop(lo_ref[i],hi_ref[i],step,0)
    for h in range(heads):
        o=acc[h]/l_s[h]
        lse_ref[h]=m_s[h]+jnp.log(l_s[h])
        ot_ref[h]=o
        ctx_ref[0,h*HD:(h+1)*HD,:]=o.astype(jnp.bfloat16)


def attend_forward(first,heads,parts,qt,ka,vt,lo,hi,BQ=384,BK=512,SUB=384):
    L=qt.shape[2]
    S=jax.ShapeDtypeStruct
    per=L//parts//BQ
    return pl.pallas_call(functools.partial(forward_body,BK,SUB),
        grid_spec=pltpu.PrefetchScalarGridSpec(num_scalar_prefetch=2,grid=(L//BQ,),
        in_specs=[pl.BlockSpec((heads,2*HD,BQ),lambda i,*_:(first//heads,0,i)),pl.BlockSpec((heads,L,2*HD),lambda i,*_:(first//heads,0,0)),pl.BlockSpec((heads,HD,L),lambda i,*_:(first//heads,0,0))],
        out_specs=[pl.BlockSpec((1,heads*HD,BQ),lambda i,*_:(i//per,0,i%per)),pl.BlockSpec((heads,HD,BQ),lambda i,*_:(0,0,i)),pl.BlockSpec((heads,1,BQ),lambda i,*_:(0,0,i))],
        scratch_shapes=[VM((heads,1,BQ),jnp.float32),VM((heads,1,BQ),jnp.float32),VM((heads,HD,BQ),jnp.float32)]),
        out_shape=[S((parts,heads*HD,L//parts),jnp.bfloat16),S((heads,HD,L),jnp.float32),S((heads,1,L),jnp.float32)],
        compiler_params=pltpu.CompilerParams(vmem_limit_bytes=56<<20),
        cost_estimate=pl.CostEstimate(flops=2*L*L*HD*2*heads,bytes_accessed=L*heads*HD*2*8,transcendentals=L*L*heads),
        name="attend_forward")(lo,hi,qt,ka,vt)


def backward_body(BQ, BK, SUB, lo_ref, hi_ref, go_ref, ot_ref, lse_ref, qt_ref, ka_ref, qn_ref, kt_ref, vn_ref, out_ref, got, gon, delta, dqt, dkt, dvt, dk_s, dv_s):
    parts,_,rows=go_ref.shape
    heads,_,L=qt_ref.shape
    CH=256
    for h in range(heads):
        for c in range(L//CH):
            p,at=c*CH//rows,c*CH%rows
            gt=go_ref[p,h*HD:(h+1)*HD,at:at+CH]
            wide=gt.astype(jnp.float32)
            got[h,:,c*CH:(c+1)*CH]=gt
            gon[h,c*CH:(c+1)*CH,:]=wide.T.astype(jnp.bfloat16)
            delta[h,:,c*CH:(c+1)*CH]=jnp.sum(wide*ot_ref[h,:,c*CH:(c+1)*CH],axis=0,keepdims=True)
    dqt[...]=jnp.zeros(dqt.shape,jnp.float32)

    def key_block(j,_):
        ka_at=pl.multiple_of(j*BK,BK)
        dk_s[...]=jnp.zeros(dk_s.shape,jnp.float32)
        dv_s[...]=jnp.zeros(dv_s.shape,jnp.float32)

        def query_block(i,_):
            for h,c in [(h,c) for h in range(heads) for c in range(BQ//SUB)]:
                at=pl.multiple_of(i*BQ+c*SUB,SUB)
                s=dot(ka_ref[h,pl.ds(ka_at,BK),:],qt_ref[h,:,pl.ds(at,SUB)])
                p=jnp.exp(s-lse_ref[h,:,pl.ds(at,SUB)])
                dp=dot(vn_ref[h,pl.ds(ka_at,BK),:],got[h,:,pl.ds(at,SUB)])
                ds=(p*(dp-delta[h,:,pl.ds(at,SUB)])).astype(jnp.bfloat16)
                dv_s[h]+=dot(p.astype(jnp.bfloat16),gon[h,pl.ds(at,SUB),:])
                dk_s[h]+=dot(ds,qn_ref[h,pl.ds(at,SUB),:])
                dqt[h,:,pl.ds(at,SUB)]+=dot(kt_ref[h,:,pl.ds(ka_at,BK)],ds)
            return 0

        lax.fori_loop(lo_ref[j],hi_ref[j],query_block,0)
        for h in range(heads):
            dkt[h,:,pl.ds(ka_at,BK)]=dk_s[h].T.astype(jnp.bfloat16)
            dvt[h,:,pl.ds(ka_at,BK)]=dv_s[h].T.astype(jnp.bfloat16)
        return 0

    lax.fori_loop(0,L//BK,key_block,0)
    for h in range(heads):
        for p in range(parts):
            cut=slice(p*rows,(p+1)*rows)
            out_ref[p,3*h*HD:(3*h+1)*HD,:]=(dqt[h,:,cut]*SCALE).astype(jnp.bfloat16)
            out_ref[p,(3*h+1)*HD:(3*h+2)*HD,:]=dkt[h,:,cut]
            out_ref[p,(3*h+2)*HD:(3*h+3)*HD,:]=dvt[h,:,cut]


def attend_backward(first,heads,go,go_first,ot,lse,qt,ka,qn,kt,vn,lo,hi,BQ=512,BK=512,SUB=512):
    parts,_,rows=go.shape; L=parts*rows
    S=jax.ShapeDtypeStruct; f32=jnp.float32; bf=jnp.bfloat16
    some=lambda a: pl.BlockSpec((heads,)+a.shape[1:],lambda i,*_:(first//heads,0,0),pipeline_mode=pl.Buffered(1))
    return pl.pallas_call(functools.partial(backward_body,BQ,BK,SUB),
        grid_spec=pltpu.PrefetchScalarGridSpec(num_scalar_prefetch=2,grid=(1,),
        in_specs=[pl.BlockSpec((parts,heads*HD,rows),lambda i,*_:(0,go_first,0),pipeline_mode=pl.Buffered(1))]+[some(a) for a in (ot,lse,qt,ka,qn,kt,vn)],
        out_specs=pl.BlockSpec((parts,3*heads*HD,rows),lambda i,*_:(0,0,0),pipeline_mode=pl.Buffered(1)),
        scratch_shapes=[VM((heads,HD,L),bf),VM((heads,L,HD),bf),VM((heads,1,L),f32),VM((heads,HD,L),f32),VM((heads,HD,L),bf),VM((heads,HD,L),bf),VM((heads,BK,HD),f32),VM((heads,BK,HD),f32)]),
        out_shape=S((parts,3*heads*HD,rows),bf),
        compiler_params=pltpu.CompilerParams(vmem_limit_bytes=60<<20),
        cost_estimate=pl.CostEstimate(flops=2*L*L*HD*5*heads,bytes_accessed=L*heads*HD*2*14,transcendentals=L*L*heads),
        name="attend_backward")(lo,hi,go,ot,lse,qt,ka,qn,kt,vn)


def ranges(seg,BQ,BK):
    first=seg.reshape(-1,BQ)[:,0]; last=seg.reshape(-1,BQ)[:,-1]
    kf=seg.reshape(-1,BK)[:,0]; kl=seg.reshape(-1,BK)[:,-1]
    lo=jnp.sum((kl[None,:]<first[:,None]).astype(jnp.int32),1)
    hi=jnp.sum((kf[None,:]<=last[:,None]).astype(jnp.int32),1)
    return lo,hi


def dot_right_t(left, right):
    return lax.dot_general(
        left, right, (((1,), (1,)), ((), ())), preferred_element_type=jnp.float32
    )


def layer_norm(values_in, gain, shift):
    mean_row = jnp.mean(values_in, -1, keepdims=True)
    centered = values_in - mean_row
    inverse = lax.rsqrt(jnp.mean(centered * centered, -1, keepdims=True) + EPS)
    normed = centered * inverse
    return (normed * gain + shift, normed, inverse)


def norm_back(grad_in, normed, inverse, gain):
    scaled = grad_in * gain
    return inverse * (
        scaled
        - jnp.mean(scaled, -1, keepdims=True)
        - normed * jnp.mean(scaled * normed, -1, keepdims=True)
    )


def gelu_value(inner):
    return 0.5 * inner * (1.0 + jax.scipy.special.erf(inner * ROOT_HALF))


def gelu_slope(inner):
    return (
        0.5 * (1.0 + jax.scipy.special.erf(inner * ROOT_HALF))
        + inner * jnp.exp(-0.5 * inner * inner) * INV_ROOT_TWO_PI
    )


MESH = pl.DeviceIdType.MESH


def chain_body(n, x_ref, out_ref, send_sem, recv_sem, keep_sem):
    me = lax.axis_index("tensor")
    barrier = pltpu.get_barrier_semaphore()

    @pl.when(me > 0)
    def _():
        pl.semaphore_signal(barrier, inc=1, device_id={"tensor": me - 1}, device_id_type=MESH)

    @pl.when(me < n - 1)
    def _():
        pl.semaphore_signal(barrier, inc=1, device_id={"tensor": me + 1}, device_id_type=MESH)

    pl.semaphore_wait(barrier, jnp.where(me > 0, 1, 0) + jnp.where(me < n - 1, 1, 0))

    keep = pltpu.make_async_copy(x_ref, out_ref.at[me], keep_sem)
    keep.start()

    def hop(side, step):
        block = me - (step - 1) if side else me + (step - 1)
        to = me + 1 if side else me - 1
        return pltpu.make_async_remote_copy(
            src_ref=x_ref if step == 1 else out_ref.at[block],
            dst_ref=out_ref.at[block],
            send_sem=send_sem.at[side, step - 1],
            recv_sem=recv_sem.at[side, step - 1],
            device_id={"tensor": to},
            device_id_type=MESH,
        )

    def sends(side, step):
        if side:
            return (me < n - 1) & (me >= step - 1)
        return (me > 0) & (me + step - 1 <= n - 1)

    def receives(side, step):
        return me >= step if side else me + step <= n - 1

    for step in range(1, n):
        for side in (0, 1):
            if step > 1:

                @pl.when(receives(side, step - 1))
                def _():
                    hop(side, step - 1).wait_recv()

            @pl.when(sends(side, step))
            def _():
                hop(side, step).start()

    for side in (0, 1):

        @pl.when(receives(side, n - 1))
        def _():
            hop(side, n - 1).wait_recv()

        for step in range(1, n):

            @pl.when(sends(side, step))
            def _():
                hop(side, step).wait_send()

    keep.wait()


def chain_gather(x):
    n = lax.axis_size("tensor")
    return pl.pallas_call(
        functools.partial(chain_body, n),
        in_specs=[pl.BlockSpec(memory_space=pltpu.VMEM)],
        out_specs=pl.BlockSpec(memory_space=pl.ANY),
        out_shape=jax.ShapeDtypeStruct((n,) + x.shape, x.dtype),
        scratch_shapes=[
            pltpu.SemaphoreType.DMA((2, n - 1)),
            pltpu.SemaphoreType.DMA((2, n - 1)),
            pltpu.SemaphoreType.DMA,
        ],
        compiler_params=pltpu.CompilerParams(collective_id=0, has_side_effects=True),
        cost_estimate=pl.CostEstimate(flops=0, bytes_accessed=200 << 20, transcendentals=0),
        name="chain_gather",
    )(x)


def weight_grads_body(parts, first_ref, second_ref, attn_ref, inner_ref, active_ref, context_ref, out_ref, ft, st):
    j = pl.program_id(0)

    @pl.when(j == 0)
    def _():
        ft[...] = first_ref[...].T
        st[...] = second_ref[...].T

    @pl.when((j < 2 * parts) & (j % 2 == 0))
    def _():
        out_ref[...] = dot(ft[...], inner_ref[0]).astype(out_ref.dtype)

    @pl.when((j < 2 * parts) & (j % 2 == 1))
    def _():
        out_ref[...] = dot(st[...], active_ref[0]).astype(out_ref.dtype)

    @pl.when(j == 2 * parts)
    def _():
        out_ref[...] = dot_right_t(attn_ref[...].T, context_ref[...]).astype(out_ref.dtype)


def weight_grads_of(first_low, second_low, attn_low, grad_inner, active, context):
    parts, rows, units = active.shape
    width = first_low.shape[1]
    features = context.shape[0]
    fixed = pl.BlockSpec((rows, width), lambda j: (0, 0))
    moving = lambda shift: pl.BlockSpec((1, rows, units), lambda j: (jnp.clip((j - shift) // 2, 0, parts - 1), 0, 0))
    return pl.pallas_call(
        functools.partial(weight_grads_body, parts),
        grid=(2 * parts + 1,),
        in_specs=[fixed, fixed, fixed, moving(0), moving(1), pl.BlockSpec((features, rows), lambda j: (0, 0))],
        out_specs=pl.BlockSpec((width, units), lambda j: (0, j)),
        out_shape=jax.ShapeDtypeStruct((width, units * 2 * parts + features), jnp.bfloat16),
        scratch_shapes=[VM((width, rows), jnp.bfloat16), VM((width, rows), jnp.bfloat16)],
        compiler_params=pltpu.CompilerParams(vmem_limit_bytes=40 << 20),
        cost_estimate=pl.CostEstimate(flops=2 * rows * width * (2 * parts * units + features), bytes_accessed=rows * units * 2 * parts * 4, transcendentals=0),
        name="weight_grads",
    )(first_low, second_low, attn_low, grad_inner, active, context)


def add_up(value):
    for axis in ("dp", "tensor"):
        size = lax.axis_size(axis)
        span = 1
        while span < size:
            value = value + lax.ppermute(value, axis, [(i, i ^ span) for i in range(size)])
            span *= 2
    return value


def rotate(blocks, axis):
    size = lax.axis_size(axis)
    me = lax.axis_index(axis)
    out = []
    for d in range(size):
        block = lax.dynamic_index_in_dim(blocks, (me + d) % size, 0, keepdims=False)
        if d:
            block = lax.ppermute(block, axis, [(i, (i + d) % size) for i in range(size)])
        out.append(block)
    return out


def body(hidden_in, segments, query_weight, key_weight, value_weight, query_bias, value_bias, mixer_weight, mixer_bias, first_gain, first_shift, inner_weight, inner_bias, outer_weight, outer_bias, second_gain, second_shift, cotangent):
    bf = jnp.bfloat16
    f32 = jnp.float32
    _, rows, width = hidden_in.shape
    parts = lax.axis_size("tensor")
    groups = lax.axis_size("dp")
    rank = lax.axis_index("tensor")
    own = query_weight.shape[1]
    heads = own // HD
    three = 3 * HD
    units = inner_weight.shape[1]
    parts_of = range(parts)
    by_head = lambda q, k, v: jnp.stack([a.reshape(a.shape[:-1] + (heads, HD)) for a in (q, k, v)], -2).reshape(q.shape[:-1] + (3 * own,))
    x_own = hidden_in[0]
    qkv_own = by_head(query_weight, key_weight, value_weight)
    qkv_all = lax.all_gather(qkv_own, "dp", axis=0, tiled=True)
    small = jnp.concatenate([segments[0].astype(f32), inner_bias])
    small = lax.all_gather(small[None], "tensor", axis=0, tiled=True)
    segment_all = small[:, :rows].astype(jnp.int32).reshape(-1)
    inner_bias_all = small[:, rows:]
    x_parts = chain_gather(x_own)
    x_all = x_parts.reshape(parts * rows, width)
    rest_own = jnp.concatenate([inner_weight, outer_weight.T, mixer_weight.T, qkv_own], 1)
    rest = lax.all_gather(rest_own, ("tensor", "dp"), axis=0, tiled=True)
    rest = rest.reshape(parts, width, rest_own.shape[1])
    biases = by_head(query_bias, jnp.zeros_like(query_bias), value_bias)

    qt, ka, vt, qn, kt, vn = project(x_all, qkv_all, biases, segment_all)
    lo, hi = ranges(segment_all, 384, 512)
    context, context_t, lse = attend_forward(0, heads, parts, qt, ka, vt, lo, hi)
    context = lax.all_to_all(context, "tensor", 0, 0, tiled=True)
    w1 = [rest[t, :, :units] for t in parts_of]
    w2t = [rest[t, :, units : 2 * units] for t in parts_of]
    mt = [rest[t, :, 2 * units : 2 * units + own] for t in parts_of]
    contract = lambda a, b, i, j: lax.dot_general(a, b, (((i,), (j,)), ((), ())), preferred_element_type=f32)
    mixed = sum(contract(context[t], mt[t], 0, 1) for t in parts_of)
    attn_in = x_own.astype(f32) + mixed + mixer_bias
    first, first_norm, first_inv = layer_norm(attn_in, first_gain, first_shift)
    first_low = first.astype(bf)
    inner = [dot(first_low, w1[t]) + inner_bias_all[t] for t in parts_of]
    active = [gelu_value(inner[t]).astype(bf) for t in parts_of]
    outer = sum(dot_right_t(active[t], w2t[t]) for t in parts_of)
    second_in = first + outer + outer_bias
    second, second_norm, second_inv = layer_norm(second_in, second_gain, second_shift)
    layer_out = second.astype(bf)
    grad_out = cotangent[0].astype(f32)
    second_gain_grad = jnp.sum(grad_out * second_norm, 0)
    second_shift_grad = jnp.sum(grad_out, 0)
    grad_second = norm_back(grad_out, second_norm, second_inv, second_gain)
    outer_bias_grad = jnp.sum(grad_second, 0)
    second_low = grad_second.astype(bf)
    grad_inner = [(dot(second_low, w2t[t]) * gelu_slope(inner[t])).astype(bf) for t in parts_of]
    inner_bias_grad = jnp.stack([jnp.sum(g, 0, dtype=f32) for g in grad_inner])
    grad_first = grad_second + sum(dot_right_t(grad_inner[t], w1[t]) for t in parts_of)
    first_gain_grad = jnp.sum(grad_first * first_norm, 0)
    first_shift_grad = jnp.sum(grad_first, 0)
    grad_attn = norm_back(grad_first, first_norm, first_inv, first_gain)
    mixer_bias_grad = jnp.sum(grad_attn, 0)
    attn_low = grad_attn.astype(bf)
    grad_context = jnp.stack([contract(mt[t], attn_low, 0, 1).astype(bf) for t in parts_of])
    go0 = lax.all_to_all(grad_context[:, :HD], "tensor", 0, 0, tiled=True)
    go1 = lax.all_to_all(grad_context[:, HD:], "tensor", 0, 0, tiled=True)
    weight_grads = weight_grads_of(
        first_low, second_low, attn_low, jnp.stack(grad_inner), jnp.stack(active), context.reshape(-1, rows)
    )
    weight_grads = lax.psum_scatter(weight_grads, "dp", scatter_dimension=0, tiled=True)
    weight_grads = jnp.concatenate(
        [
            weight_grads[:, : 2 * units * parts].reshape(-1, parts, 2 * units),
            weight_grads[:, 2 * units * parts :].reshape(-1, parts, own),
        ],
        2,
    ).transpose(1, 0, 2)
    weight_grads = rotate(weight_grads, "tensor")
    weight_grads = sum(a.astype(f32) for a in weight_grads)
    early = jnp.concatenate(
        [
            mixer_bias_grad,
            first_gain_grad,
            first_shift_grad,
            outer_bias_grad,
            second_gain_grad,
            second_shift_grad,
            inner_bias_grad.reshape(-1),
        ]
    )
    early = add_up(early)

    lo, hi = ranges(segment_all, 512, 512)
    input_back = grad_attn
    qkv_grad = []
    bias_grad = []
    for h in range(heads):
        grads = attend_backward(h, 1, go1 if h else go0, h - 1 if h else 0, context_t, lse, qt, ka, qn, kt, vn, lo, hi)
        if h < heads - 1:
            back = lax.all_to_all(grads, "tensor", 0, 0, tiled=True)
        else:
            back = rotate(grads, "tensor")
        qkv_grad.append(sum(contract(x_parts[p], grads[p], 0, 1) for p in parts_of))
        bias_grad.append(jnp.sum(grads, (0, 2), dtype=f32))
        at = 2 * units + own + h * three
        if h < heads - 1:
            weights = [rest[t, :, at : at + three] for t in parts_of]
        else:
            weights = [
                lax.dynamic_index_in_dim(rest, (rank - t) % parts, 0, keepdims=False)[:, at : at + three]
                for t in parts_of
            ]
        input_back = input_back + sum(contract(back[t], weights[t], 0, 1) for t in parts_of)
    input_grad = input_back.astype(bf)
    bias_grad = jnp.concatenate(bias_grad)
    high = bias_grad.astype(bf)
    low = (bias_grad - high.astype(f32)).astype(bf)
    each = width // groups
    qkv_grad = jnp.concatenate(qkv_grad, 1).astype(bf).reshape(groups, each, 3 * own)
    extra = jnp.pad(jnp.stack([high, low]), ((0, 14), (0, 0)))
    extra = jnp.broadcast_to(extra[None], (groups, 16, 3 * own))
    qkv_grad = lax.all_to_all(jnp.concatenate([qkv_grad, extra], 1), "dp", 0, 0, tiled=True)
    qkv_grad = jnp.sum(qkv_grad.astype(f32), 0)
    bias_grad = qkv_grad[each] + qkv_grad[each + 1]
    pick = lambda a, n: a.reshape(a.shape[:-1] + (heads, 3, HD))[..., n, :].reshape(a.shape[:-1] + (own,))
    stacked = early[: 6 * width].reshape(6, width)
    inner_bias_out = lax.dynamic_slice_in_dim(early, 6 * width + rank * units, units)
    return (
        layer_out[None],
        input_grad[None],
        pick(qkv_grad[:each], 0),
        pick(qkv_grad[:each], 1),
        pick(qkv_grad[:each], 2),
        pick(bias_grad, 0),
        pick(bias_grad, 2),
        weight_grads[:, 2 * units :].T,
        stacked[0],
        stacked[1],
        stacked[2],
        weight_grads[:, :units],
        inner_bias_out,
        weight_grads[:, units : 2 * units].T,
        stacked[3],
        stacked[4],
        stacked[5],
    )


def solution(mesh):
    placed = (
        P("dp", "tensor", None),
        P("dp", "tensor"),
        P("dp", "tensor"),
        P("dp", "tensor"),
        P("dp", "tensor"),
        P("tensor"),
        P("tensor"),
        P("tensor", "dp"),
        P(),
        P(),
        P(),
        P("dp", "tensor"),
        P("tensor"),
        P("tensor", "dp"),
        P(),
        P(),
        P(),
        P("dp", "tensor", None),
    )

    return jax.shard_map(
        body,
        mesh=mesh,
        in_specs=placed,
        out_specs=(
            P("dp", "tensor", None),
            P("dp", "tensor", None),
            P("dp", "tensor"),
            P("dp", "tensor"),
            P("dp", "tensor"),
            P("tensor"),
            P("tensor"),
            P("tensor", "dp"),
            P(),
            P(),
            P(),
            P("dp", "tensor"),
            P("tensor"),
            P("tensor", "dp"),
            P(),
            P(),
            P(),
        ),
        check_vma=False,
    )
```

```python
import functools

import jax
import jax.numpy as jnp
from jax import lax
from jax.experimental import pallas as pl
from jax.experimental.pallas import tpu as pltpu
from jax.sharding import PartitionSpec as P


EPS = 1e-12
ROOT_HALF = 0.7071067811865476
INV_ROOT_TWO_PI = 0.3989422804014327
HD=64; SCALE=0.125; APART=-1e30
VM=pltpu.VMEM


def dot(a,b): return jnp.dot(a,b,preferred_element_type=jnp.float32)


def project_body(heads, x_ref, w_ref, b_ref, scol_ref, srow_ref, qt_ref, ka_ref, vt_ref, qn_ref, kt_ref, vn_ref):
    y = dot(x_ref[...], w_ref[...]) + b_ref[...]
    low = y.astype(jnp.bfloat16)
    yt = y.T.astype(jnp.bfloat16)
    rows = y.shape[0]
    apart = jnp.where(lax.broadcasted_iota(jnp.int32,(HD,rows),0)==srow_ref[...],0.0,APART).astype(jnp.bfloat16)
    same = (lax.broadcasted_iota(jnp.int32,(rows,HD),1)==scol_ref[...]).astype(jnp.float32).astype(jnp.bfloat16)
    for h in range(heads):
        at=3*h*HD
        qt_ref[h,:HD,:]=yt[at:at+HD]*jnp.bfloat16(SCALE)
        qt_ref[h,HD:,:]=apart
        qn_ref[h]=low[:,at:at+HD]*jnp.bfloat16(SCALE)
        ka_ref[h]=jnp.concatenate([low[:,at+HD:at+2*HD],same],axis=1)
        kt_ref[h]=yt[at+HD:at+2*HD]
        vt_ref[h]=yt[at+2*HD:at+3*HD]
        vn_ref[h]=low[:,at+2*HD:at+3*HD]


def project(x,w,b,seg,rows=512):
    L,D=x.shape; heads=w.shape[1]//(3*HD)
    bf=jnp.bfloat16
    nat=lambda n: pl.BlockSpec((heads,rows,n),lambda i:(0,i,0))
    tr=lambda n: pl.BlockSpec((heads,n,rows),lambda i:(0,0,i))
    S=jax.ShapeDtypeStruct
    return pl.pallas_call(functools.partial(project_body,heads),grid=(L//rows,),
        in_specs=[pl.BlockSpec((rows,D),lambda i:(i,0)),pl.BlockSpec(w.shape,lambda i:(0,0)),pl.BlockSpec((1,w.shape[1]),lambda i:(0,0)),
                  pl.BlockSpec((rows,1),lambda i:(i,0)),pl.BlockSpec((1,rows),lambda i:(0,i))],
        out_specs=[tr(2*HD),nat(2*HD),tr(HD),nat(HD),tr(HD),nat(HD)],
        out_shape=[S((heads,2*HD,L),bf),S((heads,L,2*HD),bf),S((heads,HD,L),bf),S((heads,L,HD),bf),S((heads,HD,L),bf),S((heads,L,HD),bf)],
        compiler_params=pltpu.CompilerParams(vmem_limit_bytes=48<<20),
        cost_estimate=pl.CostEstimate(flops=2*L*D*w.shape[1],bytes_accessed=L*D*2+w.size*2+L*heads*HD*2*10,transcendentals=0),
        name="project")(x,w,b.reshape(1,-1),seg.reshape(-1,1),seg.reshape(1,-1))


def forward_body(BK, SUB, lo_ref, hi_ref, qt_ref, ka_ref, vt_ref, ctx_ref, ot_ref, lse_ref, m_s, l_s, acc):
    i=pl.program_id(0)
    heads,_,BQ=qt_ref.shape
    chains=[(h,slice(c*SUB,(c+1)*SUB)) for h in range(heads) for c in range(BQ//SUB)]
    m_s[...]=jnp.full(m_s.shape,-jnp.inf,jnp.float32)
    l_s[...]=jnp.zeros(l_s.shape,jnp.float32)
    acc[...]=jnp.zeros(acc.shape,jnp.float32)

    def step(j,_):
        at=pl.multiple_of(j*BK,BK)
        for h,cut in chains:
            s=dot(ka_ref[h,pl.ds(at,BK),:],qt_ref[h,:,cut])
            m_old=m_s[h,:,cut]
            m_new=jnp.maximum(m_old,jnp.max(s,axis=0,keepdims=True))
            p=jnp.exp(s-m_new)
            alpha=jnp.exp(m_old-m_new)
            m_s[h,:,cut]=m_new
            l_s[h,:,cut]=l_s[h,:,cut]*alpha+jnp.sum(p,axis=0,keepdims=True)
            acc[h,:,cut]=acc[h,:,cut]*alpha+dot(vt_ref[h,:,pl.ds(at,BK)],p.astype(jnp.bfloat16))
        return 0

    lax.fori_loop(lo_ref[i],hi_ref[i],step,0)
    for h in range(heads):
        o=acc[h]/l_s[h]
        lse_ref[h]=m_s[h]+jnp.log(l_s[h])
        ot_ref[h]=o
        ctx_ref[0,h*HD:(h+1)*HD,:]=o.astype(jnp.bfloat16)


def attend_forward(first,heads,parts,qt,ka,vt,lo,hi,BQ=384,BK=512,SUB=384):
    L=qt.shape[2]
    S=jax.ShapeDtypeStruct
    per=L//parts//BQ
    return pl.pallas_call(functools.partial(forward_body,BK,SUB),
        grid_spec=pltpu.PrefetchScalarGridSpec(num_scalar_prefetch=2,grid=(L//BQ,),
        in_specs=[pl.BlockSpec((heads,2*HD,BQ),lambda i,*_:(first//heads,0,i)),pl.BlockSpec((heads,L,2*HD),lambda i,*_:(first//heads,0,0)),pl.BlockSpec((heads,HD,L),lambda i,*_:(first//heads,0,0))],
        out_specs=[pl.BlockSpec((1,heads*HD,BQ),lambda i,*_:(i//per,0,i%per)),pl.BlockSpec((heads,HD,BQ),lambda i,*_:(0,0,i)),pl.BlockSpec((heads,1,BQ),lambda i,*_:(0,0,i))],
        scratch_shapes=[VM((heads,1,BQ),jnp.float32),VM((heads,1,BQ),jnp.float32),VM((heads,HD,BQ),jnp.float32)]),
        out_shape=[S((parts,heads*HD,L//parts),jnp.bfloat16),S((heads,HD,L),jnp.float32),S((heads,1,L),jnp.float32)],
        compiler_params=pltpu.CompilerParams(vmem_limit_bytes=56<<20),
        cost_estimate=pl.CostEstimate(flops=2*L*L*HD*2*heads,bytes_accessed=L*heads*HD*2*8,transcendentals=L*L*heads),
        name="attend_forward")(lo,hi,qt,ka,vt)


def backward_body(BQ, BK, SUB, lo_ref, hi_ref, go_ref, ot_ref, lse_ref, qt_ref, ka_ref, qn_ref, kt_ref, vn_ref, out_ref, got, gon, delta, dqt, dkt, dvt, dk_s, dv_s):
    parts,_,rows=go_ref.shape
    heads,_,L=qt_ref.shape
    CH=256
    for h in range(heads):
        for c in range(L//CH):
            p,at=c*CH//rows,c*CH%rows
            gt=go_ref[p,h*HD:(h+1)*HD,at:at+CH]
            wide=gt.astype(jnp.float32)
            got[h,:,c*CH:(c+1)*CH]=gt
            gon[h,c*CH:(c+1)*CH,:]=wide.T.astype(jnp.bfloat16)
            delta[h,:,c*CH:(c+1)*CH]=jnp.sum(wide*ot_ref[h,:,c*CH:(c+1)*CH],axis=0,keepdims=True)
    dqt[...]=jnp.zeros(dqt.shape,jnp.float32)

    def key_block(j,_):
        ka_at=pl.multiple_of(j*BK,BK)
        dk_s[...]=jnp.zeros(dk_s.shape,jnp.float32)
        dv_s[...]=jnp.zeros(dv_s.shape,jnp.float32)

        def query_block(i,_):
            for h,c in [(h,c) for h in range(heads) for c in range(BQ//SUB)]:
                at=pl.multiple_of(i*BQ+c*SUB,SUB)
                s=dot(ka_ref[h,pl.ds(ka_at,BK),:],qt_ref[h,:,pl.ds(at,SUB)])
                p=jnp.exp(s-lse_ref[h,:,pl.ds(at,SUB)])
                dp=dot(vn_ref[h,pl.ds(ka_at,BK),:],got[h,:,pl.ds(at,SUB)])
                ds=(p*(dp-delta[h,:,pl.ds(at,SUB)])).astype(jnp.bfloat16)
                dv_s[h]+=dot(p.astype(jnp.bfloat16),gon[h,pl.ds(at,SUB),:])
                dk_s[h]+=dot(ds,qn_ref[h,pl.ds(at,SUB),:])
                dqt[h,:,pl.ds(at,SUB)]+=dot(kt_ref[h,:,pl.ds(ka_at,BK)],ds)
            return 0

        lax.fori_loop(lo_ref[j],hi_ref[j],query_block,0)
        for h in range(heads):
            dkt[h,:,pl.ds(ka_at,BK)]=dk_s[h].T.astype(jnp.bfloat16)
            dvt[h,:,pl.ds(ka_at,BK)]=dv_s[h].T.astype(jnp.bfloat16)
        return 0

    lax.fori_loop(0,L//BK,key_block,0)
    for h in range(heads):
        for p in range(parts):
            cut=slice(p*rows,(p+1)*rows)
            out_ref[p,3*h*HD:(3*h+1)*HD,:]=(dqt[h,:,cut]*SCALE).astype(jnp.bfloat16)
            out_ref[p,(3*h+1)*HD:(3*h+2)*HD,:]=dkt[h,:,cut]
            out_ref[p,(3*h+2)*HD:(3*h+3)*HD,:]=dvt[h,:,cut]


def attend_backward(first,heads,go,go_first,ot,lse,qt,ka,qn,kt,vn,lo,hi,BQ=512,BK=512,SUB=512):
    parts,_,rows=go.shape; L=parts*rows
    S=jax.ShapeDtypeStruct; f32=jnp.float32; bf=jnp.bfloat16
    some=lambda a: pl.BlockSpec((heads,)+a.shape[1:],lambda i,*_:(first//heads,0,0),pipeline_mode=pl.Buffered(1))
    return pl.pallas_call(functools.partial(backward_body,BQ,BK,SUB),
        grid_spec=pltpu.PrefetchScalarGridSpec(num_scalar_prefetch=2,grid=(1,),
        in_specs=[pl.BlockSpec((parts,heads*HD,rows),lambda i,*_:(0,go_first,0),pipeline_mode=pl.Buffered(1))]+[some(a) for a in (ot,lse,qt,ka,qn,kt,vn)],
        out_specs=pl.BlockSpec((parts,3*heads*HD,rows),lambda i,*_:(0,0,0),pipeline_mode=pl.Buffered(1)),
        scratch_shapes=[VM((heads,HD,L),bf),VM((heads,L,HD),bf),VM((heads,1,L),f32),VM((heads,HD,L),f32),VM((heads,HD,L),bf),VM((heads,HD,L),bf),VM((heads,BK,HD),f32),VM((heads,BK,HD),f32)]),
        out_shape=S((parts,3*heads*HD,rows),bf),
        compiler_params=pltpu.CompilerParams(vmem_limit_bytes=60<<20),
        cost_estimate=pl.CostEstimate(flops=2*L*L*HD*5*heads,bytes_accessed=L*heads*HD*2*14,transcendentals=L*L*heads),
        name="attend_backward")(lo,hi,go,ot,lse,qt,ka,qn,kt,vn)


def ranges(seg,BQ,BK):
    first=seg.reshape(-1,BQ)[:,0]; last=seg.reshape(-1,BQ)[:,-1]
    kf=seg.reshape(-1,BK)[:,0]; kl=seg.reshape(-1,BK)[:,-1]
    lo=jnp.sum((kl[None,:]<first[:,None]).astype(jnp.int32),1)
    hi=jnp.sum((kf[None,:]<=last[:,None]).astype(jnp.int32),1)
    return lo,hi


def dot_right_t(left, right):
    return lax.dot_general(
        left, right, (((1,), (1,)), ((), ())), preferred_element_type=jnp.float32
    )


def layer_norm(values_in, gain, shift):
    mean_row = jnp.mean(values_in, -1, keepdims=True)
    centered = values_in - mean_row
    inverse = lax.rsqrt(jnp.mean(centered * centered, -1, keepdims=True) + EPS)
    normed = centered * inverse
    return (normed * gain + shift, normed, inverse)


def norm_back(grad_in, normed, inverse, gain):
    scaled = grad_in * gain
    return inverse * (
        scaled
        - jnp.mean(scaled, -1, keepdims=True)
        - normed * jnp.mean(scaled * normed, -1, keepdims=True)
    )


def gelu_value(inner):
    return 0.5 * inner * (1.0 + jax.scipy.special.erf(inner * ROOT_HALF))


def gelu_slope(inner):
    return (
        0.5 * (1.0 + jax.scipy.special.erf(inner * ROOT_HALF))
        + inner * jnp.exp(-0.5 * inner * inner) * INV_ROOT_TWO_PI
    )


MESH = pl.DeviceIdType.MESH


def flip(index, bit):
    span = 1 << bit
    return index + span * (1 - 2 * ((index // span) % 2))


def start_body(n, bits, x_ref, w_ref, s_ref, x_out, w_out, s_out, send_z, recv_z, send_d, recv_d, keep_sem):
    me = lax.axis_index("tensor")
    mine = lax.axis_index("dp")
    barrier = pltpu.get_barrier_semaphore()

    @pl.when(me > 0)
    def _():
        pl.semaphore_signal(barrier, inc=1, device_id={"tensor": me - 1}, device_id_type=MESH)

    @pl.when(me < n - 1)
    def _():
        pl.semaphore_signal(barrier, inc=1, device_id={"tensor": me + 1}, device_id_type=MESH)

    for bit in range(bits):
        pl.semaphore_signal(barrier, inc=1, device_id={"dp": flip(mine, bit)}, device_id_type=MESH)
    pl.semaphore_wait(barrier, bits + jnp.where(me > 0, 1, 0) + jnp.where(me < n - 1, 1, 0))

    keeps = [
        pltpu.make_async_copy(x_ref, x_out.at[me], keep_sem.at[0]),
        pltpu.make_async_copy(w_ref, w_out.at[me, mine], keep_sem.at[1]),
        pltpu.make_async_copy(s_ref, s_out.at[me], keep_sem.at[2]),
    ]
    for keep in keeps:
        keep.start()

    def hop(kind, side, step):
        block = me - (step - 1) if side else me + (step - 1)
        first, place = (
            (x_ref, x_out.at[block]),
            (w_ref, w_out.at[block, mine]),
            (s_ref, s_out.at[block]),
        )[kind]
        return pltpu.make_async_remote_copy(
            src_ref=first if step == 1 else place,
            dst_ref=place,
            send_sem=send_z.at[kind, side, step - 1],
            recv_sem=recv_z.at[kind, side, step - 1],
            device_id={"tensor": me + 1 if side else me - 1},
            device_id_type=MESH,
        )

    def sends(side, step):
        if side:
            return (me < n - 1) & (me >= step - 1)
        return (me > 0) & (me + step - 1 <= n - 1)

    def receives(side, step):
        return me >= step if side else me + step <= n - 1

    def z_start(kinds, step):
        for side in (0, 1):

            @pl.when(sends(side, step))
            def _():
                for kind in kinds:
                    hop(kind, side, step).start()

    def z_arrive(kinds, step):
        for side in (0, 1):

            @pl.when(receives(side, step))
            def _():
                for kind in kinds:
                    hop(kind, side, step).wait_recv()

    half = w_ref.shape[1] // 2
    up = list(range(bits - 1, -1, -1))
    orders = (up, [up[1], up[0]] + up[2:] if bits > 1 else up)

    def doubling(side, step):
        order = orders[side]
        held = [mine]
        for bit in order[:step]:
            held = held + [flip(d, bit) for d in held]
        cut = pl.ds(side * half, half)
        return [
            pltpu.make_async_remote_copy(
                src_ref=w_out.at[:, d, :, cut],
                dst_ref=w_out.at[:, d, :, cut],
                send_sem=send_d.at[side, (1 << step) - 1 + at],
                recv_sem=recv_d.at[side, (1 << step) - 1 + at],
                device_id={"dp": flip(mine, order[step])},
                device_id_type=MESH,
            )
            for at, d in enumerate(held)
        ]

    def d_start(step):
        for side in (0, 1):
            for copy in doubling(side, step):
                copy.start()

    def d_arrive(step):
        for side in (0, 1):
            for copy in doubling(side, step):
                copy.wait_recv()

    for step in range(1, n):
        z_start((1, 2), step)
        z_arrive((1, 2), step)
    keeps[1].wait()
    for step in range(max(n - 1, bits)):
        if step < bits:
            if step:
                d_arrive(step - 1)
            d_start(step)
        if step < n - 1:
            if step:
                z_arrive((0,), step)
            z_start((0,), step + 1)
    z_arrive((0,), n - 1)
    d_arrive(bits - 1)
    for side in (0, 1):
        for step in range(1, n):

            @pl.when(sends(side, step))
            def _():
                for kind in (0, 1, 2):
                    hop(kind, side, step).wait_send()

        for step in range(bits):
            for copy in doubling(side, step):
                copy.wait_send()
    keeps[0].wait()
    keeps[2].wait()


def start(x, w, small):
    n = lax.axis_size("tensor")
    groups = lax.axis_size("dp")
    bits = groups.bit_length() - 1
    S = jax.ShapeDtypeStruct
    anywhere = pl.BlockSpec(memory_space=pl.ANY)
    return pl.pallas_call(
        functools.partial(start_body, n, bits),
        in_specs=[pl.BlockSpec(memory_space=pltpu.VMEM)] * 3,
        out_specs=[anywhere] * 3,
        out_shape=[
            S((n,) + x.shape, x.dtype),
            S((n, groups) + w.shape, w.dtype),
            S((n,) + small.shape, small.dtype),
        ],
        scratch_shapes=[
            pltpu.SemaphoreType.DMA((3, 2, n - 1)),
            pltpu.SemaphoreType.DMA((3, 2, n - 1)),
            pltpu.SemaphoreType.DMA((2, groups - 1)),
            pltpu.SemaphoreType.DMA((2, groups - 1)),
            pltpu.SemaphoreType.DMA((3,)),
        ],
        compiler_params=pltpu.CompilerParams(collective_id=0, has_side_effects=True),
        cost_estimate=pl.CostEstimate(flops=0, bytes_accessed=200 << 20, transcendentals=0),
        name="start",
    )(x, w, small)


def weight_grads_body(parts, first_ref, second_ref, attn_ref, inner_ref, active_ref, context_ref, out_ref, ft, st):
    j = pl.program_id(0)

    @pl.when(j == 0)
    def _():
        ft[...] = first_ref[...].T
        st[...] = second_ref[...].T

    @pl.when((j < 2 * parts) & (j % 2 == 0))
    def _():
        out_ref[...] = dot(ft[...], inner_ref[0]).astype(out_ref.dtype)

    @pl.when((j < 2 * parts) & (j % 2 == 1))
    def _():
        out_ref[...] = dot(st[...], active_ref[0]).astype(out_ref.dtype)

    @pl.when(j == 2 * parts)
    def _():
        out_ref[...] = dot_right_t(attn_ref[...].T, context_ref[...]).astype(out_ref.dtype)


def weight_grads_of(first_low, second_low, attn_low, grad_inner, active, context):
    parts, rows, units = active.shape
    width = first_low.shape[1]
    features = context.shape[0]
    fixed = pl.BlockSpec((rows, width), lambda j: (0, 0))
    moving = lambda shift: pl.BlockSpec((1, rows, units), lambda j: (jnp.clip((j - shift) // 2, 0, parts - 1), 0, 0))
    return pl.pallas_call(
        functools.partial(weight_grads_body, parts),
        grid=(2 * parts + 1,),
        in_specs=[fixed, fixed, fixed, moving(0), moving(1), pl.BlockSpec((features, rows), lambda j: (0, 0))],
        out_specs=pl.BlockSpec((width, units), lambda j: (0, j)),
        out_shape=jax.ShapeDtypeStruct((width, units * 2 * parts + features), jnp.bfloat16),
        scratch_shapes=[VM((width, rows), jnp.bfloat16), VM((width, rows), jnp.bfloat16)],
        compiler_params=pltpu.CompilerParams(vmem_limit_bytes=40 << 20),
        cost_estimate=pl.CostEstimate(flops=2 * rows * width * (2 * parts * units + features), bytes_accessed=rows * units * 2 * parts * 4, transcendentals=0),
        name="weight_grads",
    )(first_low, second_low, attn_low, grad_inner, active, context)


def add_up(value):
    for axis in ("dp", "tensor"):
        size = lax.axis_size(axis)
        span = 1
        while span < size:
            value = value + lax.ppermute(value, axis, [(i, i ^ span) for i in range(size)])
            span *= 2
    return value


def rotate(blocks, axis):
    size = lax.axis_size(axis)
    me = lax.axis_index(axis)
    out = []
    for d in range(size):
        block = lax.dynamic_index_in_dim(blocks, (me + d) % size, 0, keepdims=False)
        if d:
            block = lax.ppermute(block, axis, [(i, (i + d) % size) for i in range(size)])
        out.append(block)
    return out


def body(hidden_in, segments, query_weight, key_weight, value_weight, query_bias, value_bias, mixer_weight, mixer_bias, first_gain, first_shift, inner_weight, inner_bias, outer_weight, outer_bias, second_gain, second_shift, cotangent):
    bf = jnp.bfloat16
    f32 = jnp.float32
    _, rows, width = hidden_in.shape
    parts = lax.axis_size("tensor")
    groups = lax.axis_size("dp")
    rank = lax.axis_index("tensor")
    own = query_weight.shape[1]
    heads = own // HD
    three = 3 * HD
    units = inner_weight.shape[1]
    parts_of = range(parts)
    by_head = lambda q, k, v: jnp.stack([a.reshape(a.shape[:-1] + (heads, HD)) for a in (q, k, v)], -2).reshape(q.shape[:-1] + (3 * own,))
    x_own = hidden_in[0]
    qkv_own = by_head(query_weight, key_weight, value_weight)
    small = jnp.concatenate([segments[0].astype(f32), inner_bias]).reshape(-1, 128)
    rest_own = jnp.concatenate([qkv_own, mixer_weight.T, inner_weight, outer_weight.T], 1)
    x_parts, rest, small = start(x_own, rest_own, small)
    x_all = x_parts.reshape(parts * rows, width)
    rest = rest.reshape(parts, width, rest_own.shape[1])
    small = small.reshape(parts, -1)
    segment_all = small[:, :rows].astype(jnp.int32).reshape(-1)
    inner_bias_all = small[:, rows:]
    qkv_all = lax.dynamic_index_in_dim(rest, rank, 0, keepdims=False)[:, : 3 * own]
    biases = by_head(query_bias, jnp.zeros_like(query_bias), value_bias)

    qt, ka, vt, qn, kt, vn = project(x_all, qkv_all, biases, segment_all)
    lo, hi = ranges(segment_all, 384, 512)
    context, context_t, lse = attend_forward(0, heads, parts, qt, ka, vt, lo, hi)
    context = lax.all_to_all(context, "tensor", 0, 0, tiled=True)
    w1 = [rest[t, :, 4 * own : 4 * own + units] for t in parts_of]
    w2t = [rest[t, :, 4 * own + units :] for t in parts_of]
    mt = [rest[t, :, 3 * own : 4 * own] for t in parts_of]
    contract = lambda a, b, i, j: lax.dot_general(a, b, (((i,), (j,)), ((), ())), preferred_element_type=f32)
    mixed = sum(contract(context[t], mt[t], 0, 1) for t in parts_of)
    attn_in = x_own.astype(f32) + mixed + mixer_bias
    first, first_norm, first_inv = layer_norm(attn_in, first_gain, first_shift)
    first_low = first.astype(bf)
    inner = [dot(first_low, w1[t]) + inner_bias_all[t] for t in parts_of]
    active = [gelu_value(inner[t]).astype(bf) for t in parts_of]
    outer = sum(dot_right_t(active[t], w2t[t]) for t in parts_of)
    second_in = first + outer + outer_bias
    second, second_norm, second_inv = layer_norm(second_in, second_gain, second_shift)
    layer_out = second.astype(bf)
    grad_out = cotangent[0].astype(f32)
    second_gain_grad = jnp.sum(grad_out * second_norm, 0)
    second_shift_grad = jnp.sum(grad_out, 0)
    grad_second = norm_back(grad_out, second_norm, second_inv, second_gain)
    outer_bias_grad = jnp.sum(grad_second, 0)
    second_low = grad_second.astype(bf)
    grad_inner = [(dot(second_low, w2t[t]) * gelu_slope(inner[t])).astype(bf) for t in parts_of]
    inner_bias_grad = jnp.stack([jnp.sum(g, 0, dtype=f32) for g in grad_inner])
    grad_first = grad_second + sum(dot_right_t(grad_inner[t], w1[t]) for t in parts_of)
    first_gain_grad = jnp.sum(grad_first * first_norm, 0)
    first_shift_grad = jnp.sum(grad_first, 0)
    grad_attn = norm_back(grad_first, first_norm, first_inv, first_gain)
    mixer_bias_grad = jnp.sum(grad_attn, 0)
    attn_low = grad_attn.astype(bf)
    grad_context = jnp.stack([contract(mt[t], attn_low, 0, 1).astype(bf) for t in parts_of])
    go0 = lax.all_to_all(grad_context[:, :HD], "tensor", 0, 0, tiled=True)
    go1 = lax.all_to_all(grad_context[:, HD:], "tensor", 0, 0, tiled=True)
    weight_grads = weight_grads_of(
        first_low, second_low, attn_low, jnp.stack(grad_inner), jnp.stack(active), context.reshape(-1, rows)
    )
    weight_grads = lax.psum_scatter(weight_grads, "dp", scatter_dimension=0, tiled=True)
    weight_grads = jnp.concatenate(
        [
            weight_grads[:, : 2 * units * parts].reshape(-1, parts, 2 * units),
            weight_grads[:, 2 * units * parts :].reshape(-1, parts, own),
        ],
        2,
    ).transpose(1, 0, 2)
    weight_grads = rotate(weight_grads, "tensor")
    weight_grads = sum(a.astype(f32) for a in weight_grads)
    early = jnp.concatenate(
        [
            mixer_bias_grad,
            first_gain_grad,
            first_shift_grad,
            outer_bias_grad,
            second_gain_grad,
            second_shift_grad,
            inner_bias_grad.reshape(-1),
        ]
    )
    early = add_up(early)

    lo, hi = ranges(segment_all, 512, 512)
    input_back = grad_attn
    qkv_grad = []
    bias_grad = []
    for h in range(heads):
        grads = attend_backward(h, 1, go1 if h else go0, h - 1 if h else 0, context_t, lse, qt, ka, qn, kt, vn, lo, hi)
        if h < heads - 1:
            back = lax.all_to_all(grads, "tensor", 0, 0, tiled=True)
        else:
            back = rotate(grads, "tensor")
        qkv_grad.append(sum(contract(x_parts[p], grads[p], 0, 1) for p in parts_of))
        bias_grad.append(jnp.sum(grads, (0, 2), dtype=f32))
        at = h * three
        if h < heads - 1:
            weights = [rest[t, :, at : at + three] for t in parts_of]
        else:
            weights = [
                lax.dynamic_index_in_dim(rest, (rank - t) % parts, 0, keepdims=False)[:, at : at + three]
                for t in parts_of
            ]
        input_back = input_back + sum(contract(back[t], weights[t], 0, 1) for t in parts_of)
    input_grad = input_back.astype(bf)
    bias_grad = jnp.concatenate(bias_grad)
    high = bias_grad.astype(bf)
    low = (bias_grad - high.astype(f32)).astype(bf)
    each = width // groups
    qkv_grad = jnp.concatenate(qkv_grad, 1).astype(bf).reshape(groups, each, 3 * own)
    extra = jnp.pad(jnp.stack([high, low]), ((0, 14), (0, 0)))
    extra = jnp.broadcast_to(extra[None], (groups, 16, 3 * own))
    qkv_grad = lax.all_to_all(jnp.concatenate([qkv_grad, extra], 1), "dp", 0, 0, tiled=True)
    qkv_grad = jnp.sum(qkv_grad.astype(f32), 0)
    bias_grad = qkv_grad[each] + qkv_grad[each + 1]
    pick = lambda a, n: a.reshape(a.shape[:-1] + (heads, 3, HD))[..., n, :].reshape(a.shape[:-1] + (own,))
    stacked = early[: 6 * width].reshape(6, width)
    inner_bias_out = lax.dynamic_slice_in_dim(early, 6 * width + rank * units, units)
    return (
        layer_out[None],
        input_grad[None],
        pick(qkv_grad[:each], 0),
        pick(qkv_grad[:each], 1),
        pick(qkv_grad[:each], 2),
        pick(bias_grad, 0),
        pick(bias_grad, 2),
        weight_grads[:, 2 * units :].T,
        stacked[0],
        stacked[1],
        stacked[2],
        weight_grads[:, :units],
        inner_bias_out,
        weight_grads[:, units : 2 * units].T,
        stacked[3],
        stacked[4],
        stacked[5],
    )


def solution(mesh):
    placed = (
        P("dp", "tensor", None),
        P("dp", "tensor"),
        P("dp", "tensor"),
        P("dp", "tensor"),
        P("dp", "tensor"),
        P("tensor"),
        P("tensor"),
        P("tensor", "dp"),
        P(),
        P(),
        P(),
        P("dp", "tensor"),
        P("tensor"),
        P("tensor", "dp"),
        P(),
        P(),
        P(),
        P("dp", "tensor", None),
    )

    return jax.shard_map(
        body,
        mesh=mesh,
        in_specs=placed,
        out_specs=(
            P("dp", "tensor", None),
            P("dp", "tensor", None),
            P("dp", "tensor"),
            P("dp", "tensor"),
            P("dp", "tensor"),
            P("tensor"),
            P("tensor"),
            P("tensor", "dp"),
            P(),
            P(),
            P(),
            P("dp", "tensor"),
            P("tensor"),
            P("tensor", "dp"),
            P(),
            P(),
            P(),
        ),
        check_vma=False,
    )
```

```python
import functools

import jax
import jax.numpy as jnp
from jax import lax
from jax.experimental import pallas as pl
from jax.experimental.pallas import tpu as pltpu
from jax.sharding import PartitionSpec as P


EPS = 1e-12
ROOT_HALF = 0.7071067811865476
INV_ROOT_TWO_PI = 0.3989422804014327
HD=64; SCALE=0.125; APART=-1e30
VM=pltpu.VMEM


def dot(a,b): return jnp.dot(a,b,preferred_element_type=jnp.float32)


def project_body(heads, part_ref, x_ref, w_ref, b_ref, scol_ref, srow_ref, qt_ref, ka_ref, vt_ref, qn_ref, kt_ref, vn_ref):
    y = dot(x_ref[...], w_ref[0,:,:b_ref.shape[1]]) + b_ref[...]
    low = y.astype(jnp.bfloat16)
    yt = y.T.astype(jnp.bfloat16)
    rows = y.shape[0]
    apart = jnp.where(lax.broadcasted_iota(jnp.int32,(HD,rows),0)==srow_ref[...],0.0,APART).astype(jnp.bfloat16)
    same = (lax.broadcasted_iota(jnp.int32,(rows,HD),1)==scol_ref[...]).astype(jnp.float32).astype(jnp.bfloat16)
    for h in range(heads):
        at=3*h*HD
        qt_ref[h,:HD,:]=yt[at:at+HD]*jnp.bfloat16(SCALE)
        qt_ref[h,HD:,:]=apart
        qn_ref[h]=low[:,at:at+HD]*jnp.bfloat16(SCALE)
        ka_ref[h]=jnp.concatenate([low[:,at+HD:at+2*HD],same],axis=1)
        kt_ref[h]=yt[at+HD:at+2*HD]
        vt_ref[h]=yt[at+2*HD:at+3*HD]
        vn_ref[h]=low[:,at+2*HD:at+3*HD]


def project(x,rest,part,b,seg,rows=512):
    L,D=x.shape; heads=b.shape[0]//(3*HD)
    bf=jnp.bfloat16
    cols=4*heads*HD
    nat=lambda n: pl.BlockSpec((heads,rows,n),lambda i,*_:(0,i,0))
    tr=lambda n: pl.BlockSpec((heads,n,rows),lambda i,*_:(0,0,i))
    S=jax.ShapeDtypeStruct
    return pl.pallas_call(functools.partial(project_body,heads),
        grid_spec=pltpu.PrefetchScalarGridSpec(num_scalar_prefetch=1,grid=(L//rows,),
        in_specs=[pl.BlockSpec((rows,D),lambda i,*_:(i,0)),pl.BlockSpec((1,D,cols),lambda i,p:(p[0],0,0)),pl.BlockSpec((1,b.shape[0]),lambda i,*_:(0,0)),
                  pl.BlockSpec((rows,1),lambda i,*_:(i,0)),pl.BlockSpec((1,rows),lambda i,*_:(0,i))],
        out_specs=[tr(2*HD),nat(2*HD),tr(HD),nat(HD),tr(HD),nat(HD)]),
        out_shape=[S((heads,2*HD,L),bf),S((heads,L,2*HD),bf),S((heads,HD,L),bf),S((heads,L,HD),bf),S((heads,HD,L),bf),S((heads,L,HD),bf)],
        compiler_params=pltpu.CompilerParams(vmem_limit_bytes=48<<20),
        cost_estimate=pl.CostEstimate(flops=2*L*D*b.shape[0],bytes_accessed=L*D*2+D*cols*2+L*heads*HD*2*10,transcendentals=0),
        name="project")(part.reshape(1),x,rest,b.reshape(1,-1),seg.reshape(-1,1),seg.reshape(1,-1))


def forward_body(BK, SUB, lo_ref, hi_ref, qt_ref, ka_ref, vt_ref, ctx_ref, ot_ref, lse_ref, m_s, l_s, acc):
    i=pl.program_id(0)
    heads,_,BQ=qt_ref.shape
    chains=[(h,slice(c*SUB,(c+1)*SUB)) for h in range(heads) for c in range(BQ//SUB)]
    m_s[...]=jnp.full(m_s.shape,-jnp.inf,jnp.float32)
    l_s[...]=jnp.zeros(l_s.shape,jnp.float32)
    acc[...]=jnp.zeros(acc.shape,jnp.float32)

    def step(j,_):
        at=pl.multiple_of(j*BK,BK)
        for h,cut in chains:
            s=dot(ka_ref[h,pl.ds(at,BK),:],qt_ref[h,:,cut])
            m_old=m_s[h,:,cut]
            m_new=jnp.maximum(m_old,jnp.max(s,axis=0,keepdims=True))
            p=jnp.exp(s-m_new)
            alpha=jnp.exp(m_old-m_new)
            m_s[h,:,cut]=m_new
            l_s[h,:,cut]=l_s[h,:,cut]*alpha+jnp.sum(p,axis=0,keepdims=True)
            acc[h,:,cut]=acc[h,:,cut]*alpha+dot(vt_ref[h,:,pl.ds(at,BK)],p.astype(jnp.bfloat16))
        return 0

    lax.fori_loop(lo_ref[i],hi_ref[i],step,0)
    for h in range(heads):
        o=acc[h]/l_s[h]
        lse_ref[h]=m_s[h]+jnp.log(l_s[h])
        ot_ref[h]=o
        ctx_ref[0,h*HD:(h+1)*HD,:]=o.astype(jnp.bfloat16)


def attend_forward(first,heads,parts,qt,ka,vt,lo,hi,BQ=384,BK=512,SUB=384):
    L=qt.shape[2]
    S=jax.ShapeDtypeStruct
    per=L//parts//BQ
    return pl.pallas_call(functools.partial(forward_body,BK,SUB),
        grid_spec=pltpu.PrefetchScalarGridSpec(num_scalar_prefetch=2,grid=(L//BQ,),
        in_specs=[pl.BlockSpec((heads,2*HD,BQ),lambda i,*_:(first//heads,0,i)),pl.BlockSpec((heads,L,2*HD),lambda i,*_:(first//heads,0,0)),pl.BlockSpec((heads,HD,L),lambda i,*_:(first//heads,0,0))],
        out_specs=[pl.BlockSpec((1,heads*HD,BQ),lambda i,*_:(i//per,0,i%per)),pl.BlockSpec((heads,HD,BQ),lambda i,*_:(0,0,i)),pl.BlockSpec((heads,1,BQ),lambda i,*_:(0,0,i))],
        scratch_shapes=[VM((heads,1,BQ),jnp.float32),VM((heads,1,BQ),jnp.float32),VM((heads,HD,BQ),jnp.float32)]),
        out_shape=[S((parts,heads*HD,L//parts),jnp.bfloat16),S((heads,HD,L),jnp.float32),S((heads,1,L),jnp.float32)],
        compiler_params=pltpu.CompilerParams(vmem_limit_bytes=56<<20),
        cost_estimate=pl.CostEstimate(flops=2*L*L*HD*2*heads,bytes_accessed=L*heads*HD*2*8,transcendentals=L*L*heads),
        name="attend_forward")(lo,hi,qt,ka,vt)


def backward_body(BQ, BK, SUB, lo_ref, hi_ref, go_ref, ot_ref, lse_ref, qt_ref, ka_ref, qn_ref, kt_ref, vn_ref, x_ref, out_ref, wg_ref, sum_ref, got, gon, delta, dqt, dkt, dvt, dk_s, dv_s, x_s, x_sem):
    bring=pltpu.make_async_copy(x_ref,x_s,x_sem)
    bring.start()
    parts,_,rows=go_ref.shape
    heads,_,L=qt_ref.shape
    CH=256
    for h in range(heads):
        for c in range(L//CH):
            p,at=c*CH//rows,c*CH%rows
            gt=go_ref[p,h*HD:(h+1)*HD,at:at+CH]
            wide=gt.astype(jnp.float32)
            got[h,:,c*CH:(c+1)*CH]=gt
            gon[h,c*CH:(c+1)*CH,:]=wide.T.astype(jnp.bfloat16)
            delta[h,:,c*CH:(c+1)*CH]=jnp.sum(wide*ot_ref[h,:,c*CH:(c+1)*CH],axis=0,keepdims=True)
    dqt[...]=jnp.zeros(dqt.shape,jnp.float32)

    def key_block(j,_):
        ka_at=pl.multiple_of(j*BK,BK)
        dk_s[...]=jnp.zeros(dk_s.shape,jnp.float32)
        dv_s[...]=jnp.zeros(dv_s.shape,jnp.float32)

        def query_block(i,_):
            for h,c in [(h,c) for h in range(heads) for c in range(BQ//SUB)]:
                at=pl.multiple_of(i*BQ+c*SUB,SUB)
                s=dot(ka_ref[h,pl.ds(ka_at,BK),:],qt_ref[h,:,pl.ds(at,SUB)])
                p=jnp.exp(s-lse_ref[h,:,pl.ds(at,SUB)])
                dp=dot(vn_ref[h,pl.ds(ka_at,BK),:],got[h,:,pl.ds(at,SUB)])
                ds=(p*(dp-delta[h,:,pl.ds(at,SUB)])).astype(jnp.bfloat16)
                dv_s[h]+=dot(p.astype(jnp.bfloat16),gon[h,pl.ds(at,SUB),:])
                dk_s[h]+=dot(ds,qn_ref[h,pl.ds(at,SUB),:])
                dqt[h,:,pl.ds(at,SUB)]+=dot(kt_ref[h,:,pl.ds(ka_at,BK)],ds)
            return 0

        lax.fori_loop(lo_ref[j],hi_ref[j],query_block,0)
        for h in range(heads):
            dkt[h,:,pl.ds(ka_at,BK)]=dk_s[h].T.astype(jnp.bfloat16)
            dvt[h,:,pl.ds(ka_at,BK)]=dv_s[h].T.astype(jnp.bfloat16)
        return 0

    lax.fori_loop(0,L//BK,key_block,0)
    for h in range(heads):
        for p in range(parts):
            cut=slice(p*rows,(p+1)*rows)
            out_ref[p,3*h*HD:(3*h+1)*HD,:]=(dqt[h,:,cut]*SCALE).astype(jnp.bfloat16)
            out_ref[p,(3*h+1)*HD:(3*h+2)*HD,:]=dkt[h,:,cut]
            out_ref[p,(3*h+2)*HD:(3*h+3)*HD,:]=dvt[h,:,cut]
    bring.wait()
    wg=jnp.zeros(wg_ref.shape[::-1],jnp.float32)
    total=jnp.zeros((3*heads*HD,1),jnp.float32)
    for p in range(parts):
        part=out_ref[p]
        wg=wg+dot(part,x_s[p])
        total=total+jnp.sum(part.astype(jnp.float32),axis=1,keepdims=True)
    wg_ref[...]=wg.T.astype(wg_ref.dtype)
    sum_ref[...]=jnp.broadcast_to(total,sum_ref.shape)


def attend_backward(first,heads,go,go_first,ot,lse,ot_first,qt,ka,qn,kt,vn,x,lo,hi,BQ=512,BK=512,SUB=512):
    parts,_,rows=go.shape; L=parts*rows; D=x.shape[2]
    S=jax.ShapeDtypeStruct; f32=jnp.float32; bf=jnp.bfloat16
    at=lambda a,n: pl.BlockSpec((heads,)+a.shape[1:],lambda i,*_:(n//heads,0,0),pipeline_mode=pl.Buffered(1))
    out=3*heads*HD
    return pl.pallas_call(functools.partial(backward_body,BQ,BK,SUB),
        grid_spec=pltpu.PrefetchScalarGridSpec(num_scalar_prefetch=2,grid=(1,),
        in_specs=[pl.BlockSpec((parts,heads*HD,rows),lambda i,*_:(0,go_first,0),pipeline_mode=pl.Buffered(1)),at(ot,ot_first),at(lse,ot_first)]+[at(a,first) for a in (qt,ka,qn,kt,vn)]+[pl.BlockSpec(memory_space=pl.ANY)],
        out_specs=[pl.BlockSpec((parts,out,rows),lambda i,*_:(0,0,0),pipeline_mode=pl.Buffered(1)),pl.BlockSpec((D,out),lambda i,*_:(0,0)),pl.BlockSpec((out,128),lambda i,*_:(0,0))],
        scratch_shapes=[VM((heads,HD,L),bf),VM((heads,L,HD),bf),VM((heads,1,L),f32),VM((heads,HD,L),f32),VM((heads,HD,L),bf),VM((heads,HD,L),bf),VM((heads,BK,HD),f32),VM((heads,BK,HD),f32),VM(x.shape,bf),pltpu.SemaphoreType.DMA]),
        out_shape=[S((parts,out,rows),bf),S((D,out),bf),S((out,128),f32)],
        compiler_params=pltpu.CompilerParams(vmem_limit_bytes=60<<20),
        cost_estimate=pl.CostEstimate(flops=2*L*L*HD*5*heads,bytes_accessed=L*heads*HD*2*14,transcendentals=L*L*heads),
        name="attend_backward")(lo,hi,go,ot,lse,qt,ka,qn,kt,vn,x)


def ranges(seg,BQ,BK):
    first=seg.reshape(-1,BQ)[:,0]; last=seg.reshape(-1,BQ)[:,-1]
    kf=seg.reshape(-1,BK)[:,0]; kl=seg.reshape(-1,BK)[:,-1]
    lo=jnp.sum((kl[None,:]<first[:,None]).astype(jnp.int32),1)
    hi=jnp.sum((kf[None,:]<=last[:,None]).astype(jnp.int32),1)
    return lo,hi


def dot_right_t(left, right):
    return lax.dot_general(
        left, right, (((1,), (1,)), ((), ())), preferred_element_type=jnp.float32
    )


def layer_norm(values_in, gain, shift):
    mean_row = jnp.mean(values_in, -1, keepdims=True)
    centered = values_in - mean_row
    inverse = lax.rsqrt(jnp.mean(centered * centered, -1, keepdims=True) + EPS)
    normed = centered * inverse
    return (normed * gain + shift, normed, inverse)


def norm_back(grad_in, normed, inverse, gain):
    scaled = grad_in * gain
    return inverse * (
        scaled
        - jnp.mean(scaled, -1, keepdims=True)
        - normed * jnp.mean(scaled * normed, -1, keepdims=True)
    )


def gelu_value(inner):
    return 0.5 * inner * (1.0 + jax.scipy.special.erf(inner * ROOT_HALF))


def gelu_slope(inner):
    return (
        0.5 * (1.0 + jax.scipy.special.erf(inner * ROOT_HALF))
        + inner * jnp.exp(-0.5 * inner * inner) * INV_ROOT_TWO_PI
    )


MESH = pl.DeviceIdType.MESH


def flip(index, bit):
    span = 1 << bit
    return index + span * (1 - 2 * ((index // span) % 2))


def start_body(n, bits, x_ref, w_ref, s_ref, x_out, w_out, s_out, send_z, recv_z, send_d, recv_d, keep_sem):
    me = lax.axis_index("tensor")
    mine = lax.axis_index("dp")
    barrier = pltpu.get_barrier_semaphore()

    @pl.when(me > 0)
    def _():
        pl.semaphore_signal(barrier, inc=1, device_id={"tensor": me - 1}, device_id_type=MESH)

    @pl.when(me < n - 1)
    def _():
        pl.semaphore_signal(barrier, inc=1, device_id={"tensor": me + 1}, device_id_type=MESH)

    for bit in range(bits):
        pl.semaphore_signal(barrier, inc=1, device_id={"dp": flip(mine, bit)}, device_id_type=MESH)
    pl.semaphore_wait(barrier, bits + jnp.where(me > 0, 1, 0) + jnp.where(me < n - 1, 1, 0))

    keeps = [
        pltpu.make_async_copy(x_ref, x_out.at[me], keep_sem.at[0]),
        pltpu.make_async_copy(w_ref, w_out.at[me, mine], keep_sem.at[1]),
        pltpu.make_async_copy(s_ref, s_out.at[me], keep_sem.at[2]),
    ]
    for keep in keeps:
        keep.start()

    def hop(kind, side, step):
        block = me - (step - 1) if side else me + (step - 1)
        first, place = (
            (x_ref, x_out.at[block]),
            (w_ref, w_out.at[block, mine]),
            (s_ref, s_out.at[block]),
        )[kind]
        return pltpu.make_async_remote_copy(
            src_ref=first if step == 1 else place,
            dst_ref=place,
            send_sem=send_z.at[kind, side, step - 1],
            recv_sem=recv_z.at[kind, side, step - 1],
            device_id={"tensor": me + 1 if side else me - 1},
            device_id_type=MESH,
        )

    def sends(side, step):
        if side:
            return (me < n - 1) & (me >= step - 1)
        return (me > 0) & (me + step - 1 <= n - 1)

    def receives(side, step):
        return me >= step if side else me + step <= n - 1

    def z_start(kinds, step):
        for side in (0, 1):

            @pl.when(sends(side, step))
            def _():
                for kind in kinds:
                    hop(kind, side, step).start()

    def z_arrive(kinds, step):
        for side in (0, 1):

            @pl.when(receives(side, step))
            def _():
                for kind in kinds:
                    hop(kind, side, step).wait_recv()

    half = w_ref.shape[1] // 2
    up = list(range(bits - 1, -1, -1))
    orders = (up, [up[1], up[0]] + up[2:] if bits > 1 else up)

    def doubling(side, step):
        order = orders[side]
        held = [mine]
        for bit in order[:step]:
            held = held + [flip(d, bit) for d in held]
        cut = pl.ds(side * half, half)
        return [
            pltpu.make_async_remote_copy(
                src_ref=w_out.at[:, d, :, cut],
                dst_ref=w_out.at[:, d, :, cut],
                send_sem=send_d.at[side, (1 << step) - 1 + at],
                recv_sem=recv_d.at[side, (1 << step) - 1 + at],
                device_id={"dp": flip(mine, order[step])},
                device_id_type=MESH,
            )
            for at, d in enumerate(held)
        ]

    def d_start(step):
        for side in (0, 1):
            for copy in doubling(side, step):
                copy.start()

    def d_arrive(step):
        for side in (0, 1):
            for copy in doubling(side, step):
                copy.wait_recv()

    for step in range(1, n):
        z_start((1, 2), step)
        z_arrive((1, 2), step)
    keeps[1].wait()
    for step in range(max(n - 1, bits)):
        if step < bits:
            if step:
                d_arrive(step - 1)
            d_start(step)
        if step < n - 1:
            if step:
                z_arrive((0,), step)
            z_start((0,), step + 1)
    z_arrive((0,), n - 1)
    d_arrive(bits - 1)
    for side in (0, 1):
        for step in range(1, n):

            @pl.when(sends(side, step))
            def _():
                for kind in (0, 1, 2):
                    hop(kind, side, step).wait_send()

        for step in range(bits):
            for copy in doubling(side, step):
                copy.wait_send()
    keeps[0].wait()
    keeps[2].wait()


def start(x, w, small):
    n = lax.axis_size("tensor")
    groups = lax.axis_size("dp")
    bits = groups.bit_length() - 1
    S = jax.ShapeDtypeStruct
    anywhere = pl.BlockSpec(memory_space=pl.ANY)
    return pl.pallas_call(
        functools.partial(start_body, n, bits),
        in_specs=[pl.BlockSpec(memory_space=pltpu.VMEM)] * 3,
        out_specs=[anywhere] * 3,
        out_shape=[
            S((n,) + x.shape, x.dtype),
            S((n, groups) + w.shape, w.dtype),
            S((n,) + small.shape, small.dtype),
        ],
        scratch_shapes=[
            pltpu.SemaphoreType.DMA((3, 2, n - 1)),
            pltpu.SemaphoreType.DMA((3, 2, n - 1)),
            pltpu.SemaphoreType.DMA((2, groups - 1)),
            pltpu.SemaphoreType.DMA((2, groups - 1)),
            pltpu.SemaphoreType.DMA((3,)),
        ],
        compiler_params=pltpu.CompilerParams(collective_id=0, has_side_effects=True),
        cost_estimate=pl.CostEstimate(flops=0, bytes_accessed=200 << 20, transcendentals=0),
        name="start",
    )(x, w, small)


def weight_grads_body(parts, first_ref, second_ref, attn_ref, inner_ref, active_ref, context_ref, out_ref, ft, st):
    j = pl.program_id(0)

    @pl.when(j == 0)
    def _():
        ft[...] = first_ref[...].T
        st[...] = second_ref[...].T

    @pl.when((j < 2 * parts) & (j % 2 == 0))
    def _():
        out_ref[...] = dot(ft[...], inner_ref[0]).astype(out_ref.dtype)

    @pl.when((j < 2 * parts) & (j % 2 == 1))
    def _():
        out_ref[...] = dot(st[...], active_ref[0]).astype(out_ref.dtype)

    @pl.when(j == 2 * parts)
    def _():
        out_ref[...] = dot_right_t(attn_ref[...].T, context_ref[...]).astype(out_ref.dtype)


def weight_grads_of(first_low, second_low, attn_low, grad_inner, active, context):
    parts, rows, units = active.shape
    width = first_low.shape[1]
    features = context.shape[0]
    fixed = pl.BlockSpec((rows, width), lambda j: (0, 0))
    moving = lambda shift: pl.BlockSpec((1, rows, units), lambda j: (jnp.clip((j - shift) // 2, 0, parts - 1), 0, 0))
    return pl.pallas_call(
        functools.partial(weight_grads_body, parts),
        grid=(2 * parts + 1,),
        in_specs=[fixed, fixed, fixed, moving(0), moving(1), pl.BlockSpec((features, rows), lambda j: (0, 0))],
        out_specs=pl.BlockSpec((width, units), lambda j: (0, j)),
        out_shape=jax.ShapeDtypeStruct((width, units * 2 * parts + features), jnp.bfloat16),
        scratch_shapes=[VM((width, rows), jnp.bfloat16), VM((width, rows), jnp.bfloat16)],
        compiler_params=pltpu.CompilerParams(vmem_limit_bytes=40 << 20),
        cost_estimate=pl.CostEstimate(flops=2 * rows * width * (2 * parts * units + features), bytes_accessed=rows * units * 2 * parts * 4, transcendentals=0),
        name="weight_grads",
    )(first_low, second_low, attn_low, grad_inner, active, context)


def early_back_body(w_ref, b0_ref, b1_ref, acc_ref):
    width = b0_ref.shape[1]
    total = jnp.zeros(acc_ref.shape, jnp.float32)
    for t in range(b0_ref.shape[0]):
        total = total + dot(w_ref[t, :, : 2 * width], jnp.concatenate([b0_ref[t], b1_ref[t]], axis=0))
    acc_ref[...] = total


def late_back_body(cut, part_ref, w_ref, acc_ref, grad_ref, *rest):
    backs, out_ref = rest[:-1], rest[-1]
    parts = len(backs)
    total = acc_ref[...]
    for d in range(parts):
        total = total + dot(w_ref[(part_ref[0] + parts - d) % parts, :, cut : cut + backs[d].shape[0]], backs[d][...])
    out_ref[...] = (total.T + grad_ref[...]).astype(out_ref.dtype)


def weight_block(rest, cols):
    return pl.BlockSpec(rest.shape[:2] + (cols,), lambda i, *_: (0, 0, 0), pipeline_mode=pl.Buffered(1))


def whole(a):
    return pl.BlockSpec(a.shape, lambda i, *_: (0,) * a.ndim, pipeline_mode=pl.Buffered(1))


def early_back(rest, cols, b0, b1):
    width, rows = rest.shape[1], b0.shape[2]
    return pl.pallas_call(
        early_back_body,
        grid=(1,),
        in_specs=[weight_block(rest, cols), whole(b0), whole(b1)],
        out_specs=pl.BlockSpec((width, rows), lambda i: (0, 0)),
        out_shape=jax.ShapeDtypeStruct((width, rows), jnp.float32),
        compiler_params=pltpu.CompilerParams(vmem_limit_bytes=40 << 20),
        cost_estimate=pl.CostEstimate(flops=4 * width * rows * b0.shape[0] * b0.shape[1], bytes_accessed=10 << 20, transcendentals=0),
        name="early_back",
    )(rest, b0, b1)


def late_back(rest, cols, cut, part, acc, grad, backs):
    rows, width = grad.shape
    return pl.pallas_call(
        functools.partial(late_back_body, cut),
        grid_spec=pltpu.PrefetchScalarGridSpec(
            num_scalar_prefetch=1,
            grid=(1,),
            in_specs=[weight_block(rest, cols), whole(acc), whole(grad)] + [whole(b) for b in backs],
            out_specs=pl.BlockSpec((rows, width), lambda i, *_: (0, 0)),
        ),
        out_shape=jax.ShapeDtypeStruct((rows, width), jnp.bfloat16),
        compiler_params=pltpu.CompilerParams(vmem_limit_bytes=40 << 20),
        cost_estimate=pl.CostEstimate(flops=2 * width * rows * backs[0].shape[0] * len(backs), bytes_accessed=10 << 20, transcendentals=0),
        name="late_back",
    )(part.reshape(1), rest, acc, grad, *backs)


def add_up(value):
    for axis in ("dp", "tensor"):
        size = lax.axis_size(axis)
        span = 1
        while span < size:
            other = lax.ppermute(value, axis, [(i, i ^ span) for i in range(size)])
            value = value + other
            span *= 2
    return value


def rotate(blocks, axis):
    size = lax.axis_size(axis)
    me = lax.axis_index(axis)
    out = []
    for d in range(size):
        block = lax.dynamic_index_in_dim(blocks, (me + d) % size, 0, keepdims=False)
        if d:
            block = lax.ppermute(block, axis, [(i, (i + d) % size) for i in range(size)])
        out.append(block)
    return out


def body(hidden_in, segments, query_weight, key_weight, value_weight, query_bias, value_bias, mixer_weight, mixer_bias, first_gain, first_shift, inner_weight, inner_bias, outer_weight, outer_bias, second_gain, second_shift, cotangent):
    bf = jnp.bfloat16
    f32 = jnp.float32
    _, rows, width = hidden_in.shape
    parts = lax.axis_size("tensor")
    groups = lax.axis_size("dp")
    rank = lax.axis_index("tensor")
    own = query_weight.shape[1]
    heads = own // HD
    three = 3 * HD
    units = inner_weight.shape[1]
    parts_of = range(parts)
    by_head = lambda q, k, v: jnp.stack([a.reshape(a.shape[:-1] + (heads, HD)) for a in (q, k, v)], -2).reshape(q.shape[:-1] + (3 * own,))
    x_own = hidden_in[0]
    qkv_own = by_head(query_weight, key_weight, value_weight)
    small = jnp.concatenate([segments[0].astype(f32), inner_bias]).reshape(-1, 128)
    rest_own = jnp.concatenate([qkv_own, mixer_weight.T, inner_weight, outer_weight.T], 1)
    x_parts, rest, small = start(x_own, rest_own, small)
    x_all = x_parts.reshape(parts * rows, width)
    rest = rest.reshape(parts, width, rest_own.shape[1])
    small = small.reshape(parts, -1)
    segment_all = small[:, :rows].astype(jnp.int32).reshape(-1)
    inner_bias_all = small[:, rows:]
    biases = by_head(query_bias, jnp.zeros_like(query_bias), value_bias)

    qt, ka, vt, qn, kt, vn = project(x_all, rest, rank, biases, segment_all)
    lo, hi = ranges(segment_all, 384, 512)
    lead = heads - 1
    context_t, lse, exchanged = [], [], []
    for call, (first, count) in enumerate(((0, lead), (lead, 1))):
        part, out_t, out_lse = attend_forward(first, count, parts, qt, ka, vt, lo, hi)
        context_t.append(out_t)
        lse.append(out_lse)
        exchanged.append(lax.all_to_all(part, "tensor", 0, 0, tiled=True))
    context = jnp.concatenate(exchanged, 1)
    w1 = [rest[t, :, 4 * own : 4 * own + units] for t in parts_of]
    w2t = [rest[t, :, 4 * own + units :] for t in parts_of]
    mt = [rest[t, :, 3 * own : 4 * own] for t in parts_of]
    contract = lambda a, b, i, j: lax.dot_general(a, b, (((i,), (j,)), ((), ())), preferred_element_type=f32)
    mixed = sum(contract(context[t], mt[t], 0, 1) for t in parts_of)
    attn_in = x_own.astype(f32) + mixed + mixer_bias
    first, first_norm, first_inv = layer_norm(attn_in, first_gain, first_shift)
    first_low = first.astype(bf)
    inner = [dot(first_low, w1[t]) + inner_bias_all[t] for t in parts_of]
    active = [gelu_value(inner[t]).astype(bf) for t in parts_of]
    outer = sum(dot_right_t(active[t], w2t[t]) for t in parts_of)
    second_in = first + outer + outer_bias
    second, second_norm, second_inv = layer_norm(second_in, second_gain, second_shift)
    layer_out = second.astype(bf)
    grad_out = cotangent[0].astype(f32)
    second_gain_grad = jnp.sum(grad_out * second_norm, 0)
    second_shift_grad = jnp.sum(grad_out, 0)
    grad_second = norm_back(grad_out, second_norm, second_inv, second_gain)
    outer_bias_grad = jnp.sum(grad_second, 0)
    second_low = grad_second.astype(bf)
    grad_inner = [(dot(second_low, w2t[t]) * gelu_slope(inner[t])).astype(bf) for t in parts_of]
    inner_bias_grad = jnp.stack([jnp.sum(g, 0, dtype=f32) for g in grad_inner])
    grad_first = grad_second + sum(dot_right_t(grad_inner[t], w1[t]) for t in parts_of)
    first_gain_grad = jnp.sum(grad_first * first_norm, 0)
    first_shift_grad = jnp.sum(grad_first, 0)
    grad_attn = norm_back(grad_first, first_norm, first_inv, first_gain)
    mixer_bias_grad = jnp.sum(grad_attn, 0)
    attn_low = grad_attn.astype(bf)
    grad_context = jnp.stack([contract(mt[t], attn_low, 0, 1).astype(bf) for t in parts_of])
    go0 = lax.all_to_all(grad_context[:, :HD], "tensor", 0, 0, tiled=True)
    go1 = lax.all_to_all(grad_context[:, HD:], "tensor", 0, 0, tiled=True)
    weight_grads = weight_grads_of(
        first_low, second_low, attn_low, jnp.stack(grad_inner), jnp.stack(active), context.reshape(-1, rows)
    )
    weight_grads = lax.psum_scatter(weight_grads, "dp", scatter_dimension=0, tiled=True)
    weight_grads = jnp.concatenate(
        [
            weight_grads[:, : 2 * units * parts].reshape(-1, parts, 2 * units),
            weight_grads[:, 2 * units * parts :].reshape(-1, parts, own),
        ],
        2,
    ).transpose(1, 0, 2)
    weight_grads = rotate(weight_grads, "tensor")
    weight_grads = sum(a.astype(f32) for a in weight_grads)
    early = jnp.concatenate(
        [
            mixer_bias_grad,
            first_gain_grad,
            first_shift_grad,
            outer_bias_grad,
            second_gain_grad,
            second_shift_grad,
            inner_bias_grad.reshape(-1),
        ]
    )
    early = add_up(early)

    lo, hi = ranges(segment_all, 512, 512)
    backs, qkv_grad, bias_grad = [], [], []
    for h in range(heads):
        call = 0 if h < lead else 1
        grads, weight_part, sums = attend_backward(
            h, 1, go1 if h else go0, h - 1 if h else 0, context_t[call], lse[call], h - call * lead, qt, ka, qn, kt, vn, x_parts, lo, hi
        )
        if h < heads - 1:
            backs.append(lax.all_to_all(grads, "tensor", 0, 0, tiled=True))
        else:
            backs.append(rotate(grads, "tensor"))
        qkv_grad.append(weight_part)
        bias_grad.append(sums[:, 0])
    input_back = early_back(rest, 4 * own, backs[0], backs[1])
    input_grad = late_back(rest, 4 * own, 2 * three, rank, input_back, grad_attn, backs[2])
    bias_grad = jnp.concatenate(bias_grad)
    high = bias_grad.astype(bf)
    low = (bias_grad - high.astype(f32)).astype(bf)
    each = width // groups
    qkv_grad = jnp.concatenate(qkv_grad, 1).reshape(groups, each, 3 * own)
    extra = jnp.pad(jnp.stack([high, low]), ((0, 14), (0, 0)))
    extra = jnp.broadcast_to(extra[None], (groups, 16, 3 * own))
    qkv_grad = lax.all_to_all(jnp.concatenate([qkv_grad, extra], 1), "dp", 0, 0, tiled=True)
    qkv_grad = jnp.sum(qkv_grad.astype(f32), 0)
    bias_grad = qkv_grad[each] + qkv_grad[each + 1]
    pick = lambda a, n: a.reshape(a.shape[:-1] + (heads, 3, HD))[..., n, :].reshape(a.shape[:-1] + (own,))
    stacked = early[: 6 * width].reshape(6, width)
    inner_bias_out = lax.dynamic_slice_in_dim(early, 6 * width + rank * units, units)
    return (
        layer_out[None],
        input_grad[None],
        pick(qkv_grad[:each], 0),
        pick(qkv_grad[:each], 1),
        pick(qkv_grad[:each], 2),
        pick(bias_grad, 0),
        pick(bias_grad, 2),
        weight_grads[:, 2 * units :].T,
        stacked[0],
        stacked[1],
        stacked[2],
        weight_grads[:, :units],
        inner_bias_out,
        weight_grads[:, units : 2 * units].T,
        stacked[3],
        stacked[4],
        stacked[5],
    )


def solution(mesh):
    placed = (
        P("dp", "tensor", None),
        P("dp", "tensor"),
        P("dp", "tensor"),
        P("dp", "tensor"),
        P("dp", "tensor"),
        P("tensor"),
        P("tensor"),
        P("tensor", "dp"),
        P(),
        P(),
        P(),
        P("dp", "tensor"),
        P("tensor"),
        P("tensor", "dp"),
        P(),
        P(),
        P(),
        P("dp", "tensor", None),
    )

    return jax.shard_map(
        body,
        mesh=mesh,
        in_specs=placed,
        out_specs=(
            P("dp", "tensor", None),
            P("dp", "tensor", None),
            P("dp", "tensor"),
            P("dp", "tensor"),
            P("dp", "tensor"),
            P("tensor"),
            P("tensor"),
            P("tensor", "dp"),
            P(),
            P(),
            P(),
            P("dp", "tensor"),
            P("tensor"),
            P("tensor", "dp"),
            P(),
            P(),
            P(),
        ),
        check_vma=False,
    )
```

```python
import functools

import jax
import jax.numpy as jnp
from jax import lax
from jax.experimental import pallas as pl
from jax.experimental.pallas import tpu as pltpu
from jax.sharding import PartitionSpec as P


EPS = 1e-12
ROOT_HALF = 0.7071067811865476
INV_ROOT_TWO_PI = 0.3989422804014327
HD=64; SCALE=0.125; APART=-1e30
VM=pltpu.VMEM


def dot(a,b): return jnp.dot(a,b,preferred_element_type=jnp.float32)


def project_body(heads, part_ref, x_ref, w_ref, b_ref, scol_ref, srow_ref, qt_ref, ka_ref, vt_ref, qn_ref, kt_ref, vn_ref):
    y = dot(x_ref[...], w_ref[0,:,:b_ref.shape[1]]) + b_ref[...]
    low = y.astype(jnp.bfloat16)
    yt = y.T.astype(jnp.bfloat16)
    rows = y.shape[0]
    apart = jnp.where(lax.broadcasted_iota(jnp.int32,(HD,rows),0)==srow_ref[...],0.0,APART).astype(jnp.bfloat16)
    same = (lax.broadcasted_iota(jnp.int32,(rows,HD),1)==scol_ref[...]).astype(jnp.float32).astype(jnp.bfloat16)
    for h in range(heads):
        at=3*h*HD
        qt_ref[h,:HD,:]=yt[at:at+HD]*jnp.bfloat16(SCALE)
        qt_ref[h,HD:,:]=apart
        qn_ref[h]=low[:,at:at+HD]*jnp.bfloat16(SCALE)
        ka_ref[h]=jnp.concatenate([low[:,at+HD:at+2*HD],same],axis=1)
        kt_ref[h]=yt[at+HD:at+2*HD]
        vt_ref[h]=yt[at+2*HD:at+3*HD]
        vn_ref[h]=low[:,at+2*HD:at+3*HD]


def project(x,rest,part,b,seg,rows=512):
    L,D=x.shape; heads=b.shape[0]//(3*HD)
    bf=jnp.bfloat16
    cols=4*heads*HD
    nat=lambda n: pl.BlockSpec((heads,rows,n),lambda i,*_:(0,i,0))
    tr=lambda n: pl.BlockSpec((heads,n,rows),lambda i,*_:(0,0,i))
    S=jax.ShapeDtypeStruct
    return pl.pallas_call(functools.partial(project_body,heads),
        grid_spec=pltpu.PrefetchScalarGridSpec(num_scalar_prefetch=1,grid=(L//rows,),
        in_specs=[pl.BlockSpec((rows,D),lambda i,*_:(i,0)),pl.BlockSpec((1,D,cols),lambda i,p:(p[0],0,0)),pl.BlockSpec((1,b.shape[0]),lambda i,*_:(0,0)),
                  pl.BlockSpec((rows,1),lambda i,*_:(i,0)),pl.BlockSpec((1,rows),lambda i,*_:(0,i))],
        out_specs=[tr(2*HD),nat(2*HD),tr(HD),nat(HD),tr(HD),nat(HD)]),
        out_shape=[S((heads,2*HD,L),bf),S((heads,L,2*HD),bf),S((heads,HD,L),bf),S((heads,L,HD),bf),S((heads,HD,L),bf),S((heads,L,HD),bf)],
        compiler_params=pltpu.CompilerParams(vmem_limit_bytes=48<<20),
        cost_estimate=pl.CostEstimate(flops=2*L*D*b.shape[0],bytes_accessed=L*D*2+D*cols*2+L*heads*HD*2*10,transcendentals=0),
        name="project")(part.reshape(1),x,rest,b.reshape(1,-1),seg.reshape(-1,1),seg.reshape(1,-1))


def forward_body(BK, SUB, lo_ref, hi_ref, qt_ref, ka_ref, vt_ref, ctx_ref, ot_ref, lse_ref, m_s, l_s, acc):
    i=pl.program_id(0)
    heads,_,BQ=qt_ref.shape
    chains=[(h,slice(c*SUB,(c+1)*SUB)) for h in range(heads) for c in range(BQ//SUB)]
    m_s[...]=jnp.full(m_s.shape,-jnp.inf,jnp.float32)
    l_s[...]=jnp.zeros(l_s.shape,jnp.float32)
    acc[...]=jnp.zeros(acc.shape,jnp.float32)

    def step(j,_):
        at=pl.multiple_of(j*BK,BK)
        for h,cut in chains:
            s=dot(ka_ref[h,pl.ds(at,BK),:],qt_ref[h,:,cut])
            m_old=m_s[h,:,cut]
            m_new=jnp.maximum(m_old,jnp.max(s,axis=0,keepdims=True))
            p=jnp.exp(s-m_new)
            alpha=jnp.exp(m_old-m_new)
            m_s[h,:,cut]=m_new
            l_s[h,:,cut]=l_s[h,:,cut]*alpha+jnp.sum(p,axis=0,keepdims=True)
            acc[h,:,cut]=acc[h,:,cut]*alpha+dot(vt_ref[h,:,pl.ds(at,BK)],p.astype(jnp.bfloat16))
        return 0

    lax.fori_loop(lo_ref[i],hi_ref[i],step,0)
    for h in range(heads):
        o=acc[h]/l_s[h]
        lse_ref[h]=m_s[h]+jnp.log(l_s[h])
        ot_ref[h]=o
        ctx_ref[0,h*HD:(h+1)*HD,:]=o.astype(jnp.bfloat16)


def attend_forward(first,heads,parts,qt,ka,vt,lo,hi,BQ=384,BK=512,SUB=384):
    L=qt.shape[2]
    S=jax.ShapeDtypeStruct
    per=L//parts//BQ
    return pl.pallas_call(functools.partial(forward_body,BK,SUB),
        grid_spec=pltpu.PrefetchScalarGridSpec(num_scalar_prefetch=2,grid=(L//BQ,),
        in_specs=[pl.BlockSpec((heads,2*HD,BQ),lambda i,*_:(first//heads,0,i)),pl.BlockSpec((heads,L,2*HD),lambda i,*_:(first//heads,0,0)),pl.BlockSpec((heads,HD,L),lambda i,*_:(first//heads,0,0))],
        out_specs=[pl.BlockSpec((1,heads*HD,BQ),lambda i,*_:(i//per,0,i%per)),pl.BlockSpec((heads,HD,BQ),lambda i,*_:(0,0,i)),pl.BlockSpec((heads,1,BQ),lambda i,*_:(0,0,i))],
        scratch_shapes=[VM((heads,1,BQ),jnp.float32),VM((heads,1,BQ),jnp.float32),VM((heads,HD,BQ),jnp.float32)]),
        out_shape=[S((parts,heads*HD,L//parts),jnp.bfloat16),S((heads,HD,L),jnp.float32),S((heads,1,L),jnp.float32)],
        compiler_params=pltpu.CompilerParams(vmem_limit_bytes=56<<20),
        cost_estimate=pl.CostEstimate(flops=2*L*L*HD*2*heads,bytes_accessed=L*heads*HD*2*8,transcendentals=L*L*heads),
        name="attend_forward")(lo,hi,qt,ka,vt)


def backward_body(BQ, BK, SUB, lo_ref, hi_ref, go_ref, ot_ref, lse_ref, qt_ref, ka_ref, qn_ref, kt_ref, vn_ref, x_ref, out_ref, wg_ref, sum_ref, got, gon, delta, dqt, dkt, dvt, dk_s, dv_s, x_s, x_sem):
    bring=pltpu.make_async_copy(x_ref,x_s,x_sem)
    bring.start()
    parts,_,rows=go_ref.shape
    heads,_,L=qt_ref.shape
    CH=256
    for h in range(heads):
        for c in range(L//CH):
            p,at=c*CH//rows,c*CH%rows
            gt=go_ref[p,h*HD:(h+1)*HD,at:at+CH]
            wide=gt.astype(jnp.float32)
            got[h,:,c*CH:(c+1)*CH]=gt
            gon[h,c*CH:(c+1)*CH,:]=wide.T.astype(jnp.bfloat16)
            delta[h,:,c*CH:(c+1)*CH]=jnp.sum(wide*ot_ref[h,:,c*CH:(c+1)*CH],axis=0,keepdims=True)
    dqt[...]=jnp.zeros(dqt.shape,jnp.float32)

    def key_block(j,_):
        ka_at=pl.multiple_of(j*BK,BK)
        dk_s[...]=jnp.zeros(dk_s.shape,jnp.float32)
        dv_s[...]=jnp.zeros(dv_s.shape,jnp.float32)

        def query_block(i,_):
            for h,c in [(h,c) for h in range(heads) for c in range(BQ//SUB)]:
                at=pl.multiple_of(i*BQ+c*SUB,SUB)
                s=dot(ka_ref[h,pl.ds(ka_at,BK),:],qt_ref[h,:,pl.ds(at,SUB)])
                p=jnp.exp(s-lse_ref[h,:,pl.ds(at,SUB)])
                dp=dot(vn_ref[h,pl.ds(ka_at,BK),:],got[h,:,pl.ds(at,SUB)])
                ds=(p*(dp-delta[h,:,pl.ds(at,SUB)])).astype(jnp.bfloat16)
                dv_s[h]+=dot(p.astype(jnp.bfloat16),gon[h,pl.ds(at,SUB),:])
                dk_s[h]+=dot(ds,qn_ref[h,pl.ds(at,SUB),:])
                dqt[h,:,pl.ds(at,SUB)]+=dot(kt_ref[h,:,pl.ds(ka_at,BK)],ds)
            return 0

        lax.fori_loop(lo_ref[j],hi_ref[j],query_block,0)
        for h in range(heads):
            dkt[h,:,pl.ds(ka_at,BK)]=dk_s[h].T.astype(jnp.bfloat16)
            dvt[h,:,pl.ds(ka_at,BK)]=dv_s[h].T.astype(jnp.bfloat16)
        return 0

    lax.fori_loop(0,L//BK,key_block,0)
    for h in range(heads):
        for p in range(parts):
            cut=slice(p*rows,(p+1)*rows)
            out_ref[p,3*h*HD:(3*h+1)*HD,:]=(dqt[h,:,cut]*SCALE).astype(jnp.bfloat16)
            out_ref[p,(3*h+1)*HD:(3*h+2)*HD,:]=dkt[h,:,cut]
            out_ref[p,(3*h+2)*HD:(3*h+3)*HD,:]=dvt[h,:,cut]
    bring.wait()
    wg=jnp.zeros(wg_ref.shape[::-1],jnp.float32)
    total=jnp.zeros((3*heads*HD,1),jnp.float32)
    for p in range(parts):
        part=out_ref[p]
        wg=wg+dot(part,x_s[p])
        total=total+jnp.sum(part.astype(jnp.float32),axis=1,keepdims=True)
    wg_ref[...]=wg.T.astype(wg_ref.dtype)
    sum_ref[...]=jnp.broadcast_to(total,sum_ref.shape)


def attend_backward(first,heads,go,go_first,ot,lse,ot_first,qt,ka,qn,kt,vn,x,lo,hi,BQ=512,BK=512,SUB=512):
    parts,_,rows=go.shape; L=parts*rows; D=x.shape[2]
    S=jax.ShapeDtypeStruct; f32=jnp.float32; bf=jnp.bfloat16
    at=lambda a,n: pl.BlockSpec((heads,)+a.shape[1:],lambda i,*_:(n//heads,0,0),pipeline_mode=pl.Buffered(1))
    out=3*heads*HD
    return pl.pallas_call(functools.partial(backward_body,BQ,BK,SUB),
        grid_spec=pltpu.PrefetchScalarGridSpec(num_scalar_prefetch=2,grid=(1,),
        in_specs=[pl.BlockSpec((parts,heads*HD,rows),lambda i,*_:(0,go_first,0),pipeline_mode=pl.Buffered(1)),at(ot,ot_first),at(lse,ot_first)]+[at(a,first) for a in (qt,ka,qn,kt,vn)]+[pl.BlockSpec(memory_space=pl.ANY)],
        out_specs=[pl.BlockSpec((parts,out,rows),lambda i,*_:(0,0,0),pipeline_mode=pl.Buffered(1)),pl.BlockSpec((D,out),lambda i,*_:(0,0)),pl.BlockSpec((out,128),lambda i,*_:(0,0))],
        scratch_shapes=[VM((heads,HD,L),bf),VM((heads,L,HD),bf),VM((heads,1,L),f32),VM((heads,HD,L),f32),VM((heads,HD,L),bf),VM((heads,HD,L),bf),VM((heads,BK,HD),f32),VM((heads,BK,HD),f32),VM(x.shape,bf),pltpu.SemaphoreType.DMA]),
        out_shape=[S((parts,out,rows),bf),S((D,out),bf),S((out,128),f32)],
        compiler_params=pltpu.CompilerParams(vmem_limit_bytes=60<<20),
        cost_estimate=pl.CostEstimate(flops=2*L*L*HD*5*heads,bytes_accessed=L*heads*HD*2*14,transcendentals=L*L*heads),
        name="attend_backward")(lo,hi,go,ot,lse,qt,ka,qn,kt,vn,x)


def ranges(seg,BQ,BK):
    first=seg.reshape(-1,BQ)[:,0]; last=seg.reshape(-1,BQ)[:,-1]
    kf=seg.reshape(-1,BK)[:,0]; kl=seg.reshape(-1,BK)[:,-1]
    lo=jnp.sum((kl[None,:]<first[:,None]).astype(jnp.int32),1)
    hi=jnp.sum((kf[None,:]<=last[:,None]).astype(jnp.int32),1)
    return lo,hi


def dot_right_t(left, right):
    return lax.dot_general(
        left, right, (((1,), (1,)), ((), ())), preferred_element_type=jnp.float32
    )


def layer_norm(values_in, gain, shift):
    mean_row = jnp.mean(values_in, -1, keepdims=True)
    centered = values_in - mean_row
    inverse = lax.rsqrt(jnp.mean(centered * centered, -1, keepdims=True) + EPS)
    normed = centered * inverse
    return (normed * gain + shift, normed, inverse)


def norm_back(grad_in, normed, inverse, gain):
    scaled = grad_in * gain
    return inverse * (
        scaled
        - jnp.mean(scaled, -1, keepdims=True)
        - normed * jnp.mean(scaled * normed, -1, keepdims=True)
    )


MESH = pl.DeviceIdType.MESH


def flip(index, bit):
    span = 1 << bit
    return index + span * (1 - 2 * ((index // span) % 2))


def start_body(n, bits, x_ref, w_ref, s_ref, x_out, w_out, s_out, send_z, recv_z, send_d, recv_d, keep_sem):
    me = lax.axis_index("tensor")
    mine = lax.axis_index("dp")
    barrier = pltpu.get_barrier_semaphore()

    @pl.when(me > 0)
    def _():
        pl.semaphore_signal(barrier, inc=1, device_id={"tensor": me - 1}, device_id_type=MESH)

    @pl.when(me < n - 1)
    def _():
        pl.semaphore_signal(barrier, inc=1, device_id={"tensor": me + 1}, device_id_type=MESH)

    for bit in range(bits):
        pl.semaphore_signal(barrier, inc=1, device_id={"dp": flip(mine, bit)}, device_id_type=MESH)
    pl.semaphore_wait(barrier, bits + jnp.where(me > 0, 1, 0) + jnp.where(me < n - 1, 1, 0))

    keeps = [
        pltpu.make_async_copy(x_ref, x_out.at[me], keep_sem.at[0]),
        pltpu.make_async_copy(w_ref, w_out.at[me, mine], keep_sem.at[1]),
        pltpu.make_async_copy(s_ref, s_out.at[me], keep_sem.at[2]),
    ]
    for keep in keeps:
        keep.start()

    def hop(kind, side, step):
        block = me - (step - 1) if side else me + (step - 1)
        first, place = (
            (x_ref, x_out.at[block]),
            (w_ref, w_out.at[block, mine]),
            (s_ref, s_out.at[block]),
        )[kind]
        return pltpu.make_async_remote_copy(
            src_ref=first if step == 1 else place,
            dst_ref=place,
            send_sem=send_z.at[kind, side, step - 1],
            recv_sem=recv_z.at[kind, side, step - 1],
            device_id={"tensor": me + 1 if side else me - 1},
            device_id_type=MESH,
        )

    def sends(side, step):
        if side:
            return (me < n - 1) & (me >= step - 1)
        return (me > 0) & (me + step - 1 <= n - 1)

    def receives(side, step):
        return me >= step if side else me + step <= n - 1

    def z_start(kinds, step):
        for side in (0, 1):

            @pl.when(sends(side, step))
            def _():
                for kind in kinds:
                    hop(kind, side, step).start()

    def z_arrive(kinds, step):
        for side in (0, 1):

            @pl.when(receives(side, step))
            def _():
                for kind in kinds:
                    hop(kind, side, step).wait_recv()

    half = w_ref.shape[1] // 2
    up = list(range(bits - 1, -1, -1))
    orders = (up, [up[1], up[0]] + up[2:] if bits > 1 else up)

    def doubling(side, step):
        order = orders[side]
        held = [mine]
        for bit in order[:step]:
            held = held + [flip(d, bit) for d in held]
        cut = pl.ds(side * half, half)
        return [
            pltpu.make_async_remote_copy(
                src_ref=w_out.at[:, d, :, cut],
                dst_ref=w_out.at[:, d, :, cut],
                send_sem=send_d.at[side, (1 << step) - 1 + at],
                recv_sem=recv_d.at[side, (1 << step) - 1 + at],
                device_id={"dp": flip(mine, order[step])},
                device_id_type=MESH,
            )
            for at, d in enumerate(held)
        ]

    def d_start(step):
        for side in (0, 1):
            for copy in doubling(side, step):
                copy.start()

    def d_arrive(step):
        for side in (0, 1):
            for copy in doubling(side, step):
                copy.wait_recv()

    for step in range(1, n):
        z_start((1, 2), step)
        z_arrive((1, 2), step)
    keeps[1].wait()
    for step in range(max(n - 1, bits)):
        if step < bits:
            if step:
                d_arrive(step - 1)
            d_start(step)
        if step < n - 1:
            if step:
                z_arrive((0,), step)
            z_start((0,), step + 1)
    z_arrive((0,), n - 1)
    d_arrive(bits - 1)
    for side in (0, 1):
        for step in range(1, n):

            @pl.when(sends(side, step))
            def _():
                for kind in (0, 1, 2):
                    hop(kind, side, step).wait_send()

        for step in range(bits):
            for copy in doubling(side, step):
                copy.wait_send()
    keeps[0].wait()
    keeps[2].wait()


def start(x, w, small):
    n = lax.axis_size("tensor")
    groups = lax.axis_size("dp")
    bits = groups.bit_length() - 1
    S = jax.ShapeDtypeStruct
    anywhere = pl.BlockSpec(memory_space=pl.ANY)
    return pl.pallas_call(
        functools.partial(start_body, n, bits),
        in_specs=[pl.BlockSpec(memory_space=pltpu.VMEM)] * 3,
        out_specs=[anywhere] * 3,
        out_shape=[
            S((n,) + x.shape, x.dtype),
            S((n, groups) + w.shape, w.dtype),
            S((n,) + small.shape, small.dtype),
        ],
        scratch_shapes=[
            pltpu.SemaphoreType.DMA((3, 2, n - 1)),
            pltpu.SemaphoreType.DMA((3, 2, n - 1)),
            pltpu.SemaphoreType.DMA((2, groups - 1)),
            pltpu.SemaphoreType.DMA((2, groups - 1)),
            pltpu.SemaphoreType.DMA((3,)),
        ],
        compiler_params=pltpu.CompilerParams(collective_id=0, has_side_effects=True),
        cost_estimate=pl.CostEstimate(flops=0, bytes_accessed=200 << 20, transcendentals=0),
        name="start",
    )(x, w, small)


def weight_grads_body(parts, first_ref, second_ref, attn_ref, inner_ref, active_ref, context_ref, out_ref, ft, st):
    j = pl.program_id(0)

    @pl.when(j == 0)
    def _():
        ft[...] = first_ref[...].T
        st[...] = second_ref[...].T

    @pl.when((j < 2 * parts) & (j % 2 == 0))
    def _():
        out_ref[...] = dot(ft[...], inner_ref[0]).astype(out_ref.dtype)

    @pl.when((j < 2 * parts) & (j % 2 == 1))
    def _():
        out_ref[...] = dot(st[...], active_ref[0]).astype(out_ref.dtype)

    @pl.when(j == 2 * parts)
    def _():
        out_ref[...] = dot_right_t(attn_ref[...].T, context_ref[...]).astype(out_ref.dtype)


def weight_grads_of(first_low, second_low, attn_low, grad_inner, active, context):
    parts, rows, units = active.shape
    width = first_low.shape[1]
    features = context.shape[0]
    fixed = pl.BlockSpec((rows, width), lambda j: (0, 0))
    moving = lambda shift: pl.BlockSpec((1, rows, units), lambda j: (jnp.clip((j - shift) // 2, 0, parts - 1), 0, 0))
    return pl.pallas_call(
        functools.partial(weight_grads_body, parts),
        grid=(2 * parts + 1,),
        in_specs=[fixed, fixed, fixed, moving(0), moving(1), pl.BlockSpec((features, rows), lambda j: (0, 0))],
        out_specs=pl.BlockSpec((width, units), lambda j: (0, j)),
        out_shape=jax.ShapeDtypeStruct((width, units * 2 * parts + features), jnp.bfloat16),
        scratch_shapes=[VM((width, rows), jnp.bfloat16), VM((width, rows), jnp.bfloat16)],
        compiler_params=pltpu.CompilerParams(vmem_limit_bytes=40 << 20),
        cost_estimate=pl.CostEstimate(flops=2 * rows * width * (2 * parts * units + features), bytes_accessed=rows * units * 2 * parts * 4, transcendentals=0),
        name="weight_grads",
    )(first_low, second_low, attn_low, grad_inner, active, context)


def erf(x):
    x = jnp.clip(x, -3.7439211627767994, 3.7439211627767994)
    y = x * x
    top = jnp.float32(0.00022905065861350646)
    for c in (0.0034082910107109506, 0.050955695062380861, 0.18520832239976145, 1.128379143519084):
        top = top * y + c
    low = jnp.float32(-1.1791602954361697e-7)
    for c in (0.000023547966471313185, 0.0010179625278914885, 0.014070470171167667, 0.11098505178285362, 0.49746925110067538, 1.0):
        low = low * y + c
    return x * top / low


def dense_body(own, x_ref, cot_ref, ctx0_ref, ctx1_ref, vec_ref, bias_ref, rest_ref, out_ref, first_ref, second_ref, attn_ref, grad_ref, active_ref, inner_ref, ctx_ref, go0_ref, go1_ref, sum_ref, w_s, mt_s, slope_s, first_s, acc_s, w_sem):
    i = pl.program_id(0)
    parts, _, _ = rest_ref.shape
    f32, bf = jnp.float32, jnp.bfloat16
    units = active_ref.shape[2]
    cuts = (slice(0, 4 * own), slice(4 * own, 4 * own + units), slice(4 * own + units, 4 * own + 2 * units))
    copies = [pltpu.make_async_copy(rest_ref.at[:, :, cut], w_s.at[:, :, cut], w_sem.at[c]) for c, cut in enumerate(cuts)]

    @pl.when(i == 0)
    def _():
        for copy in copies:
            copy.start()
        sum_ref[...] = jnp.zeros(sum_ref.shape, f32)
        copies[0].wait()
        for t in range(parts):
            mt_s[:, t * own : (t + 1) * own] = w_s[t, :, 3 * own : 4 * own]

    def add_sum(row, value):
        sum_ref[row : row + 1, :] += jnp.sum(value, axis=0, keepdims=True)

    for t in range(parts):
        lead = ctx0_ref.shape[1]
        ctx_ref[t * own : t * own + lead, :] = ctx0_ref[t]
        ctx_ref[t * own + lead : (t + 1) * own, :] = ctx1_ref[t]
    mixed = dot(mt_s[...], ctx_ref[...]).T
    attn_in = x_ref[...].astype(f32) + mixed + vec_ref[0:1]
    first, first_norm, first_inv = layer_norm(attn_in, vec_ref[1:2], vec_ref[2:3])
    first_ref[...] = first.astype(bf)
    first_s[...] = first_norm
    acc_s[...] = first + vec_ref[3:4]

    @pl.when(i == 0)
    def _():
        copies[1].wait()
        copies[2].wait()

    def ahead(t, _):
        inner = dot(first_ref[...], w_s[t, :, cuts[1]]) + bias_ref[t]
        half = 0.5 * (1.0 + erf(inner * ROOT_HALF))
        slope_s[t] = half + inner * jnp.exp(-0.5 * inner * inner) * INV_ROOT_TWO_PI
        active_ref[t] = (inner * half).astype(bf)
        acc_s[...] += dot_right_t(active_ref[t], w_s[t, :, cuts[2]])
        return 0

    lax.fori_loop(0, parts, ahead, 0)
    second, second_norm, second_inv = layer_norm(acc_s[...], vec_ref[4:5], vec_ref[5:6])
    out_ref[...] = second.astype(bf)
    grad_out = cot_ref[...].astype(f32)
    add_sum(4, grad_out * second_norm)
    add_sum(5, grad_out)
    grad_second = norm_back(grad_out, second_norm, second_inv, vec_ref[4:5])
    add_sum(3, grad_second)
    second_ref[...] = grad_second.astype(bf)
    acc_s[...] = grad_second

    def back(t, _):
        grad_inner = (dot(second_ref[...], w_s[t, :, cuts[2]]) * slope_s[t]).astype(bf)
        inner_ref[t] = grad_inner
        sum_ref[pl.ds(6 + t, 1), :] += jnp.sum(grad_inner.astype(f32), axis=0, keepdims=True)
        acc_s[...] += dot_right_t(grad_inner, w_s[t, :, cuts[1]])
        return 0

    lax.fori_loop(0, parts, back, 0)
    grad_first = acc_s[...]
    first_norm = first_s[...]
    add_sum(1, grad_first * first_norm)
    add_sum(2, grad_first)
    grad_attn = norm_back(grad_first, first_norm, first_inv, vec_ref[1:2])
    add_sum(0, grad_attn)
    grad_ref[...] = grad_attn
    attn_ref[...] = grad_attn.astype(bf)
    grad_context = dot(attn_ref[...], mt_s[...]).T.astype(bf)
    for t in range(parts):
        go0_ref[t] = grad_context[t * own : t * own + HD]
        go1_ref[t] = grad_context[t * own + HD : (t + 1) * own]


def dense(own, x, cot, ctx0, ctx1, vectors, inner_bias, rest, block=384):
    rows, width = x.shape
    parts, _, cols = rest.shape
    units = (cols - 4 * own) // 2
    f32, bf = jnp.float32, jnp.bfloat16
    S = jax.ShapeDtypeStruct
    tok = pl.BlockSpec((block, width), lambda i: (i, 0))
    part_tok = pl.BlockSpec((parts, block, units), lambda i: (0, i, 0))
    lanes = lambda n: pl.BlockSpec((parts, n, block), lambda i: (0, 0, i))
    fixed = lambda a: pl.BlockSpec(a.shape, lambda i: (0,) * a.ndim)
    inner_bias = inner_bias.reshape(parts, 1, units)
    return pl.pallas_call(
        functools.partial(dense_body, own),
        grid=(rows // block,),
        in_specs=[tok, tok, lanes(ctx0.shape[1]), lanes(ctx1.shape[1]), fixed(vectors), fixed(inner_bias), pl.BlockSpec(memory_space=pl.ANY)],
        out_specs=[tok] * 5 + [part_tok] * 2 + [pl.BlockSpec((parts * own, block), lambda i: (0, i)), lanes(HD), lanes(own - HD), pl.BlockSpec((16, width), lambda i: (0, 0))],
        out_shape=[S((rows, width), bf)] * 4 + [S((rows, width), f32)] + [S((parts, rows, units), bf)] * 2 + [S((parts * own, rows), bf), S((parts, HD, rows), bf), S((parts, own - HD, rows), bf), S((16, width), f32)],
        scratch_shapes=[VM((parts, width, cols), bf), VM((width, parts * own), bf), VM((parts, block, units), f32), VM((block, width), f32), VM((block, width), f32), pltpu.SemaphoreType.DMA((3,))],
        compiler_params=pltpu.CompilerParams(vmem_limit_bytes=62 << 20),
        cost_estimate=pl.CostEstimate(flops=4 * rows * width * (2 * parts * units + parts * own), bytes_accessed=40 << 20, transcendentals=rows * units * parts),
        name="dense",
    )(x, cot, ctx0, ctx1, vectors, inner_bias, rest)


def early_back_body(w_ref, b0_ref, b1_ref, acc_ref):
    width = b0_ref.shape[1]
    total = jnp.zeros(acc_ref.shape, jnp.float32)
    for t in range(b0_ref.shape[0]):
        total = total + dot(w_ref[t, :, : 2 * width], jnp.concatenate([b0_ref[t], b1_ref[t]], axis=0))
    acc_ref[...] = total


def late_back_body(cut, part_ref, w_ref, acc_ref, grad_ref, *rest):
    backs, out_ref = rest[:-1], rest[-1]
    parts = len(backs)
    total = acc_ref[...]
    for d in range(parts):
        total = total + dot(w_ref[(part_ref[0] + parts - d) % parts, :, cut : cut + backs[d].shape[0]], backs[d][...])
    out_ref[...] = (total.T + grad_ref[...]).astype(out_ref.dtype)


def weight_block(rest, cols):
    return pl.BlockSpec(rest.shape[:2] + (cols,), lambda i, *_: (0, 0, 0), pipeline_mode=pl.Buffered(1))


def whole(a):
    return pl.BlockSpec(a.shape, lambda i, *_: (0,) * a.ndim, pipeline_mode=pl.Buffered(1))


def early_back(rest, cols, b0, b1):
    width, rows = rest.shape[1], b0.shape[2]
    return pl.pallas_call(
        early_back_body,
        grid=(1,),
        in_specs=[weight_block(rest, cols), whole(b0), whole(b1)],
        out_specs=pl.BlockSpec((width, rows), lambda i: (0, 0)),
        out_shape=jax.ShapeDtypeStruct((width, rows), jnp.float32),
        compiler_params=pltpu.CompilerParams(vmem_limit_bytes=40 << 20),
        cost_estimate=pl.CostEstimate(flops=4 * width * rows * b0.shape[0] * b0.shape[1], bytes_accessed=10 << 20, transcendentals=0),
        name="early_back",
    )(rest, b0, b1)


def late_back(rest, cols, cut, part, acc, grad, backs):
    rows, width = grad.shape
    return pl.pallas_call(
        functools.partial(late_back_body, cut),
        grid_spec=pltpu.PrefetchScalarGridSpec(
            num_scalar_prefetch=1,
            grid=(1,),
            in_specs=[weight_block(rest, cols), whole(acc), whole(grad)] + [whole(b) for b in backs],
            out_specs=pl.BlockSpec((rows, width), lambda i, *_: (0, 0)),
        ),
        out_shape=jax.ShapeDtypeStruct((rows, width), jnp.bfloat16),
        compiler_params=pltpu.CompilerParams(vmem_limit_bytes=40 << 20),
        cost_estimate=pl.CostEstimate(flops=2 * width * rows * backs[0].shape[0] * len(backs), bytes_accessed=10 << 20, transcendentals=0),
        name="late_back",
    )(part.reshape(1), rest, acc, grad, *backs)


def add_up(value):
    for axis in ("dp", "tensor"):
        size = lax.axis_size(axis)
        span = 1
        while span < size:
            other = lax.ppermute(value, axis, [(i, i ^ span) for i in range(size)])
            value = value + other
            span *= 2
    return value


def rotate(blocks, axis):
    size = lax.axis_size(axis)
    me = lax.axis_index(axis)
    out = []
    for d in range(size):
        block = lax.dynamic_index_in_dim(blocks, (me + d) % size, 0, keepdims=False)
        if d:
            block = lax.ppermute(block, axis, [(i, (i + d) % size) for i in range(size)])
        out.append(block)
    return out


def body(hidden_in, segments, query_weight, key_weight, value_weight, query_bias, value_bias, mixer_weight, mixer_bias, first_gain, first_shift, inner_weight, inner_bias, outer_weight, outer_bias, second_gain, second_shift, cotangent):
    bf = jnp.bfloat16
    f32 = jnp.float32
    _, rows, width = hidden_in.shape
    parts = lax.axis_size("tensor")
    groups = lax.axis_size("dp")
    rank = lax.axis_index("tensor")
    own = query_weight.shape[1]
    heads = own // HD
    three = 3 * HD
    units = inner_weight.shape[1]
    by_head = lambda q, k, v: jnp.stack([a.reshape(a.shape[:-1] + (heads, HD)) for a in (q, k, v)], -2).reshape(q.shape[:-1] + (3 * own,))
    x_own = hidden_in[0]
    qkv_own = by_head(query_weight, key_weight, value_weight)
    small = jnp.concatenate([segments[0].astype(f32), inner_bias]).reshape(-1, 128)
    rest_own = jnp.concatenate([qkv_own, mixer_weight.T, inner_weight, outer_weight.T], 1)
    x_parts, rest, small = start(x_own, rest_own, small)
    x_all = x_parts.reshape(parts * rows, width)
    rest = rest.reshape(parts, width, rest_own.shape[1])
    small = small.reshape(parts, -1)
    segment_all = small[:, :rows].astype(jnp.int32).reshape(-1)
    inner_bias_all = small[:, rows:]
    biases = by_head(query_bias, jnp.zeros_like(query_bias), value_bias)

    qt, ka, vt, qn, kt, vn = project(x_all, rest, rank, biases, segment_all)
    lo, hi = ranges(segment_all, 384, 512)
    lead = heads - 1
    context_t, lse, exchanged = [], [], []
    for call, (first, count) in enumerate(((0, lead), (lead, 1))):
        part, out_t, out_lse = attend_forward(first, count, parts, qt, ka, vt, lo, hi)
        context_t.append(out_t)
        lse.append(out_lse)
        if exchanged:
            part, exchanged[-1] = lax.optimization_barrier((part, exchanged[-1]))
        exchanged.append(lax.all_to_all(part, "tensor", 0, 0, tiled=True))
    vectors = jnp.stack([mixer_bias, first_gain, first_shift, outer_bias, second_gain, second_shift])
    vectors = jnp.pad(vectors, ((0, 2), (0, 0)))
    layer_out, first_low, second_low, attn_low, grad_attn, active, grad_inner, context, go0, go1, early = dense(
        own, x_own, cotangent[0], exchanged[0], exchanged[1], vectors, inner_bias_all, rest, block=rows
    )
    go0 = lax.all_to_all(go0, "tensor", 0, 0, tiled=True)
    go1 = lax.all_to_all(go1, "tensor", 0, 0, tiled=True)
    weight_grads = weight_grads_of(
        first_low, second_low, attn_low, grad_inner, active, context
    )
    weight_grads = lax.psum_scatter(weight_grads, "dp", scatter_dimension=0, tiled=True)
    weight_grads = jnp.concatenate(
        [
            weight_grads[:, : 2 * units * parts].reshape(-1, parts, 2 * units),
            weight_grads[:, 2 * units * parts :].reshape(-1, parts, own),
        ],
        2,
    ).transpose(1, 0, 2)
    weight_grads = rotate(weight_grads, "tensor")
    weight_grads = sum(a.astype(f32) for a in weight_grads)
    early = add_up(early)

    lo, hi = ranges(segment_all, 512, 512)
    backs, qkv_grad, bias_grad = [], [], []
    for h in range(heads):
        call = 0 if h < lead else 1
        grads, weight_part, sums = attend_backward(
            h, 1, go1 if h else go0, h - 1 if h else 0, context_t[call], lse[call], h - call * lead, qt, ka, qn, kt, vn, x_parts, lo, hi
        )
        if h < heads - 1:
            backs.append(lax.all_to_all(grads, "tensor", 0, 0, tiled=True))
        else:
            backs.append(rotate(grads, "tensor"))
        qkv_grad.append(weight_part)
        bias_grad.append(sums[:, 0])
    input_back = early_back(rest, 4 * own, backs[0], backs[1])
    input_grad = late_back(rest, 4 * own, 2 * three, rank, input_back, grad_attn, backs[2])
    bias_grad = jnp.concatenate(bias_grad)
    high = bias_grad.astype(bf)
    low = (bias_grad - high.astype(f32)).astype(bf)
    each = width // groups
    qkv_grad = jnp.concatenate(qkv_grad, 1).reshape(groups, each, 3 * own)
    extra = jnp.pad(jnp.stack([high, low]), ((0, 14), (0, 0)))
    extra = jnp.broadcast_to(extra[None], (groups, 16, 3 * own))
    qkv_grad = lax.all_to_all(jnp.concatenate([qkv_grad, extra], 1), "dp", 0, 0, tiled=True)
    qkv_grad = jnp.sum(qkv_grad.astype(f32), 0)
    bias_grad = qkv_grad[each] + qkv_grad[each + 1]
    pick = lambda a, n: a.reshape(a.shape[:-1] + (heads, 3, HD))[..., n, :].reshape(a.shape[:-1] + (own,))
    inner_bias_out = lax.dynamic_index_in_dim(early, 6 + rank, 0, keepdims=False)
    return (
        layer_out[None],
        input_grad[None],
        pick(qkv_grad[:each], 0),
        pick(qkv_grad[:each], 1),
        pick(qkv_grad[:each], 2),
        pick(bias_grad, 0),
        pick(bias_grad, 2),
        weight_grads[:, 2 * units :].T,
        early[0],
        early[1],
        early[2],
        weight_grads[:, :units],
        inner_bias_out,
        weight_grads[:, units : 2 * units].T,
        early[3],
        early[4],
        early[5],
    )


def solution(mesh):
    placed = (
        P("dp", "tensor", None),
        P("dp", "tensor"),
        P("dp", "tensor"),
        P("dp", "tensor"),
        P("dp", "tensor"),
        P("tensor"),
        P("tensor"),
        P("tensor", "dp"),
        P(),
        P(),
        P(),
        P("dp", "tensor"),
        P("tensor"),
        P("tensor", "dp"),
        P(),
        P(),
        P(),
        P("dp", "tensor", None),
    )

    return jax.shard_map(
        body,
        mesh=mesh,
        in_specs=placed,
        out_specs=(
            P("dp", "tensor", None),
            P("dp", "tensor", None),
            P("dp", "tensor"),
            P("dp", "tensor"),
            P("dp", "tensor"),
            P("tensor"),
            P("tensor"),
            P("tensor", "dp"),
            P(),
            P(),
            P(),
            P("dp", "tensor"),
            P("tensor"),
            P("tensor", "dp"),
            P(),
            P(),
            P(),
        ),
        check_vma=False,
    )
```

```python
import functools

import jax
import jax.numpy as jnp
from jax import lax
from jax.experimental import pallas as pl
from jax.experimental.pallas import tpu as pltpu
from jax.sharding import PartitionSpec as P


EPS = 1e-12
ROOT_HALF = 0.7071067811865476
INV_ROOT_TWO_PI = 0.3989422804014327
HD=64; SCALE=0.125; APART=-1e30
VM=pltpu.VMEM


def dot(a,b): return jnp.dot(a,b,preferred_element_type=jnp.float32)


def project_body(heads, part_ref, x_ref, w_ref, b_ref, scol_ref, srow_ref, qt_ref, ka_ref, vt_ref, qn_ref, kt_ref, vn_ref):
    y = dot(x_ref[...], w_ref[0,:,:b_ref.shape[1]]) + b_ref[...]
    low = y.astype(jnp.bfloat16)
    yt = y.T.astype(jnp.bfloat16)
    rows = y.shape[0]
    apart = jnp.where(lax.broadcasted_iota(jnp.int32,(HD,rows),0)==srow_ref[...],0.0,APART).astype(jnp.bfloat16)
    same = (lax.broadcasted_iota(jnp.int32,(rows,HD),1)==scol_ref[...]).astype(jnp.float32).astype(jnp.bfloat16)
    for h in range(heads):
        at=3*h*HD
        qt_ref[h,:HD,:]=yt[at:at+HD]*jnp.bfloat16(SCALE)
        qt_ref[h,HD:,:]=apart
        qn_ref[h]=low[:,at:at+HD]*jnp.bfloat16(SCALE)
        ka_ref[h]=jnp.concatenate([low[:,at+HD:at+2*HD],same],axis=1)
        kt_ref[h]=yt[at+HD:at+2*HD]
        vt_ref[h]=yt[at+2*HD:at+3*HD]
        vn_ref[h]=low[:,at+2*HD:at+3*HD]


def project(x,rest,part,b,seg,rows=512):
    L,D=x.shape; heads=b.shape[0]//(3*HD)
    bf=jnp.bfloat16
    cols=4*heads*HD
    nat=lambda n: pl.BlockSpec((heads,rows,n),lambda i,*_:(0,i,0))
    tr=lambda n: pl.BlockSpec((heads,n,rows),lambda i,*_:(0,0,i))
    S=jax.ShapeDtypeStruct
    return pl.pallas_call(functools.partial(project_body,heads),
        grid_spec=pltpu.PrefetchScalarGridSpec(num_scalar_prefetch=1,grid=(L//rows,),
        in_specs=[pl.BlockSpec((rows,D),lambda i,*_:(i,0)),pl.BlockSpec((1,D,cols),lambda i,p:(p[0],0,0)),pl.BlockSpec((1,b.shape[0]),lambda i,*_:(0,0)),
                  pl.BlockSpec((rows,1),lambda i,*_:(i,0)),pl.BlockSpec((1,rows),lambda i,*_:(0,i))],
        out_specs=[tr(2*HD),nat(2*HD),tr(HD),nat(HD),tr(HD),nat(HD)]),
        out_shape=[S((heads,2*HD,L),bf),S((heads,L,2*HD),bf),S((heads,HD,L),bf),S((heads,L,HD),bf),S((heads,HD,L),bf),S((heads,L,HD),bf)],
        compiler_params=pltpu.CompilerParams(vmem_limit_bytes=62 << 20),
        cost_estimate=pl.CostEstimate(flops=2*L*D*b.shape[0],bytes_accessed=L*D*2+D*cols*2+L*heads*HD*2*10,transcendentals=0),
        name="project")(part.reshape(1),x,rest,b.reshape(1,-1),seg.reshape(-1,1),seg.reshape(1,-1))


def forward_body(BK, SUB, lo_ref, hi_ref, qt_ref, ka_ref, vt_ref, ctx_ref, ot_ref, lse_ref, m_s, l_s, acc):
    i=pl.program_id(0)
    heads,_,BQ=qt_ref.shape
    chains=[(h,slice(c*SUB,(c+1)*SUB)) for h in range(heads) for c in range(BQ//SUB)]
    m_s[...]=jnp.full(m_s.shape,-jnp.inf,jnp.float32)
    l_s[...]=jnp.zeros(l_s.shape,jnp.float32)
    acc[...]=jnp.zeros(acc.shape,jnp.float32)

    def step(j,_):
        at=pl.multiple_of(j*BK,BK)
        for h,cut in chains:
            s=dot(ka_ref[h,pl.ds(at,BK),:],qt_ref[h,:,cut])
            m_old=m_s[h,:,cut]
            m_new=jnp.maximum(m_old,jnp.max(s,axis=0,keepdims=True))
            p=jnp.exp(s-m_new)
            alpha=jnp.exp(m_old-m_new)
            m_s[h,:,cut]=m_new
            l_s[h,:,cut]=l_s[h,:,cut]*alpha+jnp.sum(p,axis=0,keepdims=True)
            acc[h,:,cut]=acc[h,:,cut]*alpha+dot(vt_ref[h,:,pl.ds(at,BK)],p.astype(jnp.bfloat16))
        return 0

    lax.fori_loop(lo_ref[i],hi_ref[i],step,0)
    for h in range(heads):
        o=acc[h]/l_s[h]
        lse_ref[h]=m_s[h]+jnp.log(l_s[h])
        ot_ref[h]=o
        ctx_ref[0,h*HD:(h+1)*HD,:]=o.astype(jnp.bfloat16)


def attend_forward(first,heads,parts,qt,ka,vt,lo,hi,BQ=384,BK=512,SUB=384):
    L=qt.shape[2]
    S=jax.ShapeDtypeStruct
    per=L//parts//BQ
    return pl.pallas_call(functools.partial(forward_body,BK,SUB),
        grid_spec=pltpu.PrefetchScalarGridSpec(num_scalar_prefetch=2,grid=(L//BQ,),
        in_specs=[pl.BlockSpec((heads,2*HD,BQ),lambda i,*_:(first//heads,0,i)),pl.BlockSpec((heads,L,2*HD),lambda i,*_:(first//heads,0,0)),pl.BlockSpec((heads,HD,L),lambda i,*_:(first//heads,0,0))],
        out_specs=[pl.BlockSpec((1,heads*HD,BQ),lambda i,*_:(i//per,0,i%per)),pl.BlockSpec((heads,HD,BQ),lambda i,*_:(0,0,i)),pl.BlockSpec((heads,1,BQ),lambda i,*_:(0,0,i))],
        scratch_shapes=[VM((heads,1,BQ),jnp.float32),VM((heads,1,BQ),jnp.float32),VM((heads,HD,BQ),jnp.float32)]),
        out_shape=[S((parts,heads*HD,L//parts),jnp.bfloat16),S((heads,HD,L),jnp.float32),S((heads,1,L),jnp.float32)],
        compiler_params=pltpu.CompilerParams(vmem_limit_bytes=62 << 20),
        cost_estimate=pl.CostEstimate(flops=2*L*L*HD*2*heads,bytes_accessed=L*heads*HD*2*8,transcendentals=L*L*heads),
        name="attend_forward")(lo,hi,qt,ka,vt)


def backward_body(BQ, BK, SUB, lo_ref, hi_ref, go_ref, ot_ref, lse_ref, qt_ref, ka_ref, qn_ref, kt_ref, vn_ref, x_ref, out_ref, wg_ref, sum_ref, got, gon, delta, dqt, dkt, dvt, dk_s, dv_s, x_s, x_sem):
    bring=pltpu.make_async_copy(x_ref,x_s,x_sem)
    bring.start()
    parts,_,rows=go_ref.shape
    heads,_,L=qt_ref.shape
    CH=256
    for h in range(heads):
        for c in range(L//CH):
            p,at=c*CH//rows,c*CH%rows
            gt=go_ref[p,h*HD:(h+1)*HD,at:at+CH]
            wide=gt.astype(jnp.float32)
            got[h,:,c*CH:(c+1)*CH]=gt
            gon[h,c*CH:(c+1)*CH,:]=wide.T.astype(jnp.bfloat16)
            delta[h,:,c*CH:(c+1)*CH]=jnp.sum(wide*ot_ref[h,:,c*CH:(c+1)*CH],axis=0,keepdims=True)
    dqt[...]=jnp.zeros(dqt.shape,jnp.float32)

    def key_block(j,_):
        ka_at=pl.multiple_of(j*BK,BK)
        dk_s[...]=jnp.zeros(dk_s.shape,jnp.float32)
        dv_s[...]=jnp.zeros(dv_s.shape,jnp.float32)

        def query_block(i,_):
            for h,c in [(h,c) for h in range(heads) for c in range(BQ//SUB)]:
                at=pl.multiple_of(i*BQ+c*SUB,SUB)
                s=dot(ka_ref[h,pl.ds(ka_at,BK),:],qt_ref[h,:,pl.ds(at,SUB)])
                p=jnp.exp(s-lse_ref[h,:,pl.ds(at,SUB)])
                dp=dot(vn_ref[h,pl.ds(ka_at,BK),:],got[h,:,pl.ds(at,SUB)])
                ds=(p*(dp-delta[h,:,pl.ds(at,SUB)])).astype(jnp.bfloat16)
                dv_s[h]+=dot(p.astype(jnp.bfloat16),gon[h,pl.ds(at,SUB),:])
                dk_s[h]+=dot(ds,qn_ref[h,pl.ds(at,SUB),:])
                dqt[h,:,pl.ds(at,SUB)]+=dot(kt_ref[h,:,pl.ds(ka_at,BK)],ds)
            return 0

        lax.fori_loop(lo_ref[j],hi_ref[j],query_block,0)
        for h in range(heads):
            dkt[h,:,pl.ds(ka_at,BK)]=dk_s[h].T.astype(jnp.bfloat16)
            dvt[h,:,pl.ds(ka_at,BK)]=dv_s[h].T.astype(jnp.bfloat16)
        return 0

    lax.fori_loop(0,L//BK,key_block,0)
    for h in range(heads):
        for p in range(parts):
            cut=slice(p*rows,(p+1)*rows)
            out_ref[p,3*h*HD:(3*h+1)*HD,:]=(dqt[h,:,cut]*SCALE).astype(jnp.bfloat16)
            out_ref[p,(3*h+1)*HD:(3*h+2)*HD,:]=dkt[h,:,cut]
            out_ref[p,(3*h+2)*HD:(3*h+3)*HD,:]=dvt[h,:,cut]
    bring.wait()
    wg=jnp.zeros(wg_ref.shape[::-1],jnp.float32)
    total=jnp.zeros((3*heads*HD,1),jnp.float32)
    for p in range(parts):
        part=out_ref[p]
        wg=wg+dot(part,x_s[p])
        total=total+jnp.sum(part.astype(jnp.float32),axis=1,keepdims=True)
    wg_ref[...]=wg.T.astype(wg_ref.dtype)
    sum_ref[...]=jnp.broadcast_to(total,sum_ref.shape)


def attend_backward(first,heads,go,go_first,ot,lse,ot_first,qt,ka,qn,kt,vn,x,lo,hi,BQ=512,BK=512,SUB=512):
    parts,_,rows=go.shape; L=parts*rows; D=x.shape[2]
    S=jax.ShapeDtypeStruct; f32=jnp.float32; bf=jnp.bfloat16
    at=lambda a,n: pl.BlockSpec((heads,)+a.shape[1:],lambda i,*_:(n//heads,0,0),pipeline_mode=pl.Buffered(1))
    out=3*heads*HD
    return pl.pallas_call(functools.partial(backward_body,BQ,BK,SUB),
        grid_spec=pltpu.PrefetchScalarGridSpec(num_scalar_prefetch=2,grid=(1,),
        in_specs=[pl.BlockSpec((parts,heads*HD,rows),lambda i,*_:(0,go_first,0),pipeline_mode=pl.Buffered(1)),at(ot,ot_first),at(lse,ot_first)]+[at(a,first) for a in (qt,ka,qn,kt,vn)]+[pl.BlockSpec(memory_space=pl.ANY)],
        out_specs=[pl.BlockSpec((parts,out,rows),lambda i,*_:(0,0,0),pipeline_mode=pl.Buffered(1)),pl.BlockSpec((D,out),lambda i,*_:(0,0)),pl.BlockSpec((out,128),lambda i,*_:(0,0))],
        scratch_shapes=[VM((heads,HD,L),bf),VM((heads,L,HD),bf),VM((heads,1,L),f32),VM((heads,HD,L),f32),VM((heads,HD,L),bf),VM((heads,HD,L),bf),VM((heads,BK,HD),f32),VM((heads,BK,HD),f32),VM(x.shape,bf),pltpu.SemaphoreType.DMA]),
        out_shape=[S((parts,out,rows),bf),S((D,out),bf),S((out,128),f32)],
        compiler_params=pltpu.CompilerParams(vmem_limit_bytes=62 << 20),
        cost_estimate=pl.CostEstimate(flops=2*L*L*HD*5*heads,bytes_accessed=L*heads*HD*2*14,transcendentals=L*L*heads),
        name="attend_backward")(lo,hi,go,ot,lse,qt,ka,qn,kt,vn,x)


def ranges(seg,BQ,BK):
    first=seg.reshape(-1,BQ)[:,0]; last=seg.reshape(-1,BQ)[:,-1]
    kf=seg.reshape(-1,BK)[:,0]; kl=seg.reshape(-1,BK)[:,-1]
    lo=jnp.sum((kl[None,:]<first[:,None]).astype(jnp.int32),1)
    hi=jnp.sum((kf[None,:]<=last[:,None]).astype(jnp.int32),1)
    return lo,hi


def dot_right_t(left, right):
    return lax.dot_general(
        left, right, (((1,), (1,)), ((), ())), preferred_element_type=jnp.float32
    )


def layer_norm(values_in, gain, shift):
    mean_row = jnp.mean(values_in, -1, keepdims=True)
    centered = values_in - mean_row
    inverse = lax.rsqrt(jnp.mean(centered * centered, -1, keepdims=True) + EPS)
    normed = centered * inverse
    return (normed * gain + shift, normed, inverse)


def norm_back(grad_in, normed, inverse, gain):
    scaled = grad_in * gain
    return inverse * (
        scaled
        - jnp.mean(scaled, -1, keepdims=True)
        - normed * jnp.mean(scaled * normed, -1, keepdims=True)
    )


MESH = pl.DeviceIdType.MESH


def flip(index, bit):
    span = 1 << bit
    return index + span * (1 - 2 * ((index // span) % 2))


def start_body(n, bits, x_ref, w_ref, s_ref, x_out, w_out, s_out, send_z, recv_z, send_d, recv_d, keep_sem):
    me = lax.axis_index("tensor")
    mine = lax.axis_index("dp")
    barrier = pltpu.get_barrier_semaphore()

    @pl.when(me > 0)
    def _():
        pl.semaphore_signal(barrier, inc=1, device_id={"tensor": me - 1}, device_id_type=MESH)

    @pl.when(me < n - 1)
    def _():
        pl.semaphore_signal(barrier, inc=1, device_id={"tensor": me + 1}, device_id_type=MESH)

    for bit in range(bits):
        pl.semaphore_signal(barrier, inc=1, device_id={"dp": flip(mine, bit)}, device_id_type=MESH)
    pl.semaphore_wait(barrier, bits + jnp.where(me > 0, 1, 0) + jnp.where(me < n - 1, 1, 0))

    keeps = [
        pltpu.make_async_copy(x_ref, x_out.at[me], keep_sem.at[0]),
        pltpu.make_async_copy(w_ref, w_out.at[me, mine], keep_sem.at[1]),
        pltpu.make_async_copy(s_ref, s_out.at[me], keep_sem.at[2]),
    ]
    for keep in keeps:
        keep.start()

    def hop(kind, side, step):
        block = me - (step - 1) if side else me + (step - 1)
        first, place = (
            (x_ref, x_out.at[block]),
            (w_ref, w_out.at[block, mine]),
            (s_ref, s_out.at[block]),
        )[kind]
        return pltpu.make_async_remote_copy(
            src_ref=first if step == 1 else place,
            dst_ref=place,
            send_sem=send_z.at[kind, side, step - 1],
            recv_sem=recv_z.at[kind, side, step - 1],
            device_id={"tensor": me + 1 if side else me - 1},
            device_id_type=MESH,
        )

    def sends(side, step):
        if side:
            return (me < n - 1) & (me >= step - 1)
        return (me > 0) & (me + step - 1 <= n - 1)

    def receives(side, step):
        return me >= step if side else me + step <= n - 1

    def z_start(kinds, step):
        for side in (0, 1):

            @pl.when(sends(side, step))
            def _():
                for kind in kinds:
                    hop(kind, side, step).start()

    def z_arrive(kinds, step):
        for side in (0, 1):

            @pl.when(receives(side, step))
            def _():
                for kind in kinds:
                    hop(kind, side, step).wait_recv()

    half = w_ref.shape[1] // 2
    up = list(range(bits - 1, -1, -1))
    orders = (up, [up[1], up[0]] + up[2:] if bits > 1 else up)

    def doubling(side, step):
        order = orders[side]
        held = [mine]
        for bit in order[:step]:
            held = held + [flip(d, bit) for d in held]
        cut = pl.ds(side * half, half)
        return [
            pltpu.make_async_remote_copy(
                src_ref=w_out.at[:, d, :, cut],
                dst_ref=w_out.at[:, d, :, cut],
                send_sem=send_d.at[side, (1 << step) - 1 + at],
                recv_sem=recv_d.at[side, (1 << step) - 1 + at],
                device_id={"dp": flip(mine, order[step])},
                device_id_type=MESH,
            )
            for at, d in enumerate(held)
        ]

    def d_start(step):
        for side in (0, 1):
            for copy in doubling(side, step):
                copy.start()

    def d_arrive(step):
        for side in (0, 1):
            for copy in doubling(side, step):
                copy.wait_recv()

    for step in range(1, n):
        z_start((1, 2), step)
        z_arrive((1, 2), step)
    keeps[1].wait()
    for step in range(max(n - 1, bits)):
        if step < bits:
            if step:
                d_arrive(step - 1)
            d_start(step)
        if step < n - 1:
            if step:
                z_arrive((0,), step)
            z_start((0,), step + 1)
    z_arrive((0,), n - 1)
    d_arrive(bits - 1)
    for side in (0, 1):
        for step in range(1, n):

            @pl.when(sends(side, step))
            def _():
                for kind in (0, 1, 2):
                    hop(kind, side, step).wait_send()

        for step in range(bits):
            for copy in doubling(side, step):
                copy.wait_send()
    keeps[0].wait()
    keeps[2].wait()


def start(x, w, small):
    n = lax.axis_size("tensor")
    groups = lax.axis_size("dp")
    bits = groups.bit_length() - 1
    S = jax.ShapeDtypeStruct
    anywhere = pl.BlockSpec(memory_space=pl.ANY)
    return pl.pallas_call(
        functools.partial(start_body, n, bits),
        in_specs=[pl.BlockSpec(memory_space=pltpu.VMEM)] * 3,
        out_specs=[anywhere] * 3,
        out_shape=[
            S((n,) + x.shape, x.dtype),
            S((n, groups) + w.shape, w.dtype),
            S((n,) + small.shape, small.dtype),
        ],
        scratch_shapes=[
            pltpu.SemaphoreType.DMA((3, 2, n - 1)),
            pltpu.SemaphoreType.DMA((3, 2, n - 1)),
            pltpu.SemaphoreType.DMA((2, groups - 1)),
            pltpu.SemaphoreType.DMA((2, groups - 1)),
            pltpu.SemaphoreType.DMA((3,)),
        ],
        compiler_params=pltpu.CompilerParams(collective_id=0, has_side_effects=True),
        cost_estimate=pl.CostEstimate(flops=0, bytes_accessed=200 << 20, transcendentals=0),
        name="start",
    )(x, w, small)


def weight_grads_body(parts, first_ref, second_ref, attn_ref, inner_ref, active_ref, context_ref, out_ref, ft, st):
    j = pl.program_id(0)

    @pl.when(j == 0)
    def _():
        ft[...] = first_ref[...].T
        st[...] = second_ref[...].T

    @pl.when((j < 2 * parts) & (j % 2 == 0))
    def _():
        out_ref[...] = dot(ft[...], inner_ref[0]).astype(out_ref.dtype)

    @pl.when((j < 2 * parts) & (j % 2 == 1))
    def _():
        out_ref[...] = dot(st[...], active_ref[0]).astype(out_ref.dtype)

    @pl.when(j == 2 * parts)
    def _():
        out_ref[...] = dot_right_t(attn_ref[...].T, context_ref[...]).astype(out_ref.dtype)


def weight_grads_of(first_low, second_low, attn_low, grad_inner, active, context):
    parts, rows, units = active.shape
    width = first_low.shape[1]
    features = context.shape[0]
    fixed = pl.BlockSpec((rows, width), lambda j: (0, 0))
    moving = lambda shift: pl.BlockSpec((1, rows, units), lambda j: (jnp.clip((j - shift) // 2, 0, parts - 1), 0, 0))
    return pl.pallas_call(
        functools.partial(weight_grads_body, parts),
        grid=(2 * parts + 1,),
        in_specs=[fixed, fixed, fixed, moving(0), moving(1), pl.BlockSpec((features, rows), lambda j: (0, 0))],
        out_specs=pl.BlockSpec((width, units), lambda j: (0, j)),
        out_shape=jax.ShapeDtypeStruct((width, units * 2 * parts + features), jnp.bfloat16),
        scratch_shapes=[VM((width, rows), jnp.bfloat16), VM((width, rows), jnp.bfloat16)],
        compiler_params=pltpu.CompilerParams(vmem_limit_bytes=62 << 20),
        cost_estimate=pl.CostEstimate(flops=2 * rows * width * (2 * parts * units + features), bytes_accessed=rows * units * 2 * parts * 4, transcendentals=0),
        name="weight_grads",
    )(first_low, second_low, attn_low, grad_inner, active, context)


def erf(x):
    x = jnp.clip(x, -3.7439211627767994, 3.7439211627767994)
    y = x * x
    top = jnp.float32(0.00022905065861350646)
    for c in (0.0034082910107109506, 0.050955695062380861, 0.18520832239976145, 1.128379143519084):
        top = top * y + c
    low = jnp.float32(-1.1791602954361697e-7)
    for c in (0.000023547966471313185, 0.0010179625278914885, 0.014070470171167667, 0.11098505178285362, 0.49746925110067538, 1.0):
        low = low * y + c
    return x * top / low


def dense_body(own, x_ref, cot_ref, ctx0_ref, ctx1_ref, vec_ref, bias_ref, near_ref, far_ref, out_ref, first_ref, second_ref, attn_ref, grad_ref, active_ref, inner_ref, ctx_ref, go0_ref, go1_ref, sum_ref, w_s, mt_s, slope_s, first_s, acc_s, w_sem):
    i = pl.program_id(0)
    parts, _, _ = near_ref.shape
    f32, bf = jnp.float32, jnp.bfloat16
    units = active_ref.shape[2]
    cuts = (slice(0, 4 * own), slice(4 * own, 4 * own + units), slice(4 * own + units, 4 * own + 2 * units))
    sources = (near_ref, far_ref.at[:, :, :units], far_ref.at[:, :, units:])
    copies = [pltpu.make_async_copy(sources[c], w_s.at[:, :, cut], w_sem.at[c]) for c, cut in enumerate(cuts)]

    @pl.when(i == 0)
    def _():
        for copy in copies:
            copy.start()
        sum_ref[...] = jnp.zeros(sum_ref.shape, f32)
        copies[0].wait()
        for t in range(parts):
            mt_s[:, t * own : (t + 1) * own] = w_s[t, :, 3 * own : 4 * own]

    def add_sum(row, value):
        sum_ref[row : row + 1, :] += jnp.sum(value, axis=0, keepdims=True)

    for t in range(parts):
        lead = ctx0_ref.shape[1]
        ctx_ref[t * own : t * own + lead, :] = ctx0_ref[t]
        ctx_ref[t * own + lead : (t + 1) * own, :] = ctx1_ref[t]
    mixed = dot(mt_s[...], ctx_ref[...]).T
    attn_in = x_ref[...].astype(f32) + mixed + vec_ref[0:1]
    first, first_norm, first_inv = layer_norm(attn_in, vec_ref[1:2], vec_ref[2:3])
    first_ref[...] = first.astype(bf)
    first_s[...] = first_norm
    acc_s[...] = first + vec_ref[3:4]

    @pl.when(i == 0)
    def _():
        copies[1].wait()
        copies[2].wait()

    def ahead(t, _):
        inner = dot(first_ref[...], w_s[t, :, cuts[1]]) + bias_ref[t]
        half = 0.5 * (1.0 + erf(inner * ROOT_HALF))
        slope_s[t] = half + inner * jnp.exp(-0.5 * inner * inner) * INV_ROOT_TWO_PI
        active_ref[t] = (inner * half).astype(bf)
        acc_s[...] += dot_right_t(active_ref[t], w_s[t, :, cuts[2]])
        return 0

    lax.fori_loop(0, parts, ahead, 0)
    second, second_norm, second_inv = layer_norm(acc_s[...], vec_ref[4:5], vec_ref[5:6])
    out_ref[...] = second.astype(bf)
    grad_out = cot_ref[...].astype(f32)
    add_sum(4, grad_out * second_norm)
    add_sum(5, grad_out)
    grad_second = norm_back(grad_out, second_norm, second_inv, vec_ref[4:5])
    add_sum(3, grad_second)
    second_ref[...] = grad_second.astype(bf)
    acc_s[...] = grad_second

    def back(t, _):
        grad_inner = (dot(second_ref[...], w_s[t, :, cuts[2]]) * slope_s[t]).astype(bf)
        inner_ref[t] = grad_inner
        sum_ref[pl.ds(6 + t, 1), :] += jnp.sum(grad_inner.astype(f32), axis=0, keepdims=True)
        acc_s[...] += dot_right_t(grad_inner, w_s[t, :, cuts[1]])
        return 0

    lax.fori_loop(0, parts, back, 0)
    grad_first = acc_s[...]
    first_norm = first_s[...]
    add_sum(1, grad_first * first_norm)
    add_sum(2, grad_first)
    grad_attn = norm_back(grad_first, first_norm, first_inv, vec_ref[1:2])
    add_sum(0, grad_attn)
    grad_ref[...] = grad_attn
    attn_ref[...] = grad_attn.astype(bf)
    grad_context = dot(attn_ref[...], mt_s[...]).T.astype(bf)
    for t in range(parts):
        go0_ref[t] = grad_context[t * own : t * own + HD]
        go1_ref[t] = grad_context[t * own + HD : (t + 1) * own]


def dense(own, x, cot, ctx0, ctx1, vectors, inner_bias, near, far, block):
    rows, width = x.shape
    parts = near.shape[0]
    units = far.shape[2] // 2
    cols = 4 * own + 2 * units
    f32, bf = jnp.float32, jnp.bfloat16
    S = jax.ShapeDtypeStruct
    tok = pl.BlockSpec((block, width), lambda i: (i, 0))
    part_tok = pl.BlockSpec((parts, block, units), lambda i: (0, i, 0))
    lanes = lambda n: pl.BlockSpec((parts, n, block), lambda i: (0, 0, i))
    fixed = lambda a: pl.BlockSpec(a.shape, lambda i: (0,) * a.ndim)
    inner_bias = inner_bias.reshape(parts, 1, units)
    return pl.pallas_call(
        functools.partial(dense_body, own),
        grid=(rows // block,),
        in_specs=[tok, tok, lanes(ctx0.shape[1]), lanes(ctx1.shape[1]), fixed(vectors), fixed(inner_bias), pl.BlockSpec(memory_space=pl.ANY), pl.BlockSpec(memory_space=pl.ANY)],
        out_specs=[tok] * 5 + [part_tok] * 2 + [pl.BlockSpec((parts * own, block), lambda i: (0, i)), lanes(HD), lanes(own - HD), pl.BlockSpec((16, width), lambda i: (0, 0))],
        out_shape=[S((rows, width), bf)] * 4 + [S((rows, width), f32)] + [S((parts, rows, units), bf)] * 2 + [S((parts * own, rows), bf), S((parts, HD, rows), bf), S((parts, own - HD, rows), bf), S((16, width), f32)],
        scratch_shapes=[VM((parts, width, cols), bf), VM((width, parts * own), bf), VM((parts, block, units), f32), VM((block, width), f32), VM((block, width), f32), pltpu.SemaphoreType.DMA((3,))],
        compiler_params=pltpu.CompilerParams(vmem_limit_bytes=62 << 20),
        cost_estimate=pl.CostEstimate(flops=4 * rows * width * (2 * parts * units + parts * own), bytes_accessed=40 << 20, transcendentals=rows * units * parts),
        name="dense",
    )(x, cot, ctx0, ctx1, vectors, inner_bias, near, far)


def early_back_body(w_ref, b0_ref, b1_ref, acc_ref):
    width = b0_ref.shape[1]
    total = jnp.zeros(acc_ref.shape, jnp.float32)
    for t in range(b0_ref.shape[0]):
        total = total + dot(w_ref[t, :, : 2 * width], jnp.concatenate([b0_ref[t], b1_ref[t]], axis=0))
    acc_ref[...] = total


def late_back_body(cut, part_ref, w_ref, acc_ref, grad_ref, *rest):
    backs, out_ref = rest[:-1], rest[-1]
    parts = len(backs)
    total = acc_ref[...]
    for d in range(parts):
        total = total + dot(w_ref[(part_ref[0] + parts - d) % parts, :, cut : cut + backs[d].shape[0]], backs[d][...])
    out_ref[...] = (total.T + grad_ref[...]).astype(out_ref.dtype)


def weight_block(rest, cols):
    return pl.BlockSpec(rest.shape[:2] + (cols,), lambda i, *_: (0, 0, 0), pipeline_mode=pl.Buffered(1))


def whole(a):
    return pl.BlockSpec(a.shape, lambda i, *_: (0,) * a.ndim, pipeline_mode=pl.Buffered(1))


def early_back(rest, cols, b0, b1):
    width, rows = rest.shape[1], b0.shape[2]
    return pl.pallas_call(
        early_back_body,
        grid=(1,),
        in_specs=[weight_block(rest, cols), whole(b0), whole(b1)],
        out_specs=pl.BlockSpec((width, rows), lambda i: (0, 0)),
        out_shape=jax.ShapeDtypeStruct((width, rows), jnp.float32),
        compiler_params=pltpu.CompilerParams(vmem_limit_bytes=62 << 20),
        cost_estimate=pl.CostEstimate(flops=4 * width * rows * b0.shape[0] * b0.shape[1], bytes_accessed=10 << 20, transcendentals=0),
        name="early_back",
    )(rest, b0, b1)


def late_back(rest, cols, cut, part, acc, grad, backs):
    rows, width = grad.shape
    return pl.pallas_call(
        functools.partial(late_back_body, cut),
        grid_spec=pltpu.PrefetchScalarGridSpec(
            num_scalar_prefetch=1,
            grid=(1,),
            in_specs=[weight_block(rest, cols), whole(acc), whole(grad)] + [whole(b) for b in backs],
            out_specs=pl.BlockSpec((rows, width), lambda i, *_: (0, 0)),
        ),
        out_shape=jax.ShapeDtypeStruct((rows, width), jnp.bfloat16),
        compiler_params=pltpu.CompilerParams(vmem_limit_bytes=62 << 20),
        cost_estimate=pl.CostEstimate(flops=2 * width * rows * backs[0].shape[0] * len(backs), bytes_accessed=10 << 20, transcendentals=0),
        name="late_back",
    )(part.reshape(1), rest, acc, grad, *backs)


def add_up(value):
    for axis in ("dp", "tensor"):
        size = lax.axis_size(axis)
        span = 1
        while span < size:
            other = lax.ppermute(value, axis, [(i, i ^ span) for i in range(size)])
            value = value + other
            span *= 2
    return value


def rotate(blocks, axis):
    size = lax.axis_size(axis)
    me = lax.axis_index(axis)
    out = []
    for d in range(size):
        block = lax.dynamic_index_in_dim(blocks, (me + d) % size, 0, keepdims=False)
        if d:
            block = lax.ppermute(block, axis, [(i, (i + d) % size) for i in range(size)])
        out.append(block)
    return out


def body(hidden_in, segments, query_weight, key_weight, value_weight, query_bias, value_bias, mixer_weight, mixer_bias, first_gain, first_shift, inner_weight, inner_bias, outer_weight, outer_bias, second_gain, second_shift, cotangent):
    bf = jnp.bfloat16
    f32 = jnp.float32
    _, rows, width = hidden_in.shape
    parts = lax.axis_size("tensor")
    groups = lax.axis_size("dp")
    rank = lax.axis_index("tensor")
    own = query_weight.shape[1]
    heads = own // HD
    three = 3 * HD
    units = inner_weight.shape[1]
    by_head = lambda q, k, v: jnp.stack([a.reshape(a.shape[:-1] + (heads, HD)) for a in (q, k, v)], -2).reshape(q.shape[:-1] + (3 * own,))
    x_own = hidden_in[0]
    qkv_own = by_head(query_weight, key_weight, value_weight)
    small = jnp.concatenate([segments[0].astype(f32), inner_bias]).reshape(-1, 128)
    near_own = jnp.concatenate([qkv_own, mixer_weight.T], 1)
    x_parts, near, small = start(x_own, near_own, small)
    x_all = x_parts.reshape(parts * rows, width)
    near = near.reshape(parts, width, 4 * own)
    far_own = jnp.concatenate([inner_weight, outer_weight.T], 1)
    far_own, small = lax.optimization_barrier((far_own, small))
    far = lax.all_gather(far_own, ("tensor", "dp"), axis=0, tiled=True).reshape(parts, width, 2 * units)
    small = small.reshape(parts, -1)
    segment_all = small[:, :rows].astype(jnp.int32).reshape(-1)
    inner_bias_all = small[:, rows:]
    biases = by_head(query_bias, jnp.zeros_like(query_bias), value_bias)

    qt, ka, vt, qn, kt, vn = project(x_all, near, rank, biases, segment_all)
    lo, hi = ranges(segment_all, 384, 512)
    lead = heads - 1
    context_t, lse, exchanged = [], [], []
    for call, (first, count) in enumerate(((0, lead), (lead, 1))):
        part, out_t, out_lse = attend_forward(first, count, parts, qt, ka, vt, lo, hi)
        context_t.append(out_t)
        lse.append(out_lse)
        if exchanged:
            part, exchanged[-1] = lax.optimization_barrier((part, exchanged[-1]))
        exchanged.append(lax.all_to_all(part, "tensor", 0, 0, tiled=True))
    vectors = jnp.stack([mixer_bias, first_gain, first_shift, outer_bias, second_gain, second_shift])
    vectors = jnp.pad(vectors, ((0, 2), (0, 0)))
    layer_out, first_low, second_low, attn_low, grad_attn, active, grad_inner, context, go0, go1, early = dense(
        own, x_own, cotangent[0], exchanged[0], exchanged[1], vectors, inner_bias_all, near, far, block=rows
    )
    go0 = lax.all_to_all(go0, "tensor", 0, 0, tiled=True)
    go1 = lax.all_to_all(go1, "tensor", 0, 0, tiled=True)
    weight_grads = weight_grads_of(
        first_low, second_low, attn_low, grad_inner, active, context
    )
    weight_grads = lax.psum_scatter(weight_grads, "dp", scatter_dimension=0, tiled=True)
    weight_grads = jnp.concatenate(
        [
            weight_grads[:, : 2 * units * parts].reshape(-1, parts, 2 * units),
            weight_grads[:, 2 * units * parts :].reshape(-1, parts, own),
        ],
        2,
    ).transpose(1, 0, 2)
    weight_grads = rotate(weight_grads, "tensor")
    weight_grads = sum(a.astype(f32) for a in weight_grads)
    early = add_up(early)

    lo, hi = ranges(segment_all, 512, 512)
    backs, qkv_grad, bias_grad = [], [], []
    for h in range(heads):
        call = 0 if h < lead else 1
        grads, weight_part, sums = attend_backward(
            h, 1, go1 if h else go0, h - 1 if h else 0, context_t[call], lse[call], h - call * lead, qt, ka, qn, kt, vn, x_parts, lo, hi
        )
        if h < heads - 1:
            backs.append(lax.all_to_all(grads, "tensor", 0, 0, tiled=True))
        else:
            backs.append(rotate(grads, "tensor"))
        qkv_grad.append(weight_part)
        bias_grad.append(sums[:, 0])
    input_back = early_back(near, 4 * own, backs[0], backs[1])
    input_grad = late_back(near, 4 * own, 2 * three, rank, input_back, grad_attn, backs[2])
    bias_grad = jnp.concatenate(bias_grad)
    high = bias_grad.astype(bf)
    low = (bias_grad - high.astype(f32)).astype(bf)
    each = width // groups
    qkv_grad = jnp.concatenate(qkv_grad, 1).reshape(groups, each, 3 * own)
    extra = jnp.pad(jnp.stack([high, low]), ((0, 14), (0, 0)))
    extra = jnp.broadcast_to(extra[None], (groups, 16, 3 * own))
    qkv_grad = lax.all_to_all(jnp.concatenate([qkv_grad, extra], 1), "dp", 0, 0, tiled=True)
    qkv_grad = jnp.sum(qkv_grad.astype(f32), 0)
    bias_grad = qkv_grad[each] + qkv_grad[each + 1]
    pick = lambda a, n: a.reshape(a.shape[:-1] + (heads, 3, HD))[..., n, :].reshape(a.shape[:-1] + (own,))
    inner_bias_out = lax.dynamic_index_in_dim(early, 6 + rank, 0, keepdims=False)
    return (
        layer_out[None],
        input_grad[None],
        pick(qkv_grad[:each], 0),
        pick(qkv_grad[:each], 1),
        pick(qkv_grad[:each], 2),
        pick(bias_grad, 0),
        pick(bias_grad, 2),
        weight_grads[:, 2 * units :].T,
        early[0],
        early[1],
        early[2],
        weight_grads[:, :units],
        inner_bias_out,
        weight_grads[:, units : 2 * units].T,
        early[3],
        early[4],
        early[5],
    )


def solution(mesh):
    placed = (
        P("dp", "tensor", None),
        P("dp", "tensor"),
        P("dp", "tensor"),
        P("dp", "tensor"),
        P("dp", "tensor"),
        P("tensor"),
        P("tensor"),
        P("tensor", "dp"),
        P(),
        P(),
        P(),
        P("dp", "tensor"),
        P("tensor"),
        P("tensor", "dp"),
        P(),
        P(),
        P(),
        P("dp", "tensor", None),
    )

    return jax.shard_map(
        body,
        mesh=mesh,
        in_specs=placed,
        out_specs=(
            P("dp", "tensor", None),
            P("dp", "tensor", None),
            P("dp", "tensor"),
            P("dp", "tensor"),
            P("dp", "tensor"),
            P("tensor"),
            P("tensor"),
            P("tensor", "dp"),
            P(),
            P(),
            P(),
            P("dp", "tensor"),
            P("tensor"),
            P("tensor", "dp"),
            P(),
            P(),
            P(),
        ),
        check_vma=False,
    )
```

```python
import functools

import jax
import jax.numpy as jnp
from jax import lax
from jax.experimental import pallas as pl
from jax.experimental.pallas import tpu as pltpu
from jax.sharding import PartitionSpec as P


EPS = 1e-12
ROOT_HALF = 0.7071067811865476
INV_ROOT_TWO_PI = 0.3989422804014327
HD=64; SCALE=0.125; APART=-1e30
VM=pltpu.VMEM


def dot(a,b): return jnp.dot(a,b,preferred_element_type=jnp.float32)


def project_body(heads, part_ref, x_ref, w_ref, b_ref, scol_ref, srow_ref, qt_ref, ka_ref, vt_ref, qn_ref, kt_ref, vn_ref):
    y = dot(x_ref[...], w_ref[0,:,:b_ref.shape[1]]) + b_ref[...]
    low = y.astype(jnp.bfloat16)
    yt = y.T.astype(jnp.bfloat16)
    rows = y.shape[0]
    apart = jnp.where(lax.broadcasted_iota(jnp.int32,(HD,rows),0)==srow_ref[...],0.0,APART).astype(jnp.bfloat16)
    same = (lax.broadcasted_iota(jnp.int32,(rows,HD),1)==scol_ref[...]).astype(jnp.float32).astype(jnp.bfloat16)
    for h in range(heads):
        at=3*h*HD
        qt_ref[h,:HD,:]=yt[at:at+HD]*jnp.bfloat16(SCALE)
        qt_ref[h,HD:,:]=apart
        qn_ref[h]=low[:,at:at+HD]*jnp.bfloat16(SCALE)
        ka_ref[h]=jnp.concatenate([low[:,at+HD:at+2*HD],same],axis=1)
        kt_ref[h]=yt[at+HD:at+2*HD]
        vt_ref[h]=yt[at+2*HD:at+3*HD]
        vn_ref[h]=low[:,at+2*HD:at+3*HD]


def project(x,rest,part,b,seg,rows=512):
    L,D=x.shape; heads=b.shape[0]//(3*HD)
    bf=jnp.bfloat16
    cols=4*heads*HD
    nat=lambda n: pl.BlockSpec((heads,rows,n),lambda i,*_:(0,i,0))
    tr=lambda n: pl.BlockSpec((heads,n,rows),lambda i,*_:(0,0,i))
    S=jax.ShapeDtypeStruct
    return pl.pallas_call(functools.partial(project_body,heads),
        grid_spec=pltpu.PrefetchScalarGridSpec(num_scalar_prefetch=1,grid=(L//rows,),
        in_specs=[pl.BlockSpec((rows,D),lambda i,*_:(i,0)),pl.BlockSpec((1,D,cols),lambda i,p:(p[0],0,0)),pl.BlockSpec((1,b.shape[0]),lambda i,*_:(0,0)),
                  pl.BlockSpec((rows,1),lambda i,*_:(i,0)),pl.BlockSpec((1,rows),lambda i,*_:(0,i))],
        out_specs=[tr(2*HD),nat(2*HD),tr(HD),nat(HD),tr(HD),nat(HD)]),
        out_shape=[S((heads,2*HD,L),bf),S((heads,L,2*HD),bf),S((heads,HD,L),bf),S((heads,L,HD),bf),S((heads,HD,L),bf),S((heads,L,HD),bf)],
        compiler_params=pltpu.CompilerParams(vmem_limit_bytes=62 << 20),
        cost_estimate=pl.CostEstimate(flops=2*L*D*b.shape[0],bytes_accessed=L*D*2+D*cols*2+L*heads*HD*2*10,transcendentals=0),
        name="project")(part.reshape(1),x,rest,b.reshape(1,-1),seg.reshape(-1,1),seg.reshape(1,-1))


def forward_body(BK, lo_ref, hi_ref, qt_ref, ka_ref, vt_ref, ctx_ref, ot_ref, lse_ref, m_s, l_s, acc, s_even, s_odd):
    i=pl.program_id(0)
    heads=qt_ref.shape[0]
    half=BK//2
    m_s[...]=jnp.full(m_s.shape,-jnp.inf,jnp.float32)
    l_s[...]=jnp.zeros(l_s.shape,jnp.float32)
    acc[...]=jnp.zeros(acc.shape,jnp.float32)

    def scores(h,at):
        return dot(ka_ref[h,pl.ds(pl.multiple_of(at,half),half),:],qt_ref[h])

    def use(h,at,s):
        m_old=m_s[h]
        m_new=jnp.maximum(m_old,jnp.max(s,axis=0,keepdims=True))
        p=jnp.exp(s-m_new)
        alpha=jnp.exp(m_old-m_new)
        m_s[h]=m_new
        l_s[h]=l_s[h]*alpha+jnp.sum(p,axis=0,keepdims=True)
        acc[h]=acc[h]*alpha+dot(vt_ref[h,:,pl.ds(pl.multiple_of(at,half),half)],p.astype(jnp.bfloat16))

    last=hi_ref[i]-1
    for h in range(heads):
        s_even[h]=scores(h,lo_ref[i]*BK)

    def step(j,_):
        at=j*BK
        for h in range(heads):
            s_odd[h]=scores(h,at+half)
            use(h,at,s_even[h])
        for h in range(heads):
            s_even[h]=scores(h,jnp.minimum(j+1,last)*BK)
            use(h,at+half,s_odd[h])
        return 0

    lax.fori_loop(lo_ref[i],hi_ref[i],step,0)
    for h in range(heads):
        o=acc[h]/l_s[h]
        lse_ref[h]=m_s[h]+jnp.log(l_s[h])
        ot_ref[h]=o
        ctx_ref[0,h*HD:(h+1)*HD,:]=o.astype(jnp.bfloat16)


def attend_forward(first,heads,parts,qt,ka,vt,lo,hi,BQ=384,BK=512):
    L=qt.shape[2]
    S=jax.ShapeDtypeStruct
    per=L//parts//BQ
    return pl.pallas_call(functools.partial(forward_body,BK),
        grid_spec=pltpu.PrefetchScalarGridSpec(num_scalar_prefetch=2,grid=(L//BQ,),
        in_specs=[pl.BlockSpec((heads,2*HD,BQ),lambda i,*_:(first//heads,0,i)),pl.BlockSpec((heads,L,2*HD),lambda i,*_:(first//heads,0,0)),pl.BlockSpec((heads,HD,L),lambda i,*_:(first//heads,0,0))],
        out_specs=[pl.BlockSpec((1,heads*HD,BQ),lambda i,*_:(i//per,0,i%per)),pl.BlockSpec((heads,HD,BQ),lambda i,*_:(0,0,i)),pl.BlockSpec((heads,1,BQ),lambda i,*_:(0,0,i))],
        scratch_shapes=[VM((heads,1,BQ),jnp.float32),VM((heads,1,BQ),jnp.float32),VM((heads,HD,BQ),jnp.float32)]+[VM((heads,BK//2,BQ),jnp.float32)]*2),
        out_shape=[S((parts,heads*HD,L//parts),jnp.bfloat16),S((heads,HD,L),jnp.float32),S((heads,1,L),jnp.float32)],
        compiler_params=pltpu.CompilerParams(vmem_limit_bytes=62 << 20),
        cost_estimate=pl.CostEstimate(flops=2*L*L*HD*2*heads,bytes_accessed=L*heads*HD*2*8,transcendentals=L*L*heads),
        name="attend_forward")(lo,hi,qt,ka,vt)


def backward_body(BQ, BK, SUB, lo_ref, hi_ref, go_ref, ot_ref, lse_ref, qt_ref, ka_ref, qn_ref, kt_ref, vn_ref, x_ref, out_ref, wg_ref, sum_ref, got, gon, delta, dqt, dkt, dvt, dk_s, dv_s, x_s, x_sem):
    bring=pltpu.make_async_copy(x_ref,x_s,x_sem)
    bring.start()
    parts,_,rows=go_ref.shape
    heads,_,L=qt_ref.shape
    CH=256
    for h in range(heads):
        for c in range(L//CH):
            p,at=c*CH//rows,c*CH%rows
            gt=go_ref[p,h*HD:(h+1)*HD,at:at+CH]
            wide=gt.astype(jnp.float32)
            got[h,:,c*CH:(c+1)*CH]=gt
            gon[h,c*CH:(c+1)*CH,:]=wide.T.astype(jnp.bfloat16)
            delta[h,:,c*CH:(c+1)*CH]=jnp.sum(wide*ot_ref[h,:,c*CH:(c+1)*CH],axis=0,keepdims=True)
    dqt[...]=jnp.zeros(dqt.shape,jnp.float32)

    def key_block(j,_):
        ka_at=pl.multiple_of(j*BK,BK)
        dk_s[...]=jnp.zeros(dk_s.shape,jnp.float32)
        dv_s[...]=jnp.zeros(dv_s.shape,jnp.float32)

        def query_block(i,_):
            for h,c in [(h,c) for h in range(heads) for c in range(BQ//SUB)]:
                at=pl.multiple_of(i*BQ+c*SUB,SUB)
                s=dot(ka_ref[h,pl.ds(ka_at,BK),:],qt_ref[h,:,pl.ds(at,SUB)])
                p=jnp.exp(s-lse_ref[h,:,pl.ds(at,SUB)])
                dp=dot(vn_ref[h,pl.ds(ka_at,BK),:],got[h,:,pl.ds(at,SUB)])
                ds=(p*(dp-delta[h,:,pl.ds(at,SUB)])).astype(jnp.bfloat16)
                dv_s[h]+=dot(p.astype(jnp.bfloat16),gon[h,pl.ds(at,SUB),:])
                dk_s[h]+=dot(ds,qn_ref[h,pl.ds(at,SUB),:])
                dqt[h,:,pl.ds(at,SUB)]+=dot(kt_ref[h,:,pl.ds(ka_at,BK)],ds)
            return 0

        lax.fori_loop(lo_ref[j],hi_ref[j],query_block,0)
        for h in range(heads):
            dkt[h,:,pl.ds(ka_at,BK)]=dk_s[h].T.astype(jnp.bfloat16)
            dvt[h,:,pl.ds(ka_at,BK)]=dv_s[h].T.astype(jnp.bfloat16)
        return 0

    lax.fori_loop(0,L//BK,key_block,0)
    for h in range(heads):
        for p in range(parts):
            cut=slice(p*rows,(p+1)*rows)
            out_ref[p,3*h*HD:(3*h+1)*HD,:]=(dqt[h,:,cut]*SCALE).astype(jnp.bfloat16)
            out_ref[p,(3*h+1)*HD:(3*h+2)*HD,:]=dkt[h,:,cut]
            out_ref[p,(3*h+2)*HD:(3*h+3)*HD,:]=dvt[h,:,cut]
    bring.wait()
    wg=jnp.zeros(wg_ref.shape[::-1],jnp.float32)
    total=jnp.zeros((3*heads*HD,1),jnp.float32)
    for p in range(parts):
        part=out_ref[p]
        wg=wg+dot(part,x_s[p])
        total=total+jnp.sum(part.astype(jnp.float32),axis=1,keepdims=True)
    wg_ref[...]=wg.T.astype(wg_ref.dtype)
    sum_ref[...]=jnp.broadcast_to(total,sum_ref.shape)


def attend_backward(first,heads,go,go_first,ot,lse,ot_first,qt,ka,qn,kt,vn,x,lo,hi,BQ=512,BK=512,SUB=512):
    parts,_,rows=go.shape; L=parts*rows; D=x.shape[2]
    S=jax.ShapeDtypeStruct; f32=jnp.float32; bf=jnp.bfloat16
    at=lambda a,n: pl.BlockSpec((heads,)+a.shape[1:],lambda i,*_:(n//heads,0,0),pipeline_mode=pl.Buffered(1))
    out=3*heads*HD
    return pl.pallas_call(functools.partial(backward_body,BQ,BK,SUB),
        grid_spec=pltpu.PrefetchScalarGridSpec(num_scalar_prefetch=2,grid=(1,),
        in_specs=[pl.BlockSpec((parts,heads*HD,rows),lambda i,*_:(0,go_first,0),pipeline_mode=pl.Buffered(1)),at(ot,ot_first),at(lse,ot_first)]+[at(a,first) for a in (qt,ka,qn,kt,vn)]+[pl.BlockSpec(memory_space=pl.ANY)],
        out_specs=[pl.BlockSpec((parts,out,rows),lambda i,*_:(0,0,0),pipeline_mode=pl.Buffered(1)),pl.BlockSpec((D,out),lambda i,*_:(0,0)),pl.BlockSpec((out,128),lambda i,*_:(0,0))],
        scratch_shapes=[VM((heads,HD,L),bf),VM((heads,L,HD),bf),VM((heads,1,L),f32),VM((heads,HD,L),f32),VM((heads,HD,L),bf),VM((heads,HD,L),bf),VM((heads,BK,HD),f32),VM((heads,BK,HD),f32),VM(x.shape,bf),pltpu.SemaphoreType.DMA]),
        out_shape=[S((parts,out,rows),bf),S((D,out),bf),S((out,128),f32)],
        compiler_params=pltpu.CompilerParams(vmem_limit_bytes=62 << 20),
        cost_estimate=pl.CostEstimate(flops=2*L*L*HD*5*heads,bytes_accessed=L*heads*HD*2*14,transcendentals=L*L*heads),
        name="attend_backward")(lo,hi,go,ot,lse,qt,ka,qn,kt,vn,x)


def ranges(seg,BQ,BK):
    first=seg.reshape(-1,BQ)[:,0]; last=seg.reshape(-1,BQ)[:,-1]
    kf=seg.reshape(-1,BK)[:,0]; kl=seg.reshape(-1,BK)[:,-1]
    lo=jnp.sum((kl[None,:]<first[:,None]).astype(jnp.int32),1)
    hi=jnp.sum((kf[None,:]<=last[:,None]).astype(jnp.int32),1)
    return lo,hi


def dot_right_t(left, right):
    return lax.dot_general(
        left, right, (((1,), (1,)), ((), ())), preferred_element_type=jnp.float32
    )


def layer_norm(values_in, gain, shift):
    mean_row = jnp.mean(values_in, -1, keepdims=True)
    centered = values_in - mean_row
    inverse = lax.rsqrt(jnp.mean(centered * centered, -1, keepdims=True) + EPS)
    normed = centered * inverse
    return (normed * gain + shift, normed, inverse)


def norm_back(grad_in, normed, inverse, gain):
    scaled = grad_in * gain
    return inverse * (
        scaled
        - jnp.mean(scaled, -1, keepdims=True)
        - normed * jnp.mean(scaled * normed, -1, keepdims=True)
    )


MESH = pl.DeviceIdType.MESH


def flip(index, bit):
    span = 1 << bit
    return index + span * (1 - 2 * ((index // span) % 2))


def start_body(n, bits, x_ref, w_ref, s_ref, x_out, w_out, s_out, send_z, recv_z, send_d, recv_d, keep_sem):
    me = lax.axis_index("tensor")
    mine = lax.axis_index("dp")
    barrier = pltpu.get_barrier_semaphore()

    @pl.when(me > 0)
    def _():
        pl.semaphore_signal(barrier, inc=1, device_id={"tensor": me - 1}, device_id_type=MESH)

    @pl.when(me < n - 1)
    def _():
        pl.semaphore_signal(barrier, inc=1, device_id={"tensor": me + 1}, device_id_type=MESH)

    for bit in range(bits):
        pl.semaphore_signal(barrier, inc=1, device_id={"dp": flip(mine, bit)}, device_id_type=MESH)
    pl.semaphore_wait(barrier, bits + jnp.where(me > 0, 1, 0) + jnp.where(me < n - 1, 1, 0))

    keeps = [
        pltpu.make_async_copy(x_ref, x_out.at[me], keep_sem.at[0]),
        pltpu.make_async_copy(w_ref, w_out.at[me, mine], keep_sem.at[1]),
        pltpu.make_async_copy(s_ref, s_out.at[me], keep_sem.at[2]),
    ]
    for keep in keeps:
        keep.start()

    def hop(kind, side, step):
        block = me - (step - 1) if side else me + (step - 1)
        first, place = (
            (x_ref, x_out.at[block]),
            (w_ref, w_out.at[block, mine]),
            (s_ref, s_out.at[block]),
        )[kind]
        return pltpu.make_async_remote_copy(
            src_ref=first if step == 1 else place,
            dst_ref=place,
            send_sem=send_z.at[kind, side, step - 1],
            recv_sem=recv_z.at[kind, side, step - 1],
            device_id={"tensor": me + 1 if side else me - 1},
            device_id_type=MESH,
        )

    def sends(side, step):
        if side:
            return (me < n - 1) & (me >= step - 1)
        return (me > 0) & (me + step - 1 <= n - 1)

    def receives(side, step):
        return me >= step if side else me + step <= n - 1

    def z_start(kinds, step):
        for side in (0, 1):

            @pl.when(sends(side, step))
            def _():
                for kind in kinds:
                    hop(kind, side, step).start()

    def z_arrive(kinds, step):
        for side in (0, 1):

            @pl.when(receives(side, step))
            def _():
                for kind in kinds:
                    hop(kind, side, step).wait_recv()

    half = w_ref.shape[1] // 2
    up = list(range(bits - 1, -1, -1))
    orders = (up, [up[1], up[0]] + up[2:] if bits > 1 else up)

    def doubling(side, step):
        order = orders[side]
        held = [mine]
        for bit in order[:step]:
            held = held + [flip(d, bit) for d in held]
        cut = pl.ds(side * half, half)
        return [
            pltpu.make_async_remote_copy(
                src_ref=w_out.at[:, d, :, cut],
                dst_ref=w_out.at[:, d, :, cut],
                send_sem=send_d.at[side, (1 << step) - 1 + at],
                recv_sem=recv_d.at[side, (1 << step) - 1 + at],
                device_id={"dp": flip(mine, order[step])},
                device_id_type=MESH,
            )
            for at, d in enumerate(held)
        ]

    def d_start(step):
        for side in (0, 1):
            for copy in doubling(side, step):
                copy.start()

    def d_arrive(step):
        for side in (0, 1):
            for copy in doubling(side, step):
                copy.wait_recv()

    for step in range(1, n):
        z_start((1, 2), step)
        z_arrive((1, 2), step)
    keeps[1].wait()
    for step in range(max(n - 1, bits)):
        if step < bits:
            if step:
                d_arrive(step - 1)
            d_start(step)
        if step < n - 1:
            if step:
                z_arrive((0,), step)
            z_start((0,), step + 1)
    z_arrive((0,), n - 1)
    d_arrive(bits - 1)
    for side in (0, 1):
        for step in range(1, n):

            @pl.when(sends(side, step))
            def _():
                for kind in (0, 1, 2):
                    hop(kind, side, step).wait_send()

        for step in range(bits):
            for copy in doubling(side, step):
                copy.wait_send()
    keeps[0].wait()
    keeps[2].wait()


def start(x, w, small):
    n = lax.axis_size("tensor")
    groups = lax.axis_size("dp")
    bits = groups.bit_length() - 1
    S = jax.ShapeDtypeStruct
    anywhere = pl.BlockSpec(memory_space=pl.ANY)
    return pl.pallas_call(
        functools.partial(start_body, n, bits),
        in_specs=[pl.BlockSpec(memory_space=pltpu.VMEM)] * 3,
        out_specs=[anywhere] * 3,
        out_shape=[
            S((n,) + x.shape, x.dtype),
            S((n, groups) + w.shape, w.dtype),
            S((n,) + small.shape, small.dtype),
        ],
        scratch_shapes=[
            pltpu.SemaphoreType.DMA((3, 2, n - 1)),
            pltpu.SemaphoreType.DMA((3, 2, n - 1)),
            pltpu.SemaphoreType.DMA((2, groups - 1)),
            pltpu.SemaphoreType.DMA((2, groups - 1)),
            pltpu.SemaphoreType.DMA((3,)),
        ],
        compiler_params=pltpu.CompilerParams(collective_id=0, has_side_effects=True),
        cost_estimate=pl.CostEstimate(flops=0, bytes_accessed=200 << 20, transcendentals=0),
        name="start",
    )(x, w, small)


def weight_grads_body(parts, first_ref, second_ref, attn_ref, inner_ref, active_ref, context_ref, out_ref, ft, st):
    j = pl.program_id(0)

    @pl.when(j == 0)
    def _():
        ft[...] = first_ref[...].T
        st[...] = second_ref[...].T

    @pl.when((j < 2 * parts) & (j % 2 == 0))
    def _():
        out_ref[...] = dot(ft[...], inner_ref[0]).astype(out_ref.dtype)

    @pl.when((j < 2 * parts) & (j % 2 == 1))
    def _():
        out_ref[...] = dot(st[...], active_ref[0]).astype(out_ref.dtype)

    @pl.when(j == 2 * parts)
    def _():
        out_ref[...] = dot_right_t(attn_ref[...].T, context_ref[...]).astype(out_ref.dtype)


def weight_grads_of(first_low, second_low, attn_low, grad_inner, active, context):
    parts, rows, units = active.shape
    width = first_low.shape[1]
    features = context.shape[0]
    fixed = pl.BlockSpec((rows, width), lambda j: (0, 0))
    moving = lambda shift: pl.BlockSpec((1, rows, units), lambda j: (jnp.clip((j - shift) // 2, 0, parts - 1), 0, 0))
    return pl.pallas_call(
        functools.partial(weight_grads_body, parts),
        grid=(2 * parts + 1,),
        in_specs=[fixed, fixed, fixed, moving(0), moving(1), pl.BlockSpec((features, rows), lambda j: (0, 0))],
        out_specs=pl.BlockSpec((width, units), lambda j: (0, j)),
        out_shape=jax.ShapeDtypeStruct((width, units * 2 * parts + features), jnp.bfloat16),
        scratch_shapes=[VM((width, rows), jnp.bfloat16), VM((width, rows), jnp.bfloat16)],
        compiler_params=pltpu.CompilerParams(vmem_limit_bytes=62 << 20),
        cost_estimate=pl.CostEstimate(flops=2 * rows * width * (2 * parts * units + features), bytes_accessed=rows * units * 2 * parts * 4, transcendentals=0),
        name="weight_grads",
    )(first_low, second_low, attn_low, grad_inner, active, context)


def erf(x):
    x = jnp.clip(x, -3.7439211627767994, 3.7439211627767994)
    y = x * x
    top = jnp.float32(0.00022905065861350646)
    for c in (0.0034082910107109506, 0.050955695062380861, 0.18520832239976145, 1.128379143519084):
        top = top * y + c
    low = jnp.float32(-1.1791602954361697e-7)
    for c in (0.000023547966471313185, 0.0010179625278914885, 0.014070470171167667, 0.11098505178285362, 0.49746925110067538, 1.0):
        low = low * y + c
    return x * top / low


def dense_body(own, x_ref, cot_ref, ctx0_ref, ctx1_ref, vec_ref, bias_ref, near_ref, far_ref, out_ref, first_ref, second_ref, attn_ref, grad_ref, active_ref, inner_ref, ctx_ref, go0_ref, go1_ref, sum_ref, w_s, mt_s, slope_s, first_s, acc_s, w_sem):
    i = pl.program_id(0)
    parts, _, _ = near_ref.shape
    f32, bf = jnp.float32, jnp.bfloat16
    units = active_ref.shape[2]
    cuts = (slice(0, 4 * own), slice(4 * own, 4 * own + units), slice(4 * own + units, 4 * own + 2 * units))
    sources = (near_ref.at[:, :, cuts[0]], near_ref.at[:, :, cuts[1]], far_ref)
    copies = [pltpu.make_async_copy(sources[c], w_s.at[:, :, cut], w_sem.at[c]) for c, cut in enumerate(cuts)]

    @pl.when(i == 0)
    def _():
        for copy in copies:
            copy.start()
        sum_ref[...] = jnp.zeros(sum_ref.shape, f32)
        copies[0].wait()
        for t in range(parts):
            mt_s[:, t * own : (t + 1) * own] = w_s[t, :, 3 * own : 4 * own]

    def add_sum(row, value):
        sum_ref[row : row + 1, :] += jnp.sum(value, axis=0, keepdims=True)

    for t in range(parts):
        lead = ctx0_ref.shape[1]
        ctx_ref[t * own : t * own + lead, :] = ctx0_ref[t]
        ctx_ref[t * own + lead : (t + 1) * own, :] = ctx1_ref[t]
    mixed = dot(mt_s[...], ctx_ref[...]).T
    attn_in = x_ref[...].astype(f32) + mixed + vec_ref[0:1]
    first, first_norm, first_inv = layer_norm(attn_in, vec_ref[1:2], vec_ref[2:3])
    first_ref[...] = first.astype(bf)
    first_s[...] = first_norm
    acc_s[...] = first + vec_ref[3:4]

    @pl.when(i == 0)
    def _():
        copies[1].wait()
        copies[2].wait()

    def ahead(t, _):
        inner = dot(first_ref[...], w_s[t, :, cuts[1]]) + bias_ref[t]
        half = 0.5 * (1.0 + erf(inner * ROOT_HALF))
        slope_s[t] = half + inner * jnp.exp(-0.5 * inner * inner) * INV_ROOT_TWO_PI
        active_ref[t] = (inner * half).astype(bf)
        acc_s[...] += dot_right_t(active_ref[t], w_s[t, :, cuts[2]])
        return 0

    lax.fori_loop(0, parts, ahead, 0)
    second, second_norm, second_inv = layer_norm(acc_s[...], vec_ref[4:5], vec_ref[5:6])
    out_ref[...] = second.astype(bf)
    grad_out = cot_ref[...].astype(f32)
    add_sum(4, grad_out * second_norm)
    add_sum(5, grad_out)
    grad_second = norm_back(grad_out, second_norm, second_inv, vec_ref[4:5])
    add_sum(3, grad_second)
    second_ref[...] = grad_second.astype(bf)
    acc_s[...] = grad_second

    def back(t, _):
        grad_inner = (dot(second_ref[...], w_s[t, :, cuts[2]]) * slope_s[t]).astype(bf)
        inner_ref[t] = grad_inner
        sum_ref[pl.ds(6 + t, 1), :] += jnp.sum(grad_inner.astype(f32), axis=0, keepdims=True)
        acc_s[...] += dot_right_t(grad_inner, w_s[t, :, cuts[1]])
        return 0

    lax.fori_loop(0, parts, back, 0)
    grad_first = acc_s[...]
    first_norm = first_s[...]
    add_sum(1, grad_first * first_norm)
    add_sum(2, grad_first)
    grad_attn = norm_back(grad_first, first_norm, first_inv, vec_ref[1:2])
    add_sum(0, grad_attn)
    grad_ref[...] = grad_attn
    attn_ref[...] = grad_attn.astype(bf)
    grad_context = dot(attn_ref[...], mt_s[...]).T.astype(bf)
    for t in range(parts):
        go0_ref[t] = grad_context[t * own : t * own + HD]
        go1_ref[t] = grad_context[t * own + HD : (t + 1) * own]


def dense(own, x, cot, ctx0, ctx1, vectors, inner_bias, near, far, block):
    rows, width = x.shape
    parts = near.shape[0]
    units = far.shape[2]
    cols = 4 * own + 2 * units
    f32, bf = jnp.float32, jnp.bfloat16
    S = jax.ShapeDtypeStruct
    tok = pl.BlockSpec((block, width), lambda i: (i, 0))
    part_tok = pl.BlockSpec((parts, block, units), lambda i: (0, i, 0))
    lanes = lambda n: pl.BlockSpec((parts, n, block), lambda i: (0, 0, i))
    fixed = lambda a: pl.BlockSpec(a.shape, lambda i: (0,) * a.ndim)
    inner_bias = inner_bias.reshape(parts, 1, units)
    return pl.pallas_call(
        functools.partial(dense_body, own),
        grid=(rows // block,),
        in_specs=[tok, tok, lanes(ctx0.shape[1]), lanes(ctx1.shape[1]), fixed(vectors), fixed(inner_bias), pl.BlockSpec(memory_space=pl.ANY), pl.BlockSpec(memory_space=pl.ANY)],
        out_specs=[tok] * 5 + [part_tok] * 2 + [pl.BlockSpec((parts * own, block), lambda i: (0, i)), lanes(HD), lanes(own - HD), pl.BlockSpec((16, width), lambda i: (0, 0))],
        out_shape=[S((rows, width), bf)] * 4 + [S((rows, width), f32)] + [S((parts, rows, units), bf)] * 2 + [S((parts * own, rows), bf), S((parts, HD, rows), bf), S((parts, own - HD, rows), bf), S((16, width), f32)],
        scratch_shapes=[VM((parts, width, cols), bf), VM((width, parts * own), bf), VM((parts, block, units), f32), VM((block, width), f32), VM((block, width), f32), pltpu.SemaphoreType.DMA((3,))],
        compiler_params=pltpu.CompilerParams(vmem_limit_bytes=62 << 20),
        cost_estimate=pl.CostEstimate(flops=4 * rows * width * (2 * parts * units + parts * own), bytes_accessed=40 << 20, transcendentals=rows * units * parts),
        name="dense",
    )(x, cot, ctx0, ctx1, vectors, inner_bias, near, far)


def early_back_body(w_ref, b0_ref, b1_ref, acc_ref):
    width = b0_ref.shape[1]
    total = jnp.zeros(acc_ref.shape, jnp.float32)
    for t in range(b0_ref.shape[0]):
        total = total + dot(w_ref[t, :, : 2 * width], jnp.concatenate([b0_ref[t], b1_ref[t]], axis=0))
    acc_ref[...] = total


def late_back_body(cut, part_ref, w_ref, acc_ref, grad_ref, *rest):
    backs, out_ref = rest[:-1], rest[-1]
    parts = len(backs)
    total = acc_ref[...]
    for d in range(parts):
        total = total + dot(w_ref[(part_ref[0] + parts - d) % parts, :, cut : cut + backs[d].shape[0]], backs[d][...])
    out_ref[...] = (total.T + grad_ref[...]).astype(out_ref.dtype)


def weight_block(rest, cols):
    return pl.BlockSpec(rest.shape[:2] + (cols,), lambda i, *_: (0, 0, 0), pipeline_mode=pl.Buffered(1))


def whole(a):
    return pl.BlockSpec(a.shape, lambda i, *_: (0,) * a.ndim, pipeline_mode=pl.Buffered(1))


def early_back(rest, cols, b0, b1):
    width, rows = rest.shape[1], b0.shape[2]
    return pl.pallas_call(
        early_back_body,
        grid=(1,),
        in_specs=[weight_block(rest, cols), whole(b0), whole(b1)],
        out_specs=pl.BlockSpec((width, rows), lambda i: (0, 0)),
        out_shape=jax.ShapeDtypeStruct((width, rows), jnp.float32),
        compiler_params=pltpu.CompilerParams(vmem_limit_bytes=62 << 20),
        cost_estimate=pl.CostEstimate(flops=4 * width * rows * b0.shape[0] * b0.shape[1], bytes_accessed=10 << 20, transcendentals=0),
        name="early_back",
    )(rest, b0, b1)


def late_back(rest, cols, cut, part, acc, grad, backs):
    rows, width = grad.shape
    return pl.pallas_call(
        functools.partial(late_back_body, cut),
        grid_spec=pltpu.PrefetchScalarGridSpec(
            num_scalar_prefetch=1,
            grid=(1,),
            in_specs=[weight_block(rest, cols), whole(acc), whole(grad)] + [whole(b) for b in backs],
            out_specs=pl.BlockSpec((rows, width), lambda i, *_: (0, 0)),
        ),
        out_shape=jax.ShapeDtypeStruct((rows, width), jnp.bfloat16),
        compiler_params=pltpu.CompilerParams(vmem_limit_bytes=62 << 20),
        cost_estimate=pl.CostEstimate(flops=2 * width * rows * backs[0].shape[0] * len(backs), bytes_accessed=10 << 20, transcendentals=0),
        name="late_back",
    )(part.reshape(1), rest, acc, grad, *backs)


def add_up(value):
    for axis in ("dp", "tensor"):
        size = lax.axis_size(axis)
        span = 1
        while span < size:
            other = lax.ppermute(value, axis, [(i, i ^ span) for i in range(size)])
            value = value + other
            span *= 2
    return value


def rotate(blocks, axis):
    size = lax.axis_size(axis)
    me = lax.axis_index(axis)
    out = []
    for d in range(size):
        block = lax.dynamic_index_in_dim(blocks, (me + d) % size, 0, keepdims=False)
        if d:
            block = lax.ppermute(block, axis, [(i, (i + d) % size) for i in range(size)])
        out.append(block)
    return out


def body(hidden_in, segments, query_weight, key_weight, value_weight, query_bias, value_bias, mixer_weight, mixer_bias, first_gain, first_shift, inner_weight, inner_bias, outer_weight, outer_bias, second_gain, second_shift, cotangent):
    bf = jnp.bfloat16
    f32 = jnp.float32
    _, rows, width = hidden_in.shape
    parts = lax.axis_size("tensor")
    groups = lax.axis_size("dp")
    rank = lax.axis_index("tensor")
    own = query_weight.shape[1]
    heads = own // HD
    three = 3 * HD
    units = inner_weight.shape[1]
    by_head = lambda q, k, v: jnp.stack([a.reshape(a.shape[:-1] + (heads, HD)) for a in (q, k, v)], -2).reshape(q.shape[:-1] + (3 * own,))
    x_own = hidden_in[0]
    qkv_own = by_head(query_weight, key_weight, value_weight)
    small = jnp.concatenate([segments[0].astype(f32), inner_bias]).reshape(-1, 128)
    near_own = jnp.concatenate([qkv_own, mixer_weight.T, inner_weight], 1)
    x_parts, near, small = start(x_own, near_own, small)
    x_all = x_parts.reshape(parts * rows, width)
    near = near.reshape(parts, width, 4 * own + units)
    far_own = outer_weight.T
    far_own, small = lax.optimization_barrier((far_own, small))
    far = lax.all_gather(far_own, ("tensor", "dp"), axis=0, tiled=True).reshape(parts, width, units)
    small = small.reshape(parts, -1)
    segment_all = small[:, :rows].astype(jnp.int32).reshape(-1)
    inner_bias_all = small[:, rows:]
    biases = by_head(query_bias, jnp.zeros_like(query_bias), value_bias)

    qt, ka, vt, qn, kt, vn = project(x_all, near, rank, biases, segment_all)
    lead = heads - 1
    context_t, lse, exchanged = [], [], []
    for call, (first, count, block) in enumerate(((0, lead, rows // 2), (lead, 1, rows))):
        lo, hi = ranges(segment_all, block, 512)
        part, out_t, out_lse = attend_forward(first, count, parts, qt, ka, vt, lo, hi, BQ=block)
        context_t.append(out_t)
        lse.append(out_lse)
        if exchanged:
            part, exchanged[-1] = lax.optimization_barrier((part, exchanged[-1]))
        exchanged.append(lax.all_to_all(part, "tensor", 0, 0, tiled=True))
    vectors = jnp.stack([mixer_bias, first_gain, first_shift, outer_bias, second_gain, second_shift])
    vectors = jnp.pad(vectors, ((0, 2), (0, 0)))
    layer_out, first_low, second_low, attn_low, grad_attn, active, grad_inner, context, go0, go1, early = dense(
        own, x_own, cotangent[0], exchanged[0], exchanged[1], vectors, inner_bias_all, near, far, block=rows
    )
    go0 = lax.all_to_all(go0, "tensor", 0, 0, tiled=True)
    go1 = lax.all_to_all(go1, "tensor", 0, 0, tiled=True)
    weight_grads = weight_grads_of(
        first_low, second_low, attn_low, grad_inner, active, context
    )
    weight_grads = lax.psum_scatter(weight_grads, "dp", scatter_dimension=0, tiled=True)
    weight_grads = jnp.concatenate(
        [
            weight_grads[:, : 2 * units * parts].reshape(-1, parts, 2 * units),
            weight_grads[:, 2 * units * parts :].reshape(-1, parts, own),
        ],
        2,
    ).transpose(1, 0, 2)
    weight_grads = rotate(weight_grads, "tensor")
    weight_grads = sum(a.astype(f32) for a in weight_grads)
    early = add_up(early)

    lo, hi = ranges(segment_all, 512, 512)
    backs, qkv_grad, bias_grad = [], [], []
    for h in range(heads):
        call = 0 if h < lead else 1
        grads, weight_part, sums = attend_backward(
            h, 1, go1 if h else go0, h - 1 if h else 0, context_t[call], lse[call], h - call * lead, qt, ka, qn, kt, vn, x_parts, lo, hi
        )
        if h < heads - 1:
            backs.append(lax.all_to_all(grads, "tensor", 0, 0, tiled=True))
        else:
            backs.append(rotate(grads, "tensor"))
        qkv_grad.append(weight_part)
        bias_grad.append(sums[:, 0])
    input_back = early_back(near, 4 * own, backs[0], backs[1])
    input_grad = late_back(near, 4 * own, 2 * three, rank, input_back, grad_attn, backs[2])
    bias_grad = jnp.concatenate(bias_grad)
    high = bias_grad.astype(bf)
    low = (bias_grad - high.astype(f32)).astype(bf)
    each = width // groups
    qkv_grad = jnp.concatenate(qkv_grad, 1).reshape(groups, each, 3 * own)
    extra = jnp.pad(jnp.stack([high, low]), ((0, 14), (0, 0)))
    extra = jnp.broadcast_to(extra[None], (groups, 16, 3 * own))
    qkv_grad = lax.all_to_all(jnp.concatenate([qkv_grad, extra], 1), "dp", 0, 0, tiled=True)
    qkv_grad = jnp.sum(qkv_grad.astype(f32), 0)
    bias_grad = qkv_grad[each] + qkv_grad[each + 1]
    pick = lambda a, n: a.reshape(a.shape[:-1] + (heads, 3, HD))[..., n, :].reshape(a.shape[:-1] + (own,))
    inner_bias_out = lax.dynamic_index_in_dim(early, 6 + rank, 0, keepdims=False)
    return (
        layer_out[None],
        input_grad[None],
        pick(qkv_grad[:each], 0),
        pick(qkv_grad[:each], 1),
        pick(qkv_grad[:each], 2),
        pick(bias_grad, 0),
        pick(bias_grad, 2),
        weight_grads[:, 2 * units :].T,
        early[0],
        early[1],
        early[2],
        weight_grads[:, :units],
        inner_bias_out,
        weight_grads[:, units : 2 * units].T,
        early[3],
        early[4],
        early[5],
    )


def solution(mesh):
    placed = (
        P("dp", "tensor", None),
        P("dp", "tensor"),
        P("dp", "tensor"),
        P("dp", "tensor"),
        P("dp", "tensor"),
        P("tensor"),
        P("tensor"),
        P("tensor", "dp"),
        P(),
        P(),
        P(),
        P("dp", "tensor"),
        P("tensor"),
        P("tensor", "dp"),
        P(),
        P(),
        P(),
        P("dp", "tensor", None),
    )

    return jax.shard_map(
        body,
        mesh=mesh,
        in_specs=placed,
        out_specs=(
            P("dp", "tensor", None),
            P("dp", "tensor", None),
            P("dp", "tensor"),
            P("dp", "tensor"),
            P("dp", "tensor"),
            P("tensor"),
            P("tensor"),
            P("tensor", "dp"),
            P(),
            P(),
            P(),
            P("dp", "tensor"),
            P("tensor"),
            P("tensor", "dp"),
            P(),
            P(),
            P(),
        ),
        check_vma=False,
    )
```

```python
import functools

import jax
import jax.numpy as jnp
from jax import lax
from jax.experimental import pallas as pl
from jax.experimental.pallas import tpu as pltpu
from jax.sharding import PartitionSpec as P


EPS = 1e-12
ROOT_HALF = 0.7071067811865476
INV_ROOT_TWO_PI = 0.3989422804014327
HD=64; SCALE=0.125; APART=-1e30
VM=pltpu.VMEM


def dot(a,b): return jnp.dot(a,b,preferred_element_type=jnp.float32)


def project_body(heads, part_ref, x_ref, w_ref, b_ref, scol_ref, srow_ref, qt_ref, ka_ref, vt_ref, qn_ref, kt_ref, vn_ref):
    y = dot(x_ref[...], w_ref[0,:,:b_ref.shape[1]]) + b_ref[...]
    low = y.astype(jnp.bfloat16)
    yt = y.T.astype(jnp.bfloat16)
    rows = y.shape[0]
    apart = jnp.where(lax.broadcasted_iota(jnp.int32,(HD,rows),0)==srow_ref[...],0.0,APART).astype(jnp.bfloat16)
    same = (lax.broadcasted_iota(jnp.int32,(rows,HD),1)==scol_ref[...]).astype(jnp.float32).astype(jnp.bfloat16)
    for h in range(heads):
        at=3*h*HD
        qt_ref[h,:HD,:]=yt[at:at+HD]*jnp.bfloat16(SCALE)
        qt_ref[h,HD:,:]=apart
        qn_ref[h]=low[:,at:at+HD]*jnp.bfloat16(SCALE)
        ka_ref[h]=jnp.concatenate([low[:,at+HD:at+2*HD],same],axis=1)
        kt_ref[h]=yt[at+HD:at+2*HD]
        vt_ref[h]=yt[at+2*HD:at+3*HD]
        vn_ref[h]=low[:,at+2*HD:at+3*HD]


def project(x,rest,part,b,seg,rows=512):
    L,D=x.shape; heads=b.shape[0]//(3*HD)
    bf=jnp.bfloat16
    cols=4*heads*HD
    nat=lambda n: pl.BlockSpec((heads,rows,n),lambda i,*_:(0,i,0))
    tr=lambda n: pl.BlockSpec((heads,n,rows),lambda i,*_:(0,0,i))
    S=jax.ShapeDtypeStruct
    return pl.pallas_call(functools.partial(project_body,heads),
        grid_spec=pltpu.PrefetchScalarGridSpec(num_scalar_prefetch=1,grid=(L//rows,),
        in_specs=[pl.BlockSpec((rows,D),lambda i,*_:(i,0)),pl.BlockSpec((1,D,cols),lambda i,p:(p[0],0,0)),pl.BlockSpec((1,b.shape[0]),lambda i,*_:(0,0)),
                  pl.BlockSpec((rows,1),lambda i,*_:(i,0)),pl.BlockSpec((1,rows),lambda i,*_:(0,i))],
        out_specs=[tr(2*HD),nat(2*HD),tr(HD),nat(HD),tr(HD),nat(HD)]),
        out_shape=[S((heads,2*HD,L),bf),S((heads,L,2*HD),bf),S((heads,HD,L),bf),S((heads,L,HD),bf),S((heads,HD,L),bf),S((heads,L,HD),bf)],
        compiler_params=pltpu.CompilerParams(vmem_limit_bytes=62 << 20),
        cost_estimate=pl.CostEstimate(flops=2*L*D*b.shape[0],bytes_accessed=L*D*2+D*cols*2+L*heads*HD*2*10,transcendentals=0),
        name="project")(part.reshape(1),x,rest,b.reshape(1,-1),seg.reshape(-1,1),seg.reshape(1,-1))


def forward_body(BK, lo_ref, hi_ref, qt_ref, ka_ref, vt_ref, ctx_ref, ot_ref, lse_ref, m_s, l_s, acc, s_even, s_odd):
    i=pl.program_id(0)
    heads=qt_ref.shape[0]
    half=BK//2
    m_s[...]=jnp.full(m_s.shape,-jnp.inf,jnp.float32)
    l_s[...]=jnp.zeros(l_s.shape,jnp.float32)
    acc[...]=jnp.zeros(acc.shape,jnp.float32)

    def scores(h,at):
        return dot(ka_ref[h,pl.ds(pl.multiple_of(at,half),half),:],qt_ref[h])

    def use(h,at,s):
        m_old=m_s[h]
        m_new=jnp.maximum(m_old,jnp.max(s,axis=0,keepdims=True))
        p=jnp.exp(s-m_new)
        alpha=jnp.exp(m_old-m_new)
        m_s[h]=m_new
        l_s[h]=l_s[h]*alpha+jnp.sum(p,axis=0,keepdims=True)
        acc[h]=acc[h]*alpha+dot(vt_ref[h,:,pl.ds(pl.multiple_of(at,half),half)],p.astype(jnp.bfloat16))

    last=hi_ref[i]-1
    for h in range(heads):
        s_even[h]=scores(h,lo_ref[i]*BK)

    def step(j,_):
        at=j*BK
        for h in range(heads):
            s_odd[h]=scores(h,at+half)
            use(h,at,s_even[h])
        for h in range(heads):
            s_even[h]=scores(h,jnp.minimum(j+1,last)*BK)
            use(h,at+half,s_odd[h])
        return 0

    lax.fori_loop(lo_ref[i],hi_ref[i],step,0)
    for h in range(heads):
        o=acc[h]/l_s[h]
        lse_ref[h]=m_s[h]+jnp.log(l_s[h])
        ot_ref[h]=o
        ctx_ref[0,h*HD:(h+1)*HD,:]=o.astype(jnp.bfloat16)


def attend_forward(first,heads,parts,qt,ka,vt,lo,hi,BQ=384,BK=512):
    L=qt.shape[2]
    S=jax.ShapeDtypeStruct
    per=L//parts//BQ
    return pl.pallas_call(functools.partial(forward_body,BK),
        grid_spec=pltpu.PrefetchScalarGridSpec(num_scalar_prefetch=2,grid=(L//BQ,),
        in_specs=[pl.BlockSpec((heads,2*HD,BQ),lambda i,*_:(first//heads,0,i)),pl.BlockSpec((heads,L,2*HD),lambda i,*_:(first//heads,0,0)),pl.BlockSpec((heads,HD,L),lambda i,*_:(first//heads,0,0))],
        out_specs=[pl.BlockSpec((1,heads*HD,BQ),lambda i,*_:(i//per,0,i%per)),pl.BlockSpec((heads,HD,BQ),lambda i,*_:(0,0,i)),pl.BlockSpec((heads,1,BQ),lambda i,*_:(0,0,i))],
        scratch_shapes=[VM((heads,1,BQ),jnp.float32),VM((heads,1,BQ),jnp.float32),VM((heads,HD,BQ),jnp.float32)]+[VM((heads,BK//2,BQ),jnp.float32)]*2),
        out_shape=[S((parts,heads*HD,L//parts),jnp.bfloat16),S((heads,HD,L),jnp.float32),S((heads,1,L),jnp.float32)],
        compiler_params=pltpu.CompilerParams(vmem_limit_bytes=62 << 20),
        cost_estimate=pl.CostEstimate(flops=2*L*L*HD*2*heads,bytes_accessed=L*heads*HD*2*8,transcendentals=L*L*heads),
        name="attend_forward")(lo,hi,qt,ka,vt)


def backward_body(BQ, BK, SUB, lo_ref, hi_ref, go_ref, ot_ref, lse_ref, qt_ref, ka_ref, qn_ref, kt_ref, vn_ref, x_ref, out_ref, wg_ref, sum_ref, got, gon, delta, dqt, dkt, dvt, dk_s, dv_s, x_s, x_sem):
    bring=pltpu.make_async_copy(x_ref,x_s,x_sem)
    bring.start()
    parts,_,rows=go_ref.shape
    heads,_,L=qt_ref.shape
    CH=256
    for h in range(heads):
        for c in range(L//CH):
            p,at=c*CH//rows,c*CH%rows
            gt=go_ref[p,h*HD:(h+1)*HD,at:at+CH]
            wide=gt.astype(jnp.float32)
            got[h,:,c*CH:(c+1)*CH]=gt
            gon[h,c*CH:(c+1)*CH,:]=wide.T.astype(jnp.bfloat16)
            delta[h,:,c*CH:(c+1)*CH]=jnp.sum(wide*ot_ref[h,:,c*CH:(c+1)*CH],axis=0,keepdims=True)
    dqt[...]=jnp.zeros(dqt.shape,jnp.float32)

    def key_block(j,_):
        ka_at=pl.multiple_of(j*BK,BK)
        dk_s[...]=jnp.zeros(dk_s.shape,jnp.float32)
        dv_s[...]=jnp.zeros(dv_s.shape,jnp.float32)

        def query_block(i,_):
            for h,c in [(h,c) for h in range(heads) for c in range(BQ//SUB)]:
                at=pl.multiple_of(i*BQ+c*SUB,SUB)
                s=dot(ka_ref[h,pl.ds(ka_at,BK),:],qt_ref[h,:,pl.ds(at,SUB)])
                p=jnp.exp(s-lse_ref[h,:,pl.ds(at,SUB)])
                dp=dot(vn_ref[h,pl.ds(ka_at,BK),:],got[h,:,pl.ds(at,SUB)])
                ds=(p*(dp-delta[h,:,pl.ds(at,SUB)])).astype(jnp.bfloat16)
                dv_s[h]+=dot(p.astype(jnp.bfloat16),gon[h,pl.ds(at,SUB),:])
                dk_s[h]+=dot(ds,qn_ref[h,pl.ds(at,SUB),:])
                dqt[h,:,pl.ds(at,SUB)]+=dot(kt_ref[h,:,pl.ds(ka_at,BK)],ds)
            return 0

        lax.fori_loop(lo_ref[j],hi_ref[j],query_block,0)
        for h in range(heads):
            dkt[h,:,pl.ds(ka_at,BK)]=dk_s[h].T.astype(jnp.bfloat16)
            dvt[h,:,pl.ds(ka_at,BK)]=dv_s[h].T.astype(jnp.bfloat16)
        return 0

    lax.fori_loop(0,L//BK,key_block,0)
    for h in range(heads):
        for p in range(parts):
            cut=slice(p*rows,(p+1)*rows)
            out_ref[p,3*h*HD:(3*h+1)*HD,:]=(dqt[h,:,cut]*SCALE).astype(jnp.bfloat16)
            out_ref[p,(3*h+1)*HD:(3*h+2)*HD,:]=dkt[h,:,cut]
            out_ref[p,(3*h+2)*HD:(3*h+3)*HD,:]=dvt[h,:,cut]
    bring.wait()
    wg=jnp.zeros(wg_ref.shape[::-1],jnp.float32)
    total=jnp.zeros((3*heads*HD,1),jnp.float32)
    for p in range(parts):
        part=out_ref[p]
        wg=wg+dot(part,x_s[p])
        total=total+jnp.sum(part.astype(jnp.float32),axis=1,keepdims=True)
    wg_ref[...]=wg.T.astype(wg_ref.dtype)
    sum_ref[...]=jnp.broadcast_to(total,sum_ref.shape)


def attend_backward(first,heads,go,go_first,ot,lse,ot_first,qt,ka,qn,kt,vn,x,lo,hi,BQ=512,BK=512,SUB=512):
    parts,_,rows=go.shape; L=parts*rows; D=x.shape[2]
    S=jax.ShapeDtypeStruct; f32=jnp.float32; bf=jnp.bfloat16
    at=lambda a,n: pl.BlockSpec((heads,)+a.shape[1:],lambda i,*_:(n//heads,0,0),pipeline_mode=pl.Buffered(1))
    out=3*heads*HD
    return pl.pallas_call(functools.partial(backward_body,BQ,BK,SUB),
        grid_spec=pltpu.PrefetchScalarGridSpec(num_scalar_prefetch=2,grid=(1,),
        in_specs=[pl.BlockSpec((parts,heads*HD,rows),lambda i,*_:(0,go_first,0),pipeline_mode=pl.Buffered(1)),at(ot,ot_first),at(lse,ot_first)]+[at(a,first) for a in (qt,ka,qn,kt,vn)]+[pl.BlockSpec(memory_space=pl.ANY)],
        out_specs=[pl.BlockSpec((parts,out,rows),lambda i,*_:(0,0,0),pipeline_mode=pl.Buffered(1)),pl.BlockSpec((D,out),lambda i,*_:(0,0)),pl.BlockSpec((out,128),lambda i,*_:(0,0))],
        scratch_shapes=[VM((heads,HD,L),bf),VM((heads,L,HD),bf),VM((heads,1,L),f32),VM((heads,HD,L),f32),VM((heads,HD,L),bf),VM((heads,HD,L),bf),VM((heads,BK,HD),f32),VM((heads,BK,HD),f32),VM(x.shape,bf),pltpu.SemaphoreType.DMA]),
        out_shape=[S((parts,out,rows),bf),S((D,out),bf),S((out,128),f32)],
        compiler_params=pltpu.CompilerParams(vmem_limit_bytes=62 << 20),
        cost_estimate=pl.CostEstimate(flops=2*L*L*HD*5*heads,bytes_accessed=L*heads*HD*2*14,transcendentals=L*L*heads),
        name="attend_backward")(lo,hi,go,ot,lse,qt,ka,qn,kt,vn,x)


def ranges(seg,BQ,BK):
    first=seg.reshape(-1,BQ)[:,0]; last=seg.reshape(-1,BQ)[:,-1]
    kf=seg.reshape(-1,BK)[:,0]; kl=seg.reshape(-1,BK)[:,-1]
    lo=jnp.sum((kl[None,:]<first[:,None]).astype(jnp.int32),1)
    hi=jnp.sum((kf[None,:]<=last[:,None]).astype(jnp.int32),1)
    return lo,hi


def dot_right_t(left, right):
    return lax.dot_general(
        left, right, (((1,), (1,)), ((), ())), preferred_element_type=jnp.float32
    )


def layer_norm(values_in, gain, shift):
    mean_row = jnp.mean(values_in, -1, keepdims=True)
    centered = values_in - mean_row
    inverse = lax.rsqrt(jnp.mean(centered * centered, -1, keepdims=True) + EPS)
    normed = centered * inverse
    return (normed * gain + shift, normed, inverse)


def norm_back(grad_in, normed, inverse, gain):
    scaled = grad_in * gain
    return inverse * (
        scaled
        - jnp.mean(scaled, -1, keepdims=True)
        - normed * jnp.mean(scaled * normed, -1, keepdims=True)
    )


MESH = pl.DeviceIdType.MESH


def flip(index, bit):
    span = 1 << bit
    return index + span * (1 - 2 * ((index // span) % 2))


def start_body(n, bits, x_ref, w_ref, s_ref, x_out, w_out, s_out, send_z, recv_z, send_d, recv_d, keep_sem):
    me = lax.axis_index("tensor")
    mine = lax.axis_index("dp")
    barrier = pltpu.get_barrier_semaphore()

    @pl.when(me > 0)
    def _():
        pl.semaphore_signal(barrier, inc=1, device_id={"tensor": me - 1}, device_id_type=MESH)

    @pl.when(me < n - 1)
    def _():
        pl.semaphore_signal(barrier, inc=1, device_id={"tensor": me + 1}, device_id_type=MESH)

    for bit in range(bits):
        pl.semaphore_signal(barrier, inc=1, device_id={"dp": flip(mine, bit)}, device_id_type=MESH)
    pl.semaphore_wait(barrier, bits + jnp.where(me > 0, 1, 0) + jnp.where(me < n - 1, 1, 0))

    keeps = [
        pltpu.make_async_copy(x_ref, x_out.at[me], keep_sem.at[0]),
        pltpu.make_async_copy(w_ref, w_out.at[me, mine], keep_sem.at[1]),
        pltpu.make_async_copy(s_ref, s_out.at[me], keep_sem.at[2]),
    ]
    for keep in keeps:
        keep.start()

    def hop(kind, side, step):
        block = me - (step - 1) if side else me + (step - 1)
        first, place = (
            (x_ref, x_out.at[block]),
            (w_ref, w_out.at[block, mine]),
            (s_ref, s_out.at[block]),
        )[kind]
        return pltpu.make_async_remote_copy(
            src_ref=first if step == 1 else place,
            dst_ref=place,
            send_sem=send_z.at[kind, side, step - 1],
            recv_sem=recv_z.at[kind, side, step - 1],
            device_id={"tensor": me + 1 if side else me - 1},
            device_id_type=MESH,
        )

    def sends(side, step):
        if side:
            return (me < n - 1) & (me >= step - 1)
        return (me > 0) & (me + step - 1 <= n - 1)

    def receives(side, step):
        return me >= step if side else me + step <= n - 1

    def z_start(kinds, step):
        for side in (0, 1):

            @pl.when(sends(side, step))
            def _():
                for kind in kinds:
                    hop(kind, side, step).start()

    def z_arrive(kinds, step):
        for side in (0, 1):

            @pl.when(receives(side, step))
            def _():
                for kind in kinds:
                    hop(kind, side, step).wait_recv()

    half = w_ref.shape[1] // 2
    up = list(range(bits - 1, -1, -1))
    orders = (up, [up[1], up[0]] + up[2:] if bits > 1 else up)

    def doubling(side, step):
        order = orders[side]
        held = [mine]
        for bit in order[:step]:
            held = held + [flip(d, bit) for d in held]
        cut = pl.ds(side * half, half)
        return [
            pltpu.make_async_remote_copy(
                src_ref=w_out.at[:, d, :, cut],
                dst_ref=w_out.at[:, d, :, cut],
                send_sem=send_d.at[side, (1 << step) - 1 + at],
                recv_sem=recv_d.at[side, (1 << step) - 1 + at],
                device_id={"dp": flip(mine, order[step])},
                device_id_type=MESH,
            )
            for at, d in enumerate(held)
        ]

    def d_start(step):
        for side in (0, 1):
            for copy in doubling(side, step):
                copy.start()

    def d_arrive(step):
        for side in (0, 1):
            for copy in doubling(side, step):
                copy.wait_recv()

    for step in range(1, n):
        z_start((1, 2), step)
        z_arrive((1, 2), step)
    keeps[1].wait()
    for step in range(max(n - 1, bits)):
        if step < bits:
            if step:
                d_arrive(step - 1)
            d_start(step)
        if step < n - 1:
            if step:
                z_arrive((0,), step)
            z_start((0,), step + 1)
    z_arrive((0,), n - 1)
    d_arrive(bits - 1)
    for side in (0, 1):
        for step in range(1, n):

            @pl.when(sends(side, step))
            def _():
                for kind in (0, 1, 2):
                    hop(kind, side, step).wait_send()

        for step in range(bits):
            for copy in doubling(side, step):
                copy.wait_send()
    keeps[0].wait()
    keeps[2].wait()


def start(x, w, small):
    n = lax.axis_size("tensor")
    groups = lax.axis_size("dp")
    bits = groups.bit_length() - 1
    S = jax.ShapeDtypeStruct
    anywhere = pl.BlockSpec(memory_space=pl.ANY)
    return pl.pallas_call(
        functools.partial(start_body, n, bits),
        in_specs=[pl.BlockSpec(memory_space=pltpu.VMEM)] * 3,
        out_specs=[anywhere] * 3,
        out_shape=[
            S((n,) + x.shape, x.dtype),
            S((n, groups) + w.shape, w.dtype),
            S((n,) + small.shape, small.dtype),
        ],
        scratch_shapes=[
            pltpu.SemaphoreType.DMA((3, 2, n - 1)),
            pltpu.SemaphoreType.DMA((3, 2, n - 1)),
            pltpu.SemaphoreType.DMA((2, groups - 1)),
            pltpu.SemaphoreType.DMA((2, groups - 1)),
            pltpu.SemaphoreType.DMA((3,)),
        ],
        compiler_params=pltpu.CompilerParams(collective_id=0, has_side_effects=True),
        cost_estimate=pl.CostEstimate(flops=0, bytes_accessed=200 << 20, transcendentals=0),
        name="start",
    )(x, w, small)


def weight_grads_body(parts, first_ref, second_ref, attn_ref, inner_ref, active_ref, context_ref, out_ref, ft, st):
    j = pl.program_id(0)

    @pl.when(j == 0)
    def _():
        ft[...] = first_ref[...].T
        st[...] = second_ref[...].T

    @pl.when((j < 2 * parts) & (j % 2 == 0))
    def _():
        out_ref[...] = dot(ft[...], inner_ref[0]).astype(out_ref.dtype)

    @pl.when((j < 2 * parts) & (j % 2 == 1))
    def _():
        out_ref[...] = dot(st[...], active_ref[0]).astype(out_ref.dtype)

    @pl.when(j == 2 * parts)
    def _():
        out_ref[...] = dot_right_t(attn_ref[...].T, context_ref[...]).astype(out_ref.dtype)


def weight_grads_of(first_low, second_low, attn_low, grad_inner, active, context):
    parts, rows, units = active.shape
    width = first_low.shape[1]
    features = context.shape[0]
    fixed = pl.BlockSpec((rows, width), lambda j: (0, 0))
    moving = lambda shift: pl.BlockSpec((1, rows, units), lambda j: (jnp.clip((j - shift) // 2, 0, parts - 1), 0, 0))
    return pl.pallas_call(
        functools.partial(weight_grads_body, parts),
        grid=(2 * parts + 1,),
        in_specs=[fixed, fixed, fixed, moving(0), moving(1), pl.BlockSpec((features, rows), lambda j: (0, 0))],
        out_specs=pl.BlockSpec((width, units), lambda j: (0, j)),
        out_shape=jax.ShapeDtypeStruct((width, units * 2 * parts + features), jnp.bfloat16),
        scratch_shapes=[VM((width, rows), jnp.bfloat16), VM((width, rows), jnp.bfloat16)],
        compiler_params=pltpu.CompilerParams(vmem_limit_bytes=62 << 20),
        cost_estimate=pl.CostEstimate(flops=2 * rows * width * (2 * parts * units + features), bytes_accessed=rows * units * 2 * parts * 4, transcendentals=0),
        name="weight_grads",
    )(first_low, second_low, attn_low, grad_inner, active, context)


def erf(x):
    x = jnp.clip(x, -3.7439211627767994, 3.7439211627767994)
    y = x * x
    top = jnp.float32(0.00022905065861350646)
    for c in (0.0034082910107109506, 0.050955695062380861, 0.18520832239976145, 1.128379143519084):
        top = top * y + c
    low = jnp.float32(-1.1791602954361697e-7)
    for c in (0.000023547966471313185, 0.0010179625278914885, 0.014070470171167667, 0.11098505178285362, 0.49746925110067538, 1.0):
        low = low * y + c
    return x * top / low


def dense_body(own, x_ref, cot_ref, ctx0_ref, ctx1_ref, vec_ref, bias_ref, near_ref, far_ref, out_ref, first_ref, second_ref, attn_ref, grad_ref, active_ref, inner_ref, ctx_ref, go0_ref, go1_ref, sum_ref, w_s, mt_s, slope_s, first_s, acc_s, even_s, odd_s, w_sem):
    i = pl.program_id(0)
    parts, _, _ = near_ref.shape
    f32, bf = jnp.float32, jnp.bfloat16
    units = active_ref.shape[2]
    cuts = (slice(0, 4 * own), slice(4 * own, 4 * own + units), slice(4 * own + units, 4 * own + 2 * units))
    sources = (near_ref.at[:, :, cuts[0]], near_ref.at[:, :, cuts[1]], far_ref)
    copies = [pltpu.make_async_copy(sources[c], w_s.at[:, :, cut], w_sem.at[c]) for c, cut in enumerate(cuts)]

    @pl.when(i == 0)
    def _():
        for copy in copies:
            copy.start()
        sum_ref[...] = jnp.zeros(sum_ref.shape, f32)
        copies[0].wait()
        for t in range(parts):
            mt_s[:, t * own : (t + 1) * own] = w_s[t, :, 3 * own : 4 * own]

    def add_sum(row, value):
        sum_ref[row : row + 1, :] += jnp.sum(value, axis=0, keepdims=True)

    for t in range(parts):
        lead = ctx0_ref.shape[1]
        ctx_ref[t * own : t * own + lead, :] = ctx0_ref[t]
        ctx_ref[t * own + lead : (t + 1) * own, :] = ctx1_ref[t]
    mixed = dot(mt_s[...], ctx_ref[...]).T
    attn_in = x_ref[...].astype(f32) + mixed + vec_ref[0:1]
    first, first_norm, first_inv = layer_norm(attn_in, vec_ref[1:2], vec_ref[2:3])
    first_ref[...] = first.astype(bf)
    first_s[...] = first_norm
    acc_s[...] = first + vec_ref[3:4]

    @pl.when(i == 0)
    def _():
        copies[1].wait()
        copies[2].wait()

    half_units = units // 2
    first_cut, second_cut = slice(0, half_units), slice(half_units, units)
    base = 4 * own

    def before(t, cut):
        return dot(first_ref[...], w_s[t, :, base + cut.start : base + cut.stop]) + bias_ref[t, :, cut]

    def after(t, cut, inner):
        half = 0.5 * (1.0 + erf(inner * ROOT_HALF))
        slope_s[t, :, cut] = half + inner * jnp.exp(-0.5 * inner * inner) * INV_ROOT_TWO_PI
        active = (inner * half).astype(bf)
        active_ref[t, :, cut] = active
        acc_s[...] += dot_right_t(active, w_s[t, :, base + units + cut.start : base + units + cut.stop])

    even_s[...] = before(0, first_cut)

    def ahead(t, _):
        odd_s[...] = before(t, second_cut)
        after(t, first_cut, even_s[...])
        even_s[...] = before(jnp.minimum(t + 1, parts - 1), first_cut)
        after(t, second_cut, odd_s[...])
        return 0

    lax.fori_loop(0, parts, ahead, 0)
    second, second_norm, second_inv = layer_norm(acc_s[...], vec_ref[4:5], vec_ref[5:6])
    out_ref[...] = second.astype(bf)
    grad_out = cot_ref[...].astype(f32)
    add_sum(4, grad_out * second_norm)
    add_sum(5, grad_out)
    grad_second = norm_back(grad_out, second_norm, second_inv, vec_ref[4:5])
    add_sum(3, grad_second)
    second_ref[...] = grad_second.astype(bf)
    acc_s[...] = grad_second

    def back(t, _):
        grad_inner = (dot(second_ref[...], w_s[t, :, cuts[2]]) * slope_s[t]).astype(bf)
        inner_ref[t] = grad_inner
        sum_ref[pl.ds(6 + t, 1), :] += jnp.sum(grad_inner.astype(f32), axis=0, keepdims=True)
        acc_s[...] += dot_right_t(grad_inner, w_s[t, :, cuts[1]])
        return 0

    lax.fori_loop(0, parts, back, 0)
    grad_first = acc_s[...]
    first_norm = first_s[...]
    add_sum(1, grad_first * first_norm)
    add_sum(2, grad_first)
    grad_attn = norm_back(grad_first, first_norm, first_inv, vec_ref[1:2])
    add_sum(0, grad_attn)
    grad_ref[...] = grad_attn
    attn_ref[...] = grad_attn.astype(bf)
    grad_context = dot(attn_ref[...], mt_s[...]).T.astype(bf)
    for t in range(parts):
        go0_ref[t] = grad_context[t * own : t * own + HD]
        go1_ref[t] = grad_context[t * own + HD : (t + 1) * own]


def dense(own, x, cot, ctx0, ctx1, vectors, inner_bias, near, far, block):
    rows, width = x.shape
    parts = near.shape[0]
    units = far.shape[2]
    cols = 4 * own + 2 * units
    f32, bf = jnp.float32, jnp.bfloat16
    S = jax.ShapeDtypeStruct
    tok = pl.BlockSpec((block, width), lambda i: (i, 0))
    part_tok = pl.BlockSpec((parts, block, units), lambda i: (0, i, 0))
    lanes = lambda n: pl.BlockSpec((parts, n, block), lambda i: (0, 0, i))
    fixed = lambda a: pl.BlockSpec(a.shape, lambda i: (0,) * a.ndim)
    inner_bias = inner_bias.reshape(parts, 1, units)
    return pl.pallas_call(
        functools.partial(dense_body, own),
        grid=(rows // block,),
        in_specs=[tok, tok, lanes(ctx0.shape[1]), lanes(ctx1.shape[1]), fixed(vectors), fixed(inner_bias), pl.BlockSpec(memory_space=pl.ANY), pl.BlockSpec(memory_space=pl.ANY)],
        out_specs=[tok] * 5 + [part_tok] * 2 + [pl.BlockSpec((parts * own, block), lambda i: (0, i)), lanes(HD), lanes(own - HD), pl.BlockSpec((16, width), lambda i: (0, 0))],
        out_shape=[S((rows, width), bf)] * 4 + [S((rows, width), f32)] + [S((parts, rows, units), bf)] * 2 + [S((parts * own, rows), bf), S((parts, HD, rows), bf), S((parts, own - HD, rows), bf), S((16, width), f32)],
        scratch_shapes=[VM((parts, width, cols), bf), VM((width, parts * own), bf), VM((parts, block, units), f32), VM((block, width), f32), VM((block, width), f32), VM((block, units // 2), f32), VM((block, units // 2), f32), pltpu.SemaphoreType.DMA((3,))],
        compiler_params=pltpu.CompilerParams(vmem_limit_bytes=62 << 20),
        cost_estimate=pl.CostEstimate(flops=4 * rows * width * (2 * parts * units + parts * own), bytes_accessed=40 << 20, transcendentals=rows * units * parts),
        name="dense",
    )(x, cot, ctx0, ctx1, vectors, inner_bias, near, far)


def early_back_body(w_ref, b0_ref, b1_ref, acc_ref):
    width = b0_ref.shape[1]
    acc_ref[...] = jnp.zeros(acc_ref.shape, jnp.float32)

    def add(t, _):
        both = jnp.concatenate([b0_ref[t], b1_ref[t]], axis=0)
        acc_ref[...] += dot(w_ref[t, :, : 2 * width], both)
        return 0

    lax.fori_loop(0, b0_ref.shape[0], add, 0)


def late_back_body(cut, part_ref, w_ref, acc_ref, grad_ref, *rest):
    backs, out_ref = rest[:-1], rest[-1]
    parts = len(backs)
    total = acc_ref[...]
    for d in range(parts):
        total = total + dot(w_ref[(part_ref[0] + parts - d) % parts, :, cut : cut + backs[d].shape[0]], backs[d][...])
    out_ref[...] = (total.T + grad_ref[...]).astype(out_ref.dtype)


def weight_block(rest, cols):
    return pl.BlockSpec(rest.shape[:2] + (cols,), lambda i, *_: (0, 0, 0), pipeline_mode=pl.Buffered(1))


def whole(a):
    return pl.BlockSpec(a.shape, lambda i, *_: (0,) * a.ndim, pipeline_mode=pl.Buffered(1))


def early_back(rest, cols, b0, b1):
    width, rows = rest.shape[1], b0.shape[2]
    return pl.pallas_call(
        early_back_body,
        grid=(1,),
        in_specs=[weight_block(rest, cols), whole(b0), whole(b1)],
        out_specs=pl.BlockSpec((width, rows), lambda i: (0, 0)),
        out_shape=jax.ShapeDtypeStruct((width, rows), jnp.float32),
        compiler_params=pltpu.CompilerParams(vmem_limit_bytes=62 << 20),
        cost_estimate=pl.CostEstimate(flops=4 * width * rows * b0.shape[0] * b0.shape[1], bytes_accessed=10 << 20, transcendentals=0),
        name="early_back",
    )(rest, b0, b1)


def late_back(rest, cols, cut, part, acc, grad, backs):
    rows, width = grad.shape
    return pl.pallas_call(
        functools.partial(late_back_body, cut),
        grid_spec=pltpu.PrefetchScalarGridSpec(
            num_scalar_prefetch=1,
            grid=(1,),
            in_specs=[weight_block(rest, cols), whole(acc), whole(grad)] + [whole(b) for b in backs],
            out_specs=pl.BlockSpec((rows, width), lambda i, *_: (0, 0)),
        ),
        out_shape=jax.ShapeDtypeStruct((rows, width), jnp.bfloat16),
        compiler_params=pltpu.CompilerParams(vmem_limit_bytes=62 << 20),
        cost_estimate=pl.CostEstimate(flops=2 * width * rows * backs[0].shape[0] * len(backs), bytes_accessed=10 << 20, transcendentals=0),
        name="late_back",
    )(part.reshape(1), rest, acc, grad, *backs)


def add_up(value):
    for axis in ("dp", "tensor"):
        size = lax.axis_size(axis)
        span = 1
        while span < size:
            other = lax.ppermute(value, axis, [(i, i ^ span) for i in range(size)])
            value = value + other
            span *= 2
    return value


def rotate(blocks, axis):
    size = lax.axis_size(axis)
    me = lax.axis_index(axis)
    out = []
    for d in range(size):
        block = lax.dynamic_index_in_dim(blocks, (me + d) % size, 0, keepdims=False)
        if d:
            block = lax.ppermute(block, axis, [(i, (i + d) % size) for i in range(size)])
        out.append(block)
    return out


def body(hidden_in, segments, query_weight, key_weight, value_weight, query_bias, value_bias, mixer_weight, mixer_bias, first_gain, first_shift, inner_weight, inner_bias, outer_weight, outer_bias, second_gain, second_shift, cotangent):
    bf = jnp.bfloat16
    f32 = jnp.float32
    _, rows, width = hidden_in.shape
    parts = lax.axis_size("tensor")
    groups = lax.axis_size("dp")
    rank = lax.axis_index("tensor")
    own = query_weight.shape[1]
    heads = own // HD
    three = 3 * HD
    units = inner_weight.shape[1]
    by_head = lambda q, k, v: jnp.stack([a.reshape(a.shape[:-1] + (heads, HD)) for a in (q, k, v)], -2).reshape(q.shape[:-1] + (3 * own,))
    x_own = hidden_in[0]
    qkv_own = by_head(query_weight, key_weight, value_weight)
    small = jnp.concatenate([segments[0].astype(f32), inner_bias]).reshape(-1, 128)
    near_own = jnp.concatenate([qkv_own, mixer_weight.T, inner_weight], 1)
    x_parts, near, small = start(x_own, near_own, small)
    x_all = x_parts.reshape(parts * rows, width)
    near = near.reshape(parts, width, 4 * own + units)
    far_own = outer_weight.T
    far_own, small = lax.optimization_barrier((far_own, small))
    far = lax.all_gather(far_own, ("tensor", "dp"), axis=0, tiled=True).reshape(parts, width, units)
    small = small.reshape(parts, -1)
    segment_all = small[:, :rows].astype(jnp.int32).reshape(-1)
    inner_bias_all = small[:, rows:]
    biases = by_head(query_bias, jnp.zeros_like(query_bias), value_bias)

    qt, ka, vt, qn, kt, vn = project(x_all, near, rank, biases, segment_all)
    lead = heads - 1
    context_t, lse, exchanged = [], [], []
    for call, (first, count, block) in enumerate(((0, lead, rows // 2), (lead, 1, rows))):
        lo, hi = ranges(segment_all, block, 512)
        part, out_t, out_lse = attend_forward(first, count, parts, qt, ka, vt, lo, hi, BQ=block)
        context_t.append(out_t)
        lse.append(out_lse)
        if exchanged:
            part, exchanged[-1] = lax.optimization_barrier((part, exchanged[-1]))
        exchanged.append(lax.all_to_all(part, "tensor", 0, 0, tiled=True))
    vectors = jnp.stack([mixer_bias, first_gain, first_shift, outer_bias, second_gain, second_shift])
    vectors = jnp.pad(vectors, ((0, 2), (0, 0)))
    layer_out, first_low, second_low, attn_low, grad_attn, active, grad_inner, context, go0, go1, early = dense(
        own, x_own, cotangent[0], exchanged[0], exchanged[1], vectors, inner_bias_all, near, far, block=rows // 2
    )
    go0 = lax.all_to_all(go0, "tensor", 0, 0, tiled=True)
    go1 = lax.all_to_all(go1, "tensor", 0, 0, tiled=True)
    weight_grads = weight_grads_of(
        first_low, second_low, attn_low, grad_inner, active, context
    )
    weight_grads = lax.psum_scatter(weight_grads, "dp", scatter_dimension=0, tiled=True)
    weight_grads = jnp.concatenate(
        [
            weight_grads[:, : 2 * units * parts].reshape(-1, parts, 2 * units),
            weight_grads[:, 2 * units * parts :].reshape(-1, parts, own),
        ],
        2,
    ).transpose(1, 0, 2)
    weight_grads = rotate(weight_grads, "tensor")
    weight_grads = sum(a.astype(f32) for a in weight_grads)
    early = add_up(early)

    lo, hi = ranges(segment_all, 512, 512)
    backs, qkv_grad, bias_grad = [], [], []
    for h in range(heads):
        call = 0 if h < lead else 1
        grads, weight_part, sums = attend_backward(
            h, 1, go1 if h else go0, h - 1 if h else 0, context_t[call], lse[call], h - call * lead, qt, ka, qn, kt, vn, x_parts, lo, hi
        )
        if h < heads - 1:
            backs.append(lax.all_to_all(grads, "tensor", 0, 0, tiled=True))
        else:
            backs.append(rotate(grads, "tensor"))
        qkv_grad.append(weight_part)
        bias_grad.append(sums[:, 0])
    input_back = early_back(near, 4 * own, backs[0], backs[1])
    input_grad = late_back(near, 4 * own, 2 * three, rank, input_back, grad_attn, backs[2])
    bias_grad = jnp.concatenate(bias_grad)
    high = bias_grad.astype(bf)
    low = (bias_grad - high.astype(f32)).astype(bf)
    each = width // groups
    qkv_grad = jnp.concatenate(qkv_grad, 1).reshape(groups, each, 3 * own)
    extra = jnp.pad(jnp.stack([high, low]), ((0, 14), (0, 0)))
    extra = jnp.broadcast_to(extra[None], (groups, 16, 3 * own))
    qkv_grad = lax.all_to_all(jnp.concatenate([qkv_grad, extra], 1), "dp", 0, 0, tiled=True)
    qkv_grad = jnp.sum(qkv_grad.astype(f32), 0)
    bias_grad = qkv_grad[each] + qkv_grad[each + 1]
    pick = lambda a, n: a.reshape(a.shape[:-1] + (heads, 3, HD))[..., n, :].reshape(a.shape[:-1] + (own,))
    inner_bias_out = lax.dynamic_index_in_dim(early, 6 + rank, 0, keepdims=False)
    return (
        layer_out[None],
        input_grad[None],
        pick(qkv_grad[:each], 0),
        pick(qkv_grad[:each], 1),
        pick(qkv_grad[:each], 2),
        pick(bias_grad, 0),
        pick(bias_grad, 2),
        weight_grads[:, 2 * units :].T,
        early[0],
        early[1],
        early[2],
        weight_grads[:, :units],
        inner_bias_out,
        weight_grads[:, units : 2 * units].T,
        early[3],
        early[4],
        early[5],
    )


def solution(mesh):
    placed = (
        P("dp", "tensor", None),
        P("dp", "tensor"),
        P("dp", "tensor"),
        P("dp", "tensor"),
        P("dp", "tensor"),
        P("tensor"),
        P("tensor"),
        P("tensor", "dp"),
        P(),
        P(),
        P(),
        P("dp", "tensor"),
        P("tensor"),
        P("tensor", "dp"),
        P(),
        P(),
        P(),
        P("dp", "tensor", None),
    )

    return jax.shard_map(
        body,
        mesh=mesh,
        in_specs=placed,
        out_specs=(
            P("dp", "tensor", None),
            P("dp", "tensor", None),
            P("dp", "tensor"),
            P("dp", "tensor"),
            P("dp", "tensor"),
            P("tensor"),
            P("tensor"),
            P("tensor", "dp"),
            P(),
            P(),
            P(),
            P("dp", "tensor"),
            P("tensor"),
            P("tensor", "dp"),
            P(),
            P(),
            P(),
        ),
        check_vma=False,
    )
```

```python
import functools

import jax
import jax.numpy as jnp
from jax import lax
from jax.experimental import pallas as pl
from jax.experimental.pallas import tpu as pltpu
from jax.sharding import PartitionSpec as P


EPS = 1e-12
ROOT_HALF = 0.7071067811865476
INV_ROOT_TWO_PI = 0.3989422804014327
HD=64; SCALE=0.125; APART=-1e30
VM=pltpu.VMEM


def dot(a,b): return jnp.dot(a,b,preferred_element_type=jnp.float32)


def project_body(heads, part_ref, x_ref, w_ref, b_ref, srow_ref, qt_ref, ka_ref, vt_ref, qn_ref, kt_ref, vn_ref):
    y=dot(x_ref[...], w_ref[0,:,:b_ref.shape[1]]) + b_ref[...]
    low = y.astype(jnp.bfloat16)
    yt = low.T
    rows = y.shape[0]
    match = lax.broadcasted_iota(jnp.int32,(HD,rows),0)==srow_ref[...]
    apart = jnp.where(match,0.0,APART).astype(jnp.bfloat16)
    same = jnp.where(match,1.0,0.0).T.astype(jnp.bfloat16)
    for h in range(heads):
        at=3*h*HD
        qt_ref[h,:HD,:]=yt[at:at+HD]*jnp.bfloat16(SCALE)
        qt_ref[h,HD:,:]=apart
        qn_ref[h]=low[:,at:at+HD]*jnp.bfloat16(SCALE)
        ka_ref[h]=jnp.concatenate([low[:,at+HD:at+2*HD],same],axis=1)
        kt_ref[h]=yt[at+HD:at+2*HD]
        vt_ref[h]=yt[at+2*HD:at+3*HD]
        vn_ref[h]=low[:,at+2*HD:at+3*HD]


def project(x,rest,part,b,seg,rows=512):
    L,D=x.shape; heads=b.shape[0]//(3*HD)
    bf=jnp.bfloat16
    cols=4*heads*HD
    nat=lambda n: pl.BlockSpec((heads,rows,n),lambda i,*_:(0,i,0))
    tr=lambda n: pl.BlockSpec((heads,n,rows),lambda i,*_:(0,0,i))
    S=jax.ShapeDtypeStruct
    return pl.pallas_call(functools.partial(project_body,heads),
        grid_spec=pltpu.PrefetchScalarGridSpec(num_scalar_prefetch=1,grid=(L//rows,),
        in_specs=[pl.BlockSpec((rows,D),lambda i,*_:(i,0)),pl.BlockSpec((1,D,cols),lambda i,p:(p[0],0,0)),pl.BlockSpec((1,b.shape[0]),lambda i,*_:(0,0)),
                  pl.BlockSpec((1,rows),lambda i,*_:(0,i))],
        out_specs=[tr(2*HD),nat(2*HD),tr(HD),nat(HD),tr(HD),nat(HD)]),
        out_shape=[S((heads,2*HD,L),bf),S((heads,L,2*HD),bf),S((heads,HD,L),bf),S((heads,L,HD),bf),S((heads,HD,L),bf),S((heads,L,HD),bf)],
        compiler_params=pltpu.CompilerParams(vmem_limit_bytes=62 << 20),
        cost_estimate=pl.CostEstimate(flops=2*L*D*b.shape[0],bytes_accessed=L*D*2+D*cols*2+L*heads*HD*2*10,transcendentals=0),
        name="project")(part.reshape(1),x,rest,b.reshape(1,-1),seg.reshape(1,-1))


def forward_body(BK, lo_ref, hi_ref, qt_ref, ka_ref, vt_ref, ctx_ref, ot_ref, lse_ref, m_s, l_s, acc, s_even, s_odd):
    i=pl.program_id(0)
    heads=qt_ref.shape[0]
    half=BK//2
    m_s[...]=jnp.full(m_s.shape,-jnp.inf,jnp.float32)
    l_s[...]=jnp.zeros(l_s.shape,jnp.float32)
    acc[...]=jnp.zeros(acc.shape,jnp.float32)

    def scores(h,at):
        return dot(ka_ref[h,pl.ds(pl.multiple_of(at,half),half),:],qt_ref[h])

    def use(h,at,s):
        m_old=m_s[h]
        m_new=jnp.maximum(m_old,jnp.max(s,axis=0,keepdims=True))
        p=jnp.exp(s-m_new)
        alpha=jnp.exp(m_old-m_new)
        m_s[h]=m_new
        l_s[h]=l_s[h]*alpha+jnp.sum(p,axis=0,keepdims=True)
        acc[h]=acc[h]*alpha+dot(vt_ref[h,:,pl.ds(pl.multiple_of(at,half),half)],p.astype(jnp.bfloat16))

    last=hi_ref[i]-1
    for h in range(heads):
        s_even[h]=scores(h,lo_ref[i]*BK)

    def step(j,_):
        at=j*BK
        for h in range(heads):
            s_odd[h]=scores(h,at+half)
            use(h,at,s_even[h])
        for h in range(heads):
            s_even[h]=scores(h,jnp.minimum(j+1,last)*BK)
            use(h,at+half,s_odd[h])
        return 0

    lax.fori_loop(lo_ref[i],hi_ref[i],step,0)
    for h in range(heads):
        o=acc[h]/l_s[h]
        lse_ref[h]=m_s[h]+jnp.log(l_s[h])
        ot_ref[h]=o
        ctx_ref[0,h*HD:(h+1)*HD,:]=o.astype(jnp.bfloat16)


def attend_forward(first,heads,parts,qt,ka,vt,lo,hi,BQ=384,BK=512):
    L=qt.shape[2]
    S=jax.ShapeDtypeStruct
    per=L//parts//BQ
    return pl.pallas_call(functools.partial(forward_body,BK),
        grid_spec=pltpu.PrefetchScalarGridSpec(num_scalar_prefetch=2,grid=(L//BQ,),
        in_specs=[pl.BlockSpec((heads,2*HD,BQ),lambda i,*_:(first//heads,0,i)),pl.BlockSpec((heads,L,2*HD),lambda i,*_:(first//heads,0,0)),pl.BlockSpec((heads,HD,L),lambda i,*_:(first//heads,0,0))],
        out_specs=[pl.BlockSpec((1,heads*HD,BQ),lambda i,*_:(i//per,0,i%per)),pl.BlockSpec((heads,HD,BQ),lambda i,*_:(0,0,i)),pl.BlockSpec((heads,1,BQ),lambda i,*_:(0,0,i))],
        scratch_shapes=[VM((heads,1,BQ),jnp.float32),VM((heads,1,BQ),jnp.float32),VM((heads,HD,BQ),jnp.float32)]+[VM((heads,BK//2,BQ),jnp.float32)]*2),
        out_shape=[S((parts,heads*HD,L//parts),jnp.bfloat16),S((heads,HD,L),jnp.float32),S((heads,1,L),jnp.float32)],
        compiler_params=pltpu.CompilerParams(vmem_limit_bytes=62 << 20),
        cost_estimate=pl.CostEstimate(flops=2*L*L*HD*2*heads,bytes_accessed=L*heads*HD*2*8,transcendentals=L*L*heads),
        name="attend_forward")(lo,hi,qt,ka,vt)


def backward_body(BQ, BK, SUB, lo_ref, hi_ref, go_ref, ot_ref, lse_ref, qt_ref, ka_ref, qn_ref, kt_ref, vn_ref, x_ref, out_ref, wg_ref, sum_ref, got, gon, delta, dqt, dkt, dvt, dk_s, dv_s, x_s, x_sem):
    bring=pltpu.make_async_copy(x_ref,x_s,x_sem)
    bring.start()
    parts,_,rows=go_ref.shape
    heads,_,L=qt_ref.shape
    CH=256
    for h in range(heads):
        for c in range(L//CH):
            p,at=c*CH//rows,c*CH%rows
            gt=go_ref[p,h*HD:(h+1)*HD,at:at+CH]
            wide=gt.astype(jnp.float32)
            got[h,:,c*CH:(c+1)*CH]=gt
            gon[h,c*CH:(c+1)*CH,:]=wide.T.astype(jnp.bfloat16)
            delta[h,:,c*CH:(c+1)*CH]=jnp.sum(wide*ot_ref[h,:,c*CH:(c+1)*CH],axis=0,keepdims=True)
    dqt[...]=jnp.zeros(dqt.shape,jnp.float32)

    def key_block(j,_):
        ka_at=pl.multiple_of(j*BK,BK)
        dk_s[...]=jnp.zeros(dk_s.shape,jnp.float32)
        dv_s[...]=jnp.zeros(dv_s.shape,jnp.float32)

        def query_block(i,_):
            for h,c in [(h,c) for h in range(heads) for c in range(BQ//SUB)]:
                at=pl.multiple_of(i*BQ+c*SUB,SUB)
                s=dot(ka_ref[h,pl.ds(ka_at,BK),:],qt_ref[h,:,pl.ds(at,SUB)])
                p=jnp.exp(s-lse_ref[h,:,pl.ds(at,SUB)])
                dp=dot(vn_ref[h,pl.ds(ka_at,BK),:],got[h,:,pl.ds(at,SUB)])
                ds=(p*(dp-delta[h,:,pl.ds(at,SUB)])).astype(jnp.bfloat16)
                dv_s[h]+=dot(p.astype(jnp.bfloat16),gon[h,pl.ds(at,SUB),:])
                dk_s[h]+=dot(ds,qn_ref[h,pl.ds(at,SUB),:])
                dqt[h,:,pl.ds(at,SUB)]+=dot(kt_ref[h,:,pl.ds(ka_at,BK)],ds)
            return 0

        lax.fori_loop(lo_ref[j],hi_ref[j],query_block,0)
        for h in range(heads):
            dkt[h,:,pl.ds(ka_at,BK)]=dk_s[h].T.astype(jnp.bfloat16)
            dvt[h,:,pl.ds(ka_at,BK)]=dv_s[h].T.astype(jnp.bfloat16)
        return 0

    lax.fori_loop(0,L//BK,key_block,0)
    for h in range(heads):
        for p in range(parts):
            cut=slice(p*rows,(p+1)*rows)
            out_ref[p,3*h*HD:(3*h+1)*HD,:]=(dqt[h,:,cut]*SCALE).astype(jnp.bfloat16)
            out_ref[p,(3*h+1)*HD:(3*h+2)*HD,:]=dkt[h,:,cut]
            out_ref[p,(3*h+2)*HD:(3*h+3)*HD,:]=dvt[h,:,cut]
    bring.wait()
    wg=jnp.zeros(wg_ref.shape[::-1],jnp.float32)
    total=jnp.zeros((3*heads*HD,1),jnp.float32)
    for p in range(parts):
        part=out_ref[p]
        wg=wg+dot(part,x_s[p])
        total=total+jnp.sum(part.astype(jnp.float32),axis=1,keepdims=True)
    wg_ref[...]=wg.T.astype(wg_ref.dtype)
    sum_ref[...]=jnp.broadcast_to(total,sum_ref.shape)


def attend_backward(first,heads,go,go_first,ot,lse,ot_first,qt,ka,qn,kt,vn,x,lo,hi,BQ=512,BK=512,SUB=512):
    parts,_,rows=go.shape; L=parts*rows; D=x.shape[2]
    S=jax.ShapeDtypeStruct; f32=jnp.float32; bf=jnp.bfloat16
    at=lambda a,n: pl.BlockSpec((heads,)+a.shape[1:],lambda i,*_:(n//heads,0,0),pipeline_mode=pl.Buffered(1))
    out=3*heads*HD
    return pl.pallas_call(functools.partial(backward_body,BQ,BK,SUB),
        grid_spec=pltpu.PrefetchScalarGridSpec(num_scalar_prefetch=2,grid=(1,),
        in_specs=[pl.BlockSpec((parts,heads*HD,rows),lambda i,*_:(0,go_first,0),pipeline_mode=pl.Buffered(1)),at(ot,ot_first),at(lse,ot_first)]+[at(a,first) for a in (qt,ka,qn,kt,vn)]+[pl.BlockSpec(memory_space=pl.ANY)],
        out_specs=[pl.BlockSpec((parts,out,rows),lambda i,*_:(0,0,0),pipeline_mode=pl.Buffered(1)),pl.BlockSpec((D,out),lambda i,*_:(0,0)),pl.BlockSpec((out,128),lambda i,*_:(0,0))],
        scratch_shapes=[VM((heads,HD,L),bf),VM((heads,L,HD),bf),VM((heads,1,L),f32),VM((heads,HD,L),f32),VM((heads,HD,L),bf),VM((heads,HD,L),bf),VM((heads,BK,HD),f32),VM((heads,BK,HD),f32),VM(x.shape,bf),pltpu.SemaphoreType.DMA]),
        out_shape=[S((parts,out,rows),bf),S((D,out),bf),S((out,128),f32)],
        compiler_params=pltpu.CompilerParams(vmem_limit_bytes=62 << 20),
        cost_estimate=pl.CostEstimate(flops=2*L*L*HD*5*heads,bytes_accessed=L*heads*HD*2*14,transcendentals=L*L*heads),
        name="attend_backward")(lo,hi,go,ot,lse,qt,ka,qn,kt,vn,x)


def ranges(seg,BQ,BK):
    first=seg.reshape(-1,BQ)[:,0]; last=seg.reshape(-1,BQ)[:,-1]
    kf=seg.reshape(-1,BK)[:,0]; kl=seg.reshape(-1,BK)[:,-1]
    lo=jnp.sum((kl[None,:]<first[:,None]).astype(jnp.int32),1)
    hi=jnp.sum((kf[None,:]<=last[:,None]).astype(jnp.int32),1)
    return lo,hi


def dot_right_t(left, right):
    return lax.dot_general(
        left, right, (((1,), (1,)), ((), ())), preferred_element_type=jnp.float32
    )


def layer_norm(values_in, gain, shift):
    mean_row = jnp.mean(values_in, -1, keepdims=True)
    centered = values_in - mean_row
    inverse = lax.rsqrt(jnp.mean(centered * centered, -1, keepdims=True) + EPS)
    normed = centered * inverse
    return (normed * gain + shift, normed, inverse)


def norm_back(grad_in, normed, inverse, gain):
    scaled = grad_in * gain
    return inverse * (
        scaled
        - jnp.mean(scaled, -1, keepdims=True)
        - normed * jnp.mean(scaled * normed, -1, keepdims=True)
    )


MESH = pl.DeviceIdType.MESH


def flip(index, bit):
    span = 1 << bit
    return index + span * (1 - 2 * ((index // span) % 2))


def start_body(n, bits, x_ref, w_ref, s_ref, x_out, w_out, s_out, send_z, recv_z, send_d, recv_d, keep_sem):
    me = lax.axis_index("tensor")
    mine = lax.axis_index("dp")
    barrier = pltpu.get_barrier_semaphore()

    @pl.when(me > 0)
    def _():
        pl.semaphore_signal(barrier, inc=1, device_id={"tensor": me - 1}, device_id_type=MESH)

    @pl.when(me < n - 1)
    def _():
        pl.semaphore_signal(barrier, inc=1, device_id={"tensor": me + 1}, device_id_type=MESH)

    for bit in range(bits):
        pl.semaphore_signal(barrier, inc=1, device_id={"dp": flip(mine, bit)}, device_id_type=MESH)
    pl.semaphore_wait(barrier, bits + jnp.where(me > 0, 1, 0) + jnp.where(me < n - 1, 1, 0))

    keeps = [
        pltpu.make_async_copy(x_ref, x_out.at[me], keep_sem.at[0]),
        pltpu.make_async_copy(w_ref, w_out.at[me, mine], keep_sem.at[1]),
        pltpu.make_async_copy(s_ref, s_out.at[me], keep_sem.at[2]),
    ]
    for keep in keeps:
        keep.start()

    def hop(kind, side, step):
        block = me - (step - 1) if side else me + (step - 1)
        first, place = (
            (x_ref, x_out.at[block]),
            (w_ref, w_out.at[block, mine]),
            (s_ref, s_out.at[block]),
        )[kind]
        return pltpu.make_async_remote_copy(
            src_ref=first if step == 1 else place,
            dst_ref=place,
            send_sem=send_z.at[kind, side, step - 1],
            recv_sem=recv_z.at[kind, side, step - 1],
            device_id={"tensor": me + 1 if side else me - 1},
            device_id_type=MESH,
        )

    def sends(side, step):
        if side:
            return (me < n - 1) & (me >= step - 1)
        return (me > 0) & (me + step - 1 <= n - 1)

    def receives(side, step):
        return me >= step if side else me + step <= n - 1

    def z_start(kinds, step):
        for side in (0, 1):

            @pl.when(sends(side, step))
            def _():
                for kind in kinds:
                    hop(kind, side, step).start()

    def z_arrive(kinds, step):
        for side in (0, 1):

            @pl.when(receives(side, step))
            def _():
                for kind in kinds:
                    hop(kind, side, step).wait_recv()

    half = w_ref.shape[1] // 2
    up = list(range(bits - 1, -1, -1))
    orders = (up, [up[1], up[0]] + up[2:] if bits > 1 else up)

    def doubling(side, step):
        order = orders[side]
        held = [mine]
        for bit in order[:step]:
            held = held + [flip(d, bit) for d in held]
        cut = pl.ds(side * half, half)
        return [
            pltpu.make_async_remote_copy(
                src_ref=w_out.at[:, d, :, cut],
                dst_ref=w_out.at[:, d, :, cut],
                send_sem=send_d.at[side, (1 << step) - 1 + at],
                recv_sem=recv_d.at[side, (1 << step) - 1 + at],
                device_id={"dp": flip(mine, order[step])},
                device_id_type=MESH,
            )
            for at, d in enumerate(held)
        ]

    def d_start(step):
        for side in (0, 1):
            for copy in doubling(side, step):
                copy.start()

    def d_arrive(step):
        for side in (0, 1):
            for copy in doubling(side, step):
                copy.wait_recv()

    for step in range(1, n):
        z_start((1, 2), step)
        z_arrive((1, 2), step)
    keeps[1].wait()
    for step in range(max(n - 1, bits)):
        if step < bits:
            if step:
                d_arrive(step - 1)
            d_start(step)
        if step < n - 1:
            if step:
                z_arrive((0,), step)
            z_start((0,), step + 1)
    z_arrive((0,), n - 1)
    d_arrive(bits - 1)
    for side in (0, 1):
        for step in range(1, n):

            @pl.when(sends(side, step))
            def _():
                for kind in (0, 1, 2):
                    hop(kind, side, step).wait_send()

        for step in range(bits):
            for copy in doubling(side, step):
                copy.wait_send()
    keeps[0].wait()
    keeps[2].wait()


def start(x, w, small):
    n = lax.axis_size("tensor")
    groups = lax.axis_size("dp")
    bits = groups.bit_length() - 1
    S = jax.ShapeDtypeStruct
    anywhere = pl.BlockSpec(memory_space=pl.ANY)
    return pl.pallas_call(
        functools.partial(start_body, n, bits),
        in_specs=[pl.BlockSpec(memory_space=pltpu.VMEM)] * 3,
        out_specs=[anywhere] * 3,
        out_shape=[
            S((n,) + x.shape, x.dtype),
            S((n, groups) + w.shape, w.dtype),
            S((n,) + small.shape, small.dtype),
        ],
        scratch_shapes=[
            pltpu.SemaphoreType.DMA((3, 2, n - 1)),
            pltpu.SemaphoreType.DMA((3, 2, n - 1)),
            pltpu.SemaphoreType.DMA((2, groups - 1)),
            pltpu.SemaphoreType.DMA((2, groups - 1)),
            pltpu.SemaphoreType.DMA((3,)),
        ],
        compiler_params=pltpu.CompilerParams(collective_id=0, has_side_effects=True),
        cost_estimate=pl.CostEstimate(flops=0, bytes_accessed=200 << 20, transcendentals=0),
        name="start",
    )(x, w, small)


def weight_grads_body(parts, first_ref, second_ref, attn_ref, both_ref, context_ref, out_ref, left):
    j = pl.program_id(0)

    @pl.when(j == 0)
    def _():
        left[0] = first_ref[...].T
        left[1] = second_ref[...].T

    @pl.when(j < 2 * parts)
    def _():
        out_ref[...] = dot(left[j % 2], both_ref[0]).astype(out_ref.dtype)

    @pl.when(j == 2 * parts)
    def _():
        out_ref[...] = dot_right_t(attn_ref[...].T, context_ref[...]).astype(out_ref.dtype)


def weight_grads_of(first_low, second_low, attn_low, both, context):
    steps, rows, units = both.shape
    width = first_low.shape[1]
    features = context.shape[0]
    fixed = pl.BlockSpec((rows, width), lambda j: (0, 0))
    return pl.pallas_call(
        functools.partial(weight_grads_body, steps // 2),
        grid=(steps + 1,),
        in_specs=[fixed, fixed, fixed, pl.BlockSpec((1, rows, units), lambda j: (jnp.minimum(j, steps - 1), 0, 0)), pl.BlockSpec((features, rows), lambda j: (0, 0))],
        out_specs=pl.BlockSpec((width, units), lambda j: (0, j)),
        out_shape=jax.ShapeDtypeStruct((width, units * steps + features), jnp.bfloat16),
        scratch_shapes=[VM((2, width, rows), jnp.bfloat16)],
        compiler_params=pltpu.CompilerParams(vmem_limit_bytes=62 << 20),
        cost_estimate=pl.CostEstimate(flops=2 * rows * width * (steps * units + features), bytes_accessed=rows * units * steps * 4, transcendentals=0),
        name="weight_grads",
    )(first_low, second_low, attn_low, both, context)


def erf(x):
    x = jnp.clip(x, -3.7439211627767994, 3.7439211627767994)
    y = x * x
    top = jnp.float32(0.00022905065861350646)
    for c in (0.0034082910107109506, 0.050955695062380861, 0.18520832239976145, 1.128379143519084):
        top = top * y + c
    low = jnp.float32(-1.1791602954361697e-7)
    for c in (0.000023547966471313185, 0.0010179625278914885, 0.014070470171167667, 0.11098505178285362, 0.49746925110067538, 1.0):
        low = low * y + c
    return x * top / low


def dense_body(own, x_ref, cot_ref, ctx0_ref, ctx1_ref, vec_ref, bias_ref, near_ref, out_ref, first_ref, second_ref, attn_ref, grad_ref, both_ref, ctx_ref, go0_ref, go1_ref, sum_ref, w_s, mt_s, slope_s, first_s, acc_s, even_s, odd_s, w_sem):
    i = pl.program_id(0)
    parts, _, _ = near_ref.shape
    f32, bf = jnp.float32, jnp.bfloat16
    units = both_ref.shape[2]
    cuts = (slice(0, 4 * own), slice(4 * own, 4 * own + units), slice(4 * own + units, 4 * own + 2 * units))
    sources = (near_ref.at[:, :, cuts[0]], near_ref.at[:, :, cuts[1]], near_ref.at[:, :, cuts[2]])
    copies = [pltpu.make_async_copy(sources[c], w_s.at[:, :, cut], w_sem.at[c]) for c, cut in enumerate(cuts)]

    @pl.when(i == 0)
    def _():
        for copy in copies:
            copy.start()
        sum_ref[...] = jnp.zeros(sum_ref.shape, f32)
        copies[0].wait()
        for t in range(parts):
            mt_s[:, t * own : (t + 1) * own] = w_s[t, :, 3 * own : 4 * own]

    def add_sum(row, value):
        sum_ref[row : row + 1, :] += jnp.sum(value, axis=0, keepdims=True)

    for t in range(parts):
        lead = ctx0_ref.shape[1]
        ctx_ref[t * own : t * own + lead, :] = ctx0_ref[t]
        ctx_ref[t * own + lead : (t + 1) * own, :] = ctx1_ref[t]
    mixed = dot(mt_s[...], ctx_ref[...]).T
    attn_in = x_ref[...].astype(f32) + mixed + vec_ref[0:1]
    first, first_norm, first_inv = layer_norm(attn_in, vec_ref[1:2], vec_ref[2:3])
    first_ref[...] = first.astype(bf)
    first_s[...] = first_norm
    acc_s[...] = first + vec_ref[3:4]

    @pl.when(i == 0)
    def _():
        copies[1].wait()
        copies[2].wait()

    half_units = units // 2
    first_cut, second_cut = slice(0, half_units), slice(half_units, units)
    base = 4 * own

    def before(t, cut):
        return dot(first_ref[...], w_s[t, :, base + cut.start : base + cut.stop]) + bias_ref[t, :, cut]

    def after(t, cut, inner):
        half = 0.5 * (1.0 + erf(inner * ROOT_HALF))
        slope_s[t, :, cut] = half + inner * jnp.exp(-0.5 * inner * inner) * INV_ROOT_TWO_PI
        active = (inner * half).astype(bf)
        both_ref[2 * t + 1, :, cut] = active
        acc_s[...] += dot_right_t(active, w_s[t, :, base + units + cut.start : base + units + cut.stop])

    even_s[...] = before(0, first_cut)

    def ahead(t, _):
        odd_s[...] = before(t, second_cut)
        after(t, first_cut, even_s[...])
        even_s[...] = before(jnp.minimum(t + 1, parts - 1), first_cut)
        after(t, second_cut, odd_s[...])
        return 0

    lax.fori_loop(0, parts, ahead, 0)
    second, second_norm, second_inv = layer_norm(acc_s[...], vec_ref[4:5], vec_ref[5:6])
    out_ref[...] = second.astype(bf)
    grad_out = cot_ref[...].astype(f32)
    add_sum(4, grad_out * second_norm)
    add_sum(5, grad_out)
    grad_second = norm_back(grad_out, second_norm, second_inv, vec_ref[4:5])
    add_sum(3, grad_second)
    second_ref[...] = grad_second.astype(bf)
    acc_s[...] = grad_second

    def back(t, _):
        grad_inner = (dot(second_ref[...], w_s[t, :, cuts[2]]) * slope_s[t]).astype(bf)
        both_ref[2 * t] = grad_inner
        sum_ref[pl.ds(6 + t, 1), :] += jnp.sum(grad_inner.astype(f32), axis=0, keepdims=True)
        acc_s[...] += dot_right_t(grad_inner, w_s[t, :, cuts[1]])
        return 0

    lax.fori_loop(0, parts, back, 0)
    grad_first = acc_s[...]
    first_norm = first_s[...]
    add_sum(1, grad_first * first_norm)
    add_sum(2, grad_first)
    grad_attn = norm_back(grad_first, first_norm, first_inv, vec_ref[1:2])
    add_sum(0, grad_attn)
    grad_ref[...] = grad_attn
    attn_ref[...] = grad_attn.astype(bf)
    grad_context = dot(attn_ref[...], mt_s[...]).T.astype(bf)
    for t in range(parts):
        go0_ref[t] = grad_context[t * own : t * own + HD]
        go1_ref[t] = grad_context[t * own + HD : (t + 1) * own]


def dense(own, x, cot, ctx0, ctx1, vectors, inner_bias, near, block):
    rows, width = x.shape
    parts = near.shape[0]
    cols = near.shape[2]
    units = (cols - 4 * own) // 2
    f32, bf = jnp.float32, jnp.bfloat16
    S = jax.ShapeDtypeStruct
    tok = pl.BlockSpec((block, width), lambda i: (i, 0))
    part_tok = pl.BlockSpec((2 * parts, block, units), lambda i: (0, i, 0))
    lanes = lambda n: pl.BlockSpec((parts, n, block), lambda i: (0, 0, i))
    fixed = lambda a: pl.BlockSpec(a.shape, lambda i: (0,) * a.ndim)
    inner_bias = inner_bias.reshape(parts, 1, units)
    return pl.pallas_call(
        functools.partial(dense_body, own),
        grid=(rows // block,),
        in_specs=[tok, tok, lanes(ctx0.shape[1]), lanes(ctx1.shape[1]), fixed(vectors), fixed(inner_bias), pl.BlockSpec(memory_space=pl.ANY)],
        out_specs=[tok] * 5 + [part_tok] + [pl.BlockSpec((parts * own, block), lambda i: (0, i)), lanes(HD), lanes(own - HD), pl.BlockSpec((16, width), lambda i: (0, 0))],
        out_shape=[S((rows, width), bf)] * 4 + [S((rows, width), f32)] + [S((2 * parts, rows, units), bf)] + [S((parts * own, rows), bf), S((parts, HD, rows), bf), S((parts, own - HD, rows), bf), S((16, width), f32)],
        scratch_shapes=[VM((parts, width, cols), bf), VM((width, parts * own), bf), VM((parts, block, units), f32), VM((block, width), f32), VM((block, width), f32), VM((block, units // 2), f32), VM((block, units // 2), f32), pltpu.SemaphoreType.DMA((3,))],
        compiler_params=pltpu.CompilerParams(vmem_limit_bytes=62 << 20),
        cost_estimate=pl.CostEstimate(flops=4 * rows * width * (2 * parts * units + parts * own), bytes_accessed=40 << 20, transcendentals=rows * units * parts),
        name="dense",
    )(x, cot, ctx0, ctx1, vectors, inner_bias, near)


def early_back_body(w_ref, b0_ref, b1_ref, acc_ref):
    width = b0_ref.shape[1]
    acc_ref[...] = jnp.zeros(acc_ref.shape, jnp.float32)

    def add(t, _):
        both = jnp.concatenate([b0_ref[t], b1_ref[t]], axis=0)
        acc_ref[...] += dot(w_ref[t, :, : 2 * width], both)
        return 0

    lax.fori_loop(0, b0_ref.shape[0], add, 0)


def late_back_body(cut, part_ref, w_ref, acc_ref, grad_ref, *rest):
    backs, out_ref = rest[:-1], rest[-1]
    parts = len(backs)
    total = acc_ref[...]
    for d in range(parts):
        total = total + dot(w_ref[(part_ref[0] + parts - d) % parts, :, cut : cut + backs[d].shape[0]], backs[d][...])
    out_ref[...] = (total.T + grad_ref[...]).astype(out_ref.dtype)


def weight_block(rest, cols):
    return pl.BlockSpec(rest.shape[:2] + (cols,), lambda i, *_: (0, 0, 0), pipeline_mode=pl.Buffered(1))


def whole(a):
    return pl.BlockSpec(a.shape, lambda i, *_: (0,) * a.ndim, pipeline_mode=pl.Buffered(1))


def early_back(rest, cols, b0, b1):
    width, rows = rest.shape[1], b0.shape[2]
    return pl.pallas_call(
        early_back_body,
        grid=(1,),
        in_specs=[weight_block(rest, cols), whole(b0), whole(b1)],
        out_specs=pl.BlockSpec((width, rows), lambda i: (0, 0)),
        out_shape=jax.ShapeDtypeStruct((width, rows), jnp.float32),
        compiler_params=pltpu.CompilerParams(vmem_limit_bytes=62 << 20),
        cost_estimate=pl.CostEstimate(flops=4 * width * rows * b0.shape[0] * b0.shape[1], bytes_accessed=10 << 20, transcendentals=0),
        name="early_back",
    )(rest, b0, b1)


def late_back(rest, cols, cut, part, acc, grad, backs):
    rows, width = grad.shape
    return pl.pallas_call(
        functools.partial(late_back_body, cut),
        grid_spec=pltpu.PrefetchScalarGridSpec(
            num_scalar_prefetch=1,
            grid=(1,),
            in_specs=[weight_block(rest, cols), whole(acc), whole(grad)] + [whole(b) for b in backs],
            out_specs=pl.BlockSpec((rows, width), lambda i, *_: (0, 0)),
        ),
        out_shape=jax.ShapeDtypeStruct((rows, width), jnp.bfloat16),
        compiler_params=pltpu.CompilerParams(vmem_limit_bytes=62 << 20),
        cost_estimate=pl.CostEstimate(flops=2 * width * rows * backs[0].shape[0] * len(backs), bytes_accessed=10 << 20, transcendentals=0),
        name="late_back",
    )(part.reshape(1), rest, acc, grad, *backs)


def add_up(value, axis):
    size = lax.axis_size(axis)
    span, turn = 1, 0
    while span < size:
        other = lax.ppermute(value, axis, [(i, i ^ span) for i in range(size)])
        value = value + other
        span *= 2
        turn += 1
    return value


def two_halves(value):
    high = value.astype(jnp.bfloat16)
    return high, (value - high.astype(jnp.float32)).astype(jnp.bfloat16)


def rotate(blocks, axis):
    size = lax.axis_size(axis)
    me = lax.axis_index(axis)
    out = []
    for d in range(size):
        block = lax.dynamic_index_in_dim(blocks, (me + d) % size, 0, keepdims=False)
        if d:
            block = lax.ppermute(block, axis, [(i, (i + d) % size) for i in range(size)])
        out.append(block)
    return out


def body(hidden_in, segments, query_weight, key_weight, value_weight, query_bias, value_bias, mixer_weight, mixer_bias, first_gain, first_shift, inner_weight, inner_bias, outer_weight, outer_bias, second_gain, second_shift, cotangent):
    f32 = jnp.float32
    _, rows, width = hidden_in.shape
    parts = lax.axis_size("tensor")
    groups = lax.axis_size("dp")
    rank = lax.axis_index("tensor")
    own = query_weight.shape[1]
    heads = own // HD
    three = 3 * HD
    units = inner_weight.shape[1]
    by_head = lambda q, k, v: jnp.stack([a.reshape(a.shape[:-1] + (heads, HD)) for a in (q, k, v)], -2).reshape(q.shape[:-1] + (3 * own,))
    x_own = hidden_in[0]
    qkv_own = by_head(query_weight, key_weight, value_weight)
    small = jnp.concatenate([segments[0].astype(f32), inner_bias]).reshape(-1, 128)
    near_own = jnp.concatenate([qkv_own, mixer_weight.T, inner_weight, outer_weight.T], 1)
    x_parts, near, small = start(x_own, near_own, small)
    x_all = x_parts.reshape(parts * rows, width)
    near = near.reshape(parts, width, 4 * own + 2 * units)
    small = small.reshape(parts, -1)
    segment_all = small[:, :rows].astype(jnp.int32).reshape(-1)
    inner_bias_all = small[:, rows:]
    biases = by_head(query_bias, jnp.zeros_like(query_bias), value_bias)

    qt, ka, vt, qn, kt, vn = project(x_all, near, rank, biases, segment_all)
    lead = heads - 1
    context_t, lse, exchanged = [], [], []
    for call, (first, count, block) in enumerate(((0, lead, rows // 2), (lead, 1, rows))):
        lo, hi = ranges(segment_all, block, 512)
        part, out_t, out_lse = attend_forward(first, count, parts, qt, ka, vt, lo, hi, BQ=block)
        context_t.append(out_t)
        lse.append(out_lse)
        if exchanged:
            part, exchanged[-1] = lax.optimization_barrier((part, exchanged[-1]))
        exchanged.append(lax.all_to_all(part, "tensor", 0, 0, tiled=True))
    vectors = jnp.stack([mixer_bias, first_gain, first_shift, outer_bias, second_gain, second_shift])
    vectors = jnp.pad(vectors, ((0, 2), (0, 0)))
    layer_out, first_low, second_low, attn_low, grad_attn, both, context, go0, go1, early = dense(
        own, x_own, cotangent[0], exchanged[0], exchanged[1], vectors, inner_bias_all, near, block=rows // 2
    )
    go0 = lax.all_to_all(go0, "tensor", 0, 0, tiled=True)
    go1 = lax.all_to_all(go1, "tensor", 0, 0, tiled=True)
    weight_grads = weight_grads_of(
        first_low, second_low, attn_low, both, context
    )
    weight_grads = lax.psum_scatter(weight_grads, "dp", scatter_dimension=0, tiled=True)
    weight_grads = jnp.concatenate(
        [
            weight_grads[:, : 2 * units * parts].reshape(-1, parts, 2 * units),
            weight_grads[:, 2 * units * parts :].reshape(-1, parts, own),
        ],
        2,
    ).transpose(1, 0, 2)
    weight_grads = rotate(weight_grads, "tensor")
    weight_grads = sum(a.astype(f32) for a in weight_grads)
    early = add_up(early[: 6 + parts], "tensor")
    count = 6 + parts
    lines = -(-count * width // (3 * own))
    early = jnp.pad(early.reshape(-1), (0, lines * 3 * own - count * width)).reshape(lines, 3 * own)
    early = jnp.concatenate(two_halves(early), 0)

    lo, hi = ranges(segment_all, 512, 512)
    backs, qkv_grad, bias_grad = [], [], []
    for h in range(heads):
        call = 0 if h < lead else 1
        grads, weight_part, sums = attend_backward(
            h, 1, go1 if h else go0, h - 1 if h else 0, context_t[call], lse[call], h - call * lead, qt, ka, qn, kt, vn, x_parts, lo, hi
        )
        if h < heads - 1:
            backs.append(lax.all_to_all(grads, "tensor", 0, 0, tiled=True))
        else:
            backs.append(rotate(grads, "tensor"))
        qkv_grad.append(weight_part)
        bias_grad.append(sums[:, 0])
    input_back = early_back(near, 4 * own, backs[0], backs[1])
    input_grad = late_back(near, 4 * own, 2 * three, rank, input_back, grad_attn, backs[2])
    each = width // groups
    bias_grad = jnp.stack(two_halves(jnp.concatenate(bias_grad)))
    extra = jnp.concatenate([early, bias_grad], 0)
    spare = -extra.shape[0] % 16
    extra = jnp.pad(extra, ((0, spare), (0, 0)))
    extra = jnp.broadcast_to(extra[None], (groups,) + extra.shape)
    qkv_grad = jnp.concatenate(qkv_grad, 1).reshape(groups, each, 3 * own)
    qkv_grad = jnp.concatenate([qkv_grad, extra], 1)
    qkv_grad = lax.all_to_all(qkv_grad, "dp", 0, 0, tiled=True)
    qkv_grad = jnp.sum(qkv_grad.astype(f32), 0)
    early = qkv_grad[each : each + lines] + qkv_grad[each + lines : each + 2 * lines]
    early = early.reshape(-1)[: count * width].reshape(count, width)
    bias_grad = qkv_grad[each + 2 * lines] + qkv_grad[each + 2 * lines + 1]
    pick = lambda a, n: a.reshape(a.shape[:-1] + (heads, 3, HD))[..., n, :].reshape(a.shape[:-1] + (own,))
    inner_bias_out = lax.dynamic_index_in_dim(early, 6 + rank, 0, keepdims=False)
    return (
        layer_out[None],
        input_grad[None],
        pick(qkv_grad[:each], 0),
        pick(qkv_grad[:each], 1),
        pick(qkv_grad[:each], 2),
        pick(bias_grad, 0),
        pick(bias_grad, 2),
        weight_grads[:, 2 * units :].T,
        early[0],
        early[1],
        early[2],
        weight_grads[:, :units],
        inner_bias_out,
        weight_grads[:, units : 2 * units].T,
        early[3],
        early[4],
        early[5],
    )


def solution(mesh):
    placed = (
        P("dp", "tensor", None),
        P("dp", "tensor"),
        P("dp", "tensor"),
        P("dp", "tensor"),
        P("dp", "tensor"),
        P("tensor"),
        P("tensor"),
        P("tensor", "dp"),
        P(),
        P(),
        P(),
        P("dp", "tensor"),
        P("tensor"),
        P("tensor", "dp"),
        P(),
        P(),
        P(),
        P("dp", "tensor", None),
    )

    return jax.shard_map(
        body,
        mesh=mesh,
        in_specs=placed,
        out_specs=(
            P("dp", "tensor", None),
            P("dp", "tensor", None),
            P("dp", "tensor"),
            P("dp", "tensor"),
            P("dp", "tensor"),
            P("tensor"),
            P("tensor"),
            P("tensor", "dp"),
            P(),
            P(),
            P(),
            P("dp", "tensor"),
            P("tensor"),
            P("tensor", "dp"),
            P(),
            P(),
            P(),
        ),
        check_vma=False,
    )
```

```python
import functools

import jax
import jax.numpy as jnp
from jax import lax
from jax.experimental import pallas as pl
from jax.experimental.pallas import tpu as pltpu
from jax.sharding import PartitionSpec as P


EPS = 1e-12
ROOT_HALF = 0.7071067811865476
INV_ROOT_TWO_PI = 0.3989422804014327
HD=64; SCALE=0.125; APART=-1e30
VM=pltpu.VMEM


def dot(a,b): return jnp.dot(a,b,preferred_element_type=jnp.float32)


def project_body(heads, part_ref, x_ref, w_ref, b_ref, srow_ref, qt_ref, ka_ref, vt_ref, kt_ref, vn_ref):
    y=dot(x_ref[...], w_ref[0,:,:b_ref.shape[1]]) + b_ref[...]
    low = y.astype(jnp.bfloat16)
    yt = low.T
    rows = y.shape[0]
    match = lax.broadcasted_iota(jnp.int32,(HD,rows),0)==srow_ref[...]
    apart = jnp.where(match,0.0,APART).astype(jnp.bfloat16)
    same = jnp.where(match,1.0,0.0).T.astype(jnp.bfloat16)
    width=heads*HD
    for h in range(heads):
        q_at,k_at,v_at=h*HD,width+h*HD,2*width+h*HD
        qt_ref[h,:HD,:]=yt[q_at:q_at+HD]*jnp.bfloat16(SCALE)
        qt_ref[h,HD:,:]=apart
        ka_ref[h]=jnp.concatenate([low[:,k_at:k_at+HD],same],axis=1)
        kt_ref[h]=yt[k_at:k_at+HD]
        vt_ref[h]=yt[v_at:v_at+HD]
        vn_ref[h]=low[:,v_at:v_at+HD]


def project(x,rest,part,b,seg,rows=512):
    L,D=x.shape; heads=b.shape[0]//(3*HD)
    bf=jnp.bfloat16
    cols=4*heads*HD
    nat=lambda n: pl.BlockSpec((heads,rows,n),lambda i,*_:(0,i,0))
    tr=lambda n: pl.BlockSpec((heads,n,rows),lambda i,*_:(0,0,i))
    S=jax.ShapeDtypeStruct
    return pl.pallas_call(functools.partial(project_body,heads),
        grid_spec=pltpu.PrefetchScalarGridSpec(num_scalar_prefetch=1,grid=(L//rows,),
        in_specs=[pl.BlockSpec((rows,D),lambda i,*_:(i,0)),pl.BlockSpec((1,D,cols),lambda i,p:(p[0],0,0)),pl.BlockSpec((1,b.shape[0]),lambda i,*_:(0,0)),
                  pl.BlockSpec((1,rows),lambda i,*_:(0,i))],
        out_specs=[tr(2*HD),nat(2*HD),tr(HD),tr(HD),nat(HD)]),
        out_shape=[S((heads,2*HD,L),bf),S((heads,L,2*HD),bf),S((heads,HD,L),bf),S((heads,HD,L),bf),S((heads,L,HD),bf)],
        compiler_params=pltpu.CompilerParams(vmem_limit_bytes=62 << 20),
        cost_estimate=pl.CostEstimate(flops=2*L*D*b.shape[0],bytes_accessed=L*D*2+D*cols*2+L*heads*HD*2*10,transcendentals=0),
        name="project")(part.reshape(1),x,rest,b.reshape(1,-1),seg.reshape(1,-1))


def forward_body(BK, lo_ref, hi_ref, qt_ref, ka_ref, vt_ref, ctx_ref, ot_ref, lse_ref, m_s, l_s, acc, s_even, s_odd):
    i=pl.program_id(0)
    heads=qt_ref.shape[0]
    half=BK//2
    m_s[...]=jnp.full(m_s.shape,-jnp.inf,jnp.float32)
    l_s[...]=jnp.zeros(l_s.shape,jnp.float32)
    acc[...]=jnp.zeros(acc.shape,jnp.float32)

    def scores(h,at):
        return dot(ka_ref[h,pl.ds(pl.multiple_of(at,half),half),:],qt_ref[h])

    def use(h,at,s):
        m_old=m_s[h]
        m_new=jnp.maximum(m_old,jnp.max(s,axis=0,keepdims=True))
        p=jnp.exp(s-m_new)
        alpha=jnp.exp(m_old-m_new)
        m_s[h]=m_new
        l_s[h]=l_s[h]*alpha+jnp.sum(p,axis=0,keepdims=True)
        acc[h]=acc[h]*alpha+dot(vt_ref[h,:,pl.ds(pl.multiple_of(at,half),half)],p.astype(jnp.bfloat16))

    last=hi_ref[i]-1
    for h in range(heads):
        s_even[h]=scores(h,lo_ref[i]*BK)

    def step(j,_):
        at=j*BK
        for h in range(heads):
            s_odd[h]=scores(h,at+half)
            use(h,at,s_even[h])
        for h in range(heads):
            s_even[h]=scores(h,jnp.minimum(j+1,last)*BK)
            use(h,at+half,s_odd[h])
        return 0

    lax.fori_loop(lo_ref[i],hi_ref[i],step,0)
    for h in range(heads):
        o=acc[h]/l_s[h]
        lse_ref[h]=m_s[h]+jnp.log(l_s[h])
        ot_ref[h]=o
        ctx_ref[0,h*HD:(h+1)*HD,:]=o.astype(jnp.bfloat16)


def attend_forward(first,heads,parts,qt,ka,vt,lo,hi,BQ=384,BK=512):
    L=qt.shape[2]
    S=jax.ShapeDtypeStruct
    per=L//parts//BQ
    return pl.pallas_call(functools.partial(forward_body,BK),
        grid_spec=pltpu.PrefetchScalarGridSpec(num_scalar_prefetch=2,grid=(L//BQ,),
        in_specs=[pl.BlockSpec((heads,2*HD,BQ),lambda i,*_:(first//heads,0,i)),pl.BlockSpec((heads,L,2*HD),lambda i,*_:(first//heads,0,0)),pl.BlockSpec((heads,HD,L),lambda i,*_:(first//heads,0,0))],
        out_specs=[pl.BlockSpec((1,heads*HD,BQ),lambda i,*_:(i//per,0,i%per)),pl.BlockSpec((heads,HD,BQ),lambda i,*_:(0,0,i)),pl.BlockSpec((heads,1,BQ),lambda i,*_:(0,0,i))],
        scratch_shapes=[VM((heads,1,BQ),jnp.float32),VM((heads,1,BQ),jnp.float32),VM((heads,HD,BQ),jnp.float32)]+[VM((heads,BK//2,BQ),jnp.float32)]*2),
        out_shape=[S((parts,heads*HD,L//parts),jnp.bfloat16),S((heads,HD,L),jnp.float32),S((heads,1,L),jnp.float32)],
        compiler_params=pltpu.CompilerParams(vmem_limit_bytes=62 << 20),
        cost_estimate=pl.CostEstimate(flops=2*L*L*HD*2*heads,bytes_accessed=L*heads*HD*2*8,transcendentals=L*L*heads),
        name="attend_forward")(lo,hi,qt,ka,vt)


def backward_body(BQ, BK, lo_ref, hi_ref, go_ref, ot_ref, lse_ref, qt_ref, ka_ref, kt_ref, vn_ref, x_ref, out_ref, wg_ref, sum_ref, got, delta, dqt, dkt, dvt, dk_s, dv_s, x_s, x_sem):
    bring=pltpu.make_async_copy(x_ref,x_s,x_sem)
    bring.start()
    parts,_,rows=go_ref.shape
    heads,_,L=qt_ref.shape
    CH=256
    for h in range(heads):
        for c in range(L//CH):
            p,at=c*CH//rows,c*CH%rows
            gt=go_ref[p,h*HD:(h+1)*HD,at:at+CH]
            wide=gt.astype(jnp.float32)
            got[h,:,c*CH:(c+1)*CH]=gt
            delta[h,:,c*CH:(c+1)*CH]=jnp.sum(wide*ot_ref[h,:,c*CH:(c+1)*CH],axis=0,keepdims=True)
    dqt[...]=jnp.zeros(dqt.shape,jnp.float32)

    def key_block(j,_):
        ka_at=pl.multiple_of(j*BK,BK)
        dk_s[...]=jnp.zeros(dk_s.shape,jnp.float32)
        dv_s[...]=jnp.zeros(dv_s.shape,jnp.float32)

        def query_block(i,_):
            for h in range(heads):
                at=pl.multiple_of(i*BQ,BQ)
                s=dot(ka_ref[h,pl.ds(ka_at,BK),:],qt_ref[h,:,pl.ds(at,BQ)])
                p=jnp.exp(s-lse_ref[h,:,pl.ds(at,BQ)])
                dp=dot(vn_ref[h,pl.ds(ka_at,BK),:],got[h,:,pl.ds(at,BQ)])
                ds=(p*(dp-delta[h,:,pl.ds(at,BQ)])).astype(jnp.bfloat16)
                dv_s[h]+=dot_right_t(got[h,:,pl.ds(at,BQ)],p.astype(jnp.bfloat16))
                dk_s[h]+=dot_right_t(qt_ref[h,:HD,pl.ds(at,BQ)],ds)
                dqt[h,:,pl.ds(at,BQ)]+=dot(kt_ref[h,:,pl.ds(ka_at,BK)],ds)
            return 0

        lax.fori_loop(lo_ref[j],hi_ref[j],query_block,0)
        for h in range(heads):
            dkt[h,:,pl.ds(ka_at,BK)]=dk_s[h].astype(jnp.bfloat16)
            dvt[h,:,pl.ds(ka_at,BK)]=dv_s[h].astype(jnp.bfloat16)
        return 0

    lax.fori_loop(0,L//BK,key_block,0)
    for h in range(heads):
        for p in range(parts):
            cut=slice(p*rows,(p+1)*rows)
            out_ref[p,3*h*HD:(3*h+1)*HD,:]=(dqt[h,:,cut]*SCALE).astype(jnp.bfloat16)
            out_ref[p,(3*h+1)*HD:(3*h+2)*HD,:]=dkt[h,:,cut]
            out_ref[p,(3*h+2)*HD:(3*h+3)*HD,:]=dvt[h,:,cut]
    bring.wait()
    wg=jnp.zeros(wg_ref.shape[::-1],jnp.float32)
    total=jnp.zeros((3*heads*HD,1),jnp.float32)
    for p in range(parts):
        part=out_ref[p]
        wg=wg+dot(part,x_s[p])
        total=total+jnp.sum(part.astype(jnp.float32),axis=1,keepdims=True)
    wg_ref[...]=wg.T.astype(wg_ref.dtype)
    sum_ref[...]=jnp.broadcast_to(total,sum_ref.shape)


def attend_backward(first,heads,go,go_first,ot,lse,ot_first,qt,ka,kt,vn,x,lo,hi,BQ=512,BK=512):
    parts,_,rows=go.shape; L=parts*rows; D=x.shape[2]
    S=jax.ShapeDtypeStruct; f32=jnp.float32; bf=jnp.bfloat16
    at=lambda a,n: pl.BlockSpec((heads,)+a.shape[1:],lambda i,*_:(n//heads,0,0),pipeline_mode=pl.Buffered(1))
    out=3*heads*HD
    return pl.pallas_call(functools.partial(backward_body,BQ,BK),
        grid_spec=pltpu.PrefetchScalarGridSpec(num_scalar_prefetch=2,grid=(1,),
        in_specs=[pl.BlockSpec((parts,heads*HD,rows),lambda i,*_:(0,go_first,0),pipeline_mode=pl.Buffered(1)),at(ot,ot_first),at(lse,ot_first)]+[at(a,first) for a in (qt,ka,kt,vn)]+[pl.BlockSpec(memory_space=pl.ANY)],
        out_specs=[pl.BlockSpec((parts,out,rows),lambda i,*_:(0,0,0),pipeline_mode=pl.Buffered(1)),pl.BlockSpec((D,out),lambda i,*_:(0,0)),pl.BlockSpec((out,128),lambda i,*_:(0,0))],
        scratch_shapes=[VM((heads,HD,L),bf),VM((heads,1,L),f32),VM((heads,HD,L),f32),VM((heads,HD,L),bf),VM((heads,HD,L),bf),VM((heads,HD,BK),f32),VM((heads,HD,BK),f32),VM(x.shape,bf),pltpu.SemaphoreType.DMA]),
        out_shape=[S((parts,out,rows),bf),S((D,out),bf),S((out,128),f32)],
        compiler_params=pltpu.CompilerParams(vmem_limit_bytes=62 << 20),
        cost_estimate=pl.CostEstimate(flops=2*L*L*HD*5*heads,bytes_accessed=L*heads*HD*2*14,transcendentals=L*L*heads),
        name="attend_backward")(lo,hi,go,ot,lse,qt,ka,kt,vn,x)


def ranges(seg,BQ,BK):
    first=seg.reshape(-1,BQ)[:,0]; last=seg.reshape(-1,BQ)[:,-1]
    kf=seg.reshape(-1,BK)[:,0]; kl=seg.reshape(-1,BK)[:,-1]
    lo=jnp.sum((kl[None,:]<first[:,None]).astype(jnp.int32),1)
    hi=jnp.sum((kf[None,:]<=last[:,None]).astype(jnp.int32),1)
    return lo,hi


def dot_right_t(left, right):
    return lax.dot_general(
        left, right, (((1,), (1,)), ((), ())), preferred_element_type=jnp.float32
    )


def layer_norm(values_in, gain, shift):
    mean_row = jnp.mean(values_in, -1, keepdims=True)
    centered = values_in - mean_row
    inverse = lax.rsqrt(jnp.mean(centered * centered, -1, keepdims=True) + EPS)
    normed = centered * inverse
    return (normed * gain + shift, normed, inverse)


def norm_back(grad_in, normed, inverse, gain):
    scaled = grad_in * gain
    return inverse * (
        scaled
        - jnp.mean(scaled, -1, keepdims=True)
        - normed * jnp.mean(scaled * normed, -1, keepdims=True)
    )


MESH = pl.DeviceIdType.MESH


def flip(index, bit):
    span = 1 << bit
    return index + span * (1 - 2 * ((index // span) % 2))


def start_body(n, bits, x_ref, w_ref, s_ref, x_out, w_out, s_out, send_z, recv_z, send_d, recv_d, keep_sem):
    me = lax.axis_index("tensor")
    mine = lax.axis_index("dp")
    barrier = pltpu.get_barrier_semaphore()

    @pl.when(me > 0)
    def _():
        pl.semaphore_signal(barrier, inc=1, device_id={"tensor": me - 1}, device_id_type=MESH)

    @pl.when(me < n - 1)
    def _():
        pl.semaphore_signal(barrier, inc=1, device_id={"tensor": me + 1}, device_id_type=MESH)

    for bit in range(bits):
        pl.semaphore_signal(barrier, inc=1, device_id={"dp": flip(mine, bit)}, device_id_type=MESH)
    pl.semaphore_wait(barrier, bits + jnp.where(me > 0, 1, 0) + jnp.where(me < n - 1, 1, 0))

    keeps = [
        pltpu.make_async_copy(x_ref, x_out.at[me], keep_sem.at[0]),
        pltpu.make_async_copy(w_ref, w_out.at[me, mine], keep_sem.at[1]),
        pltpu.make_async_copy(s_ref, s_out.at[me], keep_sem.at[2]),
    ]
    for keep in keeps:
        keep.start()

    def hop(kind, side, step):
        block = me - (step - 1) if side else me + (step - 1)
        first, place = (
            (x_ref, x_out.at[block]),
            (w_ref, w_out.at[block, mine]),
            (s_ref, s_out.at[block]),
        )[kind]
        return pltpu.make_async_remote_copy(
            src_ref=first if step == 1 else place,
            dst_ref=place,
            send_sem=send_z.at[kind, side, step - 1],
            recv_sem=recv_z.at[kind, side, step - 1],
            device_id={"tensor": me + 1 if side else me - 1},
            device_id_type=MESH,
        )

    def sends(side, step):
        if side:
            return (me < n - 1) & (me >= step - 1)
        return (me > 0) & (me + step - 1 <= n - 1)

    def receives(side, step):
        return me >= step if side else me + step <= n - 1

    def z_start(kinds, step):
        for side in (0, 1):

            @pl.when(sends(side, step))
            def _():
                for kind in kinds:
                    hop(kind, side, step).start()

    def z_arrive(kinds, step):
        for side in (0, 1):

            @pl.when(receives(side, step))
            def _():
                for kind in kinds:
                    hop(kind, side, step).wait_recv()

    half = w_ref.shape[1] // 2
    up = list(range(bits - 1, -1, -1))
    orders = (up, [up[1], up[0]] + up[2:] if bits > 1 else up)

    def doubling(side, step):
        order = orders[side]
        held = [mine]
        for bit in order[:step]:
            held = held + [flip(d, bit) for d in held]
        cut = pl.ds(side * half, half)
        return [
            pltpu.make_async_remote_copy(
                src_ref=w_out.at[:, d, :, cut],
                dst_ref=w_out.at[:, d, :, cut],
                send_sem=send_d.at[side, (1 << step) - 1 + at],
                recv_sem=recv_d.at[side, (1 << step) - 1 + at],
                device_id={"dp": flip(mine, order[step])},
                device_id_type=MESH,
            )
            for at, d in enumerate(held)
        ]

    def d_start(step):
        for side in (0, 1):
            for copy in doubling(side, step):
                copy.start()

    def d_arrive(step):
        for side in (0, 1):
            for copy in doubling(side, step):
                copy.wait_recv()

    for step in range(1, n):
        z_start((1, 2), step)
        z_arrive((1, 2), step)
    keeps[1].wait()
    for step in range(max(n - 1, bits)):
        if step < bits:
            if step:
                d_arrive(step - 1)
            d_start(step)
        if step < n - 1:
            if step:
                z_arrive((0,), step)
            z_start((0,), step + 1)
    z_arrive((0,), n - 1)
    d_arrive(bits - 1)
    for side in (0, 1):
        for step in range(1, n):

            @pl.when(sends(side, step))
            def _():
                for kind in (0, 1, 2):
                    hop(kind, side, step).wait_send()

        for step in range(bits):
            for copy in doubling(side, step):
                copy.wait_send()
    keeps[0].wait()
    keeps[2].wait()


def start(x, w, small):
    n = lax.axis_size("tensor")
    groups = lax.axis_size("dp")
    bits = groups.bit_length() - 1
    S = jax.ShapeDtypeStruct
    anywhere = pl.BlockSpec(memory_space=pl.ANY)
    return pl.pallas_call(
        functools.partial(start_body, n, bits),
        in_specs=[pl.BlockSpec(memory_space=pltpu.VMEM)] * 3,
        out_specs=[anywhere] * 3,
        out_shape=[
            S((n,) + x.shape, x.dtype),
            S((n, groups) + w.shape, w.dtype),
            S((n,) + small.shape, small.dtype),
        ],
        scratch_shapes=[
            pltpu.SemaphoreType.DMA((3, 2, n - 1)),
            pltpu.SemaphoreType.DMA((3, 2, n - 1)),
            pltpu.SemaphoreType.DMA((2, groups - 1)),
            pltpu.SemaphoreType.DMA((2, groups - 1)),
            pltpu.SemaphoreType.DMA((3,)),
        ],
        compiler_params=pltpu.CompilerParams(collective_id=0, has_side_effects=True),
        cost_estimate=pl.CostEstimate(flops=0, bytes_accessed=200 << 20, transcendentals=0),
        name="start",
    )(x, w, small)


def weight_grads_body(parts, first_ref, second_ref, attn_ref, both_ref, context_ref, out_ref, left):
    j = pl.program_id(0)

    @pl.when(j == 0)
    def _():
        left[0] = first_ref[...].T
        left[1] = second_ref[...].T

    @pl.when(j < 2 * parts)
    def _():
        out_ref[...] = dot(left[j % 2], both_ref[0]).astype(out_ref.dtype)

    @pl.when(j == 2 * parts)
    def _():
        out_ref[...] = dot_right_t(attn_ref[...].T, context_ref[...]).astype(out_ref.dtype)


def weight_grads_of(first_low, second_low, attn_low, both, context):
    steps, rows, units = both.shape
    width = first_low.shape[1]
    features = context.shape[0]
    fixed = pl.BlockSpec((rows, width), lambda j: (0, 0))
    return pl.pallas_call(
        functools.partial(weight_grads_body, steps // 2),
        grid=(steps + 1,),
        in_specs=[fixed, fixed, fixed, pl.BlockSpec((1, rows, units), lambda j: (jnp.minimum(j, steps - 1), 0, 0)), pl.BlockSpec((features, rows), lambda j: (0, 0))],
        out_specs=pl.BlockSpec((width, units), lambda j: (0, j)),
        out_shape=jax.ShapeDtypeStruct((width, units * steps + features), jnp.bfloat16),
        scratch_shapes=[VM((2, width, rows), jnp.bfloat16)],
        compiler_params=pltpu.CompilerParams(vmem_limit_bytes=62 << 20),
        cost_estimate=pl.CostEstimate(flops=2 * rows * width * (steps * units + features), bytes_accessed=rows * units * steps * 4, transcendentals=0),
        name="weight_grads",
    )(first_low, second_low, attn_low, both, context)


def erf(x):
    x = jnp.clip(x, -3.7439211627767994, 3.7439211627767994)
    y = x * x
    top = jnp.float32(0.00022905065861350646)
    for c in (0.0034082910107109506, 0.050955695062380861, 0.18520832239976145, 1.128379143519084):
        top = top * y + c
    low = jnp.float32(-1.1791602954361697e-7)
    for c in (0.000023547966471313185, 0.0010179625278914885, 0.014070470171167667, 0.11098505178285362, 0.49746925110067538, 1.0):
        low = low * y + c
    return x * top / low


def dense_body(own, x_ref, cot_ref, ctx0_ref, ctx1_ref, vec_ref, bias_ref, near_ref, out_ref, first_ref, second_ref, attn_ref, grad_ref, both_ref, ctx_ref, go0_ref, go1_ref, sum_ref, w_s, mt_s, slope_s, first_s, acc_s, even_s, odd_s, w_sem):
    i = pl.program_id(0)
    parts, _, _ = near_ref.shape
    f32, bf = jnp.float32, jnp.bfloat16
    units = both_ref.shape[2]
    cuts = (slice(0, 4 * own), slice(4 * own, 4 * own + units), slice(4 * own + units, 4 * own + 2 * units))
    sources = (near_ref.at[:, :, cuts[0]], near_ref.at[:, :, cuts[1]], near_ref.at[:, :, cuts[2]])
    copies = [pltpu.make_async_copy(sources[c], w_s.at[:, :, cut], w_sem.at[c]) for c, cut in enumerate(cuts)]

    @pl.when(i == 0)
    def _():
        for copy in copies:
            copy.start()
        sum_ref[...] = jnp.zeros(sum_ref.shape, f32)
        copies[0].wait()
        for t in range(parts):
            mt_s[:, t * own : (t + 1) * own] = w_s[t, :, 3 * own : 4 * own]

    def add_sum(row, value):
        sum_ref[row : row + 1, :] += jnp.sum(value, axis=0, keepdims=True)

    for t in range(parts):
        lead = ctx0_ref.shape[1]
        ctx_ref[t * own : t * own + lead, :] = ctx0_ref[t]
        ctx_ref[t * own + lead : (t + 1) * own, :] = ctx1_ref[t]
    mixed = dot(mt_s[...], ctx_ref[...]).T
    attn_in = x_ref[...].astype(f32) + mixed + vec_ref[0:1]
    first, first_norm, first_inv = layer_norm(attn_in, vec_ref[1:2], vec_ref[2:3])
    first_ref[...] = first.astype(bf)
    first_s[...] = first_norm
    acc_s[...] = first + vec_ref[3:4]

    @pl.when(i == 0)
    def _():
        copies[1].wait()
        copies[2].wait()

    half_units = units // 2
    first_cut, second_cut = slice(0, half_units), slice(half_units, units)
    base = 4 * own

    def before(t, cut):
        return dot(first_ref[...], w_s[t, :, base + cut.start : base + cut.stop]) + bias_ref[t, :, cut]

    def after(t, cut, inner):
        half = 0.5 * (1.0 + erf(inner * ROOT_HALF))
        slope_s[t, :, cut] = half + inner * jnp.exp(-0.5 * inner * inner) * INV_ROOT_TWO_PI
        active = (inner * half).astype(bf)
        both_ref[2 * t + 1, :, cut] = active
        acc_s[...] += dot_right_t(active, w_s[t, :, base + units + cut.start : base + units + cut.stop])

    even_s[...] = before(0, first_cut)

    def ahead(t, _):
        odd_s[...] = before(t, second_cut)
        after(t, first_cut, even_s[...])
        even_s[...] = before(jnp.minimum(t + 1, parts - 1), first_cut)
        after(t, second_cut, odd_s[...])
        return 0

    lax.fori_loop(0, parts, ahead, 0)
    second, second_norm, second_inv = layer_norm(acc_s[...], vec_ref[4:5], vec_ref[5:6])
    out_ref[...] = second.astype(bf)
    grad_out = cot_ref[...].astype(f32)
    add_sum(4, grad_out * second_norm)
    add_sum(5, grad_out)
    grad_second = norm_back(grad_out, second_norm, second_inv, vec_ref[4:5])
    add_sum(3, grad_second)
    second_ref[...] = grad_second.astype(bf)
    acc_s[...] = grad_second

    def back(t, _):
        grad_inner = (dot(second_ref[...], w_s[t, :, cuts[2]]) * slope_s[t]).astype(bf)
        both_ref[2 * t] = grad_inner
        sum_ref[pl.ds(6 + t, 1), :] += jnp.sum(grad_inner.astype(f32), axis=0, keepdims=True)
        acc_s[...] += dot_right_t(grad_inner, w_s[t, :, cuts[1]])
        return 0

    lax.fori_loop(0, parts, back, 0)
    grad_first = acc_s[...]
    first_norm = first_s[...]
    add_sum(1, grad_first * first_norm)
    add_sum(2, grad_first)
    grad_attn = norm_back(grad_first, first_norm, first_inv, vec_ref[1:2])
    add_sum(0, grad_attn)
    grad_ref[...] = grad_attn
    attn_ref[...] = grad_attn.astype(bf)
    grad_context = dot(attn_ref[...], mt_s[...]).T.astype(bf)
    for t in range(parts):
        go0_ref[t] = grad_context[t * own : t * own + HD]
        go1_ref[t] = grad_context[t * own + HD : (t + 1) * own]


def dense(own, x, cot, ctx0, ctx1, vectors, inner_bias, near, block):
    rows, width = x.shape
    parts = near.shape[0]
    cols = near.shape[2]
    units = (cols - 4 * own) // 2
    f32, bf = jnp.float32, jnp.bfloat16
    S = jax.ShapeDtypeStruct
    tok = pl.BlockSpec((block, width), lambda i: (i, 0))
    part_tok = pl.BlockSpec((2 * parts, block, units), lambda i: (0, i, 0))
    lanes = lambda n: pl.BlockSpec((parts, n, block), lambda i: (0, 0, i))
    fixed = lambda a: pl.BlockSpec(a.shape, lambda i: (0,) * a.ndim)
    inner_bias = inner_bias.reshape(parts, 1, units)
    return pl.pallas_call(
        functools.partial(dense_body, own),
        grid=(rows // block,),
        in_specs=[tok, tok, lanes(ctx0.shape[1]), lanes(ctx1.shape[1]), fixed(vectors), fixed(inner_bias), pl.BlockSpec(memory_space=pl.ANY)],
        out_specs=[tok] * 5 + [part_tok] + [pl.BlockSpec((parts * own, block), lambda i: (0, i)), lanes(HD), lanes(own - HD), pl.BlockSpec((16, width), lambda i: (0, 0))],
        out_shape=[S((rows, width), bf)] * 4 + [S((rows, width), f32)] + [S((2 * parts, rows, units), bf)] + [S((parts * own, rows), bf), S((parts, HD, rows), bf), S((parts, own - HD, rows), bf), S((16, width), f32)],
        scratch_shapes=[VM((parts, width, cols), bf), VM((width, parts * own), bf), VM((parts, block, units), f32), VM((block, width), f32), VM((block, width), f32), VM((block, units // 2), f32), VM((block, units // 2), f32), pltpu.SemaphoreType.DMA((3,))],
        compiler_params=pltpu.CompilerParams(vmem_limit_bytes=62 << 20),
        cost_estimate=pl.CostEstimate(flops=4 * rows * width * (2 * parts * units + parts * own), bytes_accessed=40 << 20, transcendentals=rows * units * parts),
        name="dense",
    )(x, cot, ctx0, ctx1, vectors, inner_bias, near)


def head_columns(weights, own, head):
    return [weights[:, kind * own + head * HD : kind * own + (head + 1) * HD] for kind in range(3)]


def early_back_body(own, w_ref, b0_ref, b1_ref, acc_ref):
    acc_ref[...] = jnp.zeros(acc_ref.shape, jnp.float32)

    def add(t, _):
        both = jnp.concatenate([b0_ref[t], b1_ref[t]], axis=0)
        weights = w_ref[t]
        weights = jnp.concatenate(head_columns(weights, own, 0) + head_columns(weights, own, 1), axis=1)
        acc_ref[...] += dot(weights, both)
        return 0

    lax.fori_loop(0, b0_ref.shape[0], add, 0)


def late_back_body(own, head, part_ref, w_ref, acc_ref, grad_ref, *rest):
    backs, out_ref = rest[:-1], rest[-1]
    parts = len(backs)
    total = acc_ref[...]
    for d in range(parts):
        weights = w_ref[(part_ref[0] + parts - d) % parts]
        total = total + dot(jnp.concatenate(head_columns(weights, own, head), axis=1), backs[d][...])
    out_ref[...] = (total.T + grad_ref[...]).astype(out_ref.dtype)


def weight_block(rest, cols):
    return pl.BlockSpec(rest.shape[:2] + (cols,), lambda i, *_: (0, 0, 0), pipeline_mode=pl.Buffered(1))


def whole(a):
    return pl.BlockSpec(a.shape, lambda i, *_: (0,) * a.ndim, pipeline_mode=pl.Buffered(1))


def early_back(rest, own, b0, b1):
    width, rows = rest.shape[1], b0.shape[2]
    return pl.pallas_call(
        functools.partial(early_back_body, own),
        grid=(1,),
        in_specs=[weight_block(rest, 4 * own), whole(b0), whole(b1)],
        out_specs=pl.BlockSpec((width, rows), lambda i: (0, 0)),
        out_shape=jax.ShapeDtypeStruct((width, rows), jnp.float32),
        compiler_params=pltpu.CompilerParams(vmem_limit_bytes=62 << 20),
        cost_estimate=pl.CostEstimate(flops=4 * width * rows * b0.shape[0] * b0.shape[1], bytes_accessed=10 << 20, transcendentals=0),
        name="early_back",
    )(rest, b0, b1)


def late_back(rest, own, head, part, acc, grad, backs):
    rows, width = grad.shape
    return pl.pallas_call(
        functools.partial(late_back_body, own, head),
        grid_spec=pltpu.PrefetchScalarGridSpec(
            num_scalar_prefetch=1,
            grid=(1,),
            in_specs=[weight_block(rest, 4 * own), whole(acc), whole(grad)] + [whole(b) for b in backs],
            out_specs=pl.BlockSpec((rows, width), lambda i, *_: (0, 0)),
        ),
        out_shape=jax.ShapeDtypeStruct((rows, width), jnp.bfloat16),
        compiler_params=pltpu.CompilerParams(vmem_limit_bytes=62 << 20),
        cost_estimate=pl.CostEstimate(flops=2 * width * rows * backs[0].shape[0] * len(backs), bytes_accessed=10 << 20, transcendentals=0),
        name="late_back",
    )(part.reshape(1), rest, acc, grad, *backs)


def add_up(value, axis):
    size = lax.axis_size(axis)
    span, turn = 1, 0
    while span < size:
        other = lax.ppermute(value, axis, [(i, i ^ span) for i in range(size)])
        value = value + other
        span *= 2
        turn += 1
    return value


def two_halves(value):
    high = value.astype(jnp.bfloat16)
    return high, (value - high.astype(jnp.float32)).astype(jnp.bfloat16)


def rotate(blocks, axis):
    size = lax.axis_size(axis)
    me = lax.axis_index(axis)
    out = []
    for d in range(size):
        block = lax.dynamic_index_in_dim(blocks, (me + d) % size, 0, keepdims=False)
        if d:
            block = lax.ppermute(block, axis, [(i, (i + d) % size) for i in range(size)])
        out.append(block)
    return out


def body(hidden_in, segments, query_weight, key_weight, value_weight, query_bias, value_bias, mixer_weight, mixer_bias, first_gain, first_shift, inner_weight, inner_bias, outer_weight, outer_bias, second_gain, second_shift, cotangent):
    f32 = jnp.float32
    _, rows, width = hidden_in.shape
    parts = lax.axis_size("tensor")
    groups = lax.axis_size("dp")
    rank = lax.axis_index("tensor")
    own = query_weight.shape[1]
    heads = own // HD
    units = inner_weight.shape[1]
    x_own = hidden_in[0]
    small = jnp.concatenate([segments[0].astype(f32), inner_bias]).reshape(-1, 128)
    near_own = jnp.concatenate([query_weight, key_weight, value_weight, mixer_weight.T, inner_weight, outer_weight.T], 1)
    x_parts, near, small = start(x_own, near_own, small)
    x_all = x_parts.reshape(parts * rows, width)
    near = near.reshape(parts, width, 4 * own + 2 * units)
    small = small.reshape(parts, -1)
    segment_all = small[:, :rows].astype(jnp.int32).reshape(-1)
    inner_bias_all = small[:, rows:]
    biases = jnp.concatenate([query_bias, jnp.zeros_like(query_bias), value_bias])

    qt, ka, vt, kt, vn = project(x_all, near, rank, biases, segment_all)
    lead = heads - 1
    context_t, lse, exchanged = [], [], []
    for call, (first, count, block) in enumerate(((0, lead, rows // 2), (lead, 1, rows))):
        lo, hi = ranges(segment_all, block, 512)
        part, out_t, out_lse = attend_forward(first, count, parts, qt, ka, vt, lo, hi, BQ=block)
        context_t.append(out_t)
        lse.append(out_lse)
        if exchanged:
            part, exchanged[-1] = lax.optimization_barrier((part, exchanged[-1]))
        exchanged.append(lax.all_to_all(part, "tensor", 0, 0, tiled=True))
    vectors = jnp.stack([mixer_bias, first_gain, first_shift, outer_bias, second_gain, second_shift])
    vectors = jnp.pad(vectors, ((0, 2), (0, 0)))
    layer_out, first_low, second_low, attn_low, grad_attn, both, context, go0, go1, early = dense(
        own, x_own, cotangent[0], exchanged[0], exchanged[1], vectors, inner_bias_all, near, block=rows // 2
    )
    go0 = lax.all_to_all(go0, "tensor", 0, 0, tiled=True)
    go1 = lax.all_to_all(go1, "tensor", 0, 0, tiled=True)
    weight_grads = weight_grads_of(
        first_low, second_low, attn_low, both, context
    )
    weight_grads = lax.psum_scatter(weight_grads, "dp", scatter_dimension=0, tiled=True)
    weight_grads = jnp.concatenate(
        [
            weight_grads[:, : 2 * units * parts].reshape(-1, parts, 2 * units),
            weight_grads[:, 2 * units * parts :].reshape(-1, parts, own),
        ],
        2,
    ).transpose(1, 0, 2)
    weight_grads = rotate(weight_grads, "tensor")
    weight_grads = sum(a.astype(f32) for a in weight_grads)
    early = add_up(early[: 6 + parts], "tensor")
    count = 6 + parts
    lines = -(-count * width // (3 * own))
    early = jnp.pad(early.reshape(-1), (0, lines * 3 * own - count * width)).reshape(lines, 3 * own)
    early = jnp.concatenate(two_halves(early), 0)

    lo, hi = ranges(segment_all, 512, 512)
    backs, qkv_grad, bias_grad = [], [], []
    for h in range(heads):
        call = 0 if h < lead else 1
        grads, weight_part, sums = attend_backward(
            h, 1, go1 if h else go0, h - 1 if h else 0, context_t[call], lse[call], h - call * lead, qt, ka, kt, vn, x_parts, lo, hi
        )
        if h < heads - 1:
            backs.append(lax.all_to_all(grads, "tensor", 0, 0, tiled=True))
        else:
            backs.append(rotate(grads, "tensor"))
        qkv_grad.append(weight_part)
        bias_grad.append(sums[:, 0])
    input_back = early_back(near, own, backs[0], backs[1])
    input_grad = late_back(near, own, heads - 1, rank, input_back, grad_attn, backs[2])
    each = width // groups
    by_kind = lambda per_head: [a[..., n * HD : (n + 1) * HD] for n in range(3) for a in per_head]
    bias_grad = jnp.stack(two_halves(jnp.concatenate(by_kind(bias_grad))))
    extra = jnp.concatenate([early, bias_grad], 0)
    spare = -extra.shape[0] % 16
    extra = jnp.pad(extra, ((0, spare), (0, 0)))
    extra = jnp.broadcast_to(extra[None], (groups,) + extra.shape)
    qkv_grad = jnp.concatenate(by_kind(qkv_grad), 1).reshape(groups, each, 3 * own)
    qkv_grad = jnp.concatenate([qkv_grad, extra], 1)
    qkv_grad = lax.all_to_all(qkv_grad, "dp", 0, 0, tiled=True)
    qkv_grad = jnp.sum(qkv_grad.astype(f32), 0)
    early = qkv_grad[each : each + lines] + qkv_grad[each + lines : each + 2 * lines]
    early = early.reshape(-1)[: count * width].reshape(count, width)
    bias_grad = qkv_grad[each + 2 * lines] + qkv_grad[each + 2 * lines + 1]
    inner_bias_out = lax.dynamic_index_in_dim(early, 6 + rank, 0, keepdims=False)
    return (
        layer_out[None],
        input_grad[None],
        qkv_grad[:each, 0 * own : 1 * own],
        qkv_grad[:each, 1 * own : 2 * own],
        qkv_grad[:each, 2 * own : 3 * own],
        bias_grad[:own],
        bias_grad[2 * own :],
        weight_grads[:, 2 * units :].T,
        early[0],
        early[1],
        early[2],
        weight_grads[:, :units],
        inner_bias_out,
        weight_grads[:, units : 2 * units].T,
        early[3],
        early[4],
        early[5],
    )


def solution(mesh):
    placed = (
        P("dp", "tensor", None),
        P("dp", "tensor"),
        P("dp", "tensor"),
        P("dp", "tensor"),
        P("dp", "tensor"),
        P("tensor"),
        P("tensor"),
        P("tensor", "dp"),
        P(),
        P(),
        P(),
        P("dp", "tensor"),
        P("tensor"),
        P("tensor", "dp"),
        P(),
        P(),
        P(),
        P("dp", "tensor", None),
    )

    return jax.shard_map(
        body,
        mesh=mesh,
        in_specs=placed,
        out_specs=(
            P("dp", "tensor", None),
            P("dp", "tensor", None),
            P("dp", "tensor"),
            P("dp", "tensor"),
            P("dp", "tensor"),
            P("tensor"),
            P("tensor"),
            P("tensor", "dp"),
            P(),
            P(),
            P(),
            P("dp", "tensor"),
            P("tensor"),
            P("tensor", "dp"),
            P(),
            P(),
            P(),
        ),
        check_vma=False,
    )
```

```python
import functools

import jax
import jax.numpy as jnp
from jax import lax
from jax.experimental import pallas as pl
from jax.experimental.pallas import tpu as pltpu
from jax.sharding import PartitionSpec as P


EPS = 1e-12
ROOT_HALF = 0.7071067811865476
INV_ROOT_TWO_PI = 0.3989422804014327
HD=64; SCALE=0.125; APART=-1e30
VM=pltpu.VMEM


def dot(a,b): return jnp.dot(a,b,preferred_element_type=jnp.float32)


def project_body(heads, part_ref, x_ref, w_ref, b_ref, srow_ref, qt_ref, ka_ref, vt_ref, kt_ref, vn_ref):
    y=dot(x_ref[...], w_ref[0,:,:b_ref.shape[1]]) + b_ref[...]
    low = y.astype(jnp.bfloat16)
    yt = low.T
    rows = y.shape[0]
    match = lax.broadcasted_iota(jnp.int32,(HD,rows),0)==srow_ref[...]
    apart = jnp.where(match,0.0,APART).astype(jnp.bfloat16)
    same = jnp.where(match,1.0,0.0).T.astype(jnp.bfloat16)
    width=heads*HD
    for h in range(heads):
        q_at,k_at,v_at=h*HD,width+h*HD,2*width+h*HD
        qt_ref[h,:HD,:]=yt[q_at:q_at+HD]*jnp.bfloat16(SCALE)
        qt_ref[h,HD:,:]=apart
        ka_ref[h]=jnp.concatenate([low[:,k_at:k_at+HD],same],axis=1)
        kt_ref[h]=yt[k_at:k_at+HD]
        vt_ref[h]=yt[v_at:v_at+HD]
        vn_ref[h]=low[:,v_at:v_at+HD]


def project(x,rest,part,b,seg,rows=512):
    L,D=x.shape; heads=b.shape[0]//(3*HD)
    bf=jnp.bfloat16
    cols=4*heads*HD
    nat=lambda n: pl.BlockSpec((heads,rows,n),lambda i,*_:(0,i,0))
    tr=lambda n: pl.BlockSpec((heads,n,rows),lambda i,*_:(0,0,i))
    S=jax.ShapeDtypeStruct
    return pl.pallas_call(functools.partial(project_body,heads),
        grid_spec=pltpu.PrefetchScalarGridSpec(num_scalar_prefetch=1,grid=(L//rows,),
        in_specs=[pl.BlockSpec((rows,D),lambda i,*_:(i,0)),pl.BlockSpec((1,D,cols),lambda i,p:(p[0],0,0)),pl.BlockSpec((1,b.shape[0]),lambda i,*_:(0,0)),
                  pl.BlockSpec((1,rows),lambda i,*_:(0,i))],
        out_specs=[tr(2*HD),nat(2*HD),tr(HD),tr(HD),nat(HD)]),
        out_shape=[S((heads,2*HD,L),bf),S((heads,L,2*HD),bf),S((heads,HD,L),bf),S((heads,HD,L),bf),S((heads,L,HD),bf)],
        compiler_params=pltpu.CompilerParams(vmem_limit_bytes=62 << 20),
        cost_estimate=pl.CostEstimate(flops=2*L*D*b.shape[0],bytes_accessed=L*D*2+D*cols*2+L*heads*HD*2*10,transcendentals=0),
        name="project")(part.reshape(1),x,rest,b.reshape(1,-1),seg.reshape(1,-1))


def forward_body(BK, lo_ref, hi_ref, qt_ref, ka_ref, vt_ref, ctx_ref, ot_ref, lse_ref, m_s, l_s, acc, s_even, s_odd):
    i=pl.program_id(0)
    heads=qt_ref.shape[0]
    half=BK//2
    m_s[...]=jnp.full(m_s.shape,-jnp.inf,jnp.float32)
    l_s[...]=jnp.zeros(l_s.shape,jnp.float32)
    acc[...]=jnp.zeros(acc.shape,jnp.float32)

    def scores(h,at):
        return dot(ka_ref[h,pl.ds(pl.multiple_of(at,half),half),:],qt_ref[h])

    def use(h,at,s):
        m_old=m_s[h]
        m_new=jnp.maximum(m_old,jnp.max(s,axis=0,keepdims=True))
        p=jnp.exp(s-m_new)
        alpha=jnp.exp(m_old-m_new)
        m_s[h]=m_new
        l_s[h]=l_s[h]*alpha+jnp.sum(p,axis=0,keepdims=True)
        acc[h]=acc[h]*alpha+dot(vt_ref[h,:,pl.ds(pl.multiple_of(at,half),half)],p.astype(jnp.bfloat16))

    last=hi_ref[i]-1
    for h in range(heads):
        s_even[h]=scores(h,lo_ref[i]*BK)

    def step(j,_):
        at=j*BK
        for h in range(heads):
            s_odd[h]=scores(h,at+half)
            use(h,at,s_even[h])
        for h in range(heads):
            s_even[h]=scores(h,jnp.minimum(j+1,last)*BK)
            use(h,at+half,s_odd[h])
        return 0

    lax.fori_loop(lo_ref[i],hi_ref[i],step,0)
    for h in range(heads):
        o=acc[h]/l_s[h]
        lse_ref[h]=m_s[h]+jnp.log(l_s[h])
        ot_ref[h]=o
        ctx_ref[0,h*HD:(h+1)*HD,:]=o.astype(jnp.bfloat16)


def attend_forward(first,heads,parts,qt,ka,vt,lo,hi,BQ=384,BK=512):
    L=qt.shape[2]
    S=jax.ShapeDtypeStruct
    per=L//parts//BQ
    return pl.pallas_call(functools.partial(forward_body,BK),
        grid_spec=pltpu.PrefetchScalarGridSpec(num_scalar_prefetch=2,grid=(L//BQ,),
        in_specs=[pl.BlockSpec((heads,2*HD,BQ),lambda i,*_:(first//heads,0,i)),pl.BlockSpec((heads,L,2*HD),lambda i,*_:(first//heads,0,0)),pl.BlockSpec((heads,HD,L),lambda i,*_:(first//heads,0,0))],
        out_specs=[pl.BlockSpec((1,heads*HD,BQ),lambda i,*_:(i//per,0,i%per)),pl.BlockSpec((heads,HD,BQ),lambda i,*_:(0,0,i)),pl.BlockSpec((heads,1,BQ),lambda i,*_:(0,0,i))],
        scratch_shapes=[VM((heads,1,BQ),jnp.float32),VM((heads,1,BQ),jnp.float32),VM((heads,HD,BQ),jnp.float32)]+[VM((heads,BK//2,BQ),jnp.float32)]*2),
        out_shape=[S((parts,heads*HD,L//parts),jnp.bfloat16),S((heads,HD,L),jnp.float32),S((heads,1,L),jnp.float32)],
        compiler_params=pltpu.CompilerParams(vmem_limit_bytes=62 << 20),
        cost_estimate=pl.CostEstimate(flops=2*L*L*HD*2*heads,bytes_accessed=L*heads*HD*2*8,transcendentals=L*L*heads),
        name="attend_forward")(lo,hi,qt,ka,vt)


def backward_body(BQ, BK, lo_ref, hi_ref, go_ref, ot_ref, lse_ref, qt_ref, ka_ref, kt_ref, vn_ref, x_ref, out_ref, wg_ref, sum_ref, got, delta, dqt, dkt, dvt, dk_s, dv_s, x_s, x_sem):
    bring=pltpu.make_async_copy(x_ref,x_s,x_sem)
    bring.start()
    parts,_,rows=go_ref.shape
    heads,_,L=qt_ref.shape
    CH=256
    for h in range(heads):
        for c in range(L//CH):
            p,at=c*CH//rows,c*CH%rows
            gt=go_ref[p,h*HD:(h+1)*HD,at:at+CH]
            wide=gt.astype(jnp.float32)
            got[h,:,c*CH:(c+1)*CH]=gt
            delta[h,:,c*CH:(c+1)*CH]=jnp.sum(wide*ot_ref[h,:,c*CH:(c+1)*CH],axis=0,keepdims=True)
    dqt[...]=jnp.zeros(dqt.shape,jnp.float32)

    def key_block(j,_):
        ka_at=pl.multiple_of(j*BK,BK)
        dk_s[...]=jnp.zeros(dk_s.shape,jnp.float32)
        dv_s[...]=jnp.zeros(dv_s.shape,jnp.float32)

        def query_block(i,_):
            for h in range(heads):
                at=pl.multiple_of(i*BQ,BQ)
                s=dot(ka_ref[h,pl.ds(ka_at,BK),:],qt_ref[h,:,pl.ds(at,BQ)])
                p=jnp.exp(s-lse_ref[h,:,pl.ds(at,BQ)])
                dp=dot(vn_ref[h,pl.ds(ka_at,BK),:],got[h,:,pl.ds(at,BQ)])
                ds=(p*(dp-delta[h,:,pl.ds(at,BQ)])).astype(jnp.bfloat16)
                dv_s[h]+=dot_right_t(got[h,:,pl.ds(at,BQ)],p.astype(jnp.bfloat16))
                dk_s[h]+=dot_right_t(qt_ref[h,:HD,pl.ds(at,BQ)],ds)
                dqt[h,:,pl.ds(at,BQ)]+=dot(kt_ref[h,:,pl.ds(ka_at,BK)],ds)
            return 0

        lax.fori_loop(lo_ref[j],hi_ref[j],query_block,0)
        for h in range(heads):
            dkt[h,:,pl.ds(ka_at,BK)]=dk_s[h].astype(jnp.bfloat16)
            dvt[h,:,pl.ds(ka_at,BK)]=dv_s[h].astype(jnp.bfloat16)
        return 0

    lax.fori_loop(0,L//BK,key_block,0)
    for h in range(heads):
        for p in range(parts):
            cut=slice(p*rows,(p+1)*rows)
            out_ref[p,3*h*HD:(3*h+1)*HD,:]=(dqt[h,:,cut]*SCALE).astype(jnp.bfloat16)
            out_ref[p,(3*h+1)*HD:(3*h+2)*HD,:]=dkt[h,:,cut]
            out_ref[p,(3*h+2)*HD:(3*h+3)*HD,:]=dvt[h,:,cut]
    bring.wait()
    wg=jnp.zeros(wg_ref.shape[::-1],jnp.float32)
    total=jnp.zeros((3*heads*HD,1),jnp.float32)
    for p in range(parts):
        part=out_ref[p]
        wg=wg+dot(part,x_s[p])
        total=total+jnp.sum(part.astype(jnp.float32),axis=1,keepdims=True)
    wg_ref[...]=wg.T.astype(wg_ref.dtype)
    sum_ref[...]=jnp.broadcast_to(total,sum_ref.shape)


def attend_backward(first,heads,go,go_first,ot,lse,ot_first,qt,ka,kt,vn,x,lo,hi,BQ=512,BK=512):
    parts,_,rows=go.shape; L=parts*rows; D=x.shape[2]
    S=jax.ShapeDtypeStruct; f32=jnp.float32; bf=jnp.bfloat16
    at=lambda a,n: pl.BlockSpec((heads,)+a.shape[1:],lambda i,*_:(n//heads,0,0),pipeline_mode=pl.Buffered(1))
    out=3*heads*HD
    return pl.pallas_call(functools.partial(backward_body,BQ,BK),
        grid_spec=pltpu.PrefetchScalarGridSpec(num_scalar_prefetch=2,grid=(1,),
        in_specs=[pl.BlockSpec((parts,heads*HD,rows),lambda i,*_:(0,go_first,0),pipeline_mode=pl.Buffered(1)),at(ot,ot_first),at(lse,ot_first)]+[at(a,first) for a in (qt,ka,kt,vn)]+[pl.BlockSpec(memory_space=pl.ANY)],
        out_specs=[pl.BlockSpec((parts,out,rows),lambda i,*_:(0,0,0),pipeline_mode=pl.Buffered(1)),pl.BlockSpec((D,out),lambda i,*_:(0,0)),pl.BlockSpec((out,128),lambda i,*_:(0,0))],
        scratch_shapes=[VM((heads,HD,L),bf),VM((heads,1,L),f32),VM((heads,HD,L),f32),VM((heads,HD,L),bf),VM((heads,HD,L),bf),VM((heads,HD,BK),f32),VM((heads,HD,BK),f32),VM(x.shape,bf),pltpu.SemaphoreType.DMA]),
        out_shape=[S((parts,out,rows),bf),S((D,out),bf),S((out,128),f32)],
        compiler_params=pltpu.CompilerParams(vmem_limit_bytes=62 << 20),
        cost_estimate=pl.CostEstimate(flops=2*L*L*HD*5*heads,bytes_accessed=L*heads*HD*2*14,transcendentals=L*L*heads),
        name="attend_backward")(lo,hi,go,ot,lse,qt,ka,kt,vn,x)


def ranges(seg,BQ,BK):
    first=seg.reshape(-1,BQ)[:,0]; last=seg.reshape(-1,BQ)[:,-1]
    kf=seg.reshape(-1,BK)[:,0]; kl=seg.reshape(-1,BK)[:,-1]
    lo=jnp.sum((kl[None,:]<first[:,None]).astype(jnp.int32),1)
    hi=jnp.sum((kf[None,:]<=last[:,None]).astype(jnp.int32),1)
    return lo,hi


def dot_right_t(left, right):
    return lax.dot_general(
        left, right, (((1,), (1,)), ((), ())), preferred_element_type=jnp.float32
    )


def layer_norm(values_in, gain, shift):
    mean_row = jnp.mean(values_in, -1, keepdims=True)
    centered = values_in - mean_row
    inverse = lax.rsqrt(jnp.mean(centered * centered, -1, keepdims=True) + EPS)
    normed = centered * inverse
    return (normed * gain + shift, normed, inverse)


def norm_back(grad_in, normed, inverse, gain):
    scaled = grad_in * gain
    return inverse * (
        scaled
        - jnp.mean(scaled, -1, keepdims=True)
        - normed * jnp.mean(scaled * normed, -1, keepdims=True)
    )


MESH = pl.DeviceIdType.MESH


def flip(index, bit):
    span = 1 << bit
    return index + span * (1 - 2 * ((index // span) % 2))


def start_body(n, bits, x_ref, w_ref, s_ref, x_out, w_out, s_out, send_z, recv_z, send_d, recv_d, keep_sem):
    me = lax.axis_index("tensor")
    mine = lax.axis_index("dp")
    barrier = pltpu.get_barrier_semaphore()

    @pl.when(me > 0)
    def _():
        pl.semaphore_signal(barrier, inc=1, device_id={"tensor": me - 1}, device_id_type=MESH)

    @pl.when(me < n - 1)
    def _():
        pl.semaphore_signal(barrier, inc=1, device_id={"tensor": me + 1}, device_id_type=MESH)

    for bit in range(bits):
        pl.semaphore_signal(barrier, inc=1, device_id={"dp": flip(mine, bit)}, device_id_type=MESH)
    pl.semaphore_wait(barrier, bits + jnp.where(me > 0, 1, 0) + jnp.where(me < n - 1, 1, 0))

    keeps = [
        pltpu.make_async_copy(x_ref, x_out.at[me], keep_sem.at[0]),
        pltpu.make_async_copy(w_ref, w_out.at[me, mine], keep_sem.at[1]),
        pltpu.make_async_copy(s_ref, s_out.at[me], keep_sem.at[2]),
    ]
    for keep in keeps:
        keep.start()

    def hop(kind, side, step):
        block = me - (step - 1) if side else me + (step - 1)
        first, place = (
            (x_ref, x_out.at[block]),
            (w_ref, w_out.at[block, mine]),
            (s_ref, s_out.at[block]),
        )[kind]
        return pltpu.make_async_remote_copy(
            src_ref=first if step == 1 else place,
            dst_ref=place,
            send_sem=send_z.at[kind, side, step - 1],
            recv_sem=recv_z.at[kind, side, step - 1],
            device_id={"tensor": me + 1 if side else me - 1},
            device_id_type=MESH,
        )

    def sends(side, step):
        if side:
            return (me < n - 1) & (me >= step - 1)
        return (me > 0) & (me + step - 1 <= n - 1)

    def receives(side, step):
        return me >= step if side else me + step <= n - 1

    def z_start(kinds, step):
        for side in (0, 1):

            @pl.when(sends(side, step))
            def _():
                for kind in kinds:
                    hop(kind, side, step).start()

    def z_arrive(kinds, step):
        for side in (0, 1):

            @pl.when(receives(side, step))
            def _():
                for kind in kinds:
                    hop(kind, side, step).wait_recv()

    half = w_ref.shape[1] // 2
    up = list(range(bits - 1, -1, -1))
    orders = (up, [up[1], up[0]] + up[2:] if bits > 1 else up)

    def doubling(side, step):
        order = orders[side]
        held = [mine]
        for bit in order[:step]:
            held = held + [flip(d, bit) for d in held]
        cut = pl.ds(side * half, half)
        return [
            pltpu.make_async_remote_copy(
                src_ref=w_out.at[:, d, :, cut],
                dst_ref=w_out.at[:, d, :, cut],
                send_sem=send_d.at[side, (1 << step) - 1 + at],
                recv_sem=recv_d.at[side, (1 << step) - 1 + at],
                device_id={"dp": flip(mine, order[step])},
                device_id_type=MESH,
            )
            for at, d in enumerate(held)
        ]

    def d_start(step):
        for side in (0, 1):
            for copy in doubling(side, step):
                copy.start()

    def d_arrive(step):
        for side in (0, 1):
            for copy in doubling(side, step):
                copy.wait_recv()

    for step in range(1, n):
        z_start((1, 2), step)
        z_arrive((1, 2), step)
    keeps[1].wait()
    for step in range(max(n - 1, bits)):
        if step < bits:
            if step:
                d_arrive(step - 1)
            d_start(step)
        if step < n - 1:
            if step:
                z_arrive((0,), step)
            z_start((0,), step + 1)
    z_arrive((0,), n - 1)
    d_arrive(bits - 1)
    for side in (0, 1):
        for step in range(1, n):

            @pl.when(sends(side, step))
            def _():
                for kind in (0, 1, 2):
                    hop(kind, side, step).wait_send()

        for step in range(bits):
            for copy in doubling(side, step):
                copy.wait_send()
    keeps[0].wait()
    keeps[2].wait()


def start(x, w, small):
    n = lax.axis_size("tensor")
    groups = lax.axis_size("dp")
    bits = groups.bit_length() - 1
    S = jax.ShapeDtypeStruct
    anywhere = pl.BlockSpec(memory_space=pl.ANY)
    return pl.pallas_call(
        functools.partial(start_body, n, bits),
        in_specs=[pl.BlockSpec(memory_space=pltpu.VMEM)] * 3,
        out_specs=[anywhere] * 3,
        out_shape=[
            S((n,) + x.shape, x.dtype),
            S((n, groups) + w.shape, w.dtype),
            S((n,) + small.shape, small.dtype),
        ],
        scratch_shapes=[
            pltpu.SemaphoreType.DMA((3, 2, n - 1)),
            pltpu.SemaphoreType.DMA((3, 2, n - 1)),
            pltpu.SemaphoreType.DMA((2, groups - 1)),
            pltpu.SemaphoreType.DMA((2, groups - 1)),
            pltpu.SemaphoreType.DMA((3,)),
        ],
        compiler_params=pltpu.CompilerParams(collective_id=0, has_side_effects=True),
        cost_estimate=pl.CostEstimate(flops=0, bytes_accessed=200 << 20, transcendentals=0),
        name="start",
    )(x, w, small)


def weight_grads_body(parts, first_ref, second_ref, attn_ref, both_ref, context_ref, out_ref, left):
    j = pl.program_id(0)

    @pl.when(j == 0)
    def _():
        left[0] = first_ref[...].T
        left[1] = second_ref[...].T

    @pl.when(j < 2 * parts)
    def _():
        out_ref[...] = dot(left[j % 2], both_ref[0]).astype(out_ref.dtype)

    @pl.when(j == 2 * parts)
    def _():
        out_ref[...] = dot_right_t(attn_ref[...].T, context_ref[...]).astype(out_ref.dtype)


def weight_grads_of(first_low, second_low, attn_low, both, context):
    steps, rows, units = both.shape
    width = first_low.shape[1]
    features = context.shape[0]
    fixed = pl.BlockSpec((rows, width), lambda j: (0, 0))
    return pl.pallas_call(
        functools.partial(weight_grads_body, steps // 2),
        grid=(steps + 1,),
        in_specs=[fixed, fixed, fixed, pl.BlockSpec((1, rows, units), lambda j: (jnp.minimum(j, steps - 1), 0, 0)), pl.BlockSpec((features, rows), lambda j: (0, 0))],
        out_specs=pl.BlockSpec((width, units), lambda j: (0, j)),
        out_shape=jax.ShapeDtypeStruct((width, units * steps + features), jnp.bfloat16),
        scratch_shapes=[VM((2, width, rows), jnp.bfloat16)],
        compiler_params=pltpu.CompilerParams(vmem_limit_bytes=62 << 20),
        cost_estimate=pl.CostEstimate(flops=2 * rows * width * (steps * units + features), bytes_accessed=rows * units * steps * 4, transcendentals=0),
        name="weight_grads",
    )(first_low, second_low, attn_low, both, context)


def erf(x):
    x = jnp.clip(x, -3.7439211627767994, 3.7439211627767994)
    y = x * x
    top = jnp.float32(0.00022905065861350646)
    for c in (0.0034082910107109506, 0.050955695062380861, 0.18520832239976145, 1.128379143519084):
        top = top * y + c
    low = jnp.float32(-1.1791602954361697e-7)
    for c in (0.000023547966471313185, 0.0010179625278914885, 0.014070470171167667, 0.11098505178285362, 0.49746925110067538, 1.0):
        low = low * y + c
    return x * top / low


def dense_body(own, x_ref, cot_ref, ctx0_ref, ctx1_ref, vec_ref, bias_ref, near_ref, out_ref, first_ref, second_ref, attn_ref, grad_ref, both_ref, ctx_ref, go0_ref, go1_ref, sum_ref, w_s, mt_s, slope_s, first_s, acc_s, even_s, odd_s, w_sem):
    i = pl.program_id(0)
    parts, _, _ = near_ref.shape
    f32, bf = jnp.float32, jnp.bfloat16
    units = both_ref.shape[2]
    cuts = (slice(0, 4 * own), slice(4 * own, 4 * own + units), slice(4 * own + units, 4 * own + 2 * units))
    sources = (near_ref.at[:, :, cuts[0]], near_ref.at[:, :, cuts[1]], near_ref.at[:, :, cuts[2]])
    copies = [pltpu.make_async_copy(sources[c], w_s.at[:, :, cut], w_sem.at[c]) for c, cut in enumerate(cuts)]

    @pl.when(i == 0)
    def _():
        for copy in copies:
            copy.start()
        sum_ref[...] = jnp.zeros(sum_ref.shape, f32)
        copies[0].wait()
        for t in range(parts):
            mt_s[:, t * own : (t + 1) * own] = w_s[t, :, 3 * own : 4 * own]

    def add_sum(row, value):
        sum_ref[row : row + 1, :] += jnp.sum(value, axis=0, keepdims=True)

    for t in range(parts):
        lead = ctx0_ref.shape[1]
        ctx_ref[t * own : t * own + lead, :] = ctx0_ref[t]
        ctx_ref[t * own + lead : (t + 1) * own, :] = ctx1_ref[t]
    mixed = dot(mt_s[...], ctx_ref[...]).T
    attn_in = x_ref[...].astype(f32) + mixed + vec_ref[0:1]
    first, first_norm, first_inv = layer_norm(attn_in, vec_ref[1:2], vec_ref[2:3])
    first_ref[...] = first.astype(bf)
    first_s[...] = first_norm
    acc_s[...] = first + vec_ref[3:4]

    @pl.when(i == 0)
    def _():
        copies[1].wait()
        copies[2].wait()

    half_units = units // 2
    first_cut, second_cut = slice(0, half_units), slice(half_units, units)
    base = 4 * own

    def before(t, cut):
        return dot(first_ref[...], w_s[t, :, base + cut.start : base + cut.stop]) + bias_ref[t, :, cut]

    def after(t, cut, inner):
        half = 0.5 * (1.0 + erf(inner * ROOT_HALF))
        slope_s[t, :, cut] = half + inner * jnp.exp(-0.5 * inner * inner) * INV_ROOT_TWO_PI
        active = (inner * half).astype(bf)
        both_ref[2 * t + 1, :, cut] = active
        acc_s[...] += dot_right_t(active, w_s[t, :, base + units + cut.start : base + units + cut.stop])

    even_s[...] = before(0, first_cut)

    def ahead(t, _):
        odd_s[...] = before(t, second_cut)
        after(t, first_cut, even_s[...])
        even_s[...] = before(jnp.minimum(t + 1, parts - 1), first_cut)
        after(t, second_cut, odd_s[...])
        return 0

    lax.fori_loop(0, parts, ahead, 0)
    second, second_norm, second_inv = layer_norm(acc_s[...], vec_ref[4:5], vec_ref[5:6])
    out_ref[...] = second.astype(bf)
    grad_out = cot_ref[...].astype(f32)
    add_sum(4, grad_out * second_norm)
    add_sum(5, grad_out)
    grad_second = norm_back(grad_out, second_norm, second_inv, vec_ref[4:5])
    add_sum(3, grad_second)
    second_ref[...] = grad_second.astype(bf)
    acc_s[...] = grad_second

    def back(t, _):
        grad_inner = (dot(second_ref[...], w_s[t, :, cuts[2]]) * slope_s[t]).astype(bf)
        both_ref[2 * t] = grad_inner
        sum_ref[pl.ds(6 + t, 1), :] += jnp.sum(grad_inner.astype(f32), axis=0, keepdims=True)
        acc_s[...] += dot_right_t(grad_inner, w_s[t, :, cuts[1]])
        return 0

    lax.fori_loop(0, parts, back, 0)
    grad_first = acc_s[...]
    first_norm = first_s[...]
    add_sum(1, grad_first * first_norm)
    add_sum(2, grad_first)
    grad_attn = norm_back(grad_first, first_norm, first_inv, vec_ref[1:2])
    add_sum(0, grad_attn)
    grad_ref[...] = grad_attn
    attn_ref[...] = grad_attn.astype(bf)
    grad_context = dot(attn_ref[...], mt_s[...]).T.astype(bf)
    for t in range(parts):
        go0_ref[t] = grad_context[t * own : t * own + HD]
        go1_ref[t] = grad_context[t * own + HD : (t + 1) * own]


def dense(own, x, cot, ctx0, ctx1, vectors, inner_bias, near, block):
    rows, width = x.shape
    parts = near.shape[0]
    cols = near.shape[2]
    units = (cols - 4 * own) // 2
    f32, bf = jnp.float32, jnp.bfloat16
    S = jax.ShapeDtypeStruct
    tok = pl.BlockSpec((block, width), lambda i: (i, 0))
    part_tok = pl.BlockSpec((2 * parts, block, units), lambda i: (0, i, 0))
    lanes = lambda n: pl.BlockSpec((parts, n, block), lambda i: (0, 0, i))
    fixed = lambda a: pl.BlockSpec(a.shape, lambda i: (0,) * a.ndim)
    inner_bias = inner_bias.reshape(parts, 1, units)
    return pl.pallas_call(
        functools.partial(dense_body, own),
        grid=(rows // block,),
        in_specs=[tok, tok, lanes(ctx0.shape[1]), lanes(ctx1.shape[1]), fixed(vectors), fixed(inner_bias), pl.BlockSpec(memory_space=pl.ANY)],
        out_specs=[tok] * 5 + [part_tok] + [pl.BlockSpec((parts * own, block), lambda i: (0, i)), lanes(HD), lanes(own - HD), pl.BlockSpec((16, width), lambda i: (0, 0))],
        out_shape=[S((rows, width), bf)] * 4 + [S((rows, width), f32)] + [S((2 * parts, rows, units), bf)] + [S((parts * own, rows), bf), S((parts, HD, rows), bf), S((parts, own - HD, rows), bf), S((16, width), f32)],
        scratch_shapes=[VM((parts, width, cols), bf), VM((width, parts * own), bf), VM((parts, block, units), f32), VM((block, width), f32), VM((block, width), f32), VM((block, units // 2), f32), VM((block, units // 2), f32), pltpu.SemaphoreType.DMA((3,))],
        compiler_params=pltpu.CompilerParams(vmem_limit_bytes=62 << 20),
        cost_estimate=pl.CostEstimate(flops=4 * rows * width * (2 * parts * units + parts * own), bytes_accessed=40 << 20, transcendentals=rows * units * parts),
        name="dense",
    )(x, cot, ctx0, ctx1, vectors, inner_bias, near)


def head_columns(weights, own, head):
    return [weights[:, kind * own + head * HD : kind * own + (head + 1) * HD] for kind in range(3)]


def early_back_body(own, w_ref, b0_ref, b1_ref, acc_ref):
    acc_ref[...] = jnp.zeros(acc_ref.shape, jnp.float32)

    def add(t, _):
        both = jnp.concatenate([b0_ref[t], b1_ref[t]], axis=0)
        weights = w_ref[t]
        weights = jnp.concatenate(head_columns(weights, own, 0) + head_columns(weights, own, 1), axis=1)
        acc_ref[...] += dot(weights, both)
        return 0

    lax.fori_loop(0, b0_ref.shape[0], add, 0)


def late_back_body(own, head, part_ref, w_ref, acc_ref, grad_ref, *rest):
    backs, out_ref = rest[:-1], rest[-1]
    parts = len(backs)
    total = acc_ref[...]
    for d in range(parts):
        weights = w_ref[(part_ref[0] + parts - d) % parts]
        total = total + dot(jnp.concatenate(head_columns(weights, own, head), axis=1), backs[d][...])
    out_ref[...] = (total.T + grad_ref[...]).astype(out_ref.dtype)


def weight_block(rest, cols):
    return pl.BlockSpec(rest.shape[:2] + (cols,), lambda i, *_: (0, 0, 0), pipeline_mode=pl.Buffered(1))


def whole(a):
    return pl.BlockSpec(a.shape, lambda i, *_: (0,) * a.ndim, pipeline_mode=pl.Buffered(1))


def early_back(rest, own, b0, b1):
    width, rows = rest.shape[1], b0.shape[2]
    return pl.pallas_call(
        functools.partial(early_back_body, own),
        grid=(1,),
        in_specs=[weight_block(rest, 4 * own), whole(b0), whole(b1)],
        out_specs=pl.BlockSpec((width, rows), lambda i: (0, 0)),
        out_shape=jax.ShapeDtypeStruct((width, rows), jnp.float32),
        compiler_params=pltpu.CompilerParams(vmem_limit_bytes=62 << 20),
        cost_estimate=pl.CostEstimate(flops=4 * width * rows * b0.shape[0] * b0.shape[1], bytes_accessed=10 << 20, transcendentals=0),
        name="early_back",
    )(rest, b0, b1)


def late_back(rest, own, head, part, acc, grad, backs):
    rows, width = grad.shape
    return pl.pallas_call(
        functools.partial(late_back_body, own, head),
        grid_spec=pltpu.PrefetchScalarGridSpec(
            num_scalar_prefetch=1,
            grid=(1,),
            in_specs=[weight_block(rest, 4 * own), whole(acc), whole(grad)] + [whole(b) for b in backs],
            out_specs=pl.BlockSpec((rows, width), lambda i, *_: (0, 0)),
        ),
        out_shape=jax.ShapeDtypeStruct((rows, width), jnp.bfloat16),
        compiler_params=pltpu.CompilerParams(vmem_limit_bytes=62 << 20),
        cost_estimate=pl.CostEstimate(flops=2 * width * rows * backs[0].shape[0] * len(backs), bytes_accessed=10 << 20, transcendentals=0),
        name="late_back",
    )(part.reshape(1), rest, acc, grad, *backs)


def finish_body(units, *refs):
    inner_ref, outer_ref, mixer_ref = refs[-3:]
    total = sum(a[...].astype(jnp.float32) for a in refs[:-3])
    inner_ref[...] = total[:, :units]
    outer_ref[...] = total[:, units : 2 * units].T
    mixer_ref[...] = total[:, 2 * units :].T


def finish(shares, units):
    each, cols = shares[0].shape
    own = cols - 2 * units
    shapes = ((each, units), (units, each), (own, each))
    return pl.pallas_call(
        functools.partial(finish_body, units),
        grid=(1,),
        in_specs=[whole(a) for a in shares],
        out_specs=[pl.BlockSpec(a, lambda i: (0, 0)) for a in shapes],
        out_shape=[jax.ShapeDtypeStruct(a, jnp.float32) for a in shapes],
        compiler_params=pltpu.CompilerParams(vmem_limit_bytes=62 << 20),
        name="finish",
    )(*shares)


def add_up(value, axis):
    size = lax.axis_size(axis)
    span, turn = 1, 0
    while span < size:
        other = lax.ppermute(value, axis, [(i, i ^ span) for i in range(size)])
        value = value + other
        span *= 2
        turn += 1
    return value


def two_halves(value):
    high = value.astype(jnp.bfloat16)
    return high, (value - high.astype(jnp.float32)).astype(jnp.bfloat16)


def rotate(blocks, axis):
    size = lax.axis_size(axis)
    me = lax.axis_index(axis)
    out = []
    for d in range(size):
        block = lax.dynamic_index_in_dim(blocks, (me + d) % size, 0, keepdims=False)
        if d:
            block = lax.ppermute(block, axis, [(i, (i + d) % size) for i in range(size)])
        out.append(block)
    return out


def body(hidden_in, segments, query_weight, key_weight, value_weight, query_bias, value_bias, mixer_weight, mixer_bias, first_gain, first_shift, inner_weight, inner_bias, outer_weight, outer_bias, second_gain, second_shift, cotangent):
    f32 = jnp.float32
    _, rows, width = hidden_in.shape
    parts = lax.axis_size("tensor")
    groups = lax.axis_size("dp")
    rank = lax.axis_index("tensor")
    own = query_weight.shape[1]
    heads = own // HD
    units = inner_weight.shape[1]
    x_own = hidden_in[0]
    small = jnp.concatenate([segments[0].astype(f32), inner_bias]).reshape(-1, 128)
    near_own = jnp.concatenate([query_weight, key_weight, value_weight, mixer_weight.T, inner_weight, outer_weight.T], 1)
    x_parts, near, small = start(x_own, near_own, small)
    x_all = x_parts.reshape(parts * rows, width)
    near = near.reshape(parts, width, 4 * own + 2 * units)
    small = small.reshape(parts, -1)
    segment_all = small[:, :rows].astype(jnp.int32).reshape(-1)
    inner_bias_all = small[:, rows:]
    biases = jnp.concatenate([query_bias, jnp.zeros_like(query_bias), value_bias])

    qt, ka, vt, kt, vn = project(x_all, near, rank, biases, segment_all)
    lead = heads - 1
    context_t, lse, exchanged = [], [], []
    for call, (first, count, block) in enumerate(((0, lead, rows // 2), (lead, 1, rows))):
        lo, hi = ranges(segment_all, block, 512)
        part, out_t, out_lse = attend_forward(first, count, parts, qt, ka, vt, lo, hi, BQ=block)
        context_t.append(out_t)
        lse.append(out_lse)
        if exchanged:
            part, exchanged[-1] = lax.optimization_barrier((part, exchanged[-1]))
        exchanged.append(lax.all_to_all(part, "tensor", 0, 0, tiled=True))
    vectors = jnp.stack([mixer_bias, first_gain, first_shift, outer_bias, second_gain, second_shift])
    vectors = jnp.pad(vectors, ((0, 2), (0, 0)))
    layer_out, first_low, second_low, attn_low, grad_attn, both, context, go0, go1, early = dense(
        own, x_own, cotangent[0], exchanged[0], exchanged[1], vectors, inner_bias_all, near, block=rows // 2
    )
    go0 = lax.all_to_all(go0, "tensor", 0, 0, tiled=True)
    go1 = lax.all_to_all(go1, "tensor", 0, 0, tiled=True)
    weight_grads = weight_grads_of(
        first_low, second_low, attn_low, both, context
    )
    weight_grads = lax.psum_scatter(weight_grads, "dp", scatter_dimension=0, tiled=True)
    weight_grads = jnp.concatenate(
        [
            weight_grads[:, : 2 * units * parts].reshape(-1, parts, 2 * units),
            weight_grads[:, 2 * units * parts :].reshape(-1, parts, own),
        ],
        2,
    ).transpose(1, 0, 2)
    weight_grads = rotate(weight_grads, "tensor")
    inner_grad, outer_grad, mixer_grad = finish(weight_grads, units)
    early = add_up(early[: 6 + parts], "tensor")
    count = 6 + parts
    lines = -(-count * width // (3 * own))
    early = jnp.pad(early.reshape(-1), (0, lines * 3 * own - count * width)).reshape(lines, 3 * own)
    early = jnp.concatenate(two_halves(early), 0)

    lo, hi = ranges(segment_all, 512, 512)
    backs, qkv_grad, bias_grad = [], [], []
    for h in range(heads):
        call = 0 if h < lead else 1
        grads, weight_part, sums = attend_backward(
            h, 1, go1 if h else go0, h - 1 if h else 0, context_t[call], lse[call], h - call * lead, qt, ka, kt, vn, x_parts, lo, hi
        )
        if h < heads - 1:
            backs.append(lax.all_to_all(grads, "tensor", 0, 0, tiled=True))
        else:
            backs.append(rotate(grads, "tensor"))
        qkv_grad.append(weight_part)
        bias_grad.append(sums[:, 0])
    input_back = early_back(near, own, backs[0], backs[1])
    input_grad = late_back(near, own, heads - 1, rank, input_back, grad_attn, backs[2])
    each = width // groups
    by_kind = lambda per_head: [a[..., n * HD : (n + 1) * HD] for n in range(3) for a in per_head]
    bias_grad = jnp.stack(two_halves(jnp.concatenate(by_kind(bias_grad))))
    extra = jnp.concatenate([early, bias_grad], 0)
    spare = -extra.shape[0] % 16
    extra = jnp.pad(extra, ((0, spare), (0, 0)))
    extra = jnp.broadcast_to(extra[None], (groups,) + extra.shape)
    qkv_grad = jnp.concatenate(by_kind(qkv_grad), 1).reshape(groups, each, 3 * own)
    qkv_grad = jnp.concatenate([qkv_grad, extra], 1)
    qkv_grad = lax.all_to_all(qkv_grad, "dp", 0, 0, tiled=True)
    qkv_grad = jnp.sum(qkv_grad.astype(f32), 0)
    early = qkv_grad[each : each + lines] + qkv_grad[each + lines : each + 2 * lines]
    early = early.reshape(-1)[: count * width].reshape(count, width)
    bias_grad = qkv_grad[each + 2 * lines] + qkv_grad[each + 2 * lines + 1]
    inner_bias_out = lax.dynamic_index_in_dim(early, 6 + rank, 0, keepdims=False)
    return (
        layer_out[None],
        input_grad[None],
        qkv_grad[:each, 0 * own : 1 * own],
        qkv_grad[:each, 1 * own : 2 * own],
        qkv_grad[:each, 2 * own : 3 * own],
        bias_grad[:own],
        bias_grad[2 * own :],
        mixer_grad,
        early[0],
        early[1],
        early[2],
        inner_grad,
        inner_bias_out,
        outer_grad,
        early[3],
        early[4],
        early[5],
    )


def solution(mesh):
    placed = (
        P("dp", "tensor", None),
        P("dp", "tensor"),
        P("dp", "tensor"),
        P("dp", "tensor"),
        P("dp", "tensor"),
        P("tensor"),
        P("tensor"),
        P("tensor", "dp"),
        P(),
        P(),
        P(),
        P("dp", "tensor"),
        P("tensor"),
        P("tensor", "dp"),
        P(),
        P(),
        P(),
        P("dp", "tensor", None),
    )

    return jax.shard_map(
        body,
        mesh=mesh,
        in_specs=placed,
        out_specs=(
            P("dp", "tensor", None),
            P("dp", "tensor", None),
            P("dp", "tensor"),
            P("dp", "tensor"),
            P("dp", "tensor"),
            P("tensor"),
            P("tensor"),
            P("tensor", "dp"),
            P(),
            P(),
            P(),
            P("dp", "tensor"),
            P("tensor"),
            P("tensor", "dp"),
            P(),
            P(),
            P(),
        ),
        check_vma=False,
    )
```
